16 devices in a mesh: z: 2 (over z), y: 2 (over y), x: 4 (over x, core).
Axes of the slice: x: 2, y: 2, z: 2, core: 2. Of those that a mesh axis runs over, the one named last changes fastest.
Arguments:
- atom_pos: float32 [11664, 3], P(('z', 'y', 'x'))
- atom_vel: float32 [11664, 3], P(('z', 'y', 'x'))
- atom_frc: float32 [11664, 3], P(('z', 'y', 'x'))
- atom_id: int32 [11664], P(('z', 'y', 'x'))
- atom_ok: int32 [11664], P(('z', 'y', 'x'))
- brick_side: float32 [], replicated
Outputs:
- output 1: float32 [11664, 3], P(('z', 'y', 'x'))
- output 2: float32 [11664, 3], P(('z', 'y', 'x'))
- output 3: float32 [11664, 3], P(('z', 'y', 'x'))
- output 4: int32 [11664], P(('z', 'y', 'x'))
- output 5: int32 [11664], P(('z', 'y', 'x'))
- output 6: float32 [], replicated
All inputs are finite; a program needn't handle non-finite values.
Results may differ from the reference program's by a relative error of at most 0.001.
Values sent between devices are 32-bit elements.
A program may use at most 1 GiB of HBM per device.

```python
import jax
import jax.numpy as jnp
from jax import lax

NZ = 2
NY = 2
NX = 4
GRID = 8
RHO_E4 = 5000
CAP = 729

DEVICES = NZ * NY * NX
SITES = DEVICES * GRID * GRID * GRID
MOVE_MAX = max(1, CAP // 100)
PLANE = (GRID - 1) * (GRID - 1)
SITE_SHAPE = (NZ, NY, NX, GRID, GRID, GRID)
VEC_SHAPE = (NZ, NY, NX, GRID, GRID, GRID, 3)
DT = 0.005
RC = 2.5
UCUT = 4.0 * (RC ** -12 - RC ** -6)
UPC = -48.0 * RC ** -13 + 24.0 * RC ** -7


def place_atoms(base_key, spacing, jitter, free_disp, prev_force):
    sub_keys = jax.random.split(base_key, 8)
    brick_vec = jnp.stack([lax.broadcasted_iota(jnp.int32, SITE_SHAPE, 2), lax.broadcasted_iota(jnp.int32, SITE_SHAPE, 1), lax.broadcasted_iota(jnp.int32, SITE_SHAPE, 0)], axis=-1)
    site_vec = jnp.stack([lax.broadcasted_iota(jnp.int32, SITE_SHAPE, 5), lax.broadcasted_iota(jnp.int32, SITE_SHAPE, 4), lax.broadcasted_iota(jnp.int32, SITE_SHAPE, 3)], axis=-1)
    dims_int = jnp.array([NX, NY, NZ], jnp.int32)
    on_face = site_vec == 0
    face_count = jnp.sum(on_face.astype(jnp.int32), axis=-1, keepdims=True)
    side_sign = 2 * jax.random.randint(sub_keys[0], VEC_SHAPE, 0, 2) - 1
    plane_perm = jax.random.permutation(sub_keys[1], jnp.broadcast_to(jnp.arange(PLANE), (NZ, NY, NX, 3, PLANE)), axis=-1, independent=True)
    inner_k = jnp.maximum(site_vec - 1, 0)
    plane_idx = jnp.stack([inner_k[..., (axis_d + 1) % 3] * (GRID - 1) + inner_k[..., (axis_d + 2) % 3] for axis_d in range(3)], axis=-1)
    plane_rank = jnp.take_along_axis(jnp.broadcast_to(plane_perm[:, :, :, None, None, None, :, :], VEC_SHAPE + (PLANE,)), plane_idx[..., None], axis=-1)[..., 0]
    down_count = jax.random.randint(sub_keys[2], (NZ, NY, NX, 3), 0, MOVE_MAX + 1)[:, :, :, None, None, None, :]
    up_count = jax.random.randint(sub_keys[3], (NZ, NY, NX, 3), 0, MOVE_MAX + 1).at[0, 0, 0, 0].set(MOVE_MAX)[:, :, :, None, None, None, :]
    plane_site = on_face & (face_count == 1)
    go_down = plane_site & (plane_rank < down_count)
    go_up = plane_site & (plane_rank >= down_count) & (plane_rank < down_count + up_count)
    edge_flag = (face_count == 2) & jnp.logical_not(on_face[..., 2:3]) & (site_vec[..., 2:3] == 1)
    corner_flag = face_count == 3
    crossing = go_down | go_up | (on_face & (edge_flag | corner_flag))
    side_sign = jnp.where(go_down, -1, jnp.where(go_up, 1, side_sign))
    pre_side = jnp.where(crossing, -side_sign, side_sign)
    pre_brick = jnp.mod(brick_vec + jnp.where(on_face & (pre_side < 0), -1, 0), dims_int)
    pre_dev = (pre_brick[..., 2] * NY + pre_brick[..., 1]) * NX + pre_brick[..., 0]
    fill_pct = jax.random.randint(sub_keys[4], (NZ, NY, NX, 1, 1, 1), 50, 101)
    occupied = (jax.random.randint(sub_keys[5], SITE_SHAPE, 0, 100) < fill_pct) | jnp.any(crossing, axis=-1)
    atom_ids = jax.random.permutation(sub_keys[6], SITES).astype(jnp.int32).reshape(SITE_SHAPE)
    near_gaps = jax.random.uniform(sub_keys[7], VEC_SHAPE + (2,), jnp.float32, 0.002, 0.006)
    face_gap = near_gaps[..., 0]
    cross_gap = near_gaps[..., 1]
    sign_f = side_sign.astype(jnp.float32)
    lattice = (brick_vec * GRID + site_vec).astype(jnp.float32) * spacing
    post_pos = lattice + jnp.where(on_face, sign_f * face_gap, jitter * spacing)
    displace = jnp.where(on_face, jnp.where(crossing, sign_f * (face_gap + cross_gap), 0.5 * sign_f * face_gap), free_disp)
    box_len = spacing * GRID * dims_int.astype(jnp.float32)
    start_pos = jnp.mod(post_pos - displace, box_len)
    start_vel = displace / DT - (0.5 * DT) * prev_force
    flat_ok = occupied.reshape(SITES)
    flat_dev = pre_dev.reshape(SITES)
    sort_key = jnp.where(flat_ok, flat_dev * SITES + atom_ids.reshape(SITES), DEVICES * SITES)
    sort_order = jnp.argsort(sort_key)
    counts = jax.ops.segment_sum(flat_ok.astype(jnp.int32), flat_dev, num_segments=DEVICES)
    first_row = jnp.cumsum(counts) - counts
    sorted_dev = flat_dev[sort_order]
    dest_row = jnp.where(flat_ok[sort_order], sorted_dev * CAP + jnp.arange(SITES) - first_row[sorted_dev], DEVICES * CAP)

    def spread(values):
        tail_dims = values.shape[6:]
        flat_vals = values.reshape((SITES,) + tail_dims)[sort_order]
        return jnp.zeros((DEVICES * CAP,) + tail_dims, values.dtype).at[dest_row].set(flat_vals, mode="drop")

    return {"atom_pos": spread(start_pos), "atom_vel": spread(start_vel), "atom_frc": spread(prev_force), "atom_id": spread(atom_ids), "atom_ok": spread(occupied.astype(jnp.int32)), "brick_side": spacing * GRID}


def setup_inputs(seed: int = 0) -> dict:
    value_keys = jax.random.split(jax.random.key(seed + 1), 4)
    spacing = (RHO_E4 / 10000.0) ** (-1.0 / 3.0) * (1.0 + 0.01 * jax.random.uniform(value_keys[0], (), jnp.float32, -1.0, 1.0))
    jitter = jax.random.uniform(value_keys[1], VEC_SHAPE, jnp.float32, -0.05, 0.05)
    free_disp = jax.random.uniform(value_keys[2], VEC_SHAPE, jnp.float32, -0.01, 0.01)
    prev_force = 40.0 * jax.random.normal(value_keys[3], VEC_SHAPE, jnp.float32)
    return place_atoms(jax.random.key(seed), spacing, jitter, free_disp, prev_force)


def pair_terms(own_pos, own_ok, other_pos, other_ok, box_len):
    delta_r = own_pos[..., :, None, :] - other_pos[..., None, :, :]
    delta_r = delta_r - box_len * jnp.floor(delta_r / box_len + 0.5)
    dist_sq = jnp.sum(delta_r * delta_r, axis=-1)
    in_range = own_ok[..., :, None] & other_ok[..., None, :] & (dist_sq < RC * RC) & (dist_sq > 0.01)
    safe_sq = jnp.where(in_range, dist_sq, 1.0)
    inv_r2 = 1.0 / safe_sq
    inv_r6 = inv_r2 * inv_r2 * inv_r2
    radius = jnp.sqrt(safe_sq)
    f_scale = jnp.where(in_range, (48.0 * inv_r6 * inv_r6 - 24.0 * inv_r6) * inv_r2 + UPC / radius, 0.0)
    pair_energy = jnp.where(in_range, 4.0 * (inv_r6 * inv_r6 - inv_r6) - UCUT - (radius - RC) * UPC, 0.0)
    force_sum = jnp.sum(f_scale[..., None] * delta_r, axis=-2)
    return force_sum, jnp.sum(pair_energy)


def brick_forces(own_pos, own_ok, other_pos, other_ok, box_len):
    force_sum = jnp.zeros_like(own_pos)
    energy_sum = jnp.zeros((), own_pos.dtype)
    for neighbor in range(other_pos.shape[0]):
        force_part, energy_part = pair_terms(own_pos, own_ok, other_pos[neighbor], other_ok[neighbor], box_len)
        force_sum = force_sum + force_part
        energy_sum = energy_sum + energy_part
    return force_sum, energy_sum


def reference(atom_pos, atom_vel, atom_frc, atom_id, atom_ok, brick_side):
    dims_int = jnp.array([NX, NY, NZ], jnp.int32)
    box_len = brick_side * dims_int.astype(jnp.float32)
    owned = atom_ok > 0
    half_v = atom_vel + (0.5 * DT) * atom_frc
    moved = jnp.mod(atom_pos + DT * half_v, box_len)
    new_cell = jnp.clip(jnp.floor(moved / brick_side).astype(jnp.int32), 0, dims_int - 1)
    dest_dev = (new_cell[:, 2] * NY + new_cell[:, 1]) * NX + new_cell[:, 0]
    sort_key = jnp.where(owned, dest_dev * SITES + atom_id, DEVICES * SITES)
    sort_order = jnp.argsort(sort_key)
    counts = jax.ops.segment_sum(owned.astype(jnp.int32), dest_dev, num_segments=DEVICES)
    first_row = jnp.cumsum(counts) - counts
    sorted_dev = dest_dev[sort_order]
    dest_row = jnp.where(owned[sort_order], sorted_dev * CAP + jnp.arange(DEVICES * CAP) - first_row[sorted_dev], DEVICES * CAP)

    def spread(values):
        return jnp.zeros_like(values).at[dest_row].set(values[sort_order], mode="drop")

    new_pos = spread(moved)
    new_half = spread(half_v)
    new_id = spread(atom_id)
    new_ok = spread(atom_ok)
    grid_pos = new_pos.reshape(NZ, NY, NX, CAP, 3)
    grid_ok = (new_ok > 0).reshape(NZ, NY, NX, CAP)
    steps_z = range(-1, 2) if NZ > 2 else range(0, 2)
    steps_y = range(-1, 2) if NY > 2 else range(0, 2)
    steps_x = range(-1, 2) if NX > 2 else range(0, 2)
    shell_list = [(shift_z, shift_y, shift_x) for shift_z in steps_z for shift_y in steps_y for shift_x in steps_x]
    other_pos = jnp.stack([jnp.roll(grid_pos, (-shift_zyx[0], -shift_zyx[1], -shift_zyx[2]), axis=(0, 1, 2)) for shift_zyx in shell_list], axis=3)
    other_ok = jnp.stack([jnp.roll(grid_ok, (-shift_zyx[0], -shift_zyx[1], -shift_zyx[2]), axis=(0, 1, 2)) for shift_zyx in shell_list], axis=3)
    n_shell = len(shell_list)
    force_grid, energy_grid = lax.map(lambda packed: brick_forces(packed[0], packed[1], packed[2], packed[3], box_len), (grid_pos.reshape(DEVICES, CAP, 3), grid_ok.reshape(DEVICES, CAP), other_pos.reshape(DEVICES, n_shell, CAP, 3), other_ok.reshape(DEVICES, n_shell, CAP)))
    new_force = force_grid.reshape(DEVICES * CAP, 3)
    ok_f = (new_ok > 0).astype(new_pos.dtype)[:, None]
    new_vel = (new_half + (0.5 * DT) * new_force) * ok_f
    energy = 0.5 * jnp.sum(energy_grid)
    return new_pos, new_vel, new_force, new_id, new_ok, energy
```

```python
import functools

import jax
import jax.numpy as jnp
import numpy as np
from jax import lax
from jax.experimental import pallas as pl
from jax.experimental.pallas import tpu as pltpu
from jax.sharding import PartitionSpec as P

DT = 0.005
RC = 2.5
UPC = -48.0 * RC ** -13 + 24.0 * RC ** -7
MESH_AXES = ("z", "y", "x")
MESH = pl.DeviceIdType.MESH
NZ, NY, NX = 2, 2, 4
CAP = 729
LANES = 128
BLOCKS = 6
WIDE = BLOCKS * LANES
MOVE_CAP = CAP // 100
FAR_OWN = 1.0e4
FAR_OTHER = -1.0e4
PEERS = [(dz, dy, dx) for dz in range(NZ) for dy in range(NY) for dx in range(NX)][1:]
GROUPS = [(1, 1, 1), (-1, 1, 1), (0, 1, 1), (1, 0, 0), (-1, 0, 0), (0, 1, 0), (0, 0, 1), (1, 1, 0), (-1, 1, 0), (1, 0, 1), (-1, 0, 1)]
N_GROUPS = len(GROUPS)


def lane_plan():
    starts, base = [], np.zeros((32, LANES), np.float32)
    block, lane = 0, 0
    for index, (gx, gy, gz) in enumerate(GROUPS):
        if index == 5:
            block, lane = 1, 0
        dirs = [(gx, sy, sz) for sz in ((-1, 1) if gz else (0,)) for sy in ((-1, 1) if gy else (0,))]
        starts.append((block, lane, lane + MOVE_CAP * len(dirs)))
        for dx, dy, dz in dirs:
            base[(dz + 1) * 9 + (dy + 1) * 3 + dx + 1] = block * LANES + lane
            lane += MOVE_CAP
    return starts, base


LANE_STARTS, LANE_BASE = lane_plan()
STAY = 13


def split3(values):
    hi = values.astype(jnp.bfloat16).astype(jnp.float32)
    rest = values - hi
    mid = rest.astype(jnp.bfloat16).astype(jnp.float32)
    return jnp.concatenate([hi, mid, rest - mid], axis=0).astype(jnp.bfloat16)


def join3(parts):
    rows = parts.shape[0] // 3
    return (parts[0:rows] + parts[rows:2 * rows]) + parts[2 * rows:3 * rows]


def dot_nt(a, b):
    return lax.dot_general(a, b, (((1,), (1,)), ((), ())), preferred_element_type=jnp.float32)


def dot_nn(a, b):
    return lax.dot_general(a, b, (((1,), (0,)), ((), ())), preferred_element_type=jnp.float32)


def my_coords():
    return lax.axis_index("z"), lax.axis_index("y"), lax.axis_index("x")


def peer_id(coords, offset):
    mz, my, mx = coords
    return (lax.rem(mz + offset[0], NZ), lax.rem(my + offset[1], NY), lax.rem(mx + offset[2] + NX, NX))


def entry_signals(coords):
    barrier = pltpu.get_barrier_semaphore()
    for offset in PEERS:
        pl.semaphore_signal(barrier, inc=1, device_id=peer_id(coords, offset), device_id_type=MESH)
    return barrier


def exchange_kernel(brick_ref, pos_ref, vel_ref, frc_ref, id_ref, ok_ref, base_ref, gat_ref, pkt_ref, own_ref, pad_ref, int_ref, send_pos, send_pkt, pos_send_sem, pos_recv_sem, pkt_send_sem, pkt_recv_sem):
    coords = my_coords()
    barrier = entry_signals(coords)
    brick = brick_ref[0, 0]
    tail = slice(WIDE - LANES, WIDE)
    pad_ref[:, :, tail] = jnp.zeros((3, 4, LANES), jnp.float32)
    int_ref[:, tail] = jnp.zeros((2, LANES), jnp.int32)
    pad_ref[0, 0:3, 0:CAP] = pos_ref[...]
    pad_ref[1, 0:3, 0:CAP] = vel_ref[...]
    pad_ref[2, 0:3, 0:CAP] = frc_ref[...]
    int_ref[0:1, 0:CAP] = id_ref[...]
    int_ref[1:2, 0:CAP] = ok_ref[...]
    owned = int_ref[1:2, :] > 0
    moved, half, code = [], [], jnp.zeros((1, WIDE), jnp.int32)
    for axis, (mine, size, weight) in enumerate(((coords[2], NX, 1), (coords[1], NY, 3), (coords[0], NZ, 9))):
        box = brick * float(size)
        low = mine.astype(jnp.float32) * brick
        high = (mine + 1).astype(jnp.float32) * brick
        half_v = pad_ref[1, axis:axis + 1, :] + (0.5 * DT) * pad_ref[2, axis:axis + 1, :]
        drift = pad_ref[0, axis:axis + 1, :] + DT * half_v
        step = jnp.where(drift >= high, 2, jnp.where(drift < low, 0, 1))
        code = code + step * weight
        wrapped = jnp.where(drift < 0.0, drift + box, jnp.where(drift >= box, drift - box, drift))
        moved.append(wrapped)
        half.append(half_v)
    code = jnp.where(owned, code, -1)
    for axis in range(3):
        for block in range(8):
            if block < BLOCKS:
                lanes = slice(block * LANES, (block + 1) * LANES)
                send_pos[axis, block:block + 1, :] = jnp.where(owned[:, lanes], moved[axis][:, lanes], 1.0e9)
            else:
                send_pos[axis, block:block + 1, :] = jnp.full((1, LANES), 1.0e9, jnp.float32)
    ids = int_ref[0:1, :]
    id_hi = (lax.shift_right_logical(ids, 16) + 1).astype(jnp.float32)
    id_lo = (ids & 65535).astype(jnp.float32)
    data = jnp.concatenate(moved + half + [id_hi, id_lo], axis=0)
    member = (jnp.broadcast_to(code, (32, WIDE)) == lax.broadcasted_iota(jnp.int32, (32, WIDE), 0)).astype(jnp.float32)
    tri = (lax.broadcasted_iota(jnp.int32, (LANES, LANES), 0) < lax.broadcasted_iota(jnp.int32, (LANES, LANES), 1)).astype(jnp.bfloat16)
    running = base_ref[...]
    slots = []
    for block in range(BLOCKS):
        part = member[:, block * LANES:(block + 1) * LANES]
        before = dot_nn(part.astype(jnp.bfloat16), tri)
        slots.append(jnp.sum(part * (before + running), axis=0, keepdims=True))
        running = running + jnp.sum(part, axis=1, keepdims=True)
    slot = jnp.concatenate(slots, axis=1)
    stay = code == STAY
    mover_slot = jnp.where(owned & jnp.logical_not(stay), slot, -1.0).astype(jnp.int32)
    pick = (lax.broadcasted_iota(jnp.int32, (2 * LANES, WIDE), 0) == mover_slot).astype(jnp.float32).astype(jnp.bfloat16)
    packet = join3(dot_nt(split3(data), pick))
    send_pkt[0] = packet[:, 0:LANES]
    send_pkt[1] = packet[:, LANES:2 * LANES]
    own_ref[0:8, :] = data
    own_ref[8:16, :] = jnp.concatenate([jnp.where(stay, slot, -1.0), jnp.zeros((7, WIDE), jnp.float32)], axis=0)
    pl.semaphore_wait(barrier, len(PEERS))
    copies = []
    for index, offset in enumerate(PEERS):
        copies.append(pltpu.make_async_remote_copy(src_ref=send_pos, dst_ref=gat_ref.at[index + 1], send_sem=pos_send_sem.at[index], recv_sem=pos_recv_sem.at[index], device_id=peer_id(coords, offset), device_id_type=MESH))
        copies[-1].start()
    for index, (gx, gy, gz) in enumerate(GROUPS):
        copies.append(pltpu.make_async_remote_copy(src_ref=send_pkt.at[LANE_STARTS[index][0]], dst_ref=pkt_ref.at[index], send_sem=pkt_send_sem.at[index], recv_sem=pkt_recv_sem.at[index], device_id=peer_id(coords, (gz, gy, gx)), device_id_type=MESH))
        copies[-1].start()
    gat_ref[0] = send_pos[...]
    for copy in copies:
        copy.wait()


MAX_ROWS = 6 + 16 * BLOCKS + 2
QUAD = 4


def force_kernel(brick_ref, gat_ref, pkt_ref, own_ref, pos_out, vel_out, frc_out, id_out, ok_out, eng_out, others, mine, acc, sorted_ref):
    mz, my, mx = my_coords()
    brick = brick_ref[0, 0]
    half_l = 0.5 * brick
    reach = half_l + RC
    sizes = (NX, NY, NZ)
    centre = [(index.astype(jnp.float32) + 0.5) * brick for index in (mx, my, mz)]
    box = [brick * float(size) for size in sizes]
    lane_1 = lax.broadcasted_iota(jnp.int32, (1, LANES), 1)

    arrived = []
    for block in range(2):
        total = jnp.zeros((8, LANES), jnp.float32)
        for index in range(N_GROUPS):
            where_block, first, last = LANE_STARTS[index]
            if where_block == block:
                total = total + jnp.where((lane_1 >= first) & (lane_1 < last), pkt_ref[index], 0.0)
        arrived.append(total)
    arr = jnp.concatenate(arrived, axis=1)
    data = jnp.concatenate([own_ref[0:8, :], arr], axis=1)
    int_max = 2147483647
    ids = lax.shift_left(data[6:7].astype(jnp.int32) - 1, 16) + data[7:8].astype(jnp.int32)
    stay_rank = own_ref[8:9, :]
    stay = stay_rank >= 0.0
    arr_ok = arr[6:7] > 0.5
    arr_id = jnp.where(arr_ok, ids[:, WIDE:], int_max)
    own_id = jnp.where(stay, ids[:, :WIDE], int_max)
    arr_col = jnp.transpose(jnp.broadcast_to(arr_id, (8, 2 * LANES)), (1, 0))[:, 0:1]
    own_col = jnp.transpose(jnp.broadcast_to(own_id, (8, WIDE)), (1, 0))[:, 0:1]
    all_id = jnp.concatenate([own_id, arr_id], axis=1)
    arr_before = jnp.sum((arr_col < all_id).astype(jnp.float32), axis=0, keepdims=True)
    stay_before = jnp.sum((own_col < arr_id).astype(jnp.float32), axis=0, keepdims=True)
    rank = jnp.concatenate([jnp.where(stay, stay_rank + arr_before[:, :WIDE], -1.0), jnp.where(arr_ok, stay_before + arr_before[:, WIDE:], -1.0)], axis=1).astype(jnp.int32)
    n_own = jnp.sum((rank >= 0).astype(jnp.float32)).astype(jnp.int32)
    parts = split3(data)
    for block in range(BLOCKS):
        pick = (lax.broadcasted_iota(jnp.int32, (LANES, WIDE + 2 * LANES), 0) + block * LANES == rank).astype(jnp.float32).astype(jnp.bfloat16)
        sorted_ref[block] = join3(dot_nt(parts, pick))
    for block in range(BLOCKS):
        valid = lane_1 + block * LANES < n_own
        for axis in range(3):
            rel = sorted_ref[block, axis:axis + 1, :] - centre[axis]
            others[axis, block] = jnp.broadcast_to(jnp.where(valid, rel, FAR_OTHER), (8, LANES))
            column = jnp.transpose(jnp.broadcast_to(jnp.where(valid, rel, FAR_OWN), (8, LANES)), (1, 0))[:, 0:1]
            mine[axis, pl.ds(block * 16, 16)] = jnp.broadcast_to(column, (LANES, LANES)).reshape(16, 8, LANES)
    own_rows = lax.div(n_own + (LANES - 1), LANES)

    rel = []
    for axis in range(3):
        values = gat_ref[:, axis].reshape(16 * 8, LANES) - centre[axis]
        values = jnp.where(values > 0.5 * box[axis], values - box[axis], jnp.where(values < -0.5 * box[axis], values + box[axis], values))
        rel.append(values)
    near = (jnp.abs(rel[0]) < reach) & (jnp.abs(rel[1]) < reach) & (jnp.abs(rel[2]) < reach)
    inside = (jnp.abs(rel[0]) < half_l) & (jnp.abs(rel[1]) < half_l) & (jnp.abs(rel[2]) < half_l)
    ghost = (near & jnp.logical_not(inside)).astype(jnp.float32).astype(jnp.bfloat16)
    row_i = lax.broadcasted_iota(jnp.int32, (LANES, LANES), 0)
    col_i = lax.broadcasted_iota(jnp.int32, (LANES, LANES), 1)
    cum = dot_nn(ghost, (row_i <= col_i).astype(jnp.bfloat16)).astype(jnp.int32)
    count = dot_nn(ghost, jnp.ones((LANES, LANES), jnp.bfloat16))
    base = dot_nn((col_i < row_i).astype(jnp.bfloat16), count.astype(jnp.bfloat16)).astype(jnp.int32)
    count = count.astype(jnp.int32)
    n_ghost = jnp.max(base[LANES - 8:] + count[LANES - 8:])
    place = (col_i - base) & (LANES - 1)
    source = jnp.zeros((LANES, LANES), jnp.int32)
    for step in (64, 32, 16, 8, 4, 2, 1):
        probe = jnp.take_along_axis(cum, source + (step - 1), axis=1)
        source = jnp.where(probe <= place, source + step, source)
    target = jnp.where(place < count, lax.shift_right_logical(base + place, 7), -1)
    packed = [jnp.take_along_axis(values, source, axis=1) for values in rel]
    ghost_rows = lax.div(n_ghost + (LANES - 1), LANES)

    def pack_row(row, carry):
        hit = target == row
        filled = lane_1 + row * LANES < n_ghost
        for axis in range(3):
            values = jnp.sum(jnp.where(hit, packed[axis], 0.0), axis=0, keepdims=True)
            others[axis, own_rows + row] = jnp.broadcast_to(jnp.where(filled, values, FAR_OTHER), (8, LANES))
        return carry

    lax.fori_loop(0, ghost_rows, pack_row, 0)
    rows = own_rows + ghost_rows

    rc2 = jnp.full((8, LANES), brick_ref[0, 1], jnp.float32)
    kappa = UPC / 48.0

    def radial(dist_sq):
        inv_r = lax.rsqrt(dist_sq)
        inv_2 = inv_r * inv_r
        inv_4 = inv_2 * inv_2
        term = inv_4 * inv_2 - 0.5
        tail = kappa * inv_r
        return term * (inv_4 * inv_4) + tail, term * term, tail * dist_sq

    cut_f, cut_a, cut_h = radial(rc2)
    lane_8 = lax.broadcasted_iota(jnp.int32, (8, LANES), 1)
    sub_8 = lax.broadcasted_iota(jnp.int32, (8, LANES), 0)
    zero = jnp.zeros((8, LANES), jnp.float32)

    def pair_loops(wrap):
        inv_box = [1.0 / (brick * float(size)) for size in sizes]

        def quad(index, energy):
            first = index * QUAD
            own = [[mine[axis, first + k] for axis in range(3)] for k in range(QUAD)]

            def row_body(with_self, row, sums):
                other = [others[axis, row] for axis in range(3)]
                out = []
                for k in range(QUAD):
                    fx, fy, fz, ea, eh = sums[5 * k:5 * k + 5]
                    delta = [own[k][axis] - other[axis] for axis in range(3)]
                    if wrap:
                        for axis in (1, 2):
                            delta[axis] = delta[axis] - box[axis] * jnp.floor(delta[axis] * inv_box[axis] + 0.5)
                    dist_sq = delta[0] * delta[0] + delta[1] * delta[1] + delta[2] * delta[2]
                    if with_self:
                        dist_sq = jnp.where(sub_8 + (first + k) * 8 == lane_8 + row * LANES, rc2, dist_sq)
                    scale, a, h = radial(jnp.minimum(dist_sq, rc2))
                    scale = scale - cut_f
                    out += [fx + scale * delta[0], fy + scale * delta[1], fz + scale * delta[2], ea + a, eh + h]
                return tuple(out)

            sums = (zero,) * (5 * QUAD)
            sums = lax.fori_loop(0, own_rows, functools.partial(row_body, True), sums)
            sums = lax.fori_loop(own_rows, rows, functools.partial(row_body, False), sums)
            n = rows.astype(jnp.float32)
            for k in range(QUAD):
                for axis in range(3):
                    acc[axis, first + k] = sums[5 * k + axis]
                energy = energy + (sums[5 * k + 3] - n * cut_a) - 12.0 * (sums[5 * k + 4] - n * cut_h)
            return energy

        quads = lax.div(n_own + (8 * QUAD - 1), 8 * QUAD)
        energy = lax.fori_loop(0, quads, quad, zero)
        eng_out[...] = jnp.full((8, LANES), 2.0 * jnp.sum(energy), jnp.float32)

    pl.when(brick >= 2.0 * RC)(lambda: pair_loops(False))
    pl.when(brick < 2.0 * RC)(lambda: pair_loops(True))

    for block in range(BLOCKS):
        width = min(LANES, CAP - block * LANES)
        lanes = slice(block * LANES, block * LANES + width)
        valid = lane_1 + block * LANES < n_own
        rows_s = sorted_ref[block]
        for axis in range(3):
            turned = jnp.transpose(acc[axis, pl.ds(block * 16, 16)].reshape(LANES, LANES), (1, 0))
            force = jnp.where(valid, 48.0 * jnp.sum(turned, axis=0, keepdims=True), 0.0)
            frc_out[axis:axis + 1, lanes] = force[:, :width]
            vel_out[axis:axis + 1, lanes] = (rows_s[3 + axis:4 + axis] + (0.5 * DT) * force)[:, :width]
            pos_out[axis:axis + 1, lanes] = rows_s[axis:axis + 1, :width]
        new_id = lax.shift_left(rows_s[6:7].astype(jnp.int32) - 1, 16) + rows_s[7:8].astype(jnp.int32)
        id_out[0:1, lanes] = jnp.where(valid, new_id, 0)[:, :width]
        ok_out[0:1, lanes] = valid.astype(jnp.int32)[:, :width]


def energy_kernel(eng_ref, out_ref, slots, send_sem, recv_sem):
    coords = my_coords()
    mz, my, mx = coords
    barrier = entry_signals(coords)
    pl.semaphore_wait(barrier, len(PEERS))
    place = (mz * NY + my) * NX + mx
    copies = []
    for index, offset in enumerate(PEERS):
        copies.append(pltpu.make_async_remote_copy(src_ref=eng_ref, dst_ref=slots.at[place], send_sem=send_sem.at[index], recv_sem=recv_sem.at[index], device_id=peer_id(coords, offset), device_id_type=MESH))
        copies[-1].start()
    slots[place] = eng_ref[...]
    for copy in copies:
        copy.wait()
    total = slots[0]
    for index in range(1, NZ * NY * NX):
        total = total + slots[index]
    out_ref[...] = total[0:1, :]


VMEM_SPEC = pl.BlockSpec(memory_space=pltpu.VMEM)
SMEM_SPEC = pl.BlockSpec(memory_space=pltpu.SMEM)


def solution(mesh):
    def local_step(atom_pos, atom_vel, atom_frc, atom_id, atom_ok, brick_side):
        f32 = jnp.float32
        brick = jnp.stack([brick_side, jnp.float32(RC * RC)]).reshape(1, 2)
        n_dev = NZ * NY * NX
        gat, pkt, own = pl.pallas_call(
            exchange_kernel,
            out_shape=(jax.ShapeDtypeStruct((n_dev, 3, 8, LANES), f32), jax.ShapeDtypeStruct((N_GROUPS, 8, LANES), f32), jax.ShapeDtypeStruct((16, WIDE), f32)),
            in_specs=[SMEM_SPEC] + [VMEM_SPEC] * 6,
            out_specs=(VMEM_SPEC,) * 3,
            scratch_shapes=[
                pltpu.VMEM((3, 4, WIDE), f32),
                pltpu.VMEM((2, WIDE), jnp.int32),
                pltpu.VMEM((3, 8, LANES), f32),
                pltpu.VMEM((2, 8, LANES), f32),
                pltpu.SemaphoreType.DMA((n_dev - 1,)),
                pltpu.SemaphoreType.DMA((n_dev - 1,)),
                pltpu.SemaphoreType.DMA((N_GROUPS,)),
                pltpu.SemaphoreType.DMA((N_GROUPS,)),
            ],
            compiler_params=pltpu.CompilerParams(collective_id=0, has_side_effects=True),
            name="exchange",
        )(brick, atom_pos.T, atom_vel.T, atom_frc.T, atom_id.reshape(1, CAP), atom_ok.reshape(1, CAP), jnp.asarray(LANE_BASE))
        pos, vel, frc, ids, oks, eng = pl.pallas_call(
            force_kernel,
            out_shape=(jax.ShapeDtypeStruct((3, CAP), f32),) * 3 + (jax.ShapeDtypeStruct((1, CAP), jnp.int32),) * 2 + (jax.ShapeDtypeStruct((8, LANES), f32),),
            in_specs=[SMEM_SPEC] + [VMEM_SPEC] * 3,
            out_specs=(VMEM_SPEC,) * 6,
            scratch_shapes=[
                pltpu.VMEM((3, MAX_ROWS, 8, LANES), f32),
                pltpu.VMEM((3, BLOCKS * 16, 8, LANES), f32),
                pltpu.VMEM((3, BLOCKS * 16, 8, LANES), f32),
                pltpu.VMEM((BLOCKS, 8, LANES), f32),
            ],
            name="forces",
        )(brick, gat, pkt, own)
        total = pl.pallas_call(
            energy_kernel,
            out_shape=jax.ShapeDtypeStruct((1, LANES), f32),
            in_specs=[VMEM_SPEC],
            out_specs=VMEM_SPEC,
            scratch_shapes=[pltpu.VMEM((n_dev, 8, LANES), f32), pltpu.SemaphoreType.DMA((n_dev - 1,)), pltpu.SemaphoreType.DMA((n_dev - 1,))],
            compiler_params=pltpu.CompilerParams(collective_id=1, has_side_effects=True),
            name="energy",
        )(eng)
        return pos.T, vel.T, frc.T, ids.reshape(CAP), oks.reshape(CAP), total[0, 0]

    row_spec = P(MESH_AXES, None)
    id_spec = P(MESH_AXES)
    return jax.shard_map(local_step, mesh=mesh, in_specs=(row_spec, row_spec, row_spec, id_spec, id_spec, P()), out_specs=(row_spec, row_spec, row_spec, id_spec, id_spec, P()), check_vma=False)
```

```python
import jax
import jax.numpy as jnp
from jax import lax
from jax.experimental import pallas as pl
from jax.experimental.pallas import tpu as pltpu
from jax.sharding import PartitionSpec as P

DT = 0.005
RC = 2.5
UPC = -48.0 * RC ** -13 + 24.0 * RC ** -7
MESH_AXES = ("z", "y", "x")
MESH = pl.DeviceIdType.MESH
NZ, NY, NX = 2, 2, 4
CAP = 729
LANES = 128
BLOCKS = 6
WIDE = BLOCKS * LANES
MOVE_CAP = CAP // 100
FAR_OWN = 1.0e4
FAR_OTHER = -1.0e4
NOWHERE = 1.0e9
PEERS = [(dz, dy, dx) for dz in range(NZ) for dy in range(NY) for dx in range(NX)][1:]
GROUPS = [(1, 1, 1), (-1, 1, 1), (1, 1, 0), (-1, 1, 0), (1, 0, 1), (-1, 0, 1), (1, 0, 0), (-1, 0, 0), (0, 1, 1), (0, 1, 0), (0, 0, 1)]
N_GROUPS = len(GROUPS)
DISTANT = [(2, 1, 1), (2, 1, 0), (2, 0, 1), (2, 0, 0)]
N_PACKETS = N_GROUPS + len(DISTANT)


def lane_plan():
    starts, base = [], {}
    block, lane = 0, 0
    for index, (gx, gy, gz) in enumerate(GROUPS):
        if index == 8:
            block, lane = 1, 0
        dirs = [(gx, sy, sz) for sz in ((-1, 1) if gz else (0,)) for sy in ((-1, 1) if gy else (0,))]
        starts.append((block, lane, lane + MOVE_CAP * len(dirs)))
        for dx, dy, dz in dirs:
            base[(dz + 1) * 9 + (dy + 1) * 3 + dx + 1] = block * LANES + lane
            lane += MOVE_CAP
    return starts, base


LANE_STARTS, LANE_BASE = lane_plan()
STAY = 13


def split3(values):
    hi = values.astype(jnp.bfloat16).astype(jnp.float32)
    rest = values - hi
    mid = rest.astype(jnp.bfloat16).astype(jnp.float32)
    return jnp.concatenate([hi, mid, rest - mid], axis=0).astype(jnp.bfloat16)


def join3(parts):
    rows = parts.shape[0] // 3
    return (parts[0:rows] + parts[rows:2 * rows]) + parts[2 * rows:3 * rows]


def dot_nt(a, b):
    return lax.dot_general(a, b, (((1,), (1,)), ((), ())), preferred_element_type=jnp.float32)


def dot_nn(a, b):
    return lax.dot_general(a, b, (((1,), (0,)), ((), ())), preferred_element_type=jnp.float32)


def my_coords():
    return lax.axis_index("z"), lax.axis_index("y"), lax.axis_index("x")


def peer_id(coords, offset):
    mz, my, mx = coords
    return (lax.rem(mz + offset[0], NZ), lax.rem(my + offset[1], NY), lax.rem(mx + offset[2] + NX, NX))


def entry_signals(coords):
    barrier = pltpu.get_barrier_semaphore()
    for offset in PEERS:
        pl.semaphore_signal(barrier, inc=1, device_id=peer_id(coords, offset), device_id_type=MESH)
    return barrier


def exchange_kernel(brick_ref, pos_ref, vel_ref, frc_ref, id_ref, ok_ref, gat_ref, pkt_ref, own_ref, raw, ids_in, oks_in, pad_ref, int_ref, send_pos, send_pkt, in_sem, pos_send_sem, pos_recv_sem, pkt_send_sem, pkt_recv_sem):
    coords = my_coords()
    fetches = [pltpu.make_async_copy(src, dst, in_sem.at[index]) for index, (src, dst) in enumerate(((pos_ref, raw.at[0]), (vel_ref, raw.at[1]), (frc_ref, raw.at[2]), (id_ref, ids_in), (ok_ref, oks_in)))]
    for fetch in fetches:
        fetch.start()
    barrier = entry_signals(coords)
    brick = brick_ref[0]
    tail = slice(WIDE - LANES, WIDE)
    pad_ref[:, :, tail] = jnp.zeros((3, 4, LANES), jnp.float32)
    int_ref[:, tail] = jnp.zeros((2, LANES), jnp.int32)
    for fetch in fetches:
        fetch.wait()
    for index in range(3):
        pad_ref[index, 0:3, 0:CAP] = raw[index]
    int_ref[0:1, 0:CAP] = ids_in[...].reshape(1, CAP)
    int_ref[1:2, 0:CAP] = oks_in[...].reshape(1, CAP)
    owned = int_ref[1:2, :] > 0
    moved, half, code = [], [], jnp.zeros((1, WIDE), jnp.int32)
    for axis, (mine, size, weight) in enumerate(((coords[2], NX, 1), (coords[1], NY, 3), (coords[0], NZ, 9))):
        box = brick * float(size)
        low = mine.astype(jnp.float32) * brick
        high = (mine + 1).astype(jnp.float32) * brick
        half_v = pad_ref[1, axis:axis + 1, :] + (0.5 * DT) * pad_ref[2, axis:axis + 1, :]
        drift = pad_ref[0, axis:axis + 1, :] + DT * half_v
        step = jnp.where(drift >= high, 2, jnp.where(drift < low, 0, 1))
        code = code + step * weight
        wrapped = jnp.where(drift < 0.0, drift + box, jnp.where(drift >= box, drift - box, drift))
        moved.append(wrapped)
        half.append(half_v)
    code = jnp.where(owned, code, -1)
    for axis in range(3):
        for block in range(8):
            if block < BLOCKS:
                lanes = slice(block * LANES, (block + 1) * LANES)
                send_pos[axis, block:block + 1, :] = jnp.where(owned[:, lanes], moved[axis][:, lanes], NOWHERE)
            else:
                send_pos[axis, block:block + 1, :] = jnp.full((1, LANES), NOWHERE, jnp.float32)
    ids = int_ref[0:1, :]
    id_hi = (lax.shift_right_logical(ids, 16) + 1).astype(jnp.float32)
    id_lo = (ids & 65535).astype(jnp.float32)
    data = jnp.concatenate(moved + half + [id_hi, id_lo], axis=0)
    member = (jnp.broadcast_to(code, (32, WIDE)) == lax.broadcasted_iota(jnp.int32, (32, WIDE), 0)).astype(jnp.float32)
    tri = (lax.broadcasted_iota(jnp.int32, (LANES, LANES), 0) < lax.broadcasted_iota(jnp.int32, (LANES, LANES), 1)).astype(jnp.bfloat16)
    codes = lax.broadcasted_iota(jnp.int32, (32, LANES), 0)
    running = jnp.zeros((32, LANES), jnp.float32)
    for move, first in LANE_BASE.items():
        running = jnp.where(codes == move, float(first), running)
    slots = []
    for block in range(BLOCKS):
        part = member[:, block * LANES:(block + 1) * LANES]
        before = dot_nn(part.astype(jnp.bfloat16), tri)
        slots.append(jnp.sum(part * (before + running), axis=0, keepdims=True))
        running = running + jnp.sum(part, axis=1, keepdims=True)
    slot = jnp.concatenate(slots, axis=1)
    stay = code == STAY
    mover_slot = jnp.where(owned & jnp.logical_not(stay), slot, -1.0).astype(jnp.int32)
    pick = (lax.broadcasted_iota(jnp.int32, (2 * LANES, WIDE), 0) == mover_slot).astype(jnp.float32).astype(jnp.bfloat16)
    packet = join3(dot_nt(split3(data), pick))
    send_pkt[0] = packet[:, 0:LANES]
    send_pkt[1] = packet[:, LANES:2 * LANES]
    own_ref[0:8, :] = data
    own_ref[8:16, :] = jnp.concatenate([jnp.where(stay, slot, -1.0), jnp.zeros((7, WIDE), jnp.float32)], axis=0)
    pl.semaphore_wait(barrier, len(PEERS))
    copies = []
    for index, (gx, gy, gz) in enumerate(GROUPS + DISTANT):
        peer = peer_id(coords, (gz, gy, gx))
        if index < N_GROUPS:
            copies.append(pltpu.make_async_remote_copy(src_ref=send_pos, dst_ref=gat_ref.at[index], send_sem=pos_send_sem.at[index], recv_sem=pos_recv_sem.at[index], device_id=peer, device_id_type=MESH))
            copies[-1].start()
        block = LANE_STARTS[index][0] if index < N_GROUPS else 0
        copies.append(pltpu.make_async_remote_copy(src_ref=send_pkt.at[block], dst_ref=pkt_ref.at[index], send_sem=pkt_send_sem.at[index], recv_sem=pkt_recv_sem.at[index], device_id=peer, device_id_type=MESH))
        copies[-1].start()
    gat_ref[N_GROUPS] = send_pos[...]
    for copy in copies:
        copy.wait()


CAND_ROWS = 8 * (N_GROUPS + 1) + 8
MAX_ROWS = BLOCKS + CAND_ROWS
QUAD = 4


def force_kernel(brick_ref, gat_ref, pkt_ref, own_ref, pos_out, vel_out, frc_out, id_out, ok_out, eng_out, others, mine, acc, sorted_ref):
    mz, my, mx = my_coords()
    brick = brick_ref[0]
    half_l = 0.5 * brick
    reach = half_l + RC
    sizes = (NX, NY, NZ)
    centre = [(index.astype(jnp.float32) + 0.5) * brick for index in (mx, my, mz)]
    box = [brick * float(size) for size in sizes]
    lane_1 = lax.broadcasted_iota(jnp.int32, (1, LANES), 1)

    arrived = []
    for block in range(2):
        total = jnp.zeros((8, LANES), jnp.float32)
        for index in range(N_GROUPS):
            where_block, first, last = LANE_STARTS[index]
            if where_block == block:
                total = total + jnp.where((lane_1 >= first) & (lane_1 < last), pkt_ref[index], 0.0)
        arrived.append(total)
    arr = jnp.concatenate(arrived, axis=1)
    data = jnp.concatenate([own_ref[0:8, :], arr], axis=1)
    int_max = 2147483647
    ids = lax.shift_left(data[6:7].astype(jnp.int32) - 1, 16) + data[7:8].astype(jnp.int32)
    stay_rank = own_ref[8:9, :]
    stay = stay_rank >= 0.0
    arr_ok = arr[6:7] > 0.5
    arr_id = jnp.where(arr_ok, ids[:, WIDE:], int_max)
    own_id = jnp.where(stay, ids[:, :WIDE], int_max)
    arr_col = jnp.transpose(jnp.broadcast_to(arr_id, (8, 2 * LANES)), (1, 0))[:, 0:1]
    own_col = jnp.transpose(jnp.broadcast_to(own_id, (8, WIDE)), (1, 0))[:, 0:1]
    all_id = jnp.concatenate([own_id, arr_id], axis=1)
    arr_before = jnp.sum((arr_col < all_id).astype(jnp.float32), axis=0, keepdims=True)
    stay_before = jnp.sum((own_col < arr_id).astype(jnp.float32), axis=0, keepdims=True)
    rank = jnp.concatenate([jnp.where(stay, stay_rank + arr_before[:, :WIDE], -1.0), jnp.where(arr_ok, stay_before + arr_before[:, WIDE:], -1.0)], axis=1).astype(jnp.int32)
    n_own = jnp.sum((rank >= 0).astype(jnp.float32)).astype(jnp.int32)
    parts = split3(data)
    for block in range(BLOCKS):
        pick = (lax.broadcasted_iota(jnp.int32, (LANES, WIDE + 2 * LANES), 0) + block * LANES == rank).astype(jnp.float32).astype(jnp.bfloat16)
        sorted_ref[block] = join3(dot_nt(parts, pick))
    for block in range(BLOCKS):
        valid = lane_1 + block * LANES < n_own
        for axis in range(3):
            rel = sorted_ref[block, axis:axis + 1, :] - centre[axis]
            others[axis, block] = jnp.broadcast_to(jnp.where(valid, rel, FAR_OTHER), (8, LANES))
            column = jnp.transpose(jnp.broadcast_to(jnp.where(valid, rel, FAR_OWN), (8, LANES)), (1, 0))[:, 0:1]
            mine[axis, pl.ds(block * 16, 16)] = jnp.broadcast_to(column, (LANES, LANES)).reshape(16, 8, LANES)
    own_rows = lax.div(n_own + (LANES - 1), LANES)

    rel = []
    for axis in range(3):
        distant = [jnp.where(pkt_ref[N_GROUPS + k, 6:7, :] > 0.5, pkt_ref[N_GROUPS + k, axis:axis + 1, :], NOWHERE) for k in range(len(DISTANT))]
        values = jnp.concatenate([gat_ref[:, axis].reshape(8 * (N_GROUPS + 1), LANES)] + distant + [jnp.full((4, LANES), NOWHERE, jnp.float32)], axis=0) - centre[axis]
        values = jnp.where(values > 0.5 * box[axis], values - box[axis], jnp.where(values < -0.5 * box[axis], values + box[axis], values))
        rel.append(values)
    near = (jnp.abs(rel[0]) < reach) & (jnp.abs(rel[1]) < reach) & (jnp.abs(rel[2]) < reach)
    inside = (jnp.abs(rel[0]) < half_l) & (jnp.abs(rel[1]) < half_l) & (jnp.abs(rel[2]) < half_l)
    ghost = (near & jnp.logical_not(inside)).astype(jnp.float32).astype(jnp.bfloat16)
    row_i = lax.broadcasted_iota(jnp.int32, (LANES, LANES), 0)
    col_i = lax.broadcasted_iota(jnp.int32, (LANES, LANES), 1)
    cum = dot_nn(ghost, (row_i <= col_i).astype(jnp.bfloat16)).astype(jnp.int32)
    count = dot_nn(ghost, jnp.ones((LANES, LANES), jnp.bfloat16))
    base = dot_nn((col_i < row_i).astype(jnp.bfloat16)[:CAND_ROWS, :CAND_ROWS], count.astype(jnp.bfloat16)).astype(jnp.int32)
    count = count.astype(jnp.int32)
    n_ghost = jnp.max(base[CAND_ROWS - 8:] + count[CAND_ROWS - 8:])
    lane_c = lax.broadcasted_iota(jnp.int32, (CAND_ROWS, LANES), 1)
    place = (lane_c - base) & (LANES - 1)
    source = jnp.zeros((CAND_ROWS, LANES), jnp.int32)
    for step in (64, 32, 16, 8, 4, 2, 1):
        probe = jnp.take_along_axis(cum, source + (step - 1), axis=1)
        source = jnp.where(probe <= place, source + step, source)
    target = jnp.where(place < count, lax.shift_right_logical(base + place, 7), -1)
    packed = [jnp.take_along_axis(values, source, axis=1) for values in rel]
    ghost_rows = lax.div(n_ghost + (LANES - 1), LANES)

    def pack_row(row, carry):
        hit = target == row
        filled = lane_1 + row * LANES < n_ghost
        for axis in range(3):
            values = jnp.sum(jnp.where(hit, packed[axis], 0.0), axis=0, keepdims=True)
            others[axis, own_rows + row] = jnp.broadcast_to(jnp.where(filled, values, FAR_OTHER), (8, LANES))
        return carry

    lax.fori_loop(0, ghost_rows, pack_row, 0)
    rows = own_rows + ghost_rows

    rc2 = jnp.full((8, LANES), RC * RC + 0.0 * brick, jnp.float32)
    kappa = UPC / 48.0

    def radial(dist_sq):
        inv_r = lax.rsqrt(dist_sq)
        inv_2 = inv_r * inv_r
        inv_4 = inv_2 * inv_2
        term = inv_4 * inv_2 - 0.5
        tail = kappa * inv_r
        return term * (inv_4 * inv_4) + tail, term * term, tail * dist_sq

    cut_f, cut_a, cut_h = radial(rc2)
    own_minus_lane = lax.broadcasted_iota(jnp.int32, (8, LANES), 0) - lax.broadcasted_iota(jnp.int32, (8, LANES), 1)
    zero = jnp.zeros((8, LANES), jnp.float32)

    def pair_loops(wrap):
        inv_box = [1.0 / (brick * float(size)) for size in sizes]

        def quad(index, energy):
            first = index * QUAD
            own = [[mine[axis, first + k] for axis in range(3)] for k in range(QUAD)]
            self_row = lax.div(first, 16)

            def one_row(row, sums, with_self):
                other = [others[axis, row] for axis in range(3)]
                force, sum_a, sum_h = list(sums[:-2]), sums[-2], sums[-1]
                for k in range(QUAD):
                    delta = [own[k][axis] - other[axis] for axis in range(3)]
                    if wrap:
                        for axis in (1, 2):
                            delta[axis] = delta[axis] - box[axis] * jnp.floor(delta[axis] * inv_box[axis] + 0.5)
                    dist_sq = delta[0] * delta[0] + delta[1] * delta[1] + delta[2] * delta[2]
                    if with_self:
                        dist_sq = jnp.where(own_minus_lane == row * LANES - (first + k) * 8, rc2, dist_sq)
                    dist_sq = jnp.minimum(dist_sq, rc2)
                    scale, a, h = radial(dist_sq)
                    scale = scale - cut_f
                    for axis in range(3):
                        force[3 * k + axis] = force[3 * k + axis] + scale * delta[axis]
                    sum_a, sum_h = sum_a + a, sum_h + h
                return tuple(force) + (sum_a, sum_h)

            def other_row(count, sums):
                return one_row(count + (count >= self_row).astype(jnp.int32), sums, False)

            def two_rows(count, sums):
                return other_row(2 * count + 1, other_row(2 * count, sums))

            sums = one_row(self_row, (zero,) * (3 * QUAD + 2), True)
            twos = lax.div(rows - 1, 2)
            sums = lax.fori_loop(0, twos, two_rows, sums)
            sums = lax.fori_loop(2 * twos, rows - 1, other_row, sums)
            for k in range(QUAD):
                for axis in range(3):
                    acc[axis, first + k] = sums[3 * k + axis]
            n = QUAD * rows.astype(jnp.float32)
            return energy + (sums[-2] - n * cut_a) - 12.0 * (sums[-1] - n * cut_h)

        quads = lax.div(n_own + (8 * QUAD - 1), 8 * QUAD)
        energy = lax.fori_loop(0, quads, quad, zero)
        eng_out[...] = jnp.full((8, LANES), 2.0 * jnp.sum(energy), jnp.float32)

    pl.when(brick >= 2.0 * RC)(lambda: pair_loops(False))
    pl.when(brick < 2.0 * RC)(lambda: pair_loops(True))

    for block in range(BLOCKS):
        width = min(LANES, CAP - block * LANES)
        lanes = slice(block * LANES, block * LANES + width)
        valid = lane_1 + block * LANES < n_own
        rows_s = sorted_ref[block]
        for axis in range(3):
            turned = jnp.transpose(acc[axis, pl.ds(block * 16, 16)].reshape(LANES, LANES), (1, 0))
            force = jnp.where(valid, 48.0 * jnp.sum(turned, axis=0, keepdims=True), 0.0)
            frc_out[axis:axis + 1, lanes] = force[:, :width]
            vel_out[axis:axis + 1, lanes] = (rows_s[3 + axis:4 + axis] + (0.5 * DT) * force)[:, :width]
            pos_out[axis:axis + 1, lanes] = rows_s[axis:axis + 1, :width]
        new_id = lax.shift_left(rows_s[6:7].astype(jnp.int32) - 1, 16) + rows_s[7:8].astype(jnp.int32)
        id_out[lanes] = jnp.where(valid, new_id, 0)[:, :width].reshape(width)
        ok_out[lanes] = valid.astype(jnp.int32)[:, :width].reshape(width)


def energy_kernel(eng_ref, out_ref, slots, send_sem, recv_sem):
    coords = my_coords()
    mz, my, mx = coords
    barrier = entry_signals(coords)
    pl.semaphore_wait(barrier, len(PEERS))
    place = (mz * NY + my) * NX + mx
    copies = []
    for index, offset in enumerate(PEERS):
        copies.append(pltpu.make_async_remote_copy(src_ref=eng_ref, dst_ref=slots.at[place], send_sem=send_sem.at[index], recv_sem=recv_sem.at[index], device_id=peer_id(coords, offset), device_id_type=MESH))
        copies[-1].start()
    slots[place] = eng_ref[...]
    for copy in copies:
        copy.wait()
    total = slots[0]
    for index in range(1, NZ * NY * NX):
        total = total + slots[index]
    out_ref[0, 0] = jnp.max(total)


VMEM_SPEC = pl.BlockSpec(memory_space=pltpu.VMEM)
HBM_SPEC = pl.BlockSpec(memory_space=pltpu.HBM)
VMEM_LIMIT = 8 * 1024 * 1024
SMEM_SPEC = pl.BlockSpec(memory_space=pltpu.SMEM)


def solution(mesh):
    def local_step(atom_pos, atom_vel, atom_frc, atom_id, atom_ok, brick_side):
        f32 = jnp.float32
        brick = brick_side.reshape(1)
        n_dev = NZ * NY * NX
        gat, pkt, own = pl.pallas_call(
            exchange_kernel,
            out_shape=(jax.ShapeDtypeStruct((N_GROUPS + 1, 3, 8, LANES), f32), jax.ShapeDtypeStruct((N_PACKETS, 8, LANES), f32), jax.ShapeDtypeStruct((16, WIDE), f32)),
            in_specs=[SMEM_SPEC] + [HBM_SPEC] * 5,
            out_specs=(VMEM_SPEC,) * 3,
            scratch_shapes=[
                pltpu.VMEM((3, 3, CAP), f32),
                pltpu.VMEM((CAP,), jnp.int32),
                pltpu.VMEM((CAP,), jnp.int32),
                pltpu.VMEM((3, 4, WIDE), f32),
                pltpu.VMEM((2, WIDE), jnp.int32),
                pltpu.VMEM((3, 8, LANES), f32),
                pltpu.VMEM((2, 8, LANES), f32),
                pltpu.SemaphoreType.DMA((5,)),
                pltpu.SemaphoreType.DMA((N_GROUPS,)),
                pltpu.SemaphoreType.DMA((N_GROUPS,)),
                pltpu.SemaphoreType.DMA((N_PACKETS,)),
                pltpu.SemaphoreType.DMA((N_PACKETS,)),
            ],
            compiler_params=pltpu.CompilerParams(collective_id=0, has_side_effects=True, vmem_limit_bytes=VMEM_LIMIT),
            name="exchange",
        )(brick, *(pltpu.with_memory_space_constraint(value, pltpu.HBM) for value in (atom_pos.T, atom_vel.T, atom_frc.T, atom_id, atom_ok)))
        pos, vel, frc, ids, oks, eng = pl.pallas_call(
            force_kernel,
            out_shape=(jax.ShapeDtypeStruct((3, CAP), f32),) * 3 + (jax.ShapeDtypeStruct((CAP,), jnp.int32),) * 2 + (jax.ShapeDtypeStruct((8, LANES), f32),),
            in_specs=[SMEM_SPEC] + [VMEM_SPEC] * 3,
            out_specs=(VMEM_SPEC,) * 6,
            scratch_shapes=[
                pltpu.VMEM((3, MAX_ROWS, 8, LANES), f32),
                pltpu.VMEM((3, BLOCKS * 16, 8, LANES), f32),
                pltpu.VMEM((3, BLOCKS * 16, 8, LANES), f32),
                pltpu.VMEM((BLOCKS, 8, LANES), f32),
            ],
            compiler_params=pltpu.CompilerParams(vmem_limit_bytes=VMEM_LIMIT),
            name="forces",
        )(brick, gat, pkt, own)
        total = pl.pallas_call(
            energy_kernel,
            out_shape=jax.ShapeDtypeStruct((1, 1), f32),
            in_specs=[VMEM_SPEC],
            out_specs=SMEM_SPEC,
            scratch_shapes=[pltpu.VMEM((n_dev, 8, LANES), f32), pltpu.SemaphoreType.DMA((n_dev - 1,)), pltpu.SemaphoreType.DMA((n_dev - 1,))],
            compiler_params=pltpu.CompilerParams(collective_id=1, has_side_effects=True, vmem_limit_bytes=VMEM_LIMIT),
            name="energy",
        )(eng)
        return pos.T, vel.T, frc.T, ids, oks, total.reshape(())

    row_spec = P(MESH_AXES, None)
    id_spec = P(MESH_AXES)
    return jax.shard_map(local_step, mesh=mesh, in_specs=(row_spec, row_spec, row_spec, id_spec, id_spec, P()), out_specs=(row_spec, row_spec, row_spec, id_spec, id_spec, P()), check_vma=False)
```

```python
import jax
import jax.numpy as jnp
from jax import lax
from jax.experimental import pallas as pl
from jax.experimental.pallas import tpu as pltpu
from jax.sharding import PartitionSpec as P

DT = 0.005
RC = 2.5
UPC = -48.0 * RC ** -13 + 24.0 * RC ** -7
MESH_AXES = ("z", "y", "x")
MESH = pl.DeviceIdType.MESH
NZ, NY, NX = 2, 2, 4
CAP = 729
LANES = 128
BLOCKS = 6
WIDE = BLOCKS * LANES
MOVE_CAP = CAP // 100
FAR_OWN = 1.0e4
FAR_OTHER = -1.0e4
NOWHERE = 1.0e9
PEERS = [(dz, dy, dx) for dz in range(NZ) for dy in range(NY) for dx in range(NX)][1:]
GROUPS = [(1, 1, 1), (-1, 1, 1), (1, 1, 0), (-1, 1, 0), (1, 0, 1), (-1, 0, 1), (1, 0, 0), (-1, 0, 0), (0, 1, 1), (0, 1, 0), (0, 0, 1)]
N_GROUPS = len(GROUPS)
DISTANT = [(2, 1, 1), (2, 1, 0), (2, 0, 1), (2, 0, 0)]
N_PACKETS = N_GROUPS + len(DISTANT)


def lane_plan():
    starts, base = [], {}
    block, lane = 0, 0
    for index, (gx, gy, gz) in enumerate(GROUPS):
        if index == 8:
            block, lane = 1, 0
        dirs = [(gx, sy, sz) for sz in ((-1, 1) if gz else (0,)) for sy in ((-1, 1) if gy else (0,))]
        starts.append((block, lane, lane + MOVE_CAP * len(dirs)))
        for dx, dy, dz in dirs:
            base[(dz + 1) * 9 + (dy + 1) * 3 + dx + 1] = block * LANES + lane
            lane += MOVE_CAP
    return starts, base


LANE_STARTS, LANE_BASE = lane_plan()
STAY = 13


def split3(values):
    hi = values.astype(jnp.bfloat16).astype(jnp.float32)
    rest = values - hi
    mid = rest.astype(jnp.bfloat16).astype(jnp.float32)
    return jnp.concatenate([hi, mid, rest - mid], axis=0).astype(jnp.bfloat16)


def join3(parts):
    rows = parts.shape[0] // 3
    return (parts[0:rows] + parts[rows:2 * rows]) + parts[2 * rows:3 * rows]


def dot_nt(a, b):
    return lax.dot_general(a, b, (((1,), (1,)), ((), ())), preferred_element_type=jnp.float32)


def dot_nn(a, b):
    return lax.dot_general(a, b, (((1,), (0,)), ((), ())), preferred_element_type=jnp.float32)


def my_coords():
    return lax.axis_index("z"), lax.axis_index("y"), lax.axis_index("x")


def peer_id(coords, offset):
    mz, my, mx = coords
    return (lax.rem(mz + offset[0], NZ), lax.rem(my + offset[1], NY), lax.rem(mx + offset[2] + NX, NX))


def entry_signals(coords):
    barrier = pltpu.get_barrier_semaphore()
    for offset in PEERS:
        pl.semaphore_signal(barrier, inc=1, device_id=peer_id(coords, offset), device_id_type=MESH)
    return barrier


def exchange_kernel(brick_ref, pos_ref, vel_ref, frc_ref, id_ref, ok_ref, gat_ref, pkt_ref, own_ref, raw, ids_in, oks_in, pad_ref, int_ref, send_pos, send_pkt, in_sem, pos_send_sem, pos_recv_sem, pkt_send_sem, pkt_recv_sem):
    coords = my_coords()
    fetches = [pltpu.make_async_copy(src, dst, in_sem.at[index]) for index, (src, dst) in enumerate(((pos_ref, raw.at[0]), (vel_ref, raw.at[1]), (frc_ref, raw.at[2]), (id_ref, ids_in), (ok_ref, oks_in)))]
    for fetch in fetches:
        fetch.start()
    barrier = entry_signals(coords)
    brick = brick_ref[0]
    tail = slice(WIDE - LANES, WIDE)
    pad_ref[:, :, tail] = jnp.zeros((3, 4, LANES), jnp.float32)
    int_ref[:, tail] = jnp.zeros((2, LANES), jnp.int32)
    for fetch in fetches:
        fetch.wait()
    for index in range(3):
        pad_ref[index, 0:3, 0:CAP] = raw[index]
    int_ref[0:1, 0:CAP] = ids_in[...].reshape(1, CAP)
    int_ref[1:2, 0:CAP] = oks_in[...].reshape(1, CAP)
    owned = int_ref[1:2, :] > 0
    moved, half, code = [], [], jnp.zeros((1, WIDE), jnp.int32)
    for axis, (mine, size, weight) in enumerate(((coords[2], NX, 1), (coords[1], NY, 3), (coords[0], NZ, 9))):
        box = brick * float(size)
        low = mine.astype(jnp.float32) * brick
        high = (mine + 1).astype(jnp.float32) * brick
        half_v = pad_ref[1, axis:axis + 1, :] + (0.5 * DT) * pad_ref[2, axis:axis + 1, :]
        drift = pad_ref[0, axis:axis + 1, :] + DT * half_v
        step = jnp.where(drift >= high, 2, jnp.where(drift < low, 0, 1))
        code = code + step * weight
        wrapped = jnp.where(drift < 0.0, drift + box, jnp.where(drift >= box, drift - box, drift))
        moved.append(wrapped)
        half.append(half_v)
    code = jnp.where(owned, code, -1)
    for axis in range(3):
        for block in range(8):
            if block < BLOCKS:
                lanes = slice(block * LANES, (block + 1) * LANES)
                send_pos[axis, block:block + 1, :] = jnp.where(owned[:, lanes], moved[axis][:, lanes], NOWHERE)
            else:
                send_pos[axis, block:block + 1, :] = jnp.full((1, LANES), NOWHERE, jnp.float32)
    ids = int_ref[0:1, :]
    id_hi = (lax.shift_right_logical(ids, 16) + 1).astype(jnp.float32)
    id_lo = (ids & 65535).astype(jnp.float32)
    data = jnp.concatenate(moved + half + [id_hi, id_lo], axis=0)
    member = (jnp.broadcast_to(code, (32, WIDE)) == lax.broadcasted_iota(jnp.int32, (32, WIDE), 0)).astype(jnp.float32)
    tri = (lax.broadcasted_iota(jnp.int32, (LANES, LANES), 0) < lax.broadcasted_iota(jnp.int32, (LANES, LANES), 1)).astype(jnp.bfloat16)
    codes = lax.broadcasted_iota(jnp.int32, (32, LANES), 0)
    running = jnp.zeros((32, LANES), jnp.float32)
    for move, first in LANE_BASE.items():
        running = jnp.where(codes == move, float(first), running)
    slots = []
    for block in range(BLOCKS):
        part = member[:, block * LANES:(block + 1) * LANES]
        before = dot_nn(part.astype(jnp.bfloat16), tri)
        slots.append(jnp.sum(part * (before + running), axis=0, keepdims=True))
        running = running + jnp.sum(part, axis=1, keepdims=True)
    slot = jnp.concatenate(slots, axis=1)
    stay = code == STAY
    mover_slot = jnp.where(owned & jnp.logical_not(stay), slot, -1.0).astype(jnp.int32)
    pick = (lax.broadcasted_iota(jnp.int32, (2 * LANES, WIDE), 0) == mover_slot).astype(jnp.float32).astype(jnp.bfloat16)
    packet = join3(dot_nt(split3(data), pick))
    send_pkt[0] = packet[:, 0:LANES]
    send_pkt[1] = packet[:, LANES:2 * LANES]
    own_ref[0:8, :] = data
    own_ref[8:16, :] = jnp.concatenate([jnp.where(stay, slot, -1.0), jnp.zeros((7, WIDE), jnp.float32)], axis=0)
    pl.semaphore_wait(barrier, len(PEERS))
    copies = []
    for index, (gx, gy, gz) in enumerate(GROUPS + DISTANT):
        peer = peer_id(coords, (gz, gy, gx))
        if index < N_GROUPS:
            copies.append(pltpu.make_async_remote_copy(src_ref=send_pos, dst_ref=gat_ref.at[index], send_sem=pos_send_sem.at[index], recv_sem=pos_recv_sem.at[index], device_id=peer, device_id_type=MESH))
            copies[-1].start()
        block = LANE_STARTS[index][0] if index < N_GROUPS else 0
        copies.append(pltpu.make_async_remote_copy(src_ref=send_pkt.at[block], dst_ref=pkt_ref.at[index], send_sem=pkt_send_sem.at[index], recv_sem=pkt_recv_sem.at[index], device_id=peer, device_id_type=MESH))
        copies[-1].start()
    gat_ref[N_GROUPS] = send_pos[...]
    for copy in copies:
        copy.wait()


CAND_ROWS = 8 * (N_GROUPS + 1) + 8
MAX_ROWS = BLOCKS + CAND_ROWS
GROUPS_OWN = BLOCKS * 16
QUAD = 4
FIXED_QUADS = 15
FIXED_ROWS = 12


def pair_tools(mine, others, rc2, wrap_box):
    kappa = UPC / 48.0

    def radial(dist_sq):
        inv_r = lax.rsqrt(dist_sq)
        inv_2 = inv_r * inv_r
        inv_4 = inv_2 * inv_2
        term = inv_4 * inv_2 - 0.5
        tail = kappa * inv_r
        return term * (inv_4 * inv_4) + tail, term * term, tail * dist_sq

    cut_f, cut_a, cut_h = radial(rc2)
    own_minus_lane = lax.broadcasted_iota(jnp.int32, (8, LANES), 0) - lax.broadcasted_iota(jnp.int32, (8, LANES), 1)

    def load_own(first):
        return [[mine[axis, first + k] for axis in range(3)] for k in range(QUAD)]

    def one_row(own, first, row, sums, with_self):
        other = [others[axis, row] for axis in range(3)]
        force, sum_a, sum_h = list(sums[:-2]), sums[-2], sums[-1]
        for k in range(QUAD):
            delta = [own[k][axis] - other[axis] for axis in range(3)]
            for axis, box, inv_box in wrap_box:
                delta[axis] = delta[axis] - box * jnp.floor(delta[axis] * inv_box + 0.5)
            dist_sq = delta[0] * delta[0] + delta[1] * delta[1] + delta[2] * delta[2]
            if with_self:
                dist_sq = jnp.where(own_minus_lane == row * LANES - (first + k) * 8, rc2, dist_sq)
            dist_sq = jnp.minimum(dist_sq, rc2)
            scale, a, h = radial(dist_sq)
            scale = scale - cut_f
            for axis in range(3):
                force[3 * k + axis] = force[3 * k + axis] + scale * delta[axis]
            sum_a, sum_h = sum_a + a, sum_h + h
        return tuple(force) + (sum_a, sum_h)

    def energy_of(sums, n_rows):
        return (sums[-2] - (QUAD * n_rows) * cut_a) - 12.0 * (sums[-1] - (QUAD * n_rows) * cut_h)

    return load_own, one_row, energy_of


def prepare_kernel(brick_ref, gat_ref, pkt_ref, own_ref, sorted_ref, mine, others, acc, eng_ref):
    mz, my, mx = my_coords()
    brick = brick_ref[0]
    half_l = 0.5 * brick
    reach = half_l + RC
    sizes = (NX, NY, NZ)
    centre = [(index.astype(jnp.float32) + 0.5) * brick for index in (mx, my, mz)]
    box = [brick * float(size) for size in sizes]
    lane_1 = lax.broadcasted_iota(jnp.int32, (1, LANES), 1)

    arrived = []
    for block in range(2):
        total = jnp.zeros((8, LANES), jnp.float32)
        for index in range(N_GROUPS):
            where_block, first, last = LANE_STARTS[index]
            if where_block == block:
                total = total + jnp.where((lane_1 >= first) & (lane_1 < last), pkt_ref[index], 0.0)
        arrived.append(total)
    arr = jnp.concatenate(arrived, axis=1)
    data = jnp.concatenate([own_ref[0:8, :], arr], axis=1)
    int_max = 2147483647
    ids = lax.shift_left(data[6:7].astype(jnp.int32) - 1, 16) + data[7:8].astype(jnp.int32)
    stay_rank = own_ref[8:9, :]
    stay = stay_rank >= 0.0
    arr_ok = arr[6:7] > 0.5
    arr_id = jnp.where(arr_ok, ids[:, WIDE:], int_max)
    own_id = jnp.where(stay, ids[:, :WIDE], int_max)
    arr_col = jnp.transpose(jnp.broadcast_to(arr_id, (8, 2 * LANES)), (1, 0))[:, 0:1]
    own_col = jnp.transpose(jnp.broadcast_to(own_id, (8, WIDE)), (1, 0))[:, 0:1]
    all_id = jnp.concatenate([own_id, arr_id], axis=1)
    arr_before = jnp.sum((arr_col < all_id).astype(jnp.float32), axis=0, keepdims=True)
    stay_before = jnp.sum((own_col < arr_id).astype(jnp.float32), axis=0, keepdims=True)
    rank = jnp.concatenate([jnp.where(stay, stay_rank + arr_before[:, :WIDE], -1.0), jnp.where(arr_ok, stay_before + arr_before[:, WIDE:], -1.0)], axis=1).astype(jnp.int32)
    n_own = jnp.sum((rank >= 0).astype(jnp.float32)).astype(jnp.int32)
    parts = split3(data)
    for block in range(BLOCKS):
        pick = (lax.broadcasted_iota(jnp.int32, (LANES, WIDE + 2 * LANES), 0) + block * LANES == rank).astype(jnp.float32).astype(jnp.bfloat16)
        rows_s = join3(jnp.transpose(dot_nt(pick, parts), (1, 0)))
        sorted_ref[block] = rows_s
        valid = lane_1 + block * LANES < n_own
        rel = jnp.concatenate([rows_s[axis:axis + 1] - centre[axis] for axis in range(3)] + [rows_s[3:8]], axis=0)
        columns = jnp.transpose(jnp.where(valid, rel, FAR_OWN), (1, 0))
        for axis in range(3):
            others[axis, block] = jnp.broadcast_to(jnp.where(valid, rel[axis:axis + 1], 0.0), (8, LANES))
            mine[axis, pl.ds(block * 16, 16)] = jnp.broadcast_to(columns[:, axis:axis + 1], (LANES, LANES)).reshape(16, 8, LANES)

    rel = []
    for axis in range(3):
        distant = [jnp.where(pkt_ref[N_GROUPS + k, 6:7, :] > 0.5, pkt_ref[N_GROUPS + k, axis:axis + 1, :], NOWHERE) for k in range(len(DISTANT))]
        values = jnp.concatenate([gat_ref[:, axis].reshape(8 * (N_GROUPS + 1), LANES)] + distant + [jnp.full((4, LANES), NOWHERE, jnp.float32)], axis=0) - centre[axis]
        values = jnp.where(values > 0.5 * box[axis], values - box[axis], jnp.where(values < -0.5 * box[axis], values + box[axis], values))
        rel.append(values)
    near = (jnp.abs(rel[0]) < reach) & (jnp.abs(rel[1]) < reach) & (jnp.abs(rel[2]) < reach)
    inside = (jnp.abs(rel[0]) < half_l) & (jnp.abs(rel[1]) < half_l) & (jnp.abs(rel[2]) < half_l)
    ghost = (near & jnp.logical_not(inside)).astype(jnp.float32).astype(jnp.bfloat16)
    row_i = lax.broadcasted_iota(jnp.int32, (LANES, LANES), 0)
    col_i = lax.broadcasted_iota(jnp.int32, (LANES, LANES), 1)
    cum = dot_nn(ghost, (row_i <= col_i).astype(jnp.bfloat16)).astype(jnp.int32)
    count = dot_nn(ghost, jnp.ones((LANES, LANES), jnp.bfloat16))
    base = dot_nn((col_i < row_i).astype(jnp.bfloat16)[:CAND_ROWS, :CAND_ROWS], count.astype(jnp.bfloat16)).astype(jnp.int32) + n_own
    count = count.astype(jnp.int32)
    n_all = jnp.max(base[CAND_ROWS - 8:] + count[CAND_ROWS - 8:])
    lane_c = lax.broadcasted_iota(jnp.int32, (CAND_ROWS, LANES), 1)
    place = (lane_c - base) & (LANES - 1)
    source = jnp.zeros((CAND_ROWS, LANES), jnp.int32)
    for step in (64, 32, 16, 8, 4, 2, 1):
        probe = jnp.take_along_axis(cum, source + (step - 1), axis=1)
        source = jnp.where(probe <= place, source + step, source)
    target = jnp.where(place < count, lax.shift_right_logical(base + place, 7), -1)
    packed = [jnp.take_along_axis(values, source, axis=1) for values in rel]
    rows = lax.div(n_all + (LANES - 1), LANES)
    own_rows = lax.div(n_own + (LANES - 1), LANES)

    def pack_row(row, carry):
        hit = target == row
        filled = lane_1 + row * LANES < n_all
        for axis in range(3):
            own_part = jnp.where(row < own_rows, others[axis, row], 0.0)
            values = jnp.sum(jnp.where(hit, packed[axis], 0.0), axis=0, keepdims=True)
            others[axis, row] = jnp.where(filled, own_part + values, FAR_OTHER)
        return carry

    lax.fori_loop(lax.div(n_own, LANES), rows, pack_row, 0)

    rc2 = jnp.full((8, LANES), RC * RC + 0.0 * brick, jnp.float32)
    zero = jnp.zeros((8, LANES), jnp.float32)
    acc[...] = jnp.zeros_like(acc)
    quads = lax.div(n_own + (8 * QUAD - 1), 8 * QUAD)
    far = jnp.full((8, LANES), FAR_OTHER, jnp.float32)

    def set_far(row, carry):
        for axis in range(3):
            others[axis, row] = far
        return carry

    def excess(first_quad, last_quad, first_row, wrap_box, energy):
        load_own, one_row, energy_of = pair_tools(mine, others, rc2, wrap_box)

        def quad(index, total):
            first = index * QUAD
            own = load_own(first)
            sums = (zero,) * (3 * QUAD + 2)
            sums = lax.fori_loop(first_row, rows, lambda row, part: one_row(own, first, row, part, True), sums)
            for k in range(QUAD):
                for axis in range(3):
                    acc[axis, first + k] = sums[3 * k + axis]
            return total + energy_of(sums, (rows - first_row).astype(jnp.float32))

        return lax.fori_loop(first_quad, last_quad, quad, energy)

    def plain():
        short = jnp.where(rows > FIXED_ROWS, jnp.minimum(quads, FIXED_QUADS), 0)
        energy = excess(0, short, FIXED_ROWS, [], zero)
        eng_ref[...] = excess(FIXED_QUADS, quads, 0, [], energy)
        lax.fori_loop(rows, FIXED_ROWS, set_far, 0)

    def wrapped():
        wrap_box = [(axis, box[axis], 1.0 / box[axis]) for axis in (1, 2)]
        eng_ref[...] = excess(0, quads, 0, wrap_box, zero)
        lax.fori_loop(0, FIXED_ROWS, set_far, 0)

    pl.when(brick >= 2.0 * RC)(plain)
    pl.when(brick < 2.0 * RC)(wrapped)


def tile_kernel(brick_ref, mine, others, part, eng_ref, frc_ref, out_ref, acc, eng, slots, send_sem, recv_sem):
    coords = my_coords()
    mz, my, mx = coords
    barrier = entry_signals(coords)
    brick = brick_ref[0]
    rc2 = jnp.full((8, LANES), RC * RC + 0.0 * brick, jnp.float32)
    load_own, one_row, energy_of = pair_tools(mine, others, rc2, [])

    def quad(index, energy):
        first = index * QUAD
        own = load_own(first)
        self_row = lax.div(first, 16)
        zero = jnp.zeros((8, LANES), jnp.float32)
        sums = tuple(part[axis, first + k] for k in range(QUAD) for axis in range(3)) + (zero, zero)
        sums = one_row(own, first, self_row, sums, True)
        for count in range(FIXED_ROWS - 1):
            sums = one_row(own, first, count + (count >= self_row).astype(jnp.int32), sums, False)
        for k in range(QUAD):
            for axis in range(3):
                acc[axis, first + k] = sums[3 * k + axis]
        return energy + energy_of(sums, float(FIXED_ROWS))

    energy = lax.fori_loop(0, FIXED_QUADS, quad, eng_ref[...])
    eng[...] = jnp.full((8, LANES), 2.0 * jnp.sum(energy), jnp.float32)
    for group in range(FIXED_QUADS * QUAD, 16 * (FIXED_QUADS * QUAD // 16 + 1)):
        for axis in range(3):
            acc[axis, group] = part[axis, group]
    pl.semaphore_wait(barrier, len(PEERS))
    place = (mz * NY + my) * NX + mx
    copies = []
    for index, offset in enumerate(PEERS):
        copies.append(pltpu.make_async_remote_copy(src_ref=eng, dst_ref=slots.at[place], send_sem=send_sem.at[index], recv_sem=recv_sem.at[index], device_id=peer_id(coords, offset), device_id_type=MESH))
        copies[-1].start()
    slots[place] = eng[...]
    for block in range(BLOCKS):
        held = acc if block <= FIXED_QUADS * QUAD // 16 else part
        for axis in range(3):
            turned = jnp.transpose(held[axis, pl.ds(block * 16, 16)].reshape(LANES, LANES), (1, 0))
            frc_ref[axis:axis + 1, block * LANES:(block + 1) * LANES] = 48.0 * jnp.sum(turned, axis=0, keepdims=True)
    for copy in copies:
        copy.wait()
    total = slots[0]
    for index in range(1, NZ * NY * NX):
        total = total + slots[index]
    out_ref[0, 0] = jnp.max(total)


def finish_kernel(sorted_ref, frc_ref, pos_out, vel_out, frc_out, id_out, ok_out):
    for block in range(BLOCKS):
        width = min(LANES, CAP - block * LANES)
        lanes = slice(block * LANES, block * LANES + width)
        rows_s = sorted_ref[block]
        valid = rows_s[6:7] > 0.5
        for axis in range(3):
            force = jnp.where(valid, frc_ref[axis:axis + 1, block * LANES:(block + 1) * LANES], 0.0)
            frc_out[axis:axis + 1, lanes] = force[:, :width]
            vel_out[axis:axis + 1, lanes] = (rows_s[3 + axis:4 + axis] + (0.5 * DT) * force)[:, :width]
            pos_out[axis:axis + 1, lanes] = rows_s[axis:axis + 1, :width]
        new_id = lax.shift_left(rows_s[6:7].astype(jnp.int32) - 1, 16) + rows_s[7:8].astype(jnp.int32)
        id_out[lanes] = jnp.where(valid, new_id, 0)[:, :width].reshape(width)
        ok_out[lanes] = valid.astype(jnp.int32)[:, :width].reshape(width)


VMEM_SPEC = pl.BlockSpec(memory_space=pltpu.VMEM)
HBM_SPEC = pl.BlockSpec(memory_space=pltpu.HBM)
VMEM_LIMIT = 8 * 1024 * 1024
SMEM_SPEC = pl.BlockSpec(memory_space=pltpu.SMEM)


def solution(mesh):
    def local_step(atom_pos, atom_vel, atom_frc, atom_id, atom_ok, brick_side):
        f32 = jnp.float32
        brick = brick_side.reshape(1)
        n_dev = NZ * NY * NX
        gat, pkt, own = pl.pallas_call(
            exchange_kernel,
            out_shape=(jax.ShapeDtypeStruct((N_GROUPS + 1, 3, 8, LANES), f32), jax.ShapeDtypeStruct((N_PACKETS, 8, LANES), f32), jax.ShapeDtypeStruct((16, WIDE), f32)),
            in_specs=[SMEM_SPEC] + [HBM_SPEC] * 5,
            out_specs=(VMEM_SPEC,) * 3,
            scratch_shapes=[
                pltpu.VMEM((3, 3, CAP), f32),
                pltpu.VMEM((CAP,), jnp.int32),
                pltpu.VMEM((CAP,), jnp.int32),
                pltpu.VMEM((3, 4, WIDE), f32),
                pltpu.VMEM((2, WIDE), jnp.int32),
                pltpu.VMEM((3, 8, LANES), f32),
                pltpu.VMEM((2, 8, LANES), f32),
                pltpu.SemaphoreType.DMA((5,)),
                pltpu.SemaphoreType.DMA((N_GROUPS,)),
                pltpu.SemaphoreType.DMA((N_GROUPS,)),
                pltpu.SemaphoreType.DMA((N_PACKETS,)),
                pltpu.SemaphoreType.DMA((N_PACKETS,)),
            ],
            compiler_params=pltpu.CompilerParams(collective_id=0, has_side_effects=True, vmem_limit_bytes=VMEM_LIMIT),
            name="exchange",
        )(brick, *(pltpu.with_memory_space_constraint(value, pltpu.HBM) for value in (atom_pos.T, atom_vel.T, atom_frc.T, atom_id, atom_ok)))
        own_tiles = jax.ShapeDtypeStruct((3, GROUPS_OWN, 8, LANES), f32)
        placed, mine, others, part, eng = pl.pallas_call(
            prepare_kernel,
            out_shape=(jax.ShapeDtypeStruct((BLOCKS, 8, LANES), f32), own_tiles, jax.ShapeDtypeStruct((3, MAX_ROWS, 8, LANES), f32), own_tiles, jax.ShapeDtypeStruct((8, LANES), f32)),
            in_specs=[SMEM_SPEC] + [VMEM_SPEC] * 3,
            out_specs=(VMEM_SPEC,) * 5,
            compiler_params=pltpu.CompilerParams(vmem_limit_bytes=VMEM_LIMIT),
            name="prepare",
        )(brick, gat, pkt, own)
        frc_rows, total = pl.pallas_call(
            tile_kernel,
            out_shape=(jax.ShapeDtypeStruct((8, WIDE), f32), jax.ShapeDtypeStruct((1, 1), f32)),
            in_specs=[SMEM_SPEC] + [VMEM_SPEC] * 4,
            out_specs=(VMEM_SPEC, SMEM_SPEC),
            scratch_shapes=[pltpu.VMEM((3, GROUPS_OWN, 8, LANES), f32), pltpu.VMEM((8, LANES), f32), pltpu.VMEM((n_dev, 8, LANES), f32), pltpu.SemaphoreType.DMA((n_dev - 1,)), pltpu.SemaphoreType.DMA((n_dev - 1,))],
            compiler_params=pltpu.CompilerParams(collective_id=1, has_side_effects=True, vmem_limit_bytes=VMEM_LIMIT),
            name="tile",
        )(brick, mine, others, part, eng)
        pos, vel, frc, ids, oks = pl.pallas_call(
            finish_kernel,
            out_shape=(jax.ShapeDtypeStruct((3, CAP), f32),) * 3 + (jax.ShapeDtypeStruct((CAP,), jnp.int32),) * 2,
            in_specs=[VMEM_SPEC] * 2,
            out_specs=(VMEM_SPEC,) * 5,
            compiler_params=pltpu.CompilerParams(vmem_limit_bytes=VMEM_LIMIT),
            name="finish",
        )(placed, frc_rows)
        return pos.T, vel.T, frc.T, ids, oks, total.reshape(())

    row_spec = P(MESH_AXES, None)
    id_spec = P(MESH_AXES)
    return jax.shard_map(local_step, mesh=mesh, in_specs=(row_spec, row_spec, row_spec, id_spec, id_spec, P()), out_specs=(row_spec, row_spec, row_spec, id_spec, id_spec, P()), check_vma=False)
```

```python
import jax
import jax.numpy as jnp
from jax import lax
from jax.experimental import pallas as pl
from jax.experimental.pallas import tpu as pltpu
from jax.sharding import PartitionSpec as P

DT = 0.005
RC = 2.5
UPC = -48.0 * RC ** -13 + 24.0 * RC ** -7
MESH_AXES = ("z", "y", "x")
MESH = pl.DeviceIdType.MESH
NZ, NY, NX = 2, 2, 4
CAP = 729
LANES = 128
BLOCKS = 6
WIDE = BLOCKS * LANES
MOVE_CAP = CAP // 100
FAR_OWN = 1.0e4
FAR_OTHER = -1.0e4
NOWHERE = 1.0e9
GHOST_SQ = RC * RC + 0.01
PEERS = [(dz, dy, dx) for dz in range(NZ) for dy in range(NY) for dx in range(NX)][1:]
GROUPS = [(1, 1, 1), (-1, 1, 1), (1, 1, 0), (-1, 1, 0), (1, 0, 1), (-1, 0, 1), (1, 0, 0), (-1, 0, 0), (0, 1, 1), (0, 1, 0), (0, 0, 1)]
N_GROUPS = len(GROUPS)
DISTANT = [(2, 1, 1), (2, 1, 0), (2, 0, 1), (2, 0, 0)]
N_PACKETS = N_GROUPS + len(DISTANT)


def lane_plan():
    starts, base = [], {}
    block, lane = 0, 0
    for index, (gx, gy, gz) in enumerate(GROUPS):
        if index == 8:
            block, lane = 1, 0
        dirs = [(gx, sy, sz) for sz in ((-1, 1) if gz else (0,)) for sy in ((-1, 1) if gy else (0,))]
        starts.append((block, lane, lane + MOVE_CAP * len(dirs)))
        for dx, dy, dz in dirs:
            base[(dz + 1) * 9 + (dy + 1) * 3 + dx + 1] = block * LANES + lane
            lane += MOVE_CAP
    return starts, base


LANE_STARTS, LANE_BASE = lane_plan()
STAY = 13


def split3(values):
    hi = values.astype(jnp.bfloat16).astype(jnp.float32)
    rest = values - hi
    mid = rest.astype(jnp.bfloat16).astype(jnp.float32)
    return jnp.concatenate([hi, mid, rest - mid], axis=0).astype(jnp.bfloat16)


def join3(parts):
    rows = parts.shape[0] // 3
    return (parts[0:rows] + parts[rows:2 * rows]) + parts[2 * rows:3 * rows]


def dot_nt(a, b):
    return lax.dot_general(a, b, (((1,), (1,)), ((), ())), preferred_element_type=jnp.float32)


def dot_nn(a, b):
    return lax.dot_general(a, b, (((1,), (0,)), ((), ())), preferred_element_type=jnp.float32)


def my_coords():
    return lax.axis_index("z"), lax.axis_index("y"), lax.axis_index("x")


def peer_id(coords, offset):
    mz, my, mx = coords
    return (lax.rem(mz + offset[0], NZ), lax.rem(my + offset[1], NY), lax.rem(mx + offset[2] + NX, NX))


def entry_signals(coords):
    barrier = pltpu.get_barrier_semaphore()
    for offset in PEERS:
        pl.semaphore_signal(barrier, inc=1, device_id=peer_id(coords, offset), device_id_type=MESH)
    return barrier


def exchange_kernel(brick_ref, pos_ref, vel_ref, frc_ref, id_ref, ok_ref, gat_ref, pkt_ref, own_ref, raw, ids_in, oks_in, pad_ref, int_ref, send_pos, send_pkt, in_sem, pos_send_sem, pos_recv_sem, pkt_send_sem, pkt_recv_sem):
    coords = my_coords()
    fetches = [pltpu.make_async_copy(src, dst, in_sem.at[index]) for index, (src, dst) in enumerate(((pos_ref, raw.at[0]), (vel_ref, raw.at[1]), (frc_ref, raw.at[2]), (id_ref, ids_in), (ok_ref, oks_in)))]
    for fetch in fetches:
        fetch.start()
    barrier = entry_signals(coords)
    tail = slice(WIDE - LANES, WIDE)
    pad_ref[:, :, tail] = jnp.zeros((3, 4, LANES), jnp.float32)
    int_ref[:, tail] = jnp.zeros((2, LANES), jnp.int32)
    for fetch in fetches:
        fetch.wait()
    brick = brick_ref[...]
    for index in range(3):
        pad_ref[index, 0:3, 0:CAP] = raw[index]
    int_ref[0:1, 0:CAP] = ids_in[...].reshape(1, CAP)
    int_ref[1:2, 0:CAP] = oks_in[...].reshape(1, CAP)
    owned = int_ref[1:2, :] > 0
    moved, half, code = [], [], jnp.zeros((1, WIDE), jnp.int32)
    for axis, (mine, size, weight) in enumerate(((coords[2], NX, 1), (coords[1], NY, 3), (coords[0], NZ, 9))):
        box = brick * float(size)
        low = mine.astype(jnp.float32) * brick
        high = (mine + 1).astype(jnp.float32) * brick
        half_v = pad_ref[1, axis:axis + 1, :] + (0.5 * DT) * pad_ref[2, axis:axis + 1, :]
        drift = pad_ref[0, axis:axis + 1, :] + DT * half_v
        step = jnp.where(drift >= high, 2, jnp.where(drift < low, 0, 1))
        code = code + step * weight
        wrapped = jnp.where(drift < 0.0, drift + box, jnp.where(drift >= box, drift - box, drift))
        moved.append(wrapped)
        half.append(half_v)
    code = jnp.where(owned, code, -1)
    for axis in range(3):
        for block in range(8):
            if block < BLOCKS:
                lanes = slice(block * LANES, (block + 1) * LANES)
                send_pos[axis, block:block + 1, :] = jnp.where(owned[:, lanes], moved[axis][:, lanes], NOWHERE)
            else:
                send_pos[axis, block:block + 1, :] = jnp.full((1, LANES), NOWHERE, jnp.float32)
    ids = int_ref[0:1, :]
    id_hi = (lax.shift_right_logical(ids, 16) + 1).astype(jnp.float32)
    id_lo = (ids & 65535).astype(jnp.float32)
    data = jnp.concatenate(moved + half + [id_hi, id_lo], axis=0)
    member = (jnp.broadcast_to(code, (32, WIDE)) == lax.broadcasted_iota(jnp.int32, (32, WIDE), 0)).astype(jnp.float32)
    tri = (lax.broadcasted_iota(jnp.int32, (LANES, LANES), 0) < lax.broadcasted_iota(jnp.int32, (LANES, LANES), 1)).astype(jnp.bfloat16)
    codes = lax.broadcasted_iota(jnp.int32, (32, LANES), 0)
    running = jnp.zeros((32, LANES), jnp.float32)
    for move, first in LANE_BASE.items():
        running = jnp.where(codes == move, float(first), running)
    slots = []
    for block in range(BLOCKS):
        part = member[:, block * LANES:(block + 1) * LANES]
        before = dot_nn(part.astype(jnp.bfloat16), tri)
        slots.append(jnp.sum(part * (before + running), axis=0, keepdims=True))
        running = running + jnp.sum(part, axis=1, keepdims=True)
    slot = jnp.concatenate(slots, axis=1)
    stay = code == STAY
    mover_slot = jnp.where(owned & jnp.logical_not(stay), slot, -1.0).astype(jnp.int32)
    pick = (lax.broadcasted_iota(jnp.int32, (2 * LANES, WIDE), 0) == mover_slot).astype(jnp.float32).astype(jnp.bfloat16)
    packet = join3(dot_nt(split3(data), pick))
    send_pkt[0] = packet[:, 0:LANES]
    send_pkt[1] = packet[:, LANES:2 * LANES]
    own_ref[0:8, :] = data
    own_ref[8:16, :] = jnp.concatenate([jnp.where(stay, slot, -1.0), jnp.full((7, WIDE), brick, jnp.float32)], axis=0)
    pl.semaphore_wait(barrier, len(PEERS))
    copies = []
    for index, (gx, gy, gz) in enumerate(GROUPS + DISTANT):
        peer = peer_id(coords, (gz, gy, gx))
        if index < N_GROUPS:
            copies.append(pltpu.make_async_remote_copy(src_ref=send_pos, dst_ref=gat_ref.at[index], send_sem=pos_send_sem.at[index], recv_sem=pos_recv_sem.at[index], device_id=peer, device_id_type=MESH))
            copies[-1].start()
        block = LANE_STARTS[index][0] if index < N_GROUPS else 0
        copies.append(pltpu.make_async_remote_copy(src_ref=send_pkt.at[block], dst_ref=pkt_ref.at[index], send_sem=pkt_send_sem.at[index], recv_sem=pkt_recv_sem.at[index], device_id=peer, device_id_type=MESH))
        copies[-1].start()
    gat_ref[N_GROUPS] = send_pos[...]
    for copy in copies:
        copy.wait()


CAND_ROWS = 8 * (N_GROUPS + 1) + 8
MAX_ROWS = BLOCKS + CAND_ROWS
GROUPS_OWN = BLOCKS * 16
QUAD = 4
FIXED_QUADS = 16
FIXED_ROWS = 11


def pair_tools(mine, others, rc2, wrap_box):
    kappa = UPC / 48.0

    def radial(dist_sq):
        inv_r = lax.rsqrt(dist_sq)
        inv_2 = inv_r * inv_r
        inv_4 = inv_2 * inv_2
        term = inv_4 * inv_2 - 0.5
        tail = kappa * inv_r
        return term * (inv_4 * inv_4) + tail, term * term, tail * dist_sq

    def quad_energy(a, h):
        return ((a[0] + a[1]) + (a[2] + a[3])) - 12.0 * ((h[0] + h[1]) + (h[2] + h[3]))

    cut_f, cut_a, cut_h = radial(rc2)
    cut_energy = quad_energy([cut_a] * QUAD, [cut_h] * QUAD)
    own_minus_lane = lax.broadcasted_iota(jnp.int32, (8, LANES), 0) - lax.broadcasted_iota(jnp.int32, (8, LANES), 1)

    def load_own(first):
        return [[mine[axis, first + k] for axis in range(3)] for k in range(QUAD)]

    def one_row(own, first, row, sums, with_self):
        other = [others[axis, row] for axis in range(3)]
        force, energy, parts_a, parts_h = list(sums[:-1]), sums[-1], [], []
        for k in range(QUAD):
            delta = [own[k][axis] - other[axis] for axis in range(3)]
            for axis, box, inv_box in wrap_box:
                delta[axis] = delta[axis] - box * jnp.floor(delta[axis] * inv_box + 0.5)
            dist_sq = delta[0] * delta[0] + delta[1] * delta[1] + delta[2] * delta[2]
            if with_self:
                dist_sq = jnp.where(own_minus_lane == row * LANES - (first + k) * 8, rc2, dist_sq)
            dist_sq = jnp.minimum(dist_sq, rc2)
            scale, a, h = radial(dist_sq)
            scale = scale - cut_f
            for axis in range(3):
                force[3 * k + axis] = force[3 * k + axis] + scale * delta[axis]
            parts_a.append(a)
            parts_h.append(h)
        return tuple(force) + (energy + (quad_energy(parts_a, parts_h) - cut_energy),)

    return load_own, one_row


def prepare_kernel(gat_ref, pkt_ref, own_ref, sorted_ref, mine, others, acc, eng_ref):
    mz, my, mx = my_coords()
    brick = own_ref[9:10, 0:LANES]
    half_l = 0.5 * brick
    sizes = (NX, NY, NZ)
    centre = [(index.astype(jnp.float32) + 0.5) * brick for index in (mx, my, mz)]
    box = [brick * float(size) for size in sizes]
    lane_1 = lax.broadcasted_iota(jnp.int32, (1, LANES), 1)

    arrived = []
    for block in range(2):
        total = jnp.zeros((8, LANES), jnp.float32)
        for index in range(N_GROUPS):
            where_block, first, last = LANE_STARTS[index]
            if where_block == block:
                total = total + jnp.where((lane_1 >= first) & (lane_1 < last), pkt_ref[index], 0.0)
        arrived.append(total)
    arr = jnp.concatenate(arrived, axis=1)
    data = jnp.concatenate([own_ref[0:8, :], arr], axis=1)
    int_max = 2147483647
    ids = lax.shift_left(data[6:7].astype(jnp.int32) - 1, 16) + data[7:8].astype(jnp.int32)
    stay_rank = own_ref[8:9, :]
    stay = stay_rank >= 0.0
    arr_ok = arr[6:7] > 0.5
    arr_id = jnp.where(arr_ok, ids[:, WIDE:], int_max)
    own_id = jnp.where(stay, ids[:, :WIDE], int_max)
    n_vec = jnp.sum(stay.astype(jnp.float32), axis=1, keepdims=True) + jnp.sum(arr_ok.astype(jnp.float32), axis=1, keepdims=True)
    n_own = jnp.max(n_vec).astype(jnp.int32)

    rel = []
    for axis in range(3):
        distant = [jnp.where(pkt_ref[N_GROUPS + k, 6:7, :] > 0.5, pkt_ref[N_GROUPS + k, axis:axis + 1, :], NOWHERE) for k in range(len(DISTANT))]
        values = jnp.concatenate([gat_ref[:, axis].reshape(8 * (N_GROUPS + 1), LANES)] + distant + [jnp.full((4, LANES), NOWHERE, jnp.float32)], axis=0) - centre[axis]
        values = jnp.where(values > 0.5 * box[axis], values - box[axis], jnp.where(values < -0.5 * box[axis], values + box[axis], values))
        rel.append(values)
    over = [jnp.maximum(jnp.abs(values) - half_l, 0.0) for values in rel]
    gap_sq = over[0] * over[0] + over[1] * over[1] + over[2] * over[2]
    ghost = ((gap_sq > 0.0) & (gap_sq < GHOST_SQ)).astype(jnp.float32).astype(jnp.bfloat16)
    row_i = lax.broadcasted_iota(jnp.int32, (LANES, LANES), 0)
    col_i = lax.broadcasted_iota(jnp.int32, (LANES, LANES), 1)
    cum = dot_nn(ghost, (row_i <= col_i).astype(jnp.bfloat16)).astype(jnp.int32)
    count = dot_nn(ghost, jnp.ones((LANES, LANES), jnp.bfloat16))
    base = dot_nn((col_i < row_i).astype(jnp.bfloat16)[:CAND_ROWS, :CAND_ROWS], count.astype(jnp.bfloat16)).astype(jnp.int32) + n_vec.astype(jnp.int32)
    count = count.astype(jnp.int32)
    n_all = jnp.max(base[CAND_ROWS - 8:] + count[CAND_ROWS - 8:])
    lane_c = lax.broadcasted_iota(jnp.int32, (CAND_ROWS, LANES), 1)
    place = (lane_c - base) & (LANES - 1)
    source = jnp.zeros((CAND_ROWS, LANES), jnp.int32)
    for step in (64, 32, 16, 8, 4, 2, 1):
        probe = jnp.take_along_axis(cum, source + (step - 1), axis=1)
        source = jnp.where(probe <= place, source + step, source)
    target = jnp.where(place < count, lax.shift_right_logical(base + place, 7), -1)
    packed = [jnp.take_along_axis(values, source, axis=1) for values in rel]
    arr_col = jnp.transpose(jnp.broadcast_to(arr_id, (8, 2 * LANES)), (1, 0))[:, 0:1]
    own_col = jnp.transpose(jnp.broadcast_to(own_id, (8, WIDE)), (1, 0))[:, 0:1]
    all_id = jnp.concatenate([own_id, arr_id], axis=1)
    arr_before = jnp.sum((arr_col < all_id).astype(jnp.float32), axis=0, keepdims=True)
    stay_before = jnp.sum((own_col < arr_id).astype(jnp.float32), axis=0, keepdims=True)
    rank = jnp.concatenate([jnp.where(stay, stay_rank + arr_before[:, :WIDE], -1.0), jnp.where(arr_ok, stay_before + arr_before[:, WIDE:], -1.0)], axis=1).astype(jnp.int32)
    parts = split3(data)
    for block in range(BLOCKS):
        pick = (lax.broadcasted_iota(jnp.int32, (LANES, WIDE + 2 * LANES), 0) + block * LANES == rank).astype(jnp.float32).astype(jnp.bfloat16)
        rows_s = join3(jnp.transpose(dot_nt(pick, parts), (1, 0)))
        sorted_ref[block] = rows_s
        valid = lane_1 + block * LANES < n_vec.astype(jnp.int32)
        own_rel = jnp.concatenate([rows_s[axis:axis + 1] - centre[axis] for axis in range(3)] + [rows_s[3:8]], axis=0)
        columns = jnp.transpose(jnp.where(valid, own_rel, FAR_OWN), (1, 0))
        for axis in range(3):
            others[axis, block] = jnp.broadcast_to(jnp.where(valid, own_rel[axis:axis + 1], 0.0), (8, LANES))
            mine[axis, pl.ds(block * 16, 16)] = jnp.broadcast_to(columns[:, axis:axis + 1], (LANES, LANES)).reshape(16, 8, LANES)

    rows = lax.div(n_all + (LANES - 1), LANES)
    own_rows = lax.div(n_own + (LANES - 1), LANES)

    def pack_row(row, carry):
        hit = target == row
        filled = lane_1 + row * LANES < n_all
        for axis in range(3):
            own_part = jnp.where(row < own_rows, others[axis, row], 0.0)
            values = jnp.sum(jnp.where(hit, packed[axis], 0.0), axis=0, keepdims=True)
            others[axis, row] = jnp.where(filled, own_part + values, FAR_OTHER)
        return carry

    lax.fori_loop(lax.div(n_own, LANES), rows, pack_row, 0)

    rc2 = RC * RC + 0.0 * own_ref[8:16, 0:LANES]
    zero = jnp.zeros((8, LANES), jnp.float32)
    acc[...] = jnp.zeros_like(acc)
    quads = lax.div(n_own + (8 * QUAD - 1), 8 * QUAD)
    far = jnp.full((8, LANES), FAR_OTHER, jnp.float32)

    def set_far(row, carry):
        for axis in range(3):
            others[axis, row] = far
        return carry

    def excess(first_quad, last_quad, first_row, wrap_box, energy):
        load_own, one_row = pair_tools(mine, others, rc2, wrap_box)

        def quad(index, total):
            first = index * QUAD
            own = load_own(first)
            sums = (zero,) * (3 * QUAD) + (total,)
            sums = lax.fori_loop(first_row, rows, lambda row, part: one_row(own, first, row, part, True), sums)
            for k in range(QUAD):
                for axis in range(3):
                    acc[axis, first + k] = sums[3 * k + axis]
            return sums[-1]

        return lax.fori_loop(first_quad, last_quad, quad, energy)

    def plain():
        short = jnp.where(rows > FIXED_ROWS, jnp.minimum(quads, FIXED_QUADS), 0)
        energy = excess(0, short, FIXED_ROWS, [], zero)
        eng_ref[...] = excess(FIXED_QUADS, quads, 0, [], energy)
        lax.fori_loop(rows, FIXED_ROWS, set_far, 0)

    def wrapped():
        wrap_box = [(axis, box[axis], 1.0 / box[axis]) for axis in (1, 2)]
        eng_ref[...] = excess(0, quads, 0, wrap_box, zero)
        lax.fori_loop(0, FIXED_ROWS, set_far, 0)

    wide = jnp.max(brick) >= 2.0 * RC
    pl.when(wide)(plain)
    pl.when(jnp.logical_not(wide))(wrapped)


def tile_kernel(mine, others, part, eng_ref, frc_ref, out_ref, acc, eng, slots, send_sem, recv_sem):
    coords = my_coords()
    mz, my, mx = coords
    barrier = entry_signals(coords)
    rc2 = RC * RC + 0.0 * mine[0, 0]
    load_own, one_row = pair_tools(mine, others, rc2, [])

    def quad(index, energy):
        first = index * QUAD
        own = load_own(first)
        self_row = lax.div(first, 16)
        sums = tuple(part[axis, first + k] for k in range(QUAD) for axis in range(3)) + (energy,)
        sums = one_row(own, first, self_row, sums, True)
        for count in range(FIXED_ROWS - 1):
            sums = one_row(own, first, count + (count >= self_row).astype(jnp.int32), sums, False)
        for k in range(QUAD):
            for axis in range(3):
                acc[axis, first + k] = sums[3 * k + axis]
        return sums[-1]

    energy = lax.fori_loop(0, FIXED_QUADS, quad, eng_ref[...])
    eng[...] = jnp.full((8, LANES), 2.0 * jnp.sum(energy), jnp.float32)
    pl.semaphore_wait(barrier, len(PEERS))
    place = (mz * NY + my) * NX + mx
    copies = []
    for index, offset in enumerate(PEERS):
        copies.append(pltpu.make_async_remote_copy(src_ref=eng, dst_ref=slots.at[place], send_sem=send_sem.at[index], recv_sem=recv_sem.at[index], device_id=peer_id(coords, offset), device_id_type=MESH))
        copies[-1].start()
    slots[place] = eng[...]
    for block in range(BLOCKS):
        held = acc if block < FIXED_QUADS * QUAD // 16 else part
        for axis in range(3):
            turned = jnp.transpose(held[axis, pl.ds(block * 16, 16)].reshape(LANES, LANES), (1, 0))
            frc_ref[axis:axis + 1, block * LANES:(block + 1) * LANES] = 48.0 * jnp.sum(turned, axis=0, keepdims=True)
    for copy in copies:
        copy.wait()
    total = slots[0]
    for index in range(1, NZ * NY * NX):
        total = total + slots[index]
    out_ref[...] = total


def finish_kernel(sorted_ref, frc_ref, total_ref, pos_out, vel_out, frc_out, id_out, ok_out, eng_out):
    eng_out[...] = jnp.max(total_ref[...])
    for block in range(BLOCKS):
        width = min(LANES, CAP - block * LANES)
        lanes = slice(block * LANES, block * LANES + width)
        rows_s = sorted_ref[block]
        valid = rows_s[6:7] > 0.5
        for axis in range(3):
            force = jnp.where(valid, frc_ref[axis:axis + 1, block * LANES:(block + 1) * LANES], 0.0)
            frc_out[axis:axis + 1, lanes] = force[:, :width]
            vel_out[axis:axis + 1, lanes] = (rows_s[3 + axis:4 + axis] + (0.5 * DT) * force)[:, :width]
            pos_out[axis:axis + 1, lanes] = rows_s[axis:axis + 1, :width]
        new_id = lax.shift_left(rows_s[6:7].astype(jnp.int32) - 1, 16) + rows_s[7:8].astype(jnp.int32)
        id_out[lanes] = jnp.where(valid, new_id, 0)[:, :width].reshape(width)
        ok_out[lanes] = valid.astype(jnp.int32)[:, :width].reshape(width)


VMEM_SPEC = pl.BlockSpec(memory_space=pltpu.VMEM)
HBM_SPEC = pl.BlockSpec(memory_space=pltpu.HBM)
VMEM_LIMIT = 8 * 1024 * 1024
SMEM_SPEC = pl.BlockSpec(memory_space=pltpu.SMEM)


def solution(mesh):
    def local_step(atom_pos, atom_vel, atom_frc, atom_id, atom_ok, brick_side):
        f32 = jnp.float32
        n_dev = NZ * NY * NX
        gat, pkt, own = pl.pallas_call(
            exchange_kernel,
            out_shape=(jax.ShapeDtypeStruct((N_GROUPS + 1, 3, 8, LANES), f32), jax.ShapeDtypeStruct((N_PACKETS, 8, LANES), f32), jax.ShapeDtypeStruct((16, WIDE), f32)),
            in_specs=[SMEM_SPEC] + [HBM_SPEC] * 5,
            out_specs=(VMEM_SPEC,) * 3,
            scratch_shapes=[
                pltpu.VMEM((3, 3, CAP), f32),
                pltpu.VMEM((CAP,), jnp.int32),
                pltpu.VMEM((CAP,), jnp.int32),
                pltpu.VMEM((3, 4, WIDE), f32),
                pltpu.VMEM((2, WIDE), jnp.int32),
                pltpu.VMEM((3, 8, LANES), f32),
                pltpu.VMEM((2, 8, LANES), f32),
                pltpu.SemaphoreType.DMA((5,)),
                pltpu.SemaphoreType.DMA((N_GROUPS,)),
                pltpu.SemaphoreType.DMA((N_GROUPS,)),
                pltpu.SemaphoreType.DMA((N_PACKETS,)),
                pltpu.SemaphoreType.DMA((N_PACKETS,)),
            ],
            compiler_params=pltpu.CompilerParams(collective_id=0, has_side_effects=True, vmem_limit_bytes=VMEM_LIMIT),
            name="exchange",
        )(brick_side, *(pltpu.with_memory_space_constraint(value, pltpu.HBM) for value in (atom_pos.T, atom_vel.T, atom_frc.T, atom_id, atom_ok)))
        own_tiles = jax.ShapeDtypeStruct((3, GROUPS_OWN, 8, LANES), f32)
        placed, mine, others, part, eng = pl.pallas_call(
            prepare_kernel,
            out_shape=(jax.ShapeDtypeStruct((BLOCKS, 8, LANES), f32), own_tiles, jax.ShapeDtypeStruct((3, MAX_ROWS, 8, LANES), f32), own_tiles, jax.ShapeDtypeStruct((8, LANES), f32)),
            in_specs=[VMEM_SPEC] * 3,
            out_specs=(VMEM_SPEC,) * 5,
            compiler_params=pltpu.CompilerParams(vmem_limit_bytes=VMEM_LIMIT),
            name="prepare",
        )(gat, pkt, own)
        frc_rows, total = pl.pallas_call(
            tile_kernel,
            out_shape=(jax.ShapeDtypeStruct((8, WIDE), f32), jax.ShapeDtypeStruct((8, LANES), f32)),
            in_specs=[VMEM_SPEC] * 4,
            out_specs=(VMEM_SPEC,) * 2,
            scratch_shapes=[pltpu.VMEM((3, GROUPS_OWN, 8, LANES), f32), pltpu.VMEM((8, LANES), f32), pltpu.VMEM((n_dev, 8, LANES), f32), pltpu.SemaphoreType.DMA((n_dev - 1,)), pltpu.SemaphoreType.DMA((n_dev - 1,))],
            compiler_params=pltpu.CompilerParams(collective_id=1, has_side_effects=True, vmem_limit_bytes=VMEM_LIMIT),
            name="tile",
        )(mine, others, part, eng)
        pos, vel, frc, ids, oks, energy = pl.pallas_call(
            finish_kernel,
            out_shape=(jax.ShapeDtypeStruct((3, CAP), f32),) * 3 + (jax.ShapeDtypeStruct((CAP,), jnp.int32),) * 2 + (jax.ShapeDtypeStruct((), f32),),
            in_specs=[VMEM_SPEC] * 3,
            out_specs=(VMEM_SPEC,) * 5 + (SMEM_SPEC,),
            compiler_params=pltpu.CompilerParams(vmem_limit_bytes=VMEM_LIMIT),
            name="finish",
        )(placed, frc_rows, total)
        return pos.T, vel.T, frc.T, ids, oks, energy

    row_spec = P(MESH_AXES, None)
    id_spec = P(MESH_AXES)
    return jax.shard_map(local_step, mesh=mesh, in_specs=(row_spec, row_spec, row_spec, id_spec, id_spec, P()), out_specs=(row_spec, row_spec, row_spec, id_spec, id_spec, P()), check_vma=False)
```

```python
import jax
import jax.numpy as jnp
from jax import lax
from jax.experimental import pallas as pl
from jax.experimental.pallas import tpu as pltpu
from jax.sharding import PartitionSpec as P

DT = 0.005
RC = 2.5
UPC = -48.0 * RC ** -13 + 24.0 * RC ** -7
MESH_AXES = ("z", "y", "x")
MESH = pl.DeviceIdType.MESH
NZ, NY, NX = 2, 2, 4
CAP = 729
LANES = 128
BLOCKS = 6
WIDE = BLOCKS * LANES
MOVE_CAP = CAP // 100
FAR_OWN = 1.0e4
FAR_OTHER = -1.0e4
NOWHERE = 1.0e9
GHOST_SQ = RC * RC + 0.01
PEERS = [(dz, dy, dx) for dz in range(NZ) for dy in range(NY) for dx in range(NX)][1:]
SIDES = [(1, 1), (1, 0), (0, 1), (0, 0)]
GROUPS = [(gx, *side) for side in SIDES for gx in (1, -1)] + [(0, *side) for side in SIDES[:3]]
N_GROUPS = len(GROUPS)
DISTANT = [(2, *side) for side in SIDES]
N_PACKETS = N_GROUPS + len(DISTANT)


def lane_plan():
    starts, base = [], {}
    block, lane = 0, 0
    for index, (gx, gy, gz) in enumerate(GROUPS):
        if index == 8:
            block, lane = 1, 0
        dirs = [(gx, sy, sz) for sz in ((-1, 1) if gz else (0,)) for sy in ((-1, 1) if gy else (0,))]
        starts.append((block, lane, lane + MOVE_CAP * len(dirs)))
        for dx, dy, dz in dirs:
            base[(dz + 1) * 9 + (dy + 1) * 3 + dx + 1] = block * LANES + lane
            lane += MOVE_CAP
    return starts, base


LANE_STARTS, LANE_BASE = lane_plan()
STAY = 13
NT_DIMS = (((1,), (1,)), ((), ()))
NN_DIMS = (((1,), (0,)), ((), ()))


def split3(values):
    hi = values.astype(jnp.bfloat16).astype(jnp.float32)
    rest = values - hi
    mid = rest.astype(jnp.bfloat16).astype(jnp.float32)
    return jnp.concatenate([hi, mid, rest - mid], axis=0).astype(jnp.bfloat16)


def join3(parts):
    rows = parts.shape[0] // 3
    return (parts[0:rows] + parts[rows:2 * rows]) + parts[2 * rows:3 * rows]


def dot_nt(a, b):
    return lax.dot_general(a, b, NT_DIMS, preferred_element_type=jnp.float32)


def dot_nn(a, b):
    return lax.dot_general(a, b, NN_DIMS, preferred_element_type=jnp.float32)


def my_coords():
    return lax.axis_index("z"), lax.axis_index("y"), lax.axis_index("x")


def peer_id(coords, offset):
    mz, my, mx = coords
    return (lax.rem(mz + offset[0], NZ), lax.rem(my + offset[1], NY), lax.rem(mx + offset[2] + NX, NX))


def entry_signals(coords):
    barrier = pltpu.get_barrier_semaphore()
    for offset in PEERS:
        pl.semaphore_signal(barrier, inc=1, device_id=peer_id(coords, offset), device_id_type=MESH)
    return barrier


def exchange_kernel(brick_ref, pos_ref, vel_ref, frc_ref, id_ref, ok_ref, gat_ref, pkt_ref, own_ref, raw, ids_in, oks_in, pad_ref, int_ref, send_pos, send_pkt, in_sem, pos_send_sem, pos_recv_sem, pkt_send_sem, pkt_recv_sem):
    coords = my_coords()
    fetches = [pltpu.make_async_copy(src, dst, in_sem.at[index]) for index, (src, dst) in enumerate(((pos_ref, raw.at[0]), (vel_ref, raw.at[1]), (frc_ref, raw.at[2]), (id_ref, ids_in), (ok_ref, oks_in)))]
    for fetch in fetches:
        fetch.start()
    barrier = entry_signals(coords)
    tail = slice(WIDE - LANES, WIDE)
    pad_ref[:, :, tail] = jnp.zeros((3, 4, LANES), jnp.float32)
    int_ref[:, tail] = jnp.zeros((2, LANES), jnp.int32)
    for fetch in fetches:
        fetch.wait()
    brick = brick_ref[...]
    for index in range(3):
        pad_ref[index, 0:3, 0:CAP] = raw[index]
    int_ref[0:1, 0:CAP] = ids_in[...].reshape(1, CAP)
    int_ref[1:2, 0:CAP] = oks_in[...].reshape(1, CAP)
    owned = int_ref[1:2, :] > 0
    moved, half, code = [], [], jnp.zeros((1, WIDE), jnp.int32)
    for axis, (mine, size, weight) in enumerate(((coords[2], NX, 1), (coords[1], NY, 3), (coords[0], NZ, 9))):
        box = brick * float(size)
        low = mine.astype(jnp.float32) * brick
        high = (mine + 1).astype(jnp.float32) * brick
        half_v = pad_ref[1, axis:axis + 1, :] + (0.5 * DT) * pad_ref[2, axis:axis + 1, :]
        drift = pad_ref[0, axis:axis + 1, :] + DT * half_v
        step = jnp.where(drift >= high, 2, jnp.where(drift < low, 0, 1))
        code = code + step * weight
        wrapped = jnp.where(drift < 0.0, drift + box, jnp.where(drift >= box, drift - box, drift))
        moved.append(wrapped)
        half.append(half_v)
    code = jnp.where(owned, code, -1)
    for axis in range(3):
        for block in range(8):
            if block < BLOCKS:
                lanes = slice(block * LANES, (block + 1) * LANES)
                send_pos[axis, block:block + 1, :] = jnp.where(owned[:, lanes], moved[axis][:, lanes], NOWHERE)
            else:
                send_pos[axis, block:block + 1, :] = jnp.full((1, LANES), NOWHERE, jnp.float32)
    ids = int_ref[0:1, :]
    id_hi = (lax.shift_right_logical(ids, 16) + 1).astype(jnp.float32)
    id_lo = (ids & 65535).astype(jnp.float32)
    data = jnp.concatenate(moved + half + [id_hi, id_lo], axis=0)
    member = (jnp.broadcast_to(code, (32, WIDE)) == lax.broadcasted_iota(jnp.int32, (32, WIDE), 0)).astype(jnp.float32)
    tri = (lax.broadcasted_iota(jnp.int32, (LANES, LANES), 0) < lax.broadcasted_iota(jnp.int32, (LANES, LANES), 1)).astype(jnp.bfloat16)
    codes = lax.broadcasted_iota(jnp.int32, (32, LANES), 0)
    running = jnp.zeros((32, LANES), jnp.float32)
    for move, first in LANE_BASE.items():
        running = jnp.where(codes == move, float(first), running)
    slots = []
    for block in range(BLOCKS):
        part = member[:, block * LANES:(block + 1) * LANES]
        before = dot_nn(part.astype(jnp.bfloat16), tri)
        slots.append(jnp.sum(part * (before + running), axis=0, keepdims=True))
        running = running + jnp.sum(part, axis=1, keepdims=True)
    slot = jnp.concatenate(slots, axis=1)
    stay = code == STAY
    mover_slot = jnp.where(owned & jnp.logical_not(stay), slot, -1.0).astype(jnp.int32)
    pick = (lax.broadcasted_iota(jnp.int32, (2 * LANES, WIDE), 0) == mover_slot).astype(jnp.float32).astype(jnp.bfloat16)
    packet = join3(dot_nt(split3(data), pick))
    send_pkt[0] = packet[:, 0:LANES]
    send_pkt[1] = packet[:, LANES:2 * LANES]
    own_ref[0:8, :] = data
    own_ref[8:16, :] = jnp.concatenate([jnp.where(stay, slot, -1.0), jnp.full((7, WIDE), brick, jnp.float32)], axis=0)
    pl.semaphore_wait(barrier, len(PEERS))
    copies = []
    for index, (gx, gy, gz) in enumerate(GROUPS + DISTANT):
        peer = peer_id(coords, (gz, gy, gx))
        if index < N_GROUPS:
            copies.append(pltpu.make_async_remote_copy(src_ref=send_pos, dst_ref=gat_ref.at[index], send_sem=pos_send_sem.at[index], recv_sem=pos_recv_sem.at[index], device_id=peer, device_id_type=MESH))
            copies[-1].start()
        block = LANE_STARTS[index][0] if index < N_GROUPS else 0
        copies.append(pltpu.make_async_remote_copy(src_ref=send_pkt.at[block], dst_ref=pkt_ref.at[index], send_sem=pkt_send_sem.at[index], recv_sem=pkt_recv_sem.at[index], device_id=peer, device_id_type=MESH))
        copies[-1].start()
    gat_ref[N_GROUPS] = send_pos[...]
    for copy in copies:
        copy.wait()


CAND_ROWS = 8 * (N_GROUPS + 1) + 8
MAX_ROWS = BLOCKS + CAND_ROWS
GROUPS_OWN = BLOCKS * 16
QUAD = 4
FIXED_BLOCKS = 4
FIXED_QUADS = FIXED_BLOCKS * 16 // QUAD
FIXED_ROWS = 11


def pair_tools(mine, others, rc2, wrap_box):
    def powers(dist_sq):
        inv_r = lax.rsqrt(dist_sq)
        inv_2 = inv_r * inv_r
        inv_4 = inv_2 * inv_2
        term = inv_4 * inv_2 - 0.5
        return inv_r, term, term * (inv_4 * inv_4)

    cut_inv_r, cut_term, cut_core = powers(rc2)
    kappa = -RC * cut_core
    for ulps in (-3, -2, -1, 1, 2, 3):
        trial = ulps * 2.0 ** -34 - RC * cut_core
        kappa = jnp.where(trial * cut_inv_r == -cut_core, trial, kappa)

    def radial(dist_sq):
        inv_r, term, core = powers(dist_sq)
        tail = kappa * inv_r
        return core + tail, term * term, tail * dist_sq

    def quad_energy(a, h):
        return ((a[0] + a[1]) + (a[2] + a[3])) - 12.0 * ((h[0] + h[1]) + (h[2] + h[3]))

    cut_f, cut_a, cut_h = radial(rc2)
    del cut_f
    cut_energy = quad_energy([cut_a] * QUAD, [cut_h] * QUAD)
    own_minus_lane = lax.broadcasted_iota(jnp.int32, (8, LANES), 0) - lax.broadcasted_iota(jnp.int32, (8, LANES), 1)

    def load_own(first):
        return [[mine[axis, first + k] for axis in range(3)] for k in range(QUAD)]

    def one_row(own, first, row, sums, with_self, react=None, weight=None):
        other = [others[axis, row] for axis in range(3)]
        force, energy, parts_a, parts_h, pulls = list(sums[:-1]), sums[-1], [], [], []
        for k in range(QUAD):
            delta = [own[k][axis] - other[axis] for axis in range(3)]
            for axis, box, inv_box in wrap_box:
                delta[axis] = delta[axis] - box * jnp.floor(delta[axis] * inv_box + 0.5)
            dist_sq = delta[0] * delta[0] + delta[1] * delta[1] + delta[2] * delta[2]
            if with_self:
                dist_sq = jnp.where(own_minus_lane == row * LANES - (first + k) * 8, rc2, dist_sq)
            dist_sq = jnp.minimum(dist_sq, rc2)
            scale, a, h = radial(dist_sq)
            pulls.append([scale * delta[axis] for axis in range(3)])
            for axis in range(3):
                force[3 * k + axis] = force[3 * k + axis] + pulls[k][axis]
            parts_a.append(a)
            parts_h.append(h)
        gain = quad_energy(parts_a, parts_h) - cut_energy
        if react is not None:
            gain = gain * weight
            for axis in range(3):
                react[axis, row] = react[axis, row] + ((pulls[0][axis] + pulls[1][axis]) + (pulls[2][axis] + pulls[3][axis]))
        return tuple(force) + (energy + gain,)

    return load_own, one_row


def prepare_kernel(gat_ref, pkt_ref, own_ref, sorted_ref, mine, others, acc, eng_ref):
    mz, my, mx = my_coords()
    brick = own_ref[9:10, 0:LANES]
    half_l = 0.5 * brick
    sizes = (NX, NY, NZ)
    centre = [(index.astype(jnp.float32) + 0.5) * brick for index in (mx, my, mz)]
    box = [brick * float(size) for size in sizes]
    lane_1 = lax.broadcasted_iota(jnp.int32, (1, LANES), 1)
    acc[:, pl.ds(0, FIXED_QUADS * QUAD)] = jnp.zeros((3, FIXED_QUADS * QUAD, 8, LANES), jnp.float32)

    arrived = []
    for block in range(2):
        total = jnp.zeros((8, LANES), jnp.float32)
        for index in range(N_GROUPS):
            where_block, first, last = LANE_STARTS[index]
            if where_block == block:
                total = total + jnp.where((lane_1 >= first) & (lane_1 < last), pkt_ref[index], 0.0)
        arrived.append(total)
    arr = jnp.concatenate(arrived, axis=1)
    arr_ok = arr[6:7] > 0.5
    stay_all = own_ref[8:9, :] >= 0.0
    n_vec = jnp.sum(stay_all.astype(jnp.float32), axis=1, keepdims=True) + jnp.sum(arr_ok.astype(jnp.float32), axis=1, keepdims=True)
    n_own = jnp.max(n_vec).astype(jnp.int32)
    n_int = n_vec.astype(jnp.int32)
    quads = lax.div(n_own + (8 * QUAD - 1), 8 * QUAD)
    own_rows = lax.div(n_own + (LANES - 1), LANES)
    beyond = gat_ref[0, 0, 4:6, :]
    for slot in range(1, N_GROUPS + 1):
        beyond = jnp.minimum(beyond, gat_ref[slot, 0, 4:6, :])
    small = (jnp.min(beyond) > 0.5 * NOWHERE) & (n_own <= FIXED_BLOCKS * LANES)
    eng_ref[1] = jnp.broadcast_to(n_vec, (8, LANES))
    wide = jnp.max(brick) >= 2.0 * RC
    int_max = 2147483647
    rc2 = RC * RC + 0.0 * own_ref[8:16, 0:LANES]
    zero = jnp.zeros((8, LANES), jnp.float32)
    far = jnp.full((8, LANES), FAR_OTHER, jnp.float32)

    def build(blocks, tile_rows):
        span = blocks * LANES
        data = jnp.concatenate([own_ref[0:8, 0:span], arr], axis=1)
        ids = lax.shift_left(data[6:7].astype(jnp.int32) - 1, 16) + data[7:8].astype(jnp.int32)
        stay_rank = own_ref[8:9, 0:span]
        stay = stay_rank >= 0.0
        arr_id = jnp.where(arr_ok, ids[:, span:], int_max)
        own_id = jnp.where(stay, ids[:, :span], int_max)

        count_rows = (N_GROUPS + 1) * tile_rows
        cand = -(-(count_rows + len(DISTANT)) // 8) * 8
        rel = []
        for axis in range(3):
            near = [gat_ref[slot, axis, 0:tile_rows, :] for slot in range(N_GROUPS + 1)]
            distant = [jnp.where(pkt_ref[N_GROUPS + k, 6:7, :] > 0.5, pkt_ref[N_GROUPS + k, axis:axis + 1, :], NOWHERE) for k in range(len(DISTANT))]
            values = jnp.concatenate(near + distant + [jnp.full((cand - count_rows - len(DISTANT), LANES), NOWHERE, jnp.float32)], axis=0) - centre[axis]
            rel.append(jnp.where(values > 0.5 * box[axis], values - box[axis], jnp.where(values < -0.5 * box[axis], values + box[axis], values)))
        over = [jnp.maximum(jnp.abs(values) - half_l, 0.0) for values in rel]
        gap_sq = over[0] * over[0] + over[1] * over[1] + over[2] * over[2]
        ghost = ((gap_sq > 0.0) & (gap_sq < GHOST_SQ)).astype(jnp.float32).astype(jnp.bfloat16)
        row_i = lax.broadcasted_iota(jnp.int32, (LANES, LANES), 0)
        col_i = lax.broadcasted_iota(jnp.int32, (LANES, LANES), 1)
        cum = dot_nn(ghost, (row_i <= col_i).astype(jnp.bfloat16)).astype(jnp.int32)
        count = dot_nn(ghost, jnp.ones((LANES, LANES), jnp.bfloat16))
        arr_col = jnp.transpose(jnp.broadcast_to(arr_id, (8, 2 * LANES)), (1, 0))[:, 0:1]
        own_col = jnp.transpose(jnp.broadcast_to(own_id, (8, span)), (1, 0))[:, 0:1]
        all_id = jnp.concatenate([own_id, arr_id], axis=1)
        arr_before = jnp.sum((arr_col < all_id).astype(jnp.float32), axis=0, keepdims=True)
        stay_before = jnp.sum((own_col < arr_id).astype(jnp.float32), axis=0, keepdims=True)
        rank = jnp.concatenate([jnp.where(stay, stay_rank + arr_before[:, :span], -1.0), jnp.where(arr_ok, stay_before + arr_before[:, span:], -1.0)], axis=1).astype(jnp.int32)
        base = dot_nn((col_i < row_i).astype(jnp.bfloat16)[:cand, :cand], count.astype(jnp.bfloat16)).astype(jnp.int32) + n_int
        count = count.astype(jnp.int32)
        n_all = jnp.max(base[cand - 8:] + count[cand - 8:])
        place = (lax.broadcasted_iota(jnp.int32, (cand, LANES), 1) - base) & (LANES - 1)
        parts = split3(data)

        def place_block(block):
            pick = (lax.broadcasted_iota(jnp.int32, (LANES, span + 2 * LANES), 0) + block * LANES == rank).astype(jnp.float32).astype(jnp.bfloat16)
            rows_s = join3(jnp.transpose(dot_nt(pick, parts), (1, 0)))
            sorted_ref[block] = rows_s
            valid = lane_1 + block * LANES < n_int
            own_rel = jnp.concatenate([rows_s[axis:axis + 1] - centre[axis] for axis in range(3)] + [rows_s[3:8]], axis=0)
            columns = jnp.transpose(jnp.where(valid, own_rel, FAR_OWN), (1, 0))
            for axis in range(3):
                others[axis, block] = jnp.broadcast_to(jnp.where(valid, own_rel[axis:axis + 1], 0.0), (8, LANES))
                mine[axis, pl.ds(block * 16, 16)] = jnp.broadcast_to(columns[:, axis:axis + 1], (LANES, LANES)).reshape(16, 8, LANES)

        wanted = lax.broadcasted_iota(jnp.int32, (cand, LANES), 1)
        source = jnp.zeros((cand, LANES), jnp.int32)
        waiting = list(range(blocks))
        for stride, probes in ((16, 7), (2, 7), (1, 1)):
            below = jnp.zeros((cand, LANES), jnp.int32)
            for k in range(1, probes + 1):
                probe = jnp.take_along_axis(cum, source + (stride * k - 1), axis=1)
                below = below + (probe <= wanted).astype(jnp.int32)
            source = source + stride * below
            for block in waiting[:2]:
                place_block(block)
            waiting = waiting[2:]
        source = jnp.take_along_axis(source & (LANES - 1), place, axis=1)
        for block in range(blocks, BLOCKS):
            sorted_ref[block] = zero
        target = jnp.where(place < count, lax.shift_right_logical(base + place, 7), -1)
        packed = [jnp.take_along_axis(values, source, axis=1) for values in rel]
        rows = lax.div(n_all + (LANES - 1), LANES)

        def pack_row(row, carry):
            hit = target == row
            filled = lane_1 + row * LANES < n_all
            for axis in range(3):
                own_part = jnp.where(row < own_rows, others[axis, row], 0.0)
                values = jnp.sum(jnp.where(hit, packed[axis], 0.0), axis=0, keepdims=True)
                others[axis, row] = jnp.where(filled, own_part + values, FAR_OTHER)
            return carry

        lax.fori_loop(lax.div(n_own, LANES), rows, pack_row, 0)

        def set_far(row, carry):
            for axis in range(3):
                others[axis, row] = far
            return carry

        def excess(first_quad, last_quad, first_row, wrap_box, energy):
            load_own, one_row = pair_tools(mine, others, rc2, wrap_box)

            def quad(index, total):
                first = index * QUAD
                own = load_own(first)
                sums = (zero,) * (3 * QUAD) + (total,)
                sums = lax.fori_loop(first_row, rows, lambda row, part: one_row(own, first, row, part, True), sums)
                for k in range(QUAD):
                    for axis in range(3):
                        acc[axis, first + k] = sums[3 * k + axis]
                return sums[-1]

            return lax.fori_loop(first_quad, last_quad, quad, energy)

        def plain():
            short = jnp.where(rows > FIXED_ROWS, jnp.minimum(quads, FIXED_QUADS), 0)
            energy = excess(0, short, FIXED_ROWS, [], zero)
            if blocks > FIXED_BLOCKS:
                energy = excess(FIXED_QUADS, quads, 0, [], energy)
            eng_ref[0] = energy
            lax.fori_loop(rows, FIXED_ROWS, set_far, 0)

        def wrapped():
            wrap_box = [(axis, box[axis], 1.0 / box[axis]) for axis in (1, 2)]
            eng_ref[0] = excess(0, quads, 0, wrap_box, zero)
            lax.fori_loop(0, FIXED_ROWS, set_far, 0)

        pl.when(wide)(plain)
        pl.when(jnp.logical_not(wide))(wrapped)

    pl.when(small)(lambda: build(FIXED_BLOCKS, 4))
    pl.when(jnp.logical_not(small))(lambda: build(BLOCKS, 8))


def tile_kernel(mine, others, part, eng_ref, frc_ref, out_ref, acc, react, eng, slots, send_sem, recv_sem):
    coords = my_coords()
    mz, my, mx = coords
    barrier = entry_signals(coords)
    rc2 = RC * RC + 0.0 * mine[0, 0]
    load_own, one_row = pair_tools(mine, others, rc2, [])

    lane_8 = lax.broadcasted_iota(jnp.int32, (8, LANES), 1).astype(jnp.float32)
    weights = [jnp.where(lane_8 + float(row * LANES) < eng_ref[1], 2.0, 1.0) for row in range(FIXED_BLOCKS)]
    react[...] = jnp.zeros_like(react)
    energy = eng_ref[0]
    for block in range(FIXED_BLOCKS):

        def quad(index, total, block=block):
            first = block * 16 + index * QUAD
            own = load_own(first)
            sums = tuple(part[axis, first + k] for k in range(QUAD) for axis in range(3)) + (total,)
            sums = one_row(own, first, block, sums, True)
            for row in range(block + 1, FIXED_ROWS):
                if row < FIXED_BLOCKS:
                    sums = one_row(own, first, row, sums, False, react, weights[row])
                else:
                    sums = one_row(own, first, row, sums, False)
            for k in range(QUAD):
                for axis in range(3):
                    acc[axis, first + k] = sums[3 * k + axis]
            return sums[-1]

        energy = lax.fori_loop(0, 16 // QUAD, quad, energy)
    eng[...] = jnp.full((8, LANES), 2.0 * jnp.sum(energy), jnp.float32)
    pl.semaphore_wait(barrier, len(PEERS))
    place = (mz * NY + my) * NX + mx
    copies = []
    for index, offset in enumerate(PEERS):
        copies.append(pltpu.make_async_remote_copy(src_ref=eng, dst_ref=slots.at[place], send_sem=send_sem.at[index], recv_sem=recv_sem.at[index], device_id=peer_id(coords, offset), device_id_type=MESH))
        copies[-1].start()
    slots[place] = eng[...]
    for block in range(BLOCKS):
        held = acc if block < FIXED_BLOCKS else part
        for axis in range(3):
            turned = jnp.transpose(held[axis, pl.ds(block * 16, 16)].reshape(LANES, LANES), (1, 0))
            force = jnp.sum(turned, axis=0, keepdims=True)
            if 0 < block < FIXED_BLOCKS:
                force = force - jnp.sum(react[axis, block], axis=0, keepdims=True)
            frc_ref[axis:axis + 1, block * LANES:(block + 1) * LANES] = 48.0 * force
    for copy in copies:
        copy.wait()
    total = slots[0]
    for index in range(1, NZ * NY * NX):
        total = total + slots[index]
    out_ref[...] = total


def finish_kernel(sorted_ref, frc_ref, total_ref, pos_out, vel_out, frc_out, id_out, ok_out, eng_out):
    eng_out[...] = jnp.max(total_ref[...])
    for block in range(BLOCKS):
        width = min(LANES, CAP - block * LANES)
        lanes = slice(block * LANES, block * LANES + width)
        rows_s = sorted_ref[block]
        valid = rows_s[6:7] > 0.5
        for axis in range(3):
            force = jnp.where(valid, frc_ref[axis:axis + 1, block * LANES:(block + 1) * LANES], 0.0)
            frc_out[axis:axis + 1, lanes] = force[:, :width]
            vel_out[axis:axis + 1, lanes] = (rows_s[3 + axis:4 + axis] + (0.5 * DT) * force)[:, :width]
            pos_out[axis:axis + 1, lanes] = rows_s[axis:axis + 1, :width]
        new_id = lax.shift_left(rows_s[6:7].astype(jnp.int32) - 1, 16) + rows_s[7:8].astype(jnp.int32)
        id_out[lanes] = jnp.where(valid, new_id, 0)[:, :width].reshape(width)
        ok_out[lanes] = valid.astype(jnp.int32)[:, :width].reshape(width)


VMEM_SPEC = pl.BlockSpec(memory_space=pltpu.VMEM)
HBM_SPEC = pl.BlockSpec(memory_space=pltpu.HBM)
VMEM_LIMIT = 8 * 1024 * 1024
SMEM_SPEC = pl.BlockSpec(memory_space=pltpu.SMEM)


def solution(mesh):
    def local_step(atom_pos, atom_vel, atom_frc, atom_id, atom_ok, brick_side):
        f32 = jnp.float32
        n_dev = NZ * NY * NX
        gat, pkt, own = pl.pallas_call(
            exchange_kernel,
            out_shape=(jax.ShapeDtypeStruct((N_GROUPS + 1, 3, 8, LANES), f32), jax.ShapeDtypeStruct((N_PACKETS, 8, LANES), f32), jax.ShapeDtypeStruct((16, WIDE), f32)),
            in_specs=[SMEM_SPEC] + [HBM_SPEC] * 5,
            out_specs=(VMEM_SPEC,) * 3,
            scratch_shapes=[
                pltpu.VMEM((3, 3, CAP), f32),
                pltpu.VMEM((CAP,), jnp.int32),
                pltpu.VMEM((CAP,), jnp.int32),
                pltpu.VMEM((3, 4, WIDE), f32),
                pltpu.VMEM((2, WIDE), jnp.int32),
                pltpu.VMEM((3, 8, LANES), f32),
                pltpu.VMEM((2, 8, LANES), f32),
                pltpu.SemaphoreType.DMA((5,)),
                pltpu.SemaphoreType.DMA((N_GROUPS,)),
                pltpu.SemaphoreType.DMA((N_GROUPS,)),
                pltpu.SemaphoreType.DMA((N_PACKETS,)),
                pltpu.SemaphoreType.DMA((N_PACKETS,)),
            ],
            compiler_params=pltpu.CompilerParams(collective_id=0, has_side_effects=True, vmem_limit_bytes=VMEM_LIMIT),
            name="exchange",
        )(brick_side, *(pltpu.with_memory_space_constraint(value, pltpu.HBM) for value in (atom_pos.T, atom_vel.T, atom_frc.T, atom_id, atom_ok)))
        own_tiles = jax.ShapeDtypeStruct((3, GROUPS_OWN, 8, LANES), f32)
        placed, mine, others, part, eng = pl.pallas_call(
            prepare_kernel,
            out_shape=(jax.ShapeDtypeStruct((BLOCKS, 8, LANES), f32), own_tiles, jax.ShapeDtypeStruct((3, MAX_ROWS, 8, LANES), f32), own_tiles, jax.ShapeDtypeStruct((2, 8, LANES), f32)),
            in_specs=[VMEM_SPEC] * 3,
            out_specs=(VMEM_SPEC,) * 5,
            compiler_params=pltpu.CompilerParams(vmem_limit_bytes=VMEM_LIMIT),
            name="prepare",
        )(gat, pkt, own)
        frc_rows, total = pl.pallas_call(
            tile_kernel,
            out_shape=(jax.ShapeDtypeStruct((8, WIDE), f32), jax.ShapeDtypeStruct((8, LANES), f32)),
            in_specs=[VMEM_SPEC] * 4,
            out_specs=(VMEM_SPEC,) * 2,
            scratch_shapes=[pltpu.VMEM((3, FIXED_BLOCKS * 16, 8, LANES), f32), pltpu.VMEM((3, FIXED_BLOCKS, 8, LANES), f32), pltpu.VMEM((8, LANES), f32), pltpu.VMEM((n_dev, 8, LANES), f32), pltpu.SemaphoreType.DMA((n_dev - 1,)), pltpu.SemaphoreType.DMA((n_dev - 1,))],
            compiler_params=pltpu.CompilerParams(collective_id=1, has_side_effects=True, vmem_limit_bytes=VMEM_LIMIT),
            name="tile",
        )(mine, others, part, eng)
        pos, vel, frc, ids, oks, energy = pl.pallas_call(
            finish_kernel,
            out_shape=(jax.ShapeDtypeStruct((3, CAP), f32),) * 3 + (jax.ShapeDtypeStruct((CAP,), jnp.int32),) * 2 + (jax.ShapeDtypeStruct((), f32),),
            in_specs=[VMEM_SPEC] * 3,
            out_specs=(VMEM_SPEC,) * 5 + (SMEM_SPEC,),
            compiler_params=pltpu.CompilerParams(vmem_limit_bytes=VMEM_LIMIT),
            name="finish",
        )(placed, frc_rows, total)
        return pos.T, vel.T, frc.T, ids, oks, energy

    row_spec = P(MESH_AXES, None)
    id_spec = P(MESH_AXES)
    return jax.shard_map(local_step, mesh=mesh, in_specs=(row_spec, row_spec, row_spec, id_spec, id_spec, P()), out_specs=(row_spec, row_spec, row_spec, id_spec, id_spec, P()), check_vma=False)
```

```python
import jax
import jax.numpy as jnp
from jax import lax
from jax.experimental import pallas as pl
from jax.experimental.pallas import tpu as pltpu
from jax.sharding import PartitionSpec as P

DT = 0.005
RC = 2.5
UPC = -48.0 * RC ** -13 + 24.0 * RC ** -7
MESH_AXES = ("z", "y", "x")
MESH = pl.DeviceIdType.MESH
NZ, NY, NX = 2, 2, 4
CAP = 729
LANES = 128
BLOCKS = 6
WIDE = BLOCKS * LANES
MOVE_CAP = CAP // 100
FAR_OWN = 1.0e4
FAR_OTHER = -1.0e4
NOWHERE = 1.0e9
GHOST_SQ = RC * RC + 0.01
PEERS = [(dz, dy, dx) for dz in range(NZ) for dy in range(NY) for dx in range(NX)][:0:-1]
SIDES = [(1, 1), (1, 0), (0, 1), (0, 0)]
GROUPS = [(gx, *side) for side in SIDES for gx in (1, -1)] + [(0, *side) for side in SIDES[:3]]
N_GROUPS = len(GROUPS)
DISTANT = [(2, *side) for side in SIDES]
N_PACKETS = N_GROUPS + len(DISTANT)


def lane_plan():
    starts, base = [], {}
    block, lane = 0, 0
    for index, (gx, gy, gz) in enumerate(GROUPS):
        if index == 8:
            block, lane = 1, 0
        dirs = [(gx, sy, sz) for sz in ((-1, 1) if gz else (0,)) for sy in ((-1, 1) if gy else (0,))]
        starts.append((block, lane, lane + MOVE_CAP * len(dirs)))
        for dx, dy, dz in dirs:
            base[(dz + 1) * 9 + (dy + 1) * 3 + dx + 1] = block * LANES + lane
            lane += MOVE_CAP
    return starts, base


LANE_STARTS, LANE_BASE = lane_plan()
STAY = 13
NT_DIMS = (((1,), (1,)), ((), ()))
NN_DIMS = (((1,), (0,)), ((), ()))


def split3(values):
    hi = values.astype(jnp.bfloat16).astype(jnp.float32)
    rest = values - hi
    mid = rest.astype(jnp.bfloat16).astype(jnp.float32)
    return jnp.concatenate([hi, mid, rest - mid], axis=0).astype(jnp.bfloat16)


def join3(parts):
    rows = parts.shape[0] // 3
    return (parts[0:rows] + parts[rows:2 * rows]) + parts[2 * rows:3 * rows]


def dot_nt(a, b):
    return lax.dot_general(a, b, NT_DIMS, preferred_element_type=jnp.float32)


def dot_nn(a, b):
    return lax.dot_general(a, b, NN_DIMS, preferred_element_type=jnp.float32)


def my_coords():
    return lax.axis_index("z"), lax.axis_index("y"), lax.axis_index("x")


def peer_id(coords, offset):
    mz, my, mx = coords
    return (lax.rem(mz + offset[0], NZ), lax.rem(my + offset[1], NY), lax.rem(mx + offset[2] + NX, NX))


def entry_signals(coords):
    barrier = pltpu.get_barrier_semaphore()
    for offset in PEERS:
        pl.semaphore_signal(barrier, inc=1, device_id=peer_id(coords, offset), device_id_type=MESH)
    return barrier


def exchange_kernel(brick_ref, pos_ref, vel_ref, frc_ref, id_ref, ok_ref, gat_ref, pkt_ref, own_ref, raw, ids_in, oks_in, pad_ref, int_ref, send_pos, send_pkt, in_sem, pos_send_sem, pos_recv_sem, pkt_send_sem, pkt_recv_sem):
    coords = my_coords()
    fetches = [pltpu.make_async_copy(src, dst, in_sem.at[index]) for index, (src, dst) in enumerate(((pos_ref, raw.at[0]), (vel_ref, raw.at[1]), (frc_ref, raw.at[2]), (id_ref, ids_in), (ok_ref, oks_in)))]
    for fetch in fetches:
        fetch.start()
    barrier = entry_signals(coords)
    tail = slice(WIDE - LANES, WIDE)
    pad_ref[:, :, tail] = jnp.zeros((3, 4, LANES), jnp.float32)
    int_ref[:, tail] = jnp.zeros((2, LANES), jnp.int32)
    for fetch in fetches:
        fetch.wait()
    brick = brick_ref[...]
    for index in range(3):
        pad_ref[index, 0:3, 0:CAP] = raw[index]
    int_ref[0:1, 0:CAP] = ids_in[...].reshape(1, CAP)
    int_ref[1:2, 0:CAP] = oks_in[...].reshape(1, CAP)
    owned = int_ref[1:2, :] > 0
    moved, half, code = [], [], jnp.zeros((1, WIDE), jnp.int32)
    for axis, (mine, size, weight) in enumerate(((coords[2], NX, 1), (coords[1], NY, 3), (coords[0], NZ, 9))):
        box = brick * float(size)
        low = mine.astype(jnp.float32) * brick
        high = (mine + 1).astype(jnp.float32) * brick
        half_v = pad_ref[1, axis:axis + 1, :] + (0.5 * DT) * pad_ref[2, axis:axis + 1, :]
        drift = pad_ref[0, axis:axis + 1, :] + DT * half_v
        step = jnp.where(drift >= high, 2, jnp.where(drift < low, 0, 1))
        code = code + step * weight
        wrapped = jnp.where(drift < 0.0, drift + box, jnp.where(drift >= box, drift - box, drift))
        moved.append(wrapped)
        half.append(half_v)
    code = jnp.where(owned, code, -1)
    for axis in range(3):
        for block in range(BLOCKS):
            lanes = slice(block * LANES, (block + 1) * LANES)
            send_pos[axis, block:block + 1, :] = jnp.where(owned[:, lanes], moved[axis][:, lanes], NOWHERE)
    ids = int_ref[0:1, :]
    id_hi = (lax.shift_right_logical(ids, 16) + 1).astype(jnp.float32)
    id_lo = (ids & 65535).astype(jnp.float32)
    data = jnp.concatenate(moved + [id_hi] + half + [id_lo], axis=0)
    member = (jnp.broadcast_to(code, (32, WIDE)) == lax.broadcasted_iota(jnp.int32, (32, WIDE), 0)).astype(jnp.float32)
    tri = (lax.broadcasted_iota(jnp.int32, (LANES, LANES), 0) < lax.broadcasted_iota(jnp.int32, (LANES, LANES), 1)).astype(jnp.bfloat16)
    codes = lax.broadcasted_iota(jnp.int32, (32, LANES), 0)
    running = jnp.zeros((32, LANES), jnp.float32)
    for move, first in LANE_BASE.items():
        running = jnp.where(codes == move, float(first), running)
    slots = []
    for block in range(BLOCKS):
        part = member[:, block * LANES:(block + 1) * LANES]
        before = dot_nn(part.astype(jnp.bfloat16), tri)
        slots.append(jnp.sum(part * (before + running), axis=0, keepdims=True))
        running = running + jnp.sum(part, axis=1, keepdims=True)
    slot = jnp.concatenate(slots, axis=1)
    stay = code == STAY
    mover_slot = jnp.where(owned & jnp.logical_not(stay), slot, -1.0).astype(jnp.int32)
    pick = (lax.broadcasted_iota(jnp.int32, (2 * LANES, WIDE), 0) == mover_slot).astype(jnp.float32).astype(jnp.bfloat16)
    packet = join3(dot_nt(split3(data), pick))
    send_pkt[0] = packet[:, 0:LANES]
    send_pkt[1] = packet[:, LANES:2 * LANES]
    own_ref[0:8, :] = data
    own_ref[8:16, :] = jnp.concatenate([jnp.where(stay, slot, -1.0), jnp.full((7, WIDE), brick, jnp.float32)], axis=0)
    pl.semaphore_wait(barrier, len(PEERS))
    copies = []
    for index, (gx, gy, gz) in enumerate(GROUPS + DISTANT):
        peer = peer_id(coords, (gz, gy, gx))
        if index < N_GROUPS:
            copies.append(pltpu.make_async_remote_copy(src_ref=send_pos, dst_ref=gat_ref.at[index], send_sem=pos_send_sem.at[index], recv_sem=pos_recv_sem.at[index], device_id=peer, device_id_type=MESH))
            copies[-1].start()
            source, target = send_pkt.at[LANE_STARTS[index][0]], pkt_ref.at[index]
        else:
            source, target = send_pkt.at[0, 0:4], pkt_ref.at[index, 0:4]
        copies.append(pltpu.make_async_remote_copy(src_ref=source, dst_ref=target, send_sem=pkt_send_sem.at[index], recv_sem=pkt_recv_sem.at[index], device_id=peer, device_id_type=MESH))
        copies[-1].start()
    gat_ref[N_GROUPS] = send_pos[...]
    for copy in copies:
        copy.wait()


CAND_ROWS = 8 * (N_GROUPS + 1) + 8
MAX_ROWS = BLOCKS + CAND_ROWS
GROUPS_OWN = BLOCKS * 16
QUAD = 4
FIXED_BLOCKS = 4
FIXED_QUADS = FIXED_BLOCKS * 16 // QUAD
FIXED_ROWS = 11


def pair_tools(mine, others, rc2, wrap_box):
    def powers(dist_sq):
        inv_r = lax.rsqrt(dist_sq)
        inv_2 = inv_r * inv_r
        inv_4 = inv_2 * inv_2
        term = inv_4 * inv_2 - 0.5
        return inv_r, term, term * (inv_4 * inv_4)

    cut_inv_r, cut_term, cut_core = powers(rc2)
    kappa = -RC * cut_core
    for ulps in (-3, -2, -1, 1, 2, 3):
        trial = ulps * 2.0 ** -34 - RC * cut_core
        kappa = jnp.where(trial * cut_inv_r == -cut_core, trial, kappa)

    def radial(dist_sq):
        inv_r, term, core = powers(dist_sq)
        tail = kappa * inv_r
        return core + tail, term * term, tail * dist_sq

    def quad_energy(a, h):
        return ((a[0] + a[1]) + (a[2] + a[3])) - 12.0 * ((h[0] + h[1]) + (h[2] + h[3]))

    cut_f, cut_a, cut_h = radial(rc2)
    del cut_f
    cut_energy = quad_energy([cut_a] * QUAD, [cut_h] * QUAD)
    own_minus_lane = lax.broadcasted_iota(jnp.int32, (8, LANES), 0) - lax.broadcasted_iota(jnp.int32, (8, LANES), 1)

    def load_own(first):
        return [[mine[axis, first + k] for axis in range(3)] for k in range(QUAD)]

    def one_row(own, first, row, sums, with_self, react=None, weight=None):
        other = [others[axis, row] for axis in range(3)]
        force, energy, parts_a, parts_h, pulls = list(sums[:-1]), sums[-1], [], [], []
        for k in range(QUAD):
            delta = [own[k][axis] - other[axis] for axis in range(3)]
            for axis, box, inv_box in wrap_box:
                delta[axis] = delta[axis] - box * jnp.floor(delta[axis] * inv_box + 0.5)
            dist_sq = delta[0] * delta[0] + delta[1] * delta[1] + delta[2] * delta[2]
            if with_self:
                dist_sq = jnp.where(own_minus_lane == row * LANES - (first + k) * 8, rc2, dist_sq)
            dist_sq = jnp.minimum(dist_sq, rc2)
            scale, a, h = radial(dist_sq)
            pulls.append([scale * delta[axis] for axis in range(3)])
            for axis in range(3):
                force[3 * k + axis] = force[3 * k + axis] + pulls[k][axis]
            parts_a.append(a)
            parts_h.append(h)
        gain = quad_energy(parts_a, parts_h) - cut_energy
        if react is not None:
            gain = gain * weight
            for axis in range(3):
                react[axis, row] = react[axis, row] + ((pulls[0][axis] + pulls[1][axis]) + (pulls[2][axis] + pulls[3][axis]))
        return tuple(force) + (energy + gain,)

    return load_own, one_row


def prepare_kernel(gat_ref, pkt_ref, own_ref, sorted_ref, mine, others, acc, eng_ref):
    mz, my, mx = my_coords()
    brick = own_ref[9:10, 0:LANES]
    half_l = 0.5 * brick
    sizes = (NX, NY, NZ)
    centre = [(index.astype(jnp.float32) + 0.5) * brick for index in (mx, my, mz)]
    box = [brick * float(size) for size in sizes]
    lane_1 = lax.broadcasted_iota(jnp.int32, (1, LANES), 1)
    acc[:, pl.ds(0, FIXED_QUADS * QUAD)] = jnp.zeros((3, FIXED_QUADS * QUAD, 8, LANES), jnp.float32)

    arrived = []
    for block in range(2):
        total = jnp.zeros((8, LANES), jnp.float32)
        for index in range(N_GROUPS):
            where_block, first, last = LANE_STARTS[index]
            if where_block == block:
                total = total + jnp.where((lane_1 >= first) & (lane_1 < last), pkt_ref[index], 0.0)
        arrived.append(total)
    arr = jnp.concatenate(arrived, axis=1)
    arr_ok = arr[3:4] > 0.5
    stay_all = own_ref[8:9, :] >= 0.0
    n_vec = jnp.sum(stay_all.astype(jnp.float32), axis=1, keepdims=True) + jnp.sum(arr_ok.astype(jnp.float32), axis=1, keepdims=True)
    n_own = jnp.max(n_vec).astype(jnp.int32)
    n_int = n_vec.astype(jnp.int32)
    quads = lax.div(n_own + (8 * QUAD - 1), 8 * QUAD)
    own_rows = lax.div(n_own + (LANES - 1), LANES)
    beyond = gat_ref[0, 0, 4:6, :]
    for slot in range(1, N_GROUPS + 1):
        beyond = jnp.minimum(beyond, gat_ref[slot, 0, 4:6, :])
    small = (jnp.min(beyond) > 0.5 * NOWHERE) & (n_own <= FIXED_BLOCKS * LANES)
    eng_ref[1] = jnp.broadcast_to(n_vec, (8, LANES))
    wide = jnp.max(brick) >= 2.0 * RC
    int_max = 2147483647
    rc2 = RC * RC + 0.0 * own_ref[8:16, 0:LANES]
    zero = jnp.zeros((8, LANES), jnp.float32)
    far = jnp.full((8, LANES), FAR_OTHER, jnp.float32)

    def build(blocks, tile_rows):
        span = blocks * LANES
        data = jnp.concatenate([own_ref[0:8, 0:span], arr], axis=1)
        ids = lax.shift_left(data[3:4].astype(jnp.int32) - 1, 16) + data[7:8].astype(jnp.int32)
        stay_rank = own_ref[8:9, 0:span]
        stay = stay_rank >= 0.0
        arr_id = jnp.where(arr_ok, ids[:, span:], int_max)
        own_id = jnp.where(stay, ids[:, :span], int_max)

        count_rows = (N_GROUPS + 1) * tile_rows
        cand = -(-(count_rows + len(DISTANT)) // 8) * 8
        rel = []
        for axis in range(3):
            near = [gat_ref[slot, axis, 0:tile_rows, :] for slot in range(N_GROUPS + 1)]
            distant = [jnp.where(pkt_ref[N_GROUPS + k, 3:4, :] > 0.5, pkt_ref[N_GROUPS + k, axis:axis + 1, :], NOWHERE) for k in range(len(DISTANT))]
            values = jnp.concatenate(near + distant + [jnp.full((cand - count_rows - len(DISTANT), LANES), NOWHERE, jnp.float32)], axis=0) - centre[axis]
            rel.append(jnp.where(values > 0.5 * box[axis], values - box[axis], jnp.where(values < -0.5 * box[axis], values + box[axis], values)))
        over = [jnp.maximum(jnp.abs(values) - half_l, 0.0) for values in rel]
        gap_sq = over[0] * over[0] + over[1] * over[1] + over[2] * over[2]
        ghost = ((gap_sq > 0.0) & (gap_sq < GHOST_SQ)).astype(jnp.float32).astype(jnp.bfloat16)
        row_i = lax.broadcasted_iota(jnp.int32, (LANES, LANES), 0)
        col_i = lax.broadcasted_iota(jnp.int32, (LANES, LANES), 1)
        cum = dot_nn(ghost, (row_i <= col_i).astype(jnp.bfloat16)).astype(jnp.int32)
        count = dot_nn(ghost, jnp.ones((LANES, LANES), jnp.bfloat16))
        arr_col = jnp.transpose(jnp.broadcast_to(arr_id, (8, 2 * LANES)), (1, 0))[:, 0:1]
        own_col = jnp.transpose(jnp.broadcast_to(own_id, (8, span)), (1, 0))[:, 0:1]
        all_id = jnp.concatenate([own_id, arr_id], axis=1)
        arr_before = jnp.sum((arr_col < all_id).astype(jnp.float32), axis=0, keepdims=True)
        stay_before = jnp.sum((own_col < arr_id).astype(jnp.float32), axis=0, keepdims=True)
        rank = jnp.concatenate([jnp.where(stay, stay_rank + arr_before[:, :span], -1.0), jnp.where(arr_ok, stay_before + arr_before[:, span:], -1.0)], axis=1).astype(jnp.int32)
        base = dot_nn((col_i < row_i).astype(jnp.bfloat16)[:cand, :cand], count.astype(jnp.bfloat16)).astype(jnp.int32) + n_int
        count = count.astype(jnp.int32)
        n_all = jnp.max(base[cand - 8:] + count[cand - 8:])
        place = (lax.broadcasted_iota(jnp.int32, (cand, LANES), 1) - base) & (LANES - 1)
        parts = split3(data)

        def place_block(block):
            pick = (lax.broadcasted_iota(jnp.int32, (LANES, span + 2 * LANES), 0) + block * LANES == rank).astype(jnp.float32).astype(jnp.bfloat16)
            rows_s = join3(jnp.transpose(dot_nt(pick, parts), (1, 0)))
            sorted_ref[block] = rows_s
            valid = lane_1 + block * LANES < n_int
            own_rel = jnp.concatenate([rows_s[axis:axis + 1] - centre[axis] for axis in range(3)] + [rows_s[3:8]], axis=0)
            columns = jnp.transpose(jnp.where(valid, own_rel, FAR_OWN), (1, 0))
            for axis in range(3):
                others[axis, block] = jnp.broadcast_to(jnp.where(valid, own_rel[axis:axis + 1], 0.0), (8, LANES))
                mine[axis, pl.ds(block * 16, 16)] = jnp.broadcast_to(columns[:, axis:axis + 1], (LANES, LANES)).reshape(16, 8, LANES)

        wanted = lax.broadcasted_iota(jnp.int32, (cand, LANES), 1)
        source = jnp.zeros((cand, LANES), jnp.int32)
        waiting = list(range(blocks))
        for stride, probes in ((16, 7), (2, 7), (1, 1)):
            below = jnp.zeros((cand, LANES), jnp.int32)
            for k in range(1, probes + 1):
                probe = jnp.take_along_axis(cum, source + (stride * k - 1), axis=1)
                below = below + (probe <= wanted).astype(jnp.int32)
            source = source + stride * below
            for block in waiting[:2]:
                place_block(block)
            waiting = waiting[2:]
        source = jnp.take_along_axis(source & (LANES - 1), place, axis=1)
        for block in range(blocks, BLOCKS):
            sorted_ref[block] = zero
        target = jnp.where(place < count, lax.shift_right_logical(base + place, 7), -1)
        packed = [jnp.take_along_axis(values, source, axis=1) for values in rel]
        rows = lax.div(n_all + (LANES - 1), LANES)

        def pack_row(row, carry):
            hit = target == row
            filled = lane_1 + row * LANES < n_all
            for axis in range(3):
                own_part = jnp.where(row < own_rows, others[axis, row], 0.0)
                values = jnp.sum(jnp.where(hit, packed[axis], 0.0), axis=0, keepdims=True)
                others[axis, row] = jnp.where(filled, own_part + values, FAR_OTHER)
            return carry

        lax.fori_loop(lax.div(n_own, LANES), rows, pack_row, 0)

        def set_far(row, carry):
            for axis in range(3):
                others[axis, row] = far
            return carry

        def excess(first_quad, last_quad, first_row, wrap_box, energy):
            load_own, one_row = pair_tools(mine, others, rc2, wrap_box)

            def quad(index, total):
                first = index * QUAD
                own = load_own(first)
                sums = (zero,) * (3 * QUAD) + (total,)
                sums = lax.fori_loop(first_row, rows, lambda row, part: one_row(own, first, row, part, True), sums)
                for k in range(QUAD):
                    for axis in range(3):
                        acc[axis, first + k] = sums[3 * k + axis]
                return sums[-1]

            return lax.fori_loop(first_quad, last_quad, quad, energy)

        def plain():
            short = jnp.where(rows > FIXED_ROWS, jnp.minimum(quads, FIXED_QUADS), 0)
            energy = excess(0, short, FIXED_ROWS, [], zero)
            if blocks > FIXED_BLOCKS:
                energy = excess(FIXED_QUADS, quads, 0, [], energy)
            eng_ref[0] = energy
            lax.fori_loop(rows, FIXED_ROWS, set_far, 0)

        def wrapped():
            wrap_box = [(axis, box[axis], 1.0 / box[axis]) for axis in (1, 2)]
            eng_ref[0] = excess(0, quads, 0, wrap_box, zero)
            lax.fori_loop(0, FIXED_ROWS, set_far, 0)

        pl.when(wide)(plain)
        pl.when(jnp.logical_not(wide))(wrapped)

    pl.when(small)(lambda: build(FIXED_BLOCKS, 4))
    pl.when(jnp.logical_not(small))(lambda: build(BLOCKS, BLOCKS))


def tile_kernel(mine, others, part, eng_ref, frc_ref, out_ref, acc, react, eng, slots, send_sem, recv_sem):
    coords = my_coords()
    mz, my, mx = coords
    barrier = entry_signals(coords)
    rc2 = RC * RC + 0.0 * mine[0, 0]
    load_own, one_row = pair_tools(mine, others, rc2, [])

    lane_8 = lax.broadcasted_iota(jnp.int32, (8, LANES), 1).astype(jnp.float32)
    weights = [jnp.where(lane_8 + float(row * LANES) < eng_ref[1], 2.0, 1.0) for row in range(FIXED_BLOCKS)]
    react[...] = jnp.zeros_like(react)
    energy = eng_ref[0]
    for block in range(FIXED_BLOCKS):

        def quad(index, total, block=block):
            first = block * 16 + index * QUAD
            own = load_own(first)
            sums = tuple(part[axis, first + k] for k in range(QUAD) for axis in range(3)) + (total,)
            sums = one_row(own, first, block, sums, True)
            for row in range(block + 1, FIXED_ROWS):
                if row < FIXED_BLOCKS:
                    sums = one_row(own, first, row, sums, False, react, weights[row])
                else:
                    sums = one_row(own, first, row, sums, False)
            for k in range(QUAD):
                for axis in range(3):
                    acc[axis, first + k] = sums[3 * k + axis]
            return sums[-1]

        energy = lax.fori_loop(0, 16 // QUAD, quad, energy)
    eng[...] = jnp.full((1, LANES), 2.0 * jnp.sum(energy), jnp.float32)
    pl.semaphore_wait(barrier, len(PEERS))
    place = (mz * NY + my) * NX + mx
    copies = []
    for index, offset in enumerate(PEERS):
        copies.append(pltpu.make_async_remote_copy(src_ref=eng, dst_ref=slots.at[place], send_sem=send_sem.at[index], recv_sem=recv_sem.at[index], device_id=peer_id(coords, offset), device_id_type=MESH))
        copies[-1].start()
    slots[place] = eng[...]
    for block in range(BLOCKS):
        held = acc if block < FIXED_BLOCKS else part
        for axis in range(3):
            turned = jnp.transpose(held[axis, pl.ds(block * 16, 16)].reshape(LANES, LANES), (1, 0))
            force = jnp.sum(turned, axis=0, keepdims=True)
            if 0 < block < FIXED_BLOCKS:
                force = force - jnp.sum(react[axis, block], axis=0, keepdims=True)
            frc_ref[axis:axis + 1, block * LANES:(block + 1) * LANES] = 48.0 * force
    for copy in copies:
        copy.wait()
    total = slots[0]
    for index in range(1, NZ * NY * NX):
        total = total + slots[index]
    out_ref[...] = total


def finish_kernel(sorted_ref, frc_ref, total_ref, pos_out, vel_out, frc_out, id_out, ok_out, eng_out):
    eng_out[...] = jnp.max(total_ref[...])
    for block in range(BLOCKS):
        width = min(LANES, CAP - block * LANES)
        lanes = slice(block * LANES, block * LANES + width)
        rows_s = sorted_ref[block]
        valid = rows_s[3:4] > 0.5
        for axis in range(3):
            force = jnp.where(valid, frc_ref[axis:axis + 1, block * LANES:(block + 1) * LANES], 0.0)
            frc_out[axis:axis + 1, lanes] = force[:, :width]
            vel_out[axis:axis + 1, lanes] = (rows_s[4 + axis:5 + axis] + (0.5 * DT) * force)[:, :width]
            pos_out[axis:axis + 1, lanes] = rows_s[axis:axis + 1, :width]
        new_id = lax.shift_left(rows_s[3:4].astype(jnp.int32) - 1, 16) + rows_s[7:8].astype(jnp.int32)
        id_out[lanes] = jnp.where(valid, new_id, 0)[:, :width].reshape(width)
        ok_out[lanes] = valid.astype(jnp.int32)[:, :width].reshape(width)


VMEM_SPEC = pl.BlockSpec(memory_space=pltpu.VMEM)
HBM_SPEC = pl.BlockSpec(memory_space=pltpu.HBM)
VMEM_LIMIT = 8 * 1024 * 1024
SMEM_SPEC = pl.BlockSpec(memory_space=pltpu.SMEM)


def solution(mesh):
    def local_step(atom_pos, atom_vel, atom_frc, atom_id, atom_ok, brick_side):
        f32 = jnp.float32
        n_dev = NZ * NY * NX
        gat, pkt, own = pl.pallas_call(
            exchange_kernel,
            out_shape=(jax.ShapeDtypeStruct((N_GROUPS + 1, 3, BLOCKS, LANES), f32), jax.ShapeDtypeStruct((N_PACKETS, 8, LANES), f32), jax.ShapeDtypeStruct((16, WIDE), f32)),
            in_specs=[SMEM_SPEC] + [HBM_SPEC] * 5,
            out_specs=(VMEM_SPEC,) * 3,
            scratch_shapes=[
                pltpu.VMEM((3, 3, CAP), f32),
                pltpu.VMEM((CAP,), jnp.int32),
                pltpu.VMEM((CAP,), jnp.int32),
                pltpu.VMEM((3, 4, WIDE), f32),
                pltpu.VMEM((2, WIDE), jnp.int32),
                pltpu.VMEM((3, BLOCKS, LANES), f32),
                pltpu.VMEM((2, 8, LANES), f32),
                pltpu.SemaphoreType.DMA((5,)),
                pltpu.SemaphoreType.DMA((N_GROUPS,)),
                pltpu.SemaphoreType.DMA((N_GROUPS,)),
                pltpu.SemaphoreType.DMA((N_PACKETS,)),
                pltpu.SemaphoreType.DMA((N_PACKETS,)),
            ],
            compiler_params=pltpu.CompilerParams(collective_id=0, has_side_effects=True, vmem_limit_bytes=VMEM_LIMIT),
            name="exchange",
        )(brick_side, *(pltpu.with_memory_space_constraint(value, pltpu.HBM) for value in (atom_pos.T, atom_vel.T, atom_frc.T, atom_id, atom_ok)))
        own_tiles = jax.ShapeDtypeStruct((3, GROUPS_OWN, 8, LANES), f32)
        placed, mine, others, part, eng = pl.pallas_call(
            prepare_kernel,
            out_shape=(jax.ShapeDtypeStruct((BLOCKS, 8, LANES), f32), own_tiles, jax.ShapeDtypeStruct((3, MAX_ROWS, 8, LANES), f32), own_tiles, jax.ShapeDtypeStruct((2, 8, LANES), f32)),
            in_specs=[VMEM_SPEC] * 3,
            out_specs=(VMEM_SPEC,) * 5,
            compiler_params=pltpu.CompilerParams(vmem_limit_bytes=VMEM_LIMIT),
            name="prepare",
        )(gat, pkt, own)
        frc_rows, total = pl.pallas_call(
            tile_kernel,
            out_shape=(jax.ShapeDtypeStruct((8, WIDE), f32), jax.ShapeDtypeStruct((1, LANES), f32)),
            in_specs=[VMEM_SPEC] * 4,
            out_specs=(VMEM_SPEC,) * 2,
            scratch_shapes=[pltpu.VMEM((3, FIXED_BLOCKS * 16, 8, LANES), f32), pltpu.VMEM((3, FIXED_BLOCKS, 8, LANES), f32), pltpu.VMEM((1, LANES), f32), pltpu.VMEM((n_dev, 1, LANES), f32), pltpu.SemaphoreType.DMA((n_dev - 1,)), pltpu.SemaphoreType.DMA((n_dev - 1,))],
            compiler_params=pltpu.CompilerParams(collective_id=1, has_side_effects=True, vmem_limit_bytes=VMEM_LIMIT),
            name="tile",
        )(mine, others, part, eng)
        pos, vel, frc, ids, oks, energy = pl.pallas_call(
            finish_kernel,
            out_shape=(jax.ShapeDtypeStruct((3, CAP), f32),) * 3 + (jax.ShapeDtypeStruct((CAP,), jnp.int32),) * 2 + (jax.ShapeDtypeStruct((), f32),),
            in_specs=[VMEM_SPEC] * 3,
            out_specs=(VMEM_SPEC,) * 5 + (SMEM_SPEC,),
            compiler_params=pltpu.CompilerParams(vmem_limit_bytes=VMEM_LIMIT),
            name="finish",
        )(placed, frc_rows, total)
        return pos.T, vel.T, frc.T, ids, oks, energy

    row_spec = P(MESH_AXES, None)
    id_spec = P(MESH_AXES)
    return jax.shard_map(local_step, mesh=mesh, in_specs=(row_spec, row_spec, row_spec, id_spec, id_spec, P()), out_specs=(row_spec, row_spec, row_spec, id_spec, id_spec, P()), check_vma=False)
```

```python
import jax
import jax.numpy as jnp
from jax import lax
from jax.experimental import pallas as pl
from jax.experimental.pallas import tpu as pltpu
from jax.sharding import PartitionSpec as P

DT = 0.005
RC = 2.5
UPC = -48.0 * RC ** -13 + 24.0 * RC ** -7
MESH_AXES = ("z", "y", "x")
MESH = pl.DeviceIdType.MESH
NZ, NY, NX = 2, 2, 4
CAP = 729
LANES = 128
BLOCKS = 6
WIDE = BLOCKS * LANES
MOVE_CAP = CAP // 100
FAR_OWN = 1.0e4
FAR_OTHER = -1.0e4
NOWHERE = 1.0e9
GHOST_SQ = RC * RC + 0.01
PEERS = [(dz, dy, dx) for dz in range(NZ) for dy in range(NY) for dx in range(NX)][:0:-1]
SIDES = [(1, 1), (1, 0), (0, 1), (0, 0)]
GROUPS = [(gx, *side) for side in SIDES for gx in (1, -1)] + [(0, *side) for side in SIDES[:3]]
N_GROUPS = len(GROUPS)
DISTANT = [(2, *side) for side in SIDES]
N_PACKETS = N_GROUPS + len(DISTANT)


def lane_plan():
    starts, base = [], {}
    block, lane = 0, 0
    for index, (gx, gy, gz) in enumerate(GROUPS):
        if index == 8:
            block, lane = 1, 0
        dirs = [(gx, sy, sz) for sz in ((-1, 1) if gz else (0,)) for sy in ((-1, 1) if gy else (0,))]
        starts.append((block, lane, lane + MOVE_CAP * len(dirs)))
        for dx, dy, dz in dirs:
            base[(dz + 1) * 9 + (dy + 1) * 3 + dx + 1] = block * LANES + lane
            lane += MOVE_CAP
    return starts, base


LANE_STARTS, LANE_BASE = lane_plan()
STAY = 13
NT_DIMS = (((1,), (1,)), ((), ()))
NN_DIMS = (((1,), (0,)), ((), ()))


def split3(values):
    hi = values.astype(jnp.bfloat16).astype(jnp.float32)
    rest = values - hi
    mid = rest.astype(jnp.bfloat16).astype(jnp.float32)
    return jnp.concatenate([hi, mid, rest - mid], axis=0).astype(jnp.bfloat16)


def join3(parts):
    rows = parts.shape[0] // 3
    return (parts[0:rows] + parts[rows:2 * rows]) + parts[2 * rows:3 * rows]


def dot_nt(a, b):
    return lax.dot_general(a, b, NT_DIMS, preferred_element_type=jnp.float32)


def dot_nn(a, b):
    return lax.dot_general(a, b, NN_DIMS, preferred_element_type=jnp.float32)


def my_coords():
    return lax.axis_index("z"), lax.axis_index("y"), lax.axis_index("x")


def peer_id(coords, offset):
    mz, my, mx = coords
    return (lax.rem(mz + offset[0], NZ), lax.rem(my + offset[1], NY), lax.rem(mx + offset[2] + NX, NX))


def entry_signals(coords):
    barrier = pltpu.get_barrier_semaphore()
    for offset in PEERS:
        pl.semaphore_signal(barrier, inc=1, device_id=peer_id(coords, offset), device_id_type=MESH)
    return barrier


def exchange_kernel(brick_ref, pos_ref, vel_ref, frc_ref, id_ref, ok_ref, gat_ref, pkt_ref, own_ref, raw, ids_in, oks_in, pad_ref, int_ref, send_pos, send_pkt, in_sem, pos_send_sem, pos_recv_sem, pkt_send_sem, pkt_recv_sem):
    coords = my_coords()
    fetches = [pltpu.make_async_copy(src, dst, in_sem.at[index]) for index, (src, dst) in enumerate(((pos_ref, raw.at[0]), (vel_ref, raw.at[1]), (frc_ref, raw.at[2]), (id_ref, ids_in), (ok_ref, oks_in)))]
    for fetch in fetches:
        fetch.start()
    barrier = entry_signals(coords)
    tail = slice(WIDE - LANES, WIDE)
    pad_ref[:, :, tail] = jnp.zeros((3, 4, LANES), jnp.float32)
    int_ref[:, tail] = jnp.zeros((2, LANES), jnp.int32)
    for fetch in fetches:
        fetch.wait()
    brick = brick_ref[...]
    for index in range(3):
        pad_ref[index, 0:3, 0:CAP] = raw[index]
    int_ref[0:1, 0:CAP] = ids_in[...].reshape(1, CAP)
    int_ref[1:2, 0:CAP] = oks_in[...].reshape(1, CAP)
    owned = int_ref[1:2, :] > 0
    moved, half, code = [], [], jnp.zeros((1, WIDE), jnp.int32)
    for axis, (mine, size, weight) in enumerate(((coords[2], NX, 1), (coords[1], NY, 3), (coords[0], NZ, 9))):
        box = brick * float(size)
        low = mine.astype(jnp.float32) * brick
        high = (mine + 1).astype(jnp.float32) * brick
        half_v = pad_ref[1, axis:axis + 1, :] + (0.5 * DT) * pad_ref[2, axis:axis + 1, :]
        drift = pad_ref[0, axis:axis + 1, :] + DT * half_v
        step = jnp.where(drift >= high, 2, jnp.where(drift < low, 0, 1))
        code = code + step * weight
        wrapped = jnp.where(drift < 0.0, drift + box, jnp.where(drift >= box, drift - box, drift))
        moved.append(wrapped)
        half.append(half_v)
    code = jnp.where(owned, code, -1)
    for axis in range(3):
        for block in range(BLOCKS):
            lanes = slice(block * LANES, (block + 1) * LANES)
            send_pos[axis, block:block + 1, :] = jnp.where(owned[:, lanes], moved[axis][:, lanes], NOWHERE)
    ids = int_ref[0:1, :]
    id_hi = (lax.shift_right_logical(ids, 16) + 1).astype(jnp.float32)
    id_lo = (ids & 65535).astype(jnp.float32)
    data = jnp.concatenate(moved + [id_hi] + half + [id_lo], axis=0)
    member = (jnp.broadcast_to(code, (32, WIDE)) == lax.broadcasted_iota(jnp.int32, (32, WIDE), 0)).astype(jnp.float32)
    tri = (lax.broadcasted_iota(jnp.int32, (LANES, LANES), 0) < lax.broadcasted_iota(jnp.int32, (LANES, LANES), 1)).astype(jnp.bfloat16)
    codes = lax.broadcasted_iota(jnp.int32, (32, LANES), 0)
    running = jnp.zeros((32, LANES), jnp.float32)
    for move, first in LANE_BASE.items():
        running = jnp.where(codes == move, float(first), running)
    slots = []
    for block in range(BLOCKS):
        part = member[:, block * LANES:(block + 1) * LANES]
        before = dot_nn(part.astype(jnp.bfloat16), tri)
        slots.append(jnp.sum(part * (before + running), axis=0, keepdims=True))
        running = running + jnp.sum(part, axis=1, keepdims=True)
    slot = jnp.concatenate(slots, axis=1)
    stay = code == STAY
    mover_slot = jnp.where(owned & jnp.logical_not(stay), slot, -1.0).astype(jnp.int32)
    pick = (lax.broadcasted_iota(jnp.int32, (2 * LANES, WIDE), 0) == mover_slot).astype(jnp.float32).astype(jnp.bfloat16)
    packet = join3(dot_nt(split3(data), pick))
    send_pkt[0] = packet[:, 0:LANES]
    send_pkt[1] = packet[:, LANES:2 * LANES]
    own_ref[0:8, :] = data
    own_ref[8:16, :] = jnp.concatenate([jnp.where(stay, slot, -1.0), jnp.full((7, WIDE), brick, jnp.float32)], axis=0)
    pl.semaphore_wait(barrier, len(PEERS))
    copies = []
    for index, (gx, gy, gz) in enumerate(GROUPS + DISTANT):
        peer = peer_id(coords, (gz, gy, gx))
        if index < N_GROUPS:
            copies.append(pltpu.make_async_remote_copy(src_ref=send_pos, dst_ref=gat_ref.at[index], send_sem=pos_send_sem.at[index], recv_sem=pos_recv_sem.at[index], device_id=peer, device_id_type=MESH))
            copies[-1].start()
            source, target = send_pkt.at[LANE_STARTS[index][0]], pkt_ref.at[index]
        else:
            source, target = send_pkt.at[0, 0:4], pkt_ref.at[index, 0:4]
        copies.append(pltpu.make_async_remote_copy(src_ref=source, dst_ref=target, send_sem=pkt_send_sem.at[index], recv_sem=pkt_recv_sem.at[index], device_id=peer, device_id_type=MESH))
        copies[-1].start()
    gat_ref[N_GROUPS] = send_pos[...]
    for copy in copies:
        copy.wait()


CAND_ROWS = 8 * (N_GROUPS + 1) + 8
MAX_ROWS = BLOCKS + CAND_ROWS
GROUPS_OWN = BLOCKS * 16
QUAD = 4
FIXED_BLOCKS = 4
FIXED_QUADS = FIXED_BLOCKS * 16 // QUAD
FIXED_ROWS = 11


def pair_tools(mine, others, rc2, wrap_box):
    def powers(dist_sq):
        inv_r = lax.rsqrt(dist_sq)
        inv_2 = inv_r * inv_r
        inv_4 = inv_2 * inv_2
        term = inv_4 * inv_2 - 0.5
        return inv_r, term, term * (inv_4 * inv_4)

    cut_inv_r, cut_term, cut_core = powers(rc2)
    kappa = -RC * cut_core
    for ulps in (-3, -2, -1, 1, 2, 3):
        trial = ulps * 2.0 ** -34 - RC * cut_core
        kappa = jnp.where(trial * cut_inv_r == -cut_core, trial, kappa)

    def quad_energy(dist_sqs):
        terms, tails = [], []
        for dist_sq in dist_sqs:
            inv_r = lax.rsqrt(dist_sq)
            inv_2 = inv_r * inv_r
            term = inv_2 * inv_2 * inv_2 - 0.5
            terms.append(term * term)
            tails.append(kappa * inv_r * dist_sq)
        return ((terms[0] + terms[1]) + (terms[2] + terms[3])) - 12.0 * ((tails[0] + tails[1]) + (tails[2] + tails[3]))

    cut_energy = quad_energy([rc2] * QUAD)
    own_minus_lane = lax.broadcasted_iota(jnp.int32, (8, LANES), 0) - lax.broadcasted_iota(jnp.int32, (8, LANES), 1)

    def load_own(first):
        return [[mine[axis, first + k] for axis in range(3)] for k in range(QUAD)]

    def gaps(own, first, row, with_self):
        other = [others[axis, row] for axis in range(3)]
        deltas, dist_sqs = [], []
        for k in range(QUAD):
            delta = [own[k][axis] - other[axis] for axis in range(3)]
            for axis, box, inv_box in wrap_box:
                delta[axis] = delta[axis] - box * jnp.floor(delta[axis] * inv_box + 0.5)
            dist_sq = delta[0] * delta[0] + delta[1] * delta[1] + delta[2] * delta[2]
            if with_self:
                dist_sq = jnp.where(own_minus_lane == row * LANES - (first + k) * 8, rc2, dist_sq)
            deltas.append(delta)
            dist_sqs.append(jnp.minimum(dist_sq, rc2))
        return deltas, dist_sqs

    def energy_row(own, first, row, total, with_self, weight=None):
        gain = quad_energy(gaps(own, first, row, with_self)[1]) - cut_energy
        return total + (gain if weight is None else gain * weight)

    def force_row(own, first, row, force, with_self, react=None):
        force, pulls = list(force), []
        deltas, dist_sqs = gaps(own, first, row, with_self)
        for k in range(QUAD):
            inv_r, term, core = powers(dist_sqs[k])
            scale = core + kappa * inv_r
            pulls.append([scale * deltas[k][axis] for axis in range(3)])
            for axis in range(3):
                force[3 * k + axis] = force[3 * k + axis] + pulls[k][axis]
        if react is not None:
            for axis in range(3):
                react[axis, row] = react[axis, row] + ((pulls[0][axis] + pulls[1][axis]) + (pulls[2][axis] + pulls[3][axis]))
        return tuple(force)

    return load_own, energy_row, force_row


def prepare_kernel(gat_ref, pkt_ref, own_ref, sorted_ref, mine, others, acc, eng_ref):
    mz, my, mx = my_coords()
    brick = own_ref[9:10, 0:LANES]
    half_l = 0.5 * brick
    sizes = (NX, NY, NZ)
    centre = [(index.astype(jnp.float32) + 0.5) * brick for index in (mx, my, mz)]
    box = [brick * float(size) for size in sizes]
    lane_1 = lax.broadcasted_iota(jnp.int32, (1, LANES), 1)
    acc[:, pl.ds(0, FIXED_QUADS * QUAD)] = jnp.zeros((3, FIXED_QUADS * QUAD, 8, LANES), jnp.float32)

    arrived = []
    for block in range(2):
        total = jnp.zeros((8, LANES), jnp.float32)
        for index in range(N_GROUPS):
            where_block, first, last = LANE_STARTS[index]
            if where_block == block:
                total = total + jnp.where((lane_1 >= first) & (lane_1 < last), pkt_ref[index], 0.0)
        arrived.append(total)
    arr = jnp.concatenate(arrived, axis=1)
    arr_ok = arr[3:4] > 0.5
    stay_all = own_ref[8:9, :] >= 0.0
    n_vec = jnp.sum(stay_all.astype(jnp.float32), axis=1, keepdims=True) + jnp.sum(arr_ok.astype(jnp.float32), axis=1, keepdims=True)
    n_own = jnp.max(n_vec).astype(jnp.int32)
    n_int = n_vec.astype(jnp.int32)
    quads = lax.div(n_own + (8 * QUAD - 1), 8 * QUAD)
    own_rows = lax.div(n_own + (LANES - 1), LANES)
    beyond = gat_ref[0, 0, 4:6, :]
    for slot in range(1, N_GROUPS + 1):
        beyond = jnp.minimum(beyond, gat_ref[slot, 0, 4:6, :])
    small = (jnp.min(beyond) > 0.5 * NOWHERE) & (n_own <= FIXED_BLOCKS * LANES)
    eng_ref[1] = jnp.broadcast_to(n_vec, (8, LANES))
    wide = jnp.max(brick) >= 2.0 * RC
    int_max = 2147483647
    rc2 = RC * RC + 0.0 * own_ref[8:16, 0:LANES]
    zero = jnp.zeros((8, LANES), jnp.float32)
    far = jnp.full((8, LANES), FAR_OTHER, jnp.float32)

    def build(blocks, tile_rows):
        span = blocks * LANES
        data = jnp.concatenate([own_ref[0:8, 0:span], arr], axis=1)
        ids = lax.shift_left(data[3:4].astype(jnp.int32) - 1, 16) + data[7:8].astype(jnp.int32)
        stay_rank = own_ref[8:9, 0:span]
        stay = stay_rank >= 0.0
        arr_id = jnp.where(arr_ok, ids[:, span:], int_max)
        own_id = jnp.where(stay, ids[:, :span], int_max)

        count_rows = (N_GROUPS + 1) * tile_rows
        cand = -(-(count_rows + len(DISTANT)) // 8) * 8
        rel = []
        for axis in range(3):
            near = [gat_ref[slot, axis, 0:tile_rows, :] for slot in range(N_GROUPS + 1)]
            distant = [jnp.where(pkt_ref[N_GROUPS + k, 3:4, :] > 0.5, pkt_ref[N_GROUPS + k, axis:axis + 1, :], NOWHERE) for k in range(len(DISTANT))]
            values = jnp.concatenate(near + distant + [jnp.full((cand - count_rows - len(DISTANT), LANES), NOWHERE, jnp.float32)], axis=0) - centre[axis]
            rel.append(jnp.where(values > 0.5 * box[axis], values - box[axis], jnp.where(values < -0.5 * box[axis], values + box[axis], values)))
        over = [jnp.maximum(jnp.abs(values) - half_l, 0.0) for values in rel]
        gap_sq = over[0] * over[0] + over[1] * over[1] + over[2] * over[2]
        ghost = ((gap_sq > 0.0) & (gap_sq < GHOST_SQ)).astype(jnp.float32).astype(jnp.bfloat16)
        row_i = lax.broadcasted_iota(jnp.int32, (LANES, LANES), 0)
        col_i = lax.broadcasted_iota(jnp.int32, (LANES, LANES), 1)
        cum = dot_nn(ghost, (row_i <= col_i).astype(jnp.bfloat16)).astype(jnp.int32)
        count = dot_nn(ghost, jnp.ones((LANES, LANES), jnp.bfloat16))
        arr_col = jnp.transpose(jnp.broadcast_to(arr_id, (8, 2 * LANES)), (1, 0))[:, 0:1]
        own_col = jnp.transpose(jnp.broadcast_to(own_id, (8, span)), (1, 0))[:, 0:1]
        all_id = jnp.concatenate([own_id, arr_id], axis=1)
        arr_before = jnp.sum((arr_col < all_id).astype(jnp.float32), axis=0, keepdims=True)
        stay_before = jnp.sum((own_col < arr_id).astype(jnp.float32), axis=0, keepdims=True)
        rank = jnp.concatenate([jnp.where(stay, stay_rank + arr_before[:, :span], -1.0), jnp.where(arr_ok, stay_before + arr_before[:, span:], -1.0)], axis=1).astype(jnp.int32)
        base = dot_nn((col_i < row_i).astype(jnp.bfloat16)[:cand, :cand], count.astype(jnp.bfloat16)).astype(jnp.int32) + n_int
        count = count.astype(jnp.int32)
        n_all = jnp.max(base[cand - 8:] + count[cand - 8:])
        place = (lax.broadcasted_iota(jnp.int32, (cand, LANES), 1) - base) & (LANES - 1)
        parts = split3(data)

        def place_block(block):
            pick = (lax.broadcasted_iota(jnp.int32, (LANES, span + 2 * LANES), 0) + block * LANES == rank).astype(jnp.float32).astype(jnp.bfloat16)
            rows_s = join3(jnp.transpose(dot_nt(pick, parts), (1, 0)))
            sorted_ref[block] = rows_s
            valid = lane_1 + block * LANES < n_int
            own_rel = jnp.concatenate([rows_s[axis:axis + 1] - centre[axis] for axis in range(3)] + [rows_s[3:8]], axis=0)
            columns = jnp.transpose(jnp.where(valid, own_rel, FAR_OWN), (1, 0))
            for axis in range(3):
                others[axis, block] = jnp.broadcast_to(jnp.where(valid, own_rel[axis:axis + 1], 0.0), (8, LANES))
                mine[axis, pl.ds(block * 16, 16)] = jnp.broadcast_to(columns[:, axis:axis + 1], (LANES, LANES)).reshape(16, 8, LANES)

        wanted = lax.broadcasted_iota(jnp.int32, (cand, LANES), 1)
        source = jnp.zeros((cand, LANES), jnp.int32)
        waiting = list(range(blocks))
        for stride, probes in ((16, 7), (2, 7), (1, 1)):
            below = jnp.zeros((cand, LANES), jnp.int32)
            for k in range(1, probes + 1):
                probe = jnp.take_along_axis(cum, source + (stride * k - 1), axis=1)
                below = below + (probe <= wanted).astype(jnp.int32)
            source = source + stride * below
            for block in waiting[:2]:
                place_block(block)
            waiting = waiting[2:]
        source = jnp.take_along_axis(source & (LANES - 1), place, axis=1)
        for block in range(blocks, BLOCKS):
            sorted_ref[block] = zero
        target = jnp.where(place < count, lax.shift_right_logical(base + place, 7), -1)
        packed = [jnp.take_along_axis(values, source, axis=1) for values in rel]
        rows = lax.div(n_all + (LANES - 1), LANES)

        def pack_row(row, carry):
            hit = target == row
            filled = lane_1 + row * LANES < n_all
            for axis in range(3):
                own_part = jnp.where(row < own_rows, others[axis, row], 0.0)
                values = jnp.sum(jnp.where(hit, packed[axis], 0.0), axis=0, keepdims=True)
                others[axis, row] = jnp.where(filled, own_part + values, FAR_OTHER)
            return carry

        lax.fori_loop(lax.div(n_own, LANES), rows, pack_row, 0)

        def set_far(row, carry):
            for axis in range(3):
                others[axis, row] = far
            return carry

        def excess(first_quad, last_quad, first_row, wrap_box, energy):
            load_own, energy_row, force_row = pair_tools(mine, others, rc2, wrap_box)

            def quad(index, total):
                first = index * QUAD
                own = load_own(first)
                sums = (zero,) * (3 * QUAD) + (total,)
                sums = lax.fori_loop(first_row, rows, lambda row, part: force_row(own, first, row, part[:-1], True) + (energy_row(own, first, row, part[-1], True),), sums)
                for k in range(QUAD):
                    for axis in range(3):
                        acc[axis, first + k] = sums[3 * k + axis]
                return sums[-1]

            return lax.fori_loop(first_quad, last_quad, quad, energy)

        def plain():
            short = jnp.where(rows > FIXED_ROWS, jnp.minimum(quads, FIXED_QUADS), 0)
            energy = excess(0, short, FIXED_ROWS, [], zero)
            if blocks > FIXED_BLOCKS:
                energy = excess(FIXED_QUADS, quads, 0, [], energy)
            eng_ref[0] = energy
            lax.fori_loop(rows, FIXED_ROWS, set_far, 0)

        def wrapped():
            wrap_box = [(axis, box[axis], 1.0 / box[axis]) for axis in (1, 2)]
            eng_ref[0] = excess(0, quads, 0, wrap_box, zero)
            lax.fori_loop(0, FIXED_ROWS, set_far, 0)

        pl.when(wide)(plain)
        pl.when(jnp.logical_not(wide))(wrapped)

    pl.when(small)(lambda: build(FIXED_BLOCKS, 4))
    pl.when(jnp.logical_not(small))(lambda: build(BLOCKS, BLOCKS))


def tile_kernel(mine, others, part, eng_ref, frc_ref, out_ref, acc, react, eng, slots, send_sem, recv_sem):
    coords = my_coords()
    mz, my, mx = coords
    barrier = entry_signals(coords)
    rc2 = RC * RC + 0.0 * mine[0, 0]
    load_own, energy_row, force_row = pair_tools(mine, others, rc2, [])

    lane_8 = lax.broadcasted_iota(jnp.int32, (8, LANES), 1).astype(jnp.float32)
    energy = eng_ref[0]
    for block in range(FIXED_BLOCKS):

        def energy_quad(index, total, block=block):
            first = block * 16 + index * QUAD
            own = load_own(first)
            total = energy_row(own, first, block, total, True)
            for row in range(block + 1, FIXED_ROWS):
                weight = jnp.where(lane_8 + float(row * LANES) < eng_ref[1], 2.0, 1.0) if row < FIXED_BLOCKS else None
                total = energy_row(own, first, row, total, False, weight)
            return total

        energy = lax.fori_loop(0, 16 // QUAD, energy_quad, energy)
    eng[...] = jnp.full((1, LANES), 2.0 * jnp.sum(energy), jnp.float32)
    pl.semaphore_wait(barrier, len(PEERS))
    place = (mz * NY + my) * NX + mx
    copies = []
    for index, offset in enumerate(PEERS):
        copies.append(pltpu.make_async_remote_copy(src_ref=eng, dst_ref=slots.at[place], send_sem=send_sem.at[index], recv_sem=recv_sem.at[index], device_id=peer_id(coords, offset), device_id_type=MESH))
        copies[-1].start()
    slots[place] = eng[...]
    react[...] = jnp.zeros_like(react)
    for block in range(FIXED_BLOCKS):

        def force_quad(index, carry, block=block):
            first = block * 16 + index * QUAD
            own = load_own(first)
            force = force_row(own, first, block, [part[axis, first + k] for k in range(QUAD) for axis in range(3)], True)
            for row in range(block + 1, FIXED_ROWS):
                force = force_row(own, first, row, force, False, react if row < FIXED_BLOCKS else None)
            for k in range(QUAD):
                for axis in range(3):
                    acc[axis, first + k] = force[3 * k + axis]
            return carry

        lax.fori_loop(0, 16 // QUAD, force_quad, 0)
    for block in range(BLOCKS):
        held = acc if block < FIXED_BLOCKS else part
        for axis in range(3):
            turned = jnp.transpose(held[axis, pl.ds(block * 16, 16)].reshape(LANES, LANES), (1, 0))
            force = jnp.sum(turned, axis=0, keepdims=True)
            if 0 < block < FIXED_BLOCKS:
                force = force - jnp.sum(react[axis, block], axis=0, keepdims=True)
            frc_ref[axis:axis + 1, block * LANES:(block + 1) * LANES] = 48.0 * force
    for copy in copies:
        copy.wait()
    total = slots[0]
    for index in range(1, NZ * NY * NX):
        total = total + slots[index]
    out_ref[...] = total


def finish_kernel(sorted_ref, frc_ref, total_ref, pos_out, vel_out, frc_out, id_out, ok_out, eng_out):
    eng_out[...] = jnp.max(total_ref[...])
    for block in range(BLOCKS):
        width = min(LANES, CAP - block * LANES)
        lanes = slice(block * LANES, block * LANES + width)
        rows_s = sorted_ref[block]
        valid = rows_s[3:4] > 0.5
        for axis in range(3):
            force = jnp.where(valid, frc_ref[axis:axis + 1, block * LANES:(block + 1) * LANES], 0.0)
            frc_out[axis:axis + 1, lanes] = force[:, :width]
            vel_out[axis:axis + 1, lanes] = (rows_s[4 + axis:5 + axis] + (0.5 * DT) * force)[:, :width]
            pos_out[axis:axis + 1, lanes] = rows_s[axis:axis + 1, :width]
        new_id = lax.shift_left(rows_s[3:4].astype(jnp.int32) - 1, 16) + rows_s[7:8].astype(jnp.int32)
        id_out[lanes] = jnp.where(valid, new_id, 0)[:, :width].reshape(width)
        ok_out[lanes] = valid.astype(jnp.int32)[:, :width].reshape(width)


VMEM_SPEC = pl.BlockSpec(memory_space=pltpu.VMEM)
HBM_SPEC = pl.BlockSpec(memory_space=pltpu.HBM)
VMEM_LIMIT = 8 * 1024 * 1024
SMEM_SPEC = pl.BlockSpec(memory_space=pltpu.SMEM)


def solution(mesh):
    def local_step(atom_pos, atom_vel, atom_frc, atom_id, atom_ok, brick_side):
        f32 = jnp.float32
        n_dev = NZ * NY * NX
        gat, pkt, own = pl.pallas_call(
            exchange_kernel,
            out_shape=(jax.ShapeDtypeStruct((N_GROUPS + 1, 3, BLOCKS, LANES), f32), jax.ShapeDtypeStruct((N_PACKETS, 8, LANES), f32), jax.ShapeDtypeStruct((16, WIDE), f32)),
            in_specs=[SMEM_SPEC] + [HBM_SPEC] * 5,
            out_specs=(VMEM_SPEC,) * 3,
            scratch_shapes=[
                pltpu.VMEM((3, 3, CAP), f32),
                pltpu.VMEM((CAP,), jnp.int32),
                pltpu.VMEM((CAP,), jnp.int32),
                pltpu.VMEM((3, 4, WIDE), f32),
                pltpu.VMEM((2, WIDE), jnp.int32),
                pltpu.VMEM((3, BLOCKS, LANES), f32),
                pltpu.VMEM((2, 8, LANES), f32),
                pltpu.SemaphoreType.DMA((5,)),
                pltpu.SemaphoreType.DMA((N_GROUPS,)),
                pltpu.SemaphoreType.DMA((N_GROUPS,)),
                pltpu.SemaphoreType.DMA((N_PACKETS,)),
                pltpu.SemaphoreType.DMA((N_PACKETS,)),
            ],
            compiler_params=pltpu.CompilerParams(collective_id=0, has_side_effects=True, vmem_limit_bytes=VMEM_LIMIT),
            name="exchange",
        )(brick_side, *(pltpu.with_memory_space_constraint(value, pltpu.HBM) for value in (atom_pos.T, atom_vel.T, atom_frc.T, atom_id, atom_ok)))
        own_tiles = jax.ShapeDtypeStruct((3, GROUPS_OWN, 8, LANES), f32)
        placed, mine, others, part, eng = pl.pallas_call(
            prepare_kernel,
            out_shape=(jax.ShapeDtypeStruct((BLOCKS, 8, LANES), f32), own_tiles, jax.ShapeDtypeStruct((3, MAX_ROWS, 8, LANES), f32), own_tiles, jax.ShapeDtypeStruct((2, 8, LANES), f32)),
            in_specs=[VMEM_SPEC] * 3,
            out_specs=(VMEM_SPEC,) * 5,
            compiler_params=pltpu.CompilerParams(vmem_limit_bytes=VMEM_LIMIT),
            name="prepare",
        )(gat, pkt, own)
        frc_rows, total = pl.pallas_call(
            tile_kernel,
            out_shape=(jax.ShapeDtypeStruct((8, WIDE), f32), jax.ShapeDtypeStruct((1, LANES), f32)),
            in_specs=[VMEM_SPEC] * 4,
            out_specs=(VMEM_SPEC,) * 2,
            scratch_shapes=[pltpu.VMEM((3, FIXED_BLOCKS * 16, 8, LANES), f32), pltpu.VMEM((3, FIXED_BLOCKS, 8, LANES), f32), pltpu.VMEM((1, LANES), f32), pltpu.VMEM((n_dev, 1, LANES), f32), pltpu.SemaphoreType.DMA((n_dev - 1,)), pltpu.SemaphoreType.DMA((n_dev - 1,))],
            compiler_params=pltpu.CompilerParams(collective_id=1, has_side_effects=True, vmem_limit_bytes=VMEM_LIMIT),
            name="tile",
        )(mine, others, part, eng)
        pos, vel, frc, ids, oks, energy = pl.pallas_call(
            finish_kernel,
            out_shape=(jax.ShapeDtypeStruct((3, CAP), f32),) * 3 + (jax.ShapeDtypeStruct((CAP,), jnp.int32),) * 2 + (jax.ShapeDtypeStruct((), f32),),
            in_specs=[VMEM_SPEC] * 3,
            out_specs=(VMEM_SPEC,) * 5 + (SMEM_SPEC,),
            compiler_params=pltpu.CompilerParams(vmem_limit_bytes=VMEM_LIMIT),
            name="finish",
        )(placed, frc_rows, total)
        return pos.T, vel.T, frc.T, ids, oks, energy

    row_spec = P(MESH_AXES, None)
    id_spec = P(MESH_AXES)
    return jax.shard_map(local_step, mesh=mesh, in_specs=(row_spec, row_spec, row_spec, id_spec, id_spec, P()), out_specs=(row_spec, row_spec, row_spec, id_spec, id_spec, P()), check_vma=False)
```

```python
import jax
import jax.numpy as jnp
from jax import lax
from jax.experimental import pallas as pl
from jax.experimental.pallas import tpu as pltpu
from jax.sharding import PartitionSpec as P

DT = 0.005
HALF_DT = 0.5 * DT
RC = 2.5
UPC = -48.0 * RC ** -13 + 24.0 * RC ** -7
MESH_AXES = ("z", "y", "x")
MESH = pl.DeviceIdType.MESH
NZ, NY, NX = 2, 2, 4
CAP = 729
LANES = 128
TILE = (8, LANES)
BLOCKS = 6
WIDE = BLOCKS * LANES
MOVE_CAP = CAP // 100
FAR_OWN = 1.0e4
FAR_OTHER = -1.0e4
NOWHERE = 1.0e9
GHOST_SQ = RC * RC + 0.01
PEERS = [(dz, dy, dx) for dz in range(NZ) for dy in range(NY) for dx in range(NX)][:0:-1]
SIDES = [(1, 1), (1, 0), (0, 1), (0, 0)]
GROUPS = [(gx, *side) for side in SIDES for gx in (1, -1)] + [(0, *side) for side in SIDES[:3]]
N_GROUPS = len(GROUPS)
DISTANT = [(2, *side) for side in SIDES]
N_PACKETS = N_GROUPS + len(DISTANT)


def lane_plan():
    starts, base = [], {}
    block, lane = 0, 0
    for index, (gx, gy, gz) in enumerate(GROUPS):
        if index == 8:
            block, lane = 1, 0
        dirs = [(gx, sy, sz) for sz in ((-1, 1) if gz else (0,)) for sy in ((-1, 1) if gy else (0,))]
        starts.append((block, lane, lane + MOVE_CAP * len(dirs)))
        for dx, dy, dz in dirs:
            base[(dz + 1) * 9 + (dy + 1) * 3 + dx + 1] = block * LANES + lane
            lane += MOVE_CAP
    return starts, base


LANE_STARTS, LANE_BASE = lane_plan()
STAY = 13
NT_DIMS = (((1,), (1,)), ((), ()))
NN_DIMS = (((1,), (0,)), ((), ()))
TN_DIMS = (((0,), (0,)), ((), ()))


def split3(values):
    hi = values.astype(jnp.bfloat16).astype(jnp.float32)
    rest = values - hi
    mid = rest.astype(jnp.bfloat16).astype(jnp.float32)
    return jnp.concatenate([hi, mid, rest - mid], axis=0).astype(jnp.bfloat16)


def join3(parts):
    rows = parts.shape[0] // 3
    return (parts[0:rows] + parts[rows:2 * rows]) + parts[2 * rows:3 * rows]


def dot_nt(a, b):
    return lax.dot_general(a, b, NT_DIMS, preferred_element_type=jnp.float32)


def dot_nn(a, b):
    return lax.dot_general(a, b, NN_DIMS, preferred_element_type=jnp.float32)


def down(values):
    return jnp.sum(values, axis=0, keepdims=True)


def across(values):
    return jnp.sum(values, axis=1, keepdims=True)


def stack(values):
    return jnp.concatenate(values, axis=0)


def beside(values):
    return jnp.concatenate(values, axis=1)


def iota(shape, axis):
    return lax.broadcasted_iota(jnp.int32, shape, axis)


def my_coords():
    return lax.axis_index("z"), lax.axis_index("y"), lax.axis_index("x")


def peer_id(coords, offset):
    mz, my, mx = coords
    return (lax.rem(mz + offset[0], NZ), lax.rem(my + offset[1], NY), lax.rem(mx + offset[2] + NX, NX))


def entry_signals(coords):
    barrier = pltpu.get_barrier_semaphore()
    for offset in PEERS:
        pl.semaphore_signal(barrier, inc=1, device_id=peer_id(coords, offset), device_id_type=MESH)
    return barrier


def exchange_kernel(brick_ref, pos_ref, vel_ref, frc_ref, id_ref, ok_ref, gat_ref, pkt_ref, own_ref, raw, ids_in, oks_in, pad_ref, int_ref, send_pos, send_pkt, in_sem, pos_send_sem, pos_recv_sem, pkt_send_sem, pkt_recv_sem):
    coords = my_coords()
    fetches = [pltpu.make_async_copy(src, dst, in_sem.at[index]) for index, (src, dst) in enumerate(((pos_ref, raw.at[0]), (vel_ref, raw.at[1]), (frc_ref, raw.at[2]), (id_ref, ids_in), (ok_ref, oks_in)))]
    for fetch in fetches:
        fetch.start()
    barrier = entry_signals(coords)
    tail = slice(WIDE - LANES, WIDE)
    pad_ref[:, :, tail] = jnp.zeros((3, 4, LANES), jnp.float32)
    int_ref[:, tail] = jnp.zeros((2, LANES), jnp.int32)
    for fetch in fetches:
        fetch.wait()
    brick = brick_ref[...]
    for index in range(3):
        pad_ref[index, 0:3, 0:CAP] = raw[index]
    int_ref[0:1, 0:CAP] = ids_in[...].reshape(1, CAP)
    int_ref[1:2, 0:CAP] = oks_in[...].reshape(1, CAP)
    owned = int_ref[1:2, :] > 0
    moved, half, code = [], [], jnp.zeros((1, WIDE), jnp.int32)
    for axis, (mine, size, weight) in enumerate(((coords[2], NX, 1), (coords[1], NY, 3), (coords[0], NZ, 9))):
        box = brick * float(size)
        low = mine.astype(jnp.float32) * brick
        high = (mine + 1).astype(jnp.float32) * brick
        half_v = pad_ref[1, axis:axis + 1, :] + HALF_DT * pad_ref[2, axis:axis + 1, :]
        drift = pad_ref[0, axis:axis + 1, :] + DT * half_v
        step = jnp.where(drift >= high, 2, jnp.where(drift < low, 0, 1))
        code = code + step * weight
        wrapped = jnp.where(drift < 0.0, drift + box, jnp.where(drift >= box, drift - box, drift))
        moved.append(wrapped)
        half.append(half_v)
    code = jnp.where(owned, code, -1)
    for axis in range(3):
        for block in range(BLOCKS):
            lanes = slice(block * LANES, (block + 1) * LANES)
            send_pos[axis, block:block + 1, :] = jnp.where(owned[:, lanes], moved[axis][:, lanes], NOWHERE)
    ids = int_ref[0:1, :]
    id_hi = (lax.shift_right_logical(ids, 16) + 1).astype(jnp.float32)
    id_lo = (ids & 65535).astype(jnp.float32)
    data = stack(moved + [id_hi] + half + [id_lo])
    member = (jnp.broadcast_to(code, (32, WIDE)) == iota((32, WIDE), 0)).astype(jnp.float32)
    tri = (iota((LANES, LANES), 0) < iota((LANES, LANES), 1)).astype(jnp.bfloat16)
    codes = iota((32, LANES), 0)
    running = jnp.zeros((32, LANES), jnp.float32)
    for move, first in LANE_BASE.items():
        running = jnp.where(codes == move, float(first), running)
    slots = []
    for block in range(BLOCKS):
        part = member[:, block * LANES:(block + 1) * LANES]
        before = dot_nn(part.astype(jnp.bfloat16), tri)
        slots.append(down(part * (before + running)))
        running = running + across(part)
    slot = beside(slots)
    stay = code == STAY
    mover_slot = jnp.where(owned & jnp.logical_not(stay), slot, -1.0).astype(jnp.int32)
    pick = (iota((2 * LANES, WIDE), 0) == mover_slot).astype(jnp.float32).astype(jnp.bfloat16)
    packet = join3(dot_nt(split3(data), pick))
    send_pkt[0] = packet[:, 0:LANES]
    send_pkt[1] = packet[:, LANES:2 * LANES]
    own_ref[0:8, :] = data
    own_ref[8:16, :] = stack([jnp.where(stay, slot, -1.0), jnp.full((7, WIDE), brick, jnp.float32)])
    pl.semaphore_wait(barrier, len(PEERS))
    copies = []
    for index, (gx, gy, gz) in enumerate(GROUPS + DISTANT):
        peer = peer_id(coords, (gz, gy, gx))
        if index < N_GROUPS:
            copies.append(pltpu.make_async_remote_copy(src_ref=send_pos, dst_ref=gat_ref.at[index], send_sem=pos_send_sem.at[index], recv_sem=pos_recv_sem.at[index], device_id=peer, device_id_type=MESH))
            copies[-1].start()
            source, target = send_pkt.at[LANE_STARTS[index][0]], pkt_ref.at[index]
        else:
            source, target = send_pkt.at[0, 0:4], pkt_ref.at[index, 0:4]
        copies.append(pltpu.make_async_remote_copy(src_ref=source, dst_ref=target, send_sem=pkt_send_sem.at[index], recv_sem=pkt_recv_sem.at[index], device_id=peer, device_id_type=MESH))
        copies[-1].start()
    gat_ref[N_GROUPS] = send_pos[...]
    for copy in copies:
        copy.wait()


CAND_ROWS = 8 * (N_GROUPS + 1) + 8
MAX_ROWS = BLOCKS + CAND_ROWS
GROUPS_OWN = BLOCKS * 16
QUAD = 4
FIXED_BLOCKS = 4
PER_BLOCK = 16
FIXED_QUADS = FIXED_BLOCKS * PER_BLOCK // QUAD
FIXED_ROWS = 11
ENERGY_ROWS = 8


def pair_tools(mine, others, rc2, wrap_box):
    def powers(dist_sq):
        inv_r = lax.rsqrt(dist_sq)
        inv_2 = inv_r * inv_r
        inv_4 = inv_2 * inv_2
        term = inv_4 * inv_2 - 0.5
        return inv_r, term, term * (inv_4 * inv_4)

    cut_inv_r, cut_term, cut_core = powers(rc2)
    kappa = -RC * cut_core
    for ulps in (-3, -2, -1, 1, 2, 3):
        trial = ulps * 2.0 ** -34 - RC * cut_core
        kappa = jnp.where(trial * cut_inv_r == -cut_core, trial, kappa)

    def quad_energy(dist_sqs):
        terms, tails = [], []
        for dist_sq in dist_sqs:
            inv_r = lax.rsqrt(dist_sq)
            inv_2 = inv_r * inv_r
            term = inv_2 * inv_2 * inv_2 - 0.5
            terms.append(term * term)
            tails.append(kappa * inv_r * dist_sq)
        return ((terms[0] + terms[1]) + (terms[2] + terms[3])) - 12.0 * ((tails[0] + tails[1]) + (tails[2] + tails[3]))

    cut_energy = quad_energy([rc2] * QUAD)
    own_minus_lane = iota(TILE, 0) - iota(TILE, 1)

    def load_own(first):
        return [[mine[axis, first + k] for axis in range(3)] for k in range(QUAD)]

    def gaps(own, first, row, with_self):
        other = [others[axis, row] for axis in range(3)]
        deltas, dist_sqs = [], []
        for k in range(QUAD):
            delta = [own[k][axis] - other[axis] for axis in range(3)]
            for axis, box, inv_box in wrap_box:
                delta[axis] = delta[axis] - box * jnp.floor(delta[axis] * inv_box + 0.5)
            dist_sq = delta[0] * delta[0] + delta[1] * delta[1] + delta[2] * delta[2]
            if with_self:
                dist_sq = jnp.where(own_minus_lane == row * LANES - (first + k) * 8, rc2, dist_sq)
            deltas.append(delta)
            dist_sqs.append(jnp.minimum(dist_sq, rc2))
        return deltas, dist_sqs

    def energy_row(own, first, row, total, with_self, weight=None):
        gain = quad_energy(gaps(own, first, row, with_self)[1]) - cut_energy
        return total + (gain if weight is None else gain * weight)

    def force_row(own, first, row, force, with_self, react=None):
        force, pulls = list(force), []
        deltas, dist_sqs = gaps(own, first, row, with_self)
        for k in range(QUAD):
            inv_r, term, core = powers(dist_sqs[k])
            scale = core + kappa * inv_r
            pulls.append([scale * deltas[k][axis] for axis in range(3)])
            for axis in range(3):
                force[3 * k + axis] = force[3 * k + axis] + pulls[k][axis]
        if react is not None:
            for axis in range(3):
                react[axis, row] = react[axis, row] + ((pulls[0][axis] + pulls[1][axis]) + (pulls[2][axis] + pulls[3][axis]))
        return tuple(force)

    return load_own, energy_row, force_row


def prepare_kernel(gat_ref, pkt_ref, own_ref, sorted_ref, mine, others, acc, eng_ref):
    mz, my, mx = my_coords()
    brick = own_ref[9:10, 0:LANES]
    half_l = 0.5 * brick
    sizes = (NX, NY, NZ)
    centre = [(index.astype(jnp.float32) + 0.5) * brick for index in (mx, my, mz)]
    box = [brick * float(size) for size in sizes]
    lane_1 = iota((1, LANES), 1)
    acc[:, pl.ds(0, FIXED_QUADS * QUAD)] = jnp.zeros((3, FIXED_QUADS * QUAD, 8, LANES), jnp.float32)

    arrived = []
    for block in range(2):
        total = jnp.zeros(TILE, jnp.float32)
        for index in range(N_GROUPS):
            where_block, first, last = LANE_STARTS[index]
            if where_block == block:
                total = total + jnp.where((lane_1 >= first) & (lane_1 < last), pkt_ref[index], 0.0)
        arrived.append(total)
    arr = beside(arrived)
    arr_ok = arr[3:4] > 0.5
    stay_all = own_ref[8:9, :] >= 0.0
    n_vec = across(stay_all.astype(jnp.float32)) + across(arr_ok.astype(jnp.float32))
    n_own = jnp.max(n_vec).astype(jnp.int32)
    n_int = n_vec.astype(jnp.int32)
    quads = lax.div(n_own + (8 * QUAD - 1), 8 * QUAD)
    own_rows = lax.div(n_own + (LANES - 1), LANES)
    beyond = gat_ref[0, 0, 4:6, :]
    for slot in range(1, N_GROUPS + 1):
        beyond = jnp.minimum(beyond, gat_ref[slot, 0, 4:6, :])
    small = (jnp.min(beyond) > 0.5 * NOWHERE) & (n_own <= FIXED_BLOCKS * LANES)
    eng_ref[1] = jnp.broadcast_to(n_vec, TILE)
    wide = jnp.max(brick) >= 2.0 * RC
    int_max = 2147483647
    rc2 = RC * RC + 0.0 * own_ref[8:16, 0:LANES]
    zero = jnp.zeros(TILE, jnp.float32)
    far = jnp.full(TILE, FAR_OTHER, jnp.float32)

    def build(blocks, tile_rows):
        span = blocks * LANES
        data = beside([own_ref[0:8, 0:span], arr])
        ids = lax.shift_left(data[3:4].astype(jnp.int32) - 1, 16) + data[7:8].astype(jnp.int32)
        stay_rank = own_ref[8:9, 0:span]
        stay = stay_rank >= 0.0
        arr_id = jnp.where(arr_ok, ids[:, span:], int_max)
        own_id = jnp.where(stay, ids[:, :span], int_max)

        count_rows = (N_GROUPS + 1) * tile_rows
        cand = -(-(count_rows + len(DISTANT)) // 8) * 8
        rel = []
        for axis in range(3):
            near = [gat_ref[slot, axis, 0:tile_rows, :] for slot in range(N_GROUPS + 1)]
            distant = [jnp.where(pkt_ref[N_GROUPS + k, 3:4, :] > 0.5, pkt_ref[N_GROUPS + k, axis:axis + 1, :], NOWHERE) for k in range(len(DISTANT))]
            values = stack(near + distant + [jnp.full((cand - count_rows - len(DISTANT), LANES), NOWHERE, jnp.float32)]) - centre[axis]
            rel.append(jnp.where(values > 0.5 * box[axis], values - box[axis], jnp.where(values < -0.5 * box[axis], values + box[axis], values)))
        over = [jnp.maximum(jnp.abs(values) - half_l, 0.0) for values in rel]
        gap_sq = over[0] * over[0] + over[1] * over[1] + over[2] * over[2]
        side = jnp.zeros((cand, LANES), jnp.float32)
        for axis in range(3):
            side = 3.0 * side + jnp.where(over[2 - axis] > 0.0, jnp.where(rel[2 - axis] > 0.0, 1.0, -1.0), 0.0)
        near = gap_sq < GHOST_SQ
        mixed = jnp.where(near & (side > 0.0), 256.0, jnp.where(near & (side < 0.0), 1.0, 0.0)).astype(jnp.bfloat16)
        row_l, col_l = iota((LANES, LANES), 0), iota((LANES, LANES), 1)

        def counts(chosen):
            return dot_nn(mixed, chosen.astype(jnp.bfloat16)).astype(jnp.int32)

        cum = counts(row_l <= col_l)
        total = counts(row_l >= 0)
        marks = [counts(row_l < 16 * k) for k in range(1, 8)]
        arr_col = jnp.broadcast_to(arr_id, (8, 2 * LANES)).T[:, 0:1]
        arr_first = (arr_col < beside([own_id, arr_id])).astype(jnp.float32)
        arr_before = down(arr_first)
        stay_after = dot_nt(jnp.broadcast_to(stay.astype(jnp.float32), (8, span)).astype(jnp.bfloat16), arr_first[:, :span].astype(jnp.bfloat16))[0:1]
        stay_before = across(stay.astype(jnp.float32)) - stay_after
        rank = beside([jnp.where(stay, stay_rank + arr_before[:, :span], -1.0), jnp.where(arr_ok, stay_before + arr_before[:, span:], -1.0)]).astype(jnp.int32)
        earlier = (iota((cand, cand), 1) < iota((cand, cand), 0)).astype(jnp.bfloat16)
        uppers, lowers = lax.shift_right_logical(total, 8), total & 255

        def starts(each, first):
            base = dot_nn(earlier, each.astype(jnp.float32).astype(jnp.bfloat16)).astype(jnp.int32) + first
            return base, base[cand - 1:] + each[cand - 1:]

        upper_base, upper_end = starts(uppers, n_int)
        lower_base, all_end = starts(lowers, upper_end)
        n_upper, n_all = jnp.max(upper_end), jnp.max(all_end)
        eng_ref[2] = jnp.broadcast_to(upper_end.astype(jnp.float32), TILE)
        fits = n_upper <= ENERGY_ROWS * LANES
        parts = split3(data)
        spread = ((iota((24, 3 * LANES), 0) & 7) == lax.shift_right_logical(iota((24, 3 * LANES), 1), 7)).astype(jnp.bfloat16)

        def place_block(block):
            pick = (iota((LANES, span + 2 * LANES), 0) + block * LANES == rank).astype(jnp.float32).astype(jnp.bfloat16)
            rows_s = join3((dot_nt(pick, parts)).T)
            sorted_ref[block] = rows_s
            valid = lane_1 + block * LANES < n_int
            own_rel = stack([rows_s[axis:axis + 1] - centre[axis] for axis in range(3)] + [rows_s[3:8]])
            tiles = lax.dot_general(split3(jnp.where(valid, own_rel, FAR_OWN)), spread, TN_DIMS, preferred_element_type=jnp.float32)
            for axis in range(3):
                others[axis, block] = jnp.broadcast_to(jnp.where(valid, own_rel[axis:axis + 1], 0.0), TILE)
                mine[axis, pl.ds(block * PER_BLOCK, PER_BLOCK)] = tiles[:, axis * LANES:(axis + 1) * LANES].reshape(16, 8, LANES)

        lane_c = iota((cand, LANES), 1)
        is_upper = lane_c < uppers
        keep = jnp.where(is_upper, -1, 255)
        bound = jnp.where(is_upper, lane_c * 256 + 255, lane_c - uppers)

        def passed(probes):
            return sum(((probe & keep) <= bound).astype(jnp.int32) for probe in probes)

        def probe_at(source, stride, number):
            return [jnp.take_along_axis(cum, source + (stride * k - 1), axis=1) for k in range(1, number + 1)]

        source = 16 * passed(marks)
        place_block(0)
        place_block(1)
        source = source + 2 * passed(probe_at(source, 2, 7))
        for block in range(2, blocks):
            place_block(block)
        source = source + passed(probe_at(source, 1, 1))
        for block in range(blocks, BLOCKS):
            sorted_ref[block] = zero

        def turned(base, each, first):
            place = (lane_c - base) & (LANES - 1)
            lane = jnp.take_along_axis(source, (first + place) & (LANES - 1), axis=1)
            target = jnp.where(place < each, lax.shift_right_logical(base + place, 7), -1)
            return target, [jnp.take_along_axis(values, lane, axis=1) for values in rel]

        def pack(target, packed, start, stop, held_rows, empty):
            def pack_row(row, carry):
                hit = target == row
                filled = lane_1 + row * LANES < n_all
                for axis in range(3):
                    held = jnp.where(row < held_rows, others[axis, row], 0.0)
                    values = held + down(jnp.where(hit, packed[axis], 0.0))
                    others[axis, row] = jnp.where(filled, values, empty)
                return carry

            lax.fori_loop(lax.div(start, LANES), lax.div(stop + (LANES - 1), LANES), pack_row, 0)

        upper_rows = lax.div(n_upper + (LANES - 1), LANES)
        rows = lax.div(n_all + (LANES - 1), LANES)
        upper_set, lower_set = turned(upper_base, uppers, 0), turned(lower_base, lowers, uppers)
        pack(*upper_set, n_own, n_upper, own_rows, 0.0)
        pack(*lower_set, n_upper, n_all, upper_rows, FAR_OTHER)

        def set_far(row, carry):
            for axis in range(3):
                others[axis, row] = far
            return carry

        def excess(first_quad, last_quad, first_row, wrap_box, energy):
            slot_8 = iota(TILE, 1)
            load_own, energy_row, force_row = pair_tools(mine, others, rc2, wrap_box)

            def quad(index, total):
                first = index * QUAD
                own = load_own(first)
                sums = (zero,) * (3 * QUAD) + (total,)

                def both(row, part):
                    slot = slot_8 + row * LANES
                    weight = 1.0 if wrap_box else jnp.where(slot < n_int, 1.0, jnp.where(slot < upper_end, 2.0, 0.0))
                    return force_row(own, first, row, part[:-1], True) + (energy_row(own, first, row, part[-1], True, weight),)

                sums = lax.fori_loop(first_row, rows, both, sums)
                for k in range(QUAD):
                    for axis in range(3):
                        acc[axis, first + k] = sums[3 * k + axis]
                return sums[-1]

            return lax.fori_loop(first_quad, last_quad, quad, energy)

        def plain():
            short = jnp.where(rows > FIXED_ROWS, jnp.minimum(quads, FIXED_QUADS), 0)
            energy = excess(0, short, FIXED_ROWS, [], zero)
            if blocks > FIXED_BLOCKS:
                energy = excess(FIXED_QUADS, quads, 0, [], energy)
            eng_ref[0] = energy
            lax.fori_loop(rows, FIXED_ROWS, set_far, 0)

        def alone(wrap_box):
            eng_ref[0] = excess(0, quads, 0, wrap_box, zero)
            lax.fori_loop(0, FIXED_ROWS, set_far, 0)

        pl.when(wide & fits)(plain)
        pl.when(wide & jnp.logical_not(fits))(lambda: alone([]))
        pl.when(jnp.logical_not(wide))(lambda: alone([(axis, box[axis], 1.0 / box[axis]) for axis in (1, 2)]))

    pl.when(small)(lambda: build(FIXED_BLOCKS, 4))
    pl.when(jnp.logical_not(small))(lambda: build(BLOCKS, BLOCKS))


def tile_kernel(mine, others, part, eng_ref, frc_ref, out_ref, acc, react, eng, slots, send_sem, recv_sem):
    coords = my_coords()
    mz, my, mx = coords
    barrier = entry_signals(coords)
    rc2 = RC * RC + 0.0 * mine[0, 0]
    load_own, energy_row, force_row = pair_tools(mine, others, rc2, [])

    lane_8 = iota(TILE, 1).astype(jnp.float32)
    energy = eng_ref[0]

    def weight_of(row, own_weight):
        slot = lane_8 + float(row * LANES)
        return jnp.where(slot < eng_ref[1], own_weight, jnp.where(slot < eng_ref[2], 2.0, 0.0))

    for block in range(FIXED_BLOCKS):

        def energy_quad(index, total, block=block):
            first = block * PER_BLOCK + index * QUAD
            own = load_own(first)
            for row in range(block, ENERGY_ROWS):
                weight = weight_of(row, 2.0 if block < row < FIXED_BLOCKS else 1.0)
                total = energy_row(own, first, row, total, row == block, weight)
            return total

        energy = lax.fori_loop(0, PER_BLOCK // QUAD, energy_quad, energy)
    eng[...] = jnp.full((1, LANES), 2.0 * jnp.sum(energy), jnp.float32)
    pl.semaphore_wait(barrier, len(PEERS))
    place = (mz * NY + my) * NX + mx
    copies = []
    for index, offset in enumerate(PEERS):
        copies.append(pltpu.make_async_remote_copy(src_ref=eng, dst_ref=slots.at[place], send_sem=send_sem.at[index], recv_sem=recv_sem.at[index], device_id=peer_id(coords, offset), device_id_type=MESH))
        copies[-1].start()
    slots[place] = eng[...]
    react[...] = jnp.zeros_like(react)
    for block in range(FIXED_BLOCKS):

        def force_quad(index, carry, block=block):
            first = block * PER_BLOCK + index * QUAD
            own = load_own(first)
            force = force_row(own, first, block, [part[axis, first + k] for k in range(QUAD) for axis in range(3)], True)
            for row in range(block + 1, FIXED_ROWS):
                force = force_row(own, first, row, force, False, react if row < FIXED_BLOCKS else None)
            for k in range(QUAD):
                for axis in range(3):
                    acc[axis, first + k] = force[3 * k + axis]
            return carry

        lax.fori_loop(0, PER_BLOCK // QUAD, force_quad, 0)
    for block in range(BLOCKS):
        held = acc if block < FIXED_BLOCKS else part
        for axis in range(3):
            turned = (held[axis, pl.ds(block * PER_BLOCK, PER_BLOCK)].reshape(LANES, LANES)).T
            force = down(turned)
            if 0 < block < FIXED_BLOCKS:
                force = force - down(react[axis, block])
            frc_ref[axis:axis + 1, block * LANES:(block + 1) * LANES] = 48.0 * force
    for copy in copies:
        copy.wait()
    total = slots[0]
    for index in range(1, NZ * NY * NX):
        total = total + slots[index]
    out_ref[...] = total


def finish_kernel(sorted_ref, frc_ref, total_ref, pos_out, vel_out, frc_out, id_out, ok_out, eng_out):
    eng_out[...] = jnp.max(total_ref[...])
    for block in range(BLOCKS):
        width = min(LANES, CAP - block * LANES)
        lanes = slice(block * LANES, block * LANES + width)
        rows_s = sorted_ref[block]
        valid = rows_s[3:4] > 0.5
        for axis in range(3):
            force = jnp.where(valid, frc_ref[axis:axis + 1, block * LANES:(block + 1) * LANES], 0.0)
            frc_out[axis:axis + 1, lanes] = force[:, :width]
            vel_out[axis:axis + 1, lanes] = (rows_s[4 + axis:5 + axis] + HALF_DT * force)[:, :width]
            pos_out[axis:axis + 1, lanes] = rows_s[axis:axis + 1, :width]
        new_id = lax.shift_left(rows_s[3:4].astype(jnp.int32) - 1, 16) + rows_s[7:8].astype(jnp.int32)
        id_out[lanes] = jnp.where(valid, new_id, 0)[:, :width].reshape(width)
        ok_out[lanes] = valid.astype(jnp.int32)[:, :width].reshape(width)


VMEM_SPEC = pl.BlockSpec(memory_space=pltpu.VMEM)
HBM_SPEC = pl.BlockSpec(memory_space=pltpu.HBM)
VMEM_LIMIT = 8 * 1024 * 1024
SMEM_SPEC = pl.BlockSpec(memory_space=pltpu.SMEM)


def solution(mesh):
    def local_step(atom_pos, atom_vel, atom_frc, atom_id, atom_ok, brick_side):
        f32 = jnp.float32
        n_dev = NZ * NY * NX
        gat, pkt, own = pl.pallas_call(
            exchange_kernel,
            out_shape=(jax.ShapeDtypeStruct((N_GROUPS + 1, 3, BLOCKS, LANES), f32), jax.ShapeDtypeStruct((N_PACKETS, 8, LANES), f32), jax.ShapeDtypeStruct((16, WIDE), f32)),
            in_specs=[SMEM_SPEC] + [HBM_SPEC] * 5,
            out_specs=(VMEM_SPEC,) * 3,
            scratch_shapes=[
                pltpu.VMEM((3, 3, CAP), f32),
                pltpu.VMEM((CAP,), jnp.int32),
                pltpu.VMEM((CAP,), jnp.int32),
                pltpu.VMEM((3, 4, WIDE), f32),
                pltpu.VMEM((2, WIDE), jnp.int32),
                pltpu.VMEM((3, BLOCKS, LANES), f32),
                pltpu.VMEM((2, 8, LANES), f32),
                pltpu.SemaphoreType.DMA((5,)),
                pltpu.SemaphoreType.DMA((N_GROUPS,)),
                pltpu.SemaphoreType.DMA((N_GROUPS,)),
                pltpu.SemaphoreType.DMA((N_PACKETS,)),
                pltpu.SemaphoreType.DMA((N_PACKETS,)),
            ],
            compiler_params=pltpu.CompilerParams(collective_id=0, has_side_effects=True, vmem_limit_bytes=VMEM_LIMIT),
            name="exchange",
        )(brick_side, *(pltpu.with_memory_space_constraint(value, pltpu.HBM) for value in (atom_pos.T, atom_vel.T, atom_frc.T, atom_id, atom_ok)))
        own_tiles = jax.ShapeDtypeStruct((3, GROUPS_OWN, 8, LANES), f32)
        placed, mine, others, part, eng = pl.pallas_call(
            prepare_kernel,
            out_shape=(jax.ShapeDtypeStruct((BLOCKS, 8, LANES), f32), own_tiles, jax.ShapeDtypeStruct((3, MAX_ROWS, 8, LANES), f32), own_tiles, jax.ShapeDtypeStruct((3, 8, LANES), f32)),
            in_specs=[VMEM_SPEC] * 3,
            out_specs=(VMEM_SPEC,) * 5,
            compiler_params=pltpu.CompilerParams(vmem_limit_bytes=VMEM_LIMIT),
            name="prepare",
        )(gat, pkt, own)
        frc_rows, total = pl.pallas_call(
            tile_kernel,
            out_shape=(jax.ShapeDtypeStruct((8, WIDE), f32), jax.ShapeDtypeStruct((1, LANES), f32)),
            in_specs=[VMEM_SPEC] * 4,
            out_specs=(VMEM_SPEC,) * 2,
            scratch_shapes=[pltpu.VMEM((3, FIXED_BLOCKS * 16, 8, LANES), f32), pltpu.VMEM((3, FIXED_BLOCKS, 8, LANES), f32), pltpu.VMEM((1, LANES), f32), pltpu.VMEM((n_dev, 1, LANES), f32), pltpu.SemaphoreType.DMA((n_dev - 1,)), pltpu.SemaphoreType.DMA((n_dev - 1,))],
            compiler_params=pltpu.CompilerParams(collective_id=1, has_side_effects=True, vmem_limit_bytes=VMEM_LIMIT),
            name="tile",
        )(mine, others, part, eng)
        pos, vel, frc, ids, oks, energy = pl.pallas_call(
            finish_kernel,
            out_shape=(jax.ShapeDtypeStruct((3, CAP), f32),) * 3 + (jax.ShapeDtypeStruct((CAP,), jnp.int32),) * 2 + (jax.ShapeDtypeStruct((), f32),),
            in_specs=[VMEM_SPEC] * 3,
            out_specs=(VMEM_SPEC,) * 5 + (SMEM_SPEC,),
            compiler_params=pltpu.CompilerParams(vmem_limit_bytes=VMEM_LIMIT),
            name="finish",
        )(placed, frc_rows, total)
        return pos.T, vel.T, frc.T, ids, oks, energy

    row_spec = P(MESH_AXES, None)
    id_spec = P(MESH_AXES)
    return jax.shard_map(local_step, mesh=mesh, in_specs=(row_spec, row_spec, row_spec, id_spec, id_spec, P()), out_specs=(row_spec, row_spec, row_spec, id_spec, id_spec, P()), check_vma=False)
```

```python
import jax
import jax.numpy as jnp
from jax import lax
from jax.experimental import pallas as pl
from jax.experimental.pallas import tpu as pltpu
from jax.sharding import PartitionSpec as P

DT = 0.005
HALF_DT = 0.5 * DT
RC = 2.5
UPC = -48.0 * RC ** -13 + 24.0 * RC ** -7
MESH_AXES = ("z", "y", "x")
MESH = pl.DeviceIdType.MESH
NZ, NY, NX = 2, 2, 4
CAP = 729
LANES = 128
TILE = (8, LANES)
BLOCKS = 6
WIDE = BLOCKS * LANES
MOVE_CAP = CAP // 100
FAR_OWN = 1.0e4
FAR_OTHER = -1.0e4
NOWHERE = 1.0e9
GHOST_SQ = RC * RC + 0.01
PEERS = [(dz, dy, dx) for dz in range(NZ) for dy in range(NY) for dx in range(NX)][:0:-1]
SIDES = [(1, 1), (1, 0), (0, 1), (0, 0)]
GROUPS = [(gx, *side) for side in SIDES for gx in (1, -1)] + [(0, *side) for side in SIDES[:3]]
N_GROUPS = len(GROUPS)
DISTANT = [(2, *side) for side in SIDES]
N_PACKETS = N_GROUPS + len(DISTANT)


def lane_plan():
    starts, base = [], {}
    block, lane = 0, 0
    for index, (gx, gy, gz) in enumerate(GROUPS):
        if index == 8:
            block, lane = 1, 0
        dirs = [(gx, sy, sz) for sz in ((-1, 1) if gz else (0,)) for sy in ((-1, 1) if gy else (0,))]
        starts.append((block, lane, lane + MOVE_CAP * len(dirs)))
        for dx, dy, dz in dirs:
            base[(dz + 1) * 9 + (dy + 1) * 3 + dx + 1] = block * LANES + lane
            lane += MOVE_CAP
    return starts, base


LANE_STARTS, LANE_BASE = lane_plan()
STAY = 13
NT_DIMS = (((1,), (1,)), ((), ()))
NN_DIMS = (((1,), (0,)), ((), ()))


def split3(values):
    hi = values.astype(jnp.bfloat16).astype(jnp.float32)
    rest = values - hi
    mid = rest.astype(jnp.bfloat16).astype(jnp.float32)
    return jnp.concatenate([hi, mid, rest - mid], axis=0).astype(jnp.bfloat16)


def join3(parts):
    rows = parts.shape[0] // 3
    return (parts[0:rows] + parts[rows:2 * rows]) + parts[2 * rows:3 * rows]


def dot_nt(a, b):
    return lax.dot_general(a, b, NT_DIMS, preferred_element_type=jnp.float32)


def dot_nn(a, b):
    return lax.dot_general(a, b, NN_DIMS, preferred_element_type=jnp.float32)


def down(values):
    return jnp.sum(values, axis=0, keepdims=True)


def across(values):
    return jnp.sum(values, axis=1, keepdims=True)


def stack(values):
    return jnp.concatenate(values, axis=0)


def beside(values):
    return jnp.concatenate(values, axis=1)


def iota(shape, axis):
    return lax.broadcasted_iota(jnp.int32, shape, axis)


def my_coords():
    return lax.axis_index("z"), lax.axis_index("y"), lax.axis_index("x")


def peer_id(coords, offset):
    mz, my, mx = coords
    return (lax.rem(mz + offset[0], NZ), lax.rem(my + offset[1], NY), lax.rem(mx + offset[2] + NX, NX))


def entry_signals(coords):
    barrier = pltpu.get_barrier_semaphore()
    for offset in PEERS:
        pl.semaphore_signal(barrier, inc=1, device_id=peer_id(coords, offset), device_id_type=MESH)
    return barrier


def exchange_kernel(brick_ref, pos_ref, vel_ref, frc_ref, id_ref, ok_ref, gat_ref, pkt_ref, own_ref, raw, ids_in, oks_in, pad_ref, int_ref, send_pos, send_pkt, in_sem, pos_send_sem, pos_recv_sem, pkt_send_sem, pkt_recv_sem):
    coords = my_coords()
    fetches = [pltpu.make_async_copy(src, dst, in_sem.at[index]) for index, (src, dst) in enumerate(((pos_ref, raw.at[0]), (vel_ref, raw.at[1]), (frc_ref, raw.at[2]), (id_ref, ids_in), (ok_ref, oks_in)))]
    for fetch in fetches:
        fetch.start()
    barrier = entry_signals(coords)
    tail = slice(WIDE - LANES, WIDE)
    pad_ref[:, :, tail] = jnp.zeros((3, 4, LANES), jnp.float32)
    int_ref[:, tail] = jnp.zeros((2, LANES), jnp.int32)
    for fetch in fetches:
        fetch.wait()
    brick = brick_ref[...]
    for index in range(3):
        pad_ref[index, 0:3, 0:CAP] = raw[index]
    int_ref[0:1, 0:CAP] = ids_in[...].reshape(1, CAP)
    int_ref[1:2, 0:CAP] = oks_in[...].reshape(1, CAP)
    owned = int_ref[1:2, :] > 0
    moved, half, code = [], [], jnp.zeros((1, WIDE), jnp.int32)
    for axis, (mine, size, weight) in enumerate(((coords[2], NX, 1), (coords[1], NY, 3), (coords[0], NZ, 9))):
        box = brick * float(size)
        low = mine.astype(jnp.float32) * brick
        high = (mine + 1).astype(jnp.float32) * brick
        half_v = pad_ref[1, axis:axis + 1, :] + HALF_DT * pad_ref[2, axis:axis + 1, :]
        drift = pad_ref[0, axis:axis + 1, :] + DT * half_v
        step = jnp.where(drift >= high, 2, jnp.where(drift < low, 0, 1))
        code = code + step * weight
        wrapped = jnp.where(drift < 0.0, drift + box, jnp.where(drift >= box, drift - box, drift))
        moved.append(wrapped)
        half.append(half_v)
    code = jnp.where(owned, code, -1)
    for axis in range(3):
        for block in range(BLOCKS):
            lanes = slice(block * LANES, (block + 1) * LANES)
            send_pos[axis, block:block + 1, :] = jnp.where(owned[:, lanes], moved[axis][:, lanes], NOWHERE)
    ids = int_ref[0:1, :]
    id_hi = (lax.shift_right_logical(ids, 16) + 1).astype(jnp.float32)
    id_lo = (ids & 65535).astype(jnp.float32)
    data = stack(moved + [id_hi] + half + [id_lo])
    member = (jnp.broadcast_to(code, (32, WIDE)) == iota((32, WIDE), 0)).astype(jnp.float32)
    tri = (iota((LANES, LANES), 0) < iota((LANES, LANES), 1)).astype(jnp.bfloat16)
    codes = iota((32, LANES), 0)
    running = jnp.zeros((32, LANES), jnp.float32)
    for move, first in LANE_BASE.items():
        running = jnp.where(codes == move, float(first), running)
    slots = []
    for block in range(BLOCKS):
        part = member[:, block * LANES:(block + 1) * LANES]
        before = dot_nn(part.astype(jnp.bfloat16), tri)
        slots.append(down(part * (before + running)))
        running = running + across(part)
    slot = beside(slots)
    stay = code == STAY
    mover_slot = jnp.where(owned & jnp.logical_not(stay), slot, -1.0).astype(jnp.int32)
    pick = (iota((2 * LANES, WIDE), 0) == mover_slot).astype(jnp.float32).astype(jnp.bfloat16)
    packet = join3(dot_nt(split3(data), pick))
    send_pkt[0] = packet[:, 0:LANES]
    send_pkt[1] = packet[:, LANES:2 * LANES]
    own_ref[0:8, :] = data
    own_ref[8:16, :] = stack([jnp.where(stay, slot, -1.0), jnp.full((7, WIDE), brick, jnp.float32)])
    pl.semaphore_wait(barrier, len(PEERS))
    copies = []
    for index, (gx, gy, gz) in enumerate(GROUPS + DISTANT):
        peer = peer_id(coords, (gz, gy, gx))
        if index < N_GROUPS:
            copies.append(pltpu.make_async_remote_copy(src_ref=send_pos, dst_ref=gat_ref.at[index], send_sem=pos_send_sem.at[index], recv_sem=pos_recv_sem.at[index], device_id=peer, device_id_type=MESH))
            copies[-1].start()
            source, target = send_pkt.at[LANE_STARTS[index][0]], pkt_ref.at[index]
        else:
            source, target = send_pkt.at[0, 0:4], pkt_ref.at[index, 0:4]
        copies.append(pltpu.make_async_remote_copy(src_ref=source, dst_ref=target, send_sem=pkt_send_sem.at[index], recv_sem=pkt_recv_sem.at[index], device_id=peer, device_id_type=MESH))
        copies[-1].start()
    gat_ref[N_GROUPS] = send_pos[...]
    for copy in copies:
        copy.wait()


CAND_ROWS = 8 * (N_GROUPS + 1) + 8
MAX_ROWS = BLOCKS + CAND_ROWS
GROUPS_OWN = BLOCKS * 16
QUAD = 4
FIXED_BLOCKS = 4
PER_BLOCK = 16
FIXED_QUADS = FIXED_BLOCKS * PER_BLOCK // QUAD
FIXED_ROWS = 11
ENERGY_ROWS = 8


def pair_tools(mine, others, rc2, wrap_box):
    def powers(dist_sq):
        inv_r = lax.rsqrt(dist_sq)
        inv_2 = inv_r * inv_r
        inv_4 = inv_2 * inv_2
        term = inv_4 * inv_2 - 0.5
        return inv_r, term, term * (inv_4 * inv_4)

    cut_inv_r, cut_term, cut_core = powers(rc2)
    kappa = -RC * cut_core
    for ulps in (-3, -2, -1, 1, 2, 3):
        trial = ulps * 2.0 ** -34 - RC * cut_core
        kappa = jnp.where(trial * cut_inv_r == -cut_core, trial, kappa)

    def quad_energy(dist_sqs):
        terms, tails = [], []
        for dist_sq in dist_sqs:
            inv_r = lax.rsqrt(dist_sq)
            inv_2 = inv_r * inv_r
            term = inv_2 * inv_2 * inv_2 - 0.5
            terms.append(term * term)
            tails.append(kappa * inv_r * dist_sq)
        return ((terms[0] + terms[1]) + (terms[2] + terms[3])) - 12.0 * ((tails[0] + tails[1]) + (tails[2] + tails[3]))

    cut_energy = quad_energy([rc2] * QUAD)
    own_minus_lane = iota(TILE, 0) - iota(TILE, 1)

    def load_own(first):
        return [[mine[axis, first + k] for axis in range(3)] for k in range(QUAD)]

    def gaps(own, first, row, with_self):
        other = [others[axis, row] for axis in range(3)]
        deltas, dist_sqs = [], []
        for k in range(QUAD):
            delta = [own[k][axis] - other[axis] for axis in range(3)]
            for axis, box, inv_box in wrap_box:
                delta[axis] = delta[axis] - box * jnp.floor(delta[axis] * inv_box + 0.5)
            dist_sq = delta[0] * delta[0] + delta[1] * delta[1] + delta[2] * delta[2]
            if with_self:
                dist_sq = jnp.where(own_minus_lane == row * LANES - (first + k) * 8, rc2, dist_sq)
            deltas.append(delta)
            dist_sqs.append(jnp.minimum(dist_sq, rc2))
        return deltas, dist_sqs

    def energy_row(own, first, row, total, with_self, weight=None):
        gain = quad_energy(gaps(own, first, row, with_self)[1]) - cut_energy
        return total + (gain if weight is None else gain * weight)

    def force_row(own, first, row, force, with_self, react=None):
        force, pulls = list(force), []
        deltas, dist_sqs = gaps(own, first, row, with_self)
        for k in range(QUAD):
            inv_r, term, core = powers(dist_sqs[k])
            scale = core + kappa * inv_r
            pulls.append([scale * deltas[k][axis] for axis in range(3)])
            for axis in range(3):
                force[3 * k + axis] = force[3 * k + axis] + pulls[k][axis]
        if react is not None:
            for axis in range(3):
                react[axis, row] = react[axis, row] + ((pulls[0][axis] + pulls[1][axis]) + (pulls[2][axis] + pulls[3][axis]))
        return tuple(force)

    return load_own, energy_row, force_row


def prepare_kernel(gat_ref, pkt_ref, own_ref, sorted_ref, mine, others, acc, eng_ref):
    mz, my, mx = my_coords()
    brick = own_ref[9:10, 0:LANES]
    half_l = 0.5 * brick
    sizes = (NX, NY, NZ)
    centre = [(index.astype(jnp.float32) + 0.5) * brick for index in (mx, my, mz)]
    box = [brick * float(size) for size in sizes]
    lane_1 = iota((1, LANES), 1)
    acc[:, pl.ds(0, FIXED_QUADS * QUAD)] = jnp.zeros((3, FIXED_QUADS * QUAD, 8, LANES), jnp.float32)

    arrived = []
    for block in range(2):
        total = jnp.zeros(TILE, jnp.float32)
        for index in range(N_GROUPS):
            where_block, first, last = LANE_STARTS[index]
            if where_block == block:
                total = total + jnp.where((lane_1 >= first) & (lane_1 < last), pkt_ref[index], 0.0)
        arrived.append(total)
    arr = beside(arrived)
    arr_ok = arr[3:4] > 0.5
    stay_all = own_ref[8:9, :] >= 0.0
    n_vec = across(stay_all.astype(jnp.float32)) + across(arr_ok.astype(jnp.float32))
    n_own = jnp.max(n_vec).astype(jnp.int32)
    n_int = n_vec.astype(jnp.int32)
    quads = lax.div(n_own + (8 * QUAD - 1), 8 * QUAD)
    own_rows = lax.div(n_own + (LANES - 1), LANES)
    beyond = gat_ref[0, 0, 4:6, :]
    for slot in range(1, N_GROUPS + 1):
        beyond = jnp.minimum(beyond, gat_ref[slot, 0, 4:6, :])
    small = (jnp.min(beyond) > 0.5 * NOWHERE) & (n_own <= FIXED_BLOCKS * LANES)
    eng_ref[1] = jnp.broadcast_to(n_vec, TILE)
    wide = jnp.max(brick) >= 2.0 * RC
    int_max = 2147483647
    rc2 = RC * RC + 0.0 * own_ref[8:16, 0:LANES]
    zero = jnp.zeros(TILE, jnp.float32)
    far = jnp.full(TILE, FAR_OTHER, jnp.float32)

    def build(blocks, tile_rows):
        span = blocks * LANES
        data = beside([own_ref[0:8, 0:span], arr])
        ids = lax.shift_left(data[3:4].astype(jnp.int32) - 1, 16) + data[7:8].astype(jnp.int32)
        stay_rank = own_ref[8:9, 0:span]
        stay = stay_rank >= 0.0
        arr_id = jnp.where(arr_ok, ids[:, span:], int_max)
        own_id = jnp.where(stay, ids[:, :span], int_max)

        count_rows = (N_GROUPS + 1) * tile_rows
        cand = -(-(count_rows + len(DISTANT)) // 8) * 8
        rel = []
        for axis in range(3):
            near = [gat_ref[slot, axis, 0:tile_rows, :] for slot in range(N_GROUPS + 1)]
            distant = [jnp.where(pkt_ref[N_GROUPS + k, 3:4, :] > 0.5, pkt_ref[N_GROUPS + k, axis:axis + 1, :], NOWHERE) for k in range(len(DISTANT))]
            values = stack(near + distant + [jnp.full((cand - count_rows - len(DISTANT), LANES), NOWHERE, jnp.float32)]) - centre[axis]
            rel.append(jnp.where(values > 0.5 * box[axis], values - box[axis], jnp.where(values < -0.5 * box[axis], values + box[axis], values)))
        over = [jnp.maximum(jnp.abs(values) - half_l, 0.0) for values in rel]
        gap_sq = over[0] * over[0] + over[1] * over[1] + over[2] * over[2]
        side = jnp.zeros((cand, LANES), jnp.float32)
        for axis in range(3):
            side = 3.0 * side + jnp.where(over[2 - axis] > 0.0, jnp.where(rel[2 - axis] > 0.0, 1.0, -1.0), 0.0)
        near = gap_sq < GHOST_SQ
        mixed = jnp.where(near & (side > 0.0), 256.0, jnp.where(near & (side < 0.0), 1.0, 0.0)).astype(jnp.bfloat16)
        row_l, col_l = iota((LANES, LANES), 0), iota((LANES, LANES), 1)

        def counts(chosen):
            return dot_nn(mixed, chosen.astype(jnp.bfloat16)).astype(jnp.int32)

        cum = counts(row_l <= col_l)
        total = counts(row_l >= 0)
        marks = [counts(row_l < 16 * k) for k in range(1, 8)]
        arr_col = jnp.broadcast_to(arr_id, (8, 2 * LANES)).T[:, 0:1]
        arr_first = (arr_col < beside([own_id, arr_id])).astype(jnp.float32)
        arr_before = down(arr_first)
        stay_after = dot_nt(jnp.broadcast_to(stay.astype(jnp.float32), (8, span)).astype(jnp.bfloat16), arr_first[:, :span].astype(jnp.bfloat16))[0:1]
        stay_before = across(stay.astype(jnp.float32)) - stay_after
        rank = beside([jnp.where(stay, stay_rank + arr_before[:, :span], -1.0), jnp.where(arr_ok, stay_before + arr_before[:, span:], -1.0)]).astype(jnp.int32)
        earlier = (iota((cand, cand), 1) < iota((cand, cand), 0)).astype(jnp.bfloat16)
        uppers, lowers = lax.shift_right_logical(total, 8), total & 255

        def starts(each, first):
            base = dot_nn(earlier, each.astype(jnp.float32).astype(jnp.bfloat16)).astype(jnp.int32) + first
            return base, base[cand - 1:] + each[cand - 1:]

        upper_base, upper_end = starts(uppers, n_int)
        lower_base, all_end = starts(lowers, upper_end)
        n_upper, n_all = jnp.max(upper_end), jnp.max(all_end)
        eng_ref[2] = jnp.broadcast_to(upper_end.astype(jnp.float32), TILE)
        fits = n_upper <= ENERGY_ROWS * LANES
        parts = split3(data)

        def place_block(block):
            pick = (iota((LANES, span + 2 * LANES), 0) + block * LANES == rank).astype(jnp.float32).astype(jnp.bfloat16)
            rows_s = join3((dot_nt(pick, parts)).T)
            sorted_ref[block] = rows_s
            valid = lane_1 + block * LANES < n_int
            own_rel = stack([rows_s[axis:axis + 1] - centre[axis] for axis in range(3)] + [rows_s[3:8]])
            columns = jnp.where(valid, own_rel, FAR_OWN).T
            for axis in range(3):
                others[axis, block] = jnp.broadcast_to(jnp.where(valid, own_rel[axis:axis + 1], 0.0), TILE)
                mine[axis, pl.ds(block * PER_BLOCK, PER_BLOCK)] = jnp.broadcast_to(columns[:, axis:axis + 1], (LANES, LANES)).reshape(16, 8, LANES)

        lane_c = iota((cand, LANES), 1)
        is_upper = lane_c < uppers
        keep = jnp.where(is_upper, -1, 255)
        bound = jnp.where(is_upper, lane_c * 256 + 255, lane_c - uppers)

        def passed(probes):
            return sum(((probe & keep) <= bound).astype(jnp.int32) for probe in probes)

        def probe_at(source, stride, number):
            return [jnp.take_along_axis(cum, source + (stride * k - 1), axis=1) for k in range(1, number + 1)]

        source = 16 * passed(marks)
        place_block(0)
        place_block(1)
        source = source + 2 * passed(probe_at(source, 2, 7))
        for block in range(2, blocks):
            place_block(block)
        source = source + passed(probe_at(source, 1, 1))
        for block in range(blocks, BLOCKS):
            sorted_ref[block] = zero

        def turned(base, each, first):
            place = (lane_c - base) & (LANES - 1)
            lane = jnp.take_along_axis(source, (first + place) & (LANES - 1), axis=1)
            target = jnp.where(place < each, lax.shift_right_logical(base + place, 7), -1)
            return target, [jnp.take_along_axis(values, lane, axis=1) for values in rel]

        def pack(target, packed, start, stop, held_rows, empty):
            def pack_row(row, carry):
                hit = target == row
                filled = lane_1 + row * LANES < n_all
                for axis in range(3):
                    held = jnp.where(row < held_rows, others[axis, row], 0.0)
                    values = held + down(jnp.where(hit, packed[axis], 0.0))
                    others[axis, row] = jnp.where(filled, values, empty)
                return carry

            lax.fori_loop(lax.div(start, LANES), lax.div(stop + (LANES - 1), LANES), pack_row, 0)

        upper_rows = lax.div(n_upper + (LANES - 1), LANES)
        rows = lax.div(n_all + (LANES - 1), LANES)
        upper_set, lower_set = turned(upper_base, uppers, 0), turned(lower_base, lowers, uppers)
        pack(*upper_set, n_own, n_upper, own_rows, 0.0)
        pack(*lower_set, n_upper, n_all, upper_rows, FAR_OTHER)

        def set_far(row, carry):
            for axis in range(3):
                others[axis, row] = far
            return carry

        def excess(first_quad, last_quad, first_row, wrap_box, energy):
            slot_8 = iota(TILE, 1)
            load_own, energy_row, force_row = pair_tools(mine, others, rc2, wrap_box)

            def quad(index, total):
                first = index * QUAD
                own = load_own(first)
                sums = (zero,) * (3 * QUAD) + (total,)

                def both(row, part):
                    slot = slot_8 + row * LANES
                    weight = 1.0 if wrap_box else jnp.where(slot < n_int, 1.0, jnp.where(slot < upper_end, 2.0, 0.0))
                    return force_row(own, first, row, part[:-1], True) + (energy_row(own, first, row, part[-1], True, weight),)

                sums = lax.fori_loop(first_row, rows, both, sums)
                for k in range(QUAD):
                    for axis in range(3):
                        acc[axis, first + k] = sums[3 * k + axis]
                return sums[-1]

            return lax.fori_loop(first_quad, last_quad, quad, energy)

        def plain():
            short = jnp.where(rows > FIXED_ROWS, jnp.minimum(quads, FIXED_QUADS), 0)
            energy = excess(0, short, FIXED_ROWS, [], zero)
            if blocks > FIXED_BLOCKS:
                energy = excess(FIXED_QUADS, quads, 0, [], energy)
            eng_ref[0] = energy
            lax.fori_loop(rows, FIXED_ROWS, set_far, 0)

        def alone(wrap_box):
            eng_ref[0] = excess(0, quads, 0, wrap_box, zero)
            lax.fori_loop(0, FIXED_ROWS, set_far, 0)

        pl.when(wide & fits)(plain)
        pl.when(wide & jnp.logical_not(fits))(lambda: alone([]))
        pl.when(jnp.logical_not(wide))(lambda: alone([(axis, box[axis], 1.0 / box[axis]) for axis in (1, 2)]))

    pl.when(small)(lambda: build(FIXED_BLOCKS, 4))
    pl.when(jnp.logical_not(small))(lambda: build(BLOCKS, BLOCKS))


def tile_kernel(mine, others, part, eng_ref, frc_ref, out_ref, acc, react, eng, slots, send_sem, recv_sem):
    coords = my_coords()
    mz, my, mx = coords
    barrier = entry_signals(coords)
    rc2 = RC * RC + 0.0 * mine[0, 0]
    load_own, energy_row, force_row = pair_tools(mine, others, rc2, [])

    lane_8 = iota(TILE, 1).astype(jnp.float32)
    energy = eng_ref[0]

    def weight_of(row, own_weight):
        slot = lane_8 + float(row * LANES)
        return jnp.where(slot < eng_ref[1], own_weight, jnp.where(slot < eng_ref[2], 2.0, 0.0))

    for block in range(FIXED_BLOCKS):

        def energy_quad(index, total, block=block):
            first = block * PER_BLOCK + index * QUAD
            own = load_own(first)
            for row in range(block, ENERGY_ROWS):
                weight = weight_of(row, 2.0 if block < row < FIXED_BLOCKS else 1.0)
                total = energy_row(own, first, row, total, row == block, weight)
            return total

        energy = lax.fori_loop(0, PER_BLOCK // QUAD, energy_quad, energy)
    eng[...] = 2.0 * down(energy)
    pl.semaphore_wait(barrier, len(PEERS))
    place = (mz * NY + my) * NX + mx
    copies = []
    for index, offset in enumerate(PEERS):
        copies.append(pltpu.make_async_remote_copy(src_ref=eng, dst_ref=slots.at[place], send_sem=send_sem.at[index], recv_sem=recv_sem.at[index], device_id=peer_id(coords, offset), device_id_type=MESH))
        copies[-1].start()
    slots[place] = eng[...]
    react[...] = jnp.zeros_like(react)
    for block in range(FIXED_BLOCKS):

        def force_quad(index, carry, block=block):
            first = block * PER_BLOCK + index * QUAD
            own = load_own(first)
            force = force_row(own, first, block, [part[axis, first + k] for k in range(QUAD) for axis in range(3)], True)
            for row in range(block + 1, FIXED_ROWS):
                force = force_row(own, first, row, force, False, react if row < FIXED_BLOCKS else None)
            for k in range(QUAD):
                for axis in range(3):
                    acc[axis, first + k] = force[3 * k + axis]
            return carry

        lax.fori_loop(0, PER_BLOCK // QUAD, force_quad, 0)
    for block in range(BLOCKS):
        held = acc if block < FIXED_BLOCKS else part
        for axis in range(3):
            turned = (held[axis, pl.ds(block * PER_BLOCK, PER_BLOCK)].reshape(LANES, LANES)).T
            force = down(turned)
            if 0 < block < FIXED_BLOCKS:
                force = force - down(react[axis, block])
            frc_ref[axis:axis + 1, block * LANES:(block + 1) * LANES] = 48.0 * force
    for copy in copies:
        copy.wait()
    total = slots[0]
    for index in range(1, NZ * NY * NX):
        total = total + slots[index]
    out_ref[...] = total


def finish_kernel(sorted_ref, frc_ref, total_ref, pos_out, vel_out, frc_out, id_out, ok_out, eng_out):
    eng_out[...] = jnp.sum(total_ref[...])
    for block in range(BLOCKS):
        width = min(LANES, CAP - block * LANES)
        lanes = slice(block * LANES, block * LANES + width)
        rows_s = sorted_ref[block]
        valid = rows_s[3:4] > 0.5
        for axis in range(3):
            force = jnp.where(valid, frc_ref[axis:axis + 1, block * LANES:(block + 1) * LANES], 0.0)
            frc_out[axis:axis + 1, lanes] = force[:, :width]
            vel_out[axis:axis + 1, lanes] = (rows_s[4 + axis:5 + axis] + HALF_DT * force)[:, :width]
            pos_out[axis:axis + 1, lanes] = rows_s[axis:axis + 1, :width]
        new_id = lax.shift_left(rows_s[3:4].astype(jnp.int32) - 1, 16) + rows_s[7:8].astype(jnp.int32)
        id_out[lanes] = jnp.where(valid, new_id, 0)[:, :width].reshape(width)
        ok_out[lanes] = valid.astype(jnp.int32)[:, :width].reshape(width)


VMEM_SPEC = pl.BlockSpec(memory_space=pltpu.VMEM)
HBM_SPEC = pl.BlockSpec(memory_space=pltpu.HBM)
VMEM_LIMIT = 8 * 1024 * 1024
SMEM_SPEC = pl.BlockSpec(memory_space=pltpu.SMEM)


def solution(mesh):
    def local_step(atom_pos, atom_vel, atom_frc, atom_id, atom_ok, brick_side):
        f32 = jnp.float32
        n_dev = NZ * NY * NX
        gat, pkt, own = pl.pallas_call(
            exchange_kernel,
            out_shape=(jax.ShapeDtypeStruct((N_GROUPS + 1, 3, BLOCKS, LANES), f32), jax.ShapeDtypeStruct((N_PACKETS, 8, LANES), f32), jax.ShapeDtypeStruct((16, WIDE), f32)),
            in_specs=[SMEM_SPEC] + [HBM_SPEC] * 5,
            out_specs=(VMEM_SPEC,) * 3,
            scratch_shapes=[
                pltpu.VMEM((3, 3, CAP), f32),
                pltpu.VMEM((CAP,), jnp.int32),
                pltpu.VMEM((CAP,), jnp.int32),
                pltpu.VMEM((3, 4, WIDE), f32),
                pltpu.VMEM((2, WIDE), jnp.int32),
                pltpu.VMEM((3, BLOCKS, LANES), f32),
                pltpu.VMEM((2, 8, LANES), f32),
                pltpu.SemaphoreType.DMA((5,)),
                pltpu.SemaphoreType.DMA((N_GROUPS,)),
                pltpu.SemaphoreType.DMA((N_GROUPS,)),
                pltpu.SemaphoreType.DMA((N_PACKETS,)),
                pltpu.SemaphoreType.DMA((N_PACKETS,)),
            ],
            compiler_params=pltpu.CompilerParams(collective_id=0, has_side_effects=True, vmem_limit_bytes=VMEM_LIMIT),
            name="exchange",
        )(brick_side, *(pltpu.with_memory_space_constraint(value, pltpu.HBM) for value in (atom_pos.T, atom_vel.T, atom_frc.T, atom_id, atom_ok)))
        own_tiles = jax.ShapeDtypeStruct((3, GROUPS_OWN, 8, LANES), f32)
        placed, mine, others, part, eng = pl.pallas_call(
            prepare_kernel,
            out_shape=(jax.ShapeDtypeStruct((BLOCKS, 8, LANES), f32), own_tiles, jax.ShapeDtypeStruct((3, MAX_ROWS, 8, LANES), f32), own_tiles, jax.ShapeDtypeStruct((3, 8, LANES), f32)),
            in_specs=[VMEM_SPEC] * 3,
            out_specs=(VMEM_SPEC,) * 5,
            compiler_params=pltpu.CompilerParams(vmem_limit_bytes=VMEM_LIMIT),
            name="prepare",
        )(gat, pkt, own)
        frc_rows, total = pl.pallas_call(
            tile_kernel,
            out_shape=(jax.ShapeDtypeStruct((8, WIDE), f32), jax.ShapeDtypeStruct((1, LANES), f32)),
            in_specs=[VMEM_SPEC] * 4,
            out_specs=(VMEM_SPEC,) * 2,
            scratch_shapes=[pltpu.VMEM((3, FIXED_BLOCKS * 16, 8, LANES), f32), pltpu.VMEM((3, FIXED_BLOCKS, 8, LANES), f32), pltpu.VMEM((1, LANES), f32), pltpu.VMEM((n_dev, 1, LANES), f32), pltpu.SemaphoreType.DMA((n_dev - 1,)), pltpu.SemaphoreType.DMA((n_dev - 1,))],
            compiler_params=pltpu.CompilerParams(collective_id=1, has_side_effects=True, vmem_limit_bytes=VMEM_LIMIT),
            name="tile",
        )(mine, others, part, eng)
        pos, vel, frc, ids, oks, energy = pl.pallas_call(
            finish_kernel,
            out_shape=(jax.ShapeDtypeStruct((3, CAP), f32),) * 3 + (jax.ShapeDtypeStruct((CAP,), jnp.int32),) * 2 + (jax.ShapeDtypeStruct((), f32),),
            in_specs=[VMEM_SPEC] * 3,
            out_specs=(VMEM_SPEC,) * 5 + (SMEM_SPEC,),
            compiler_params=pltpu.CompilerParams(vmem_limit_bytes=VMEM_LIMIT),
            name="finish",
        )(placed, frc_rows, total)
        return pos.T, vel.T, frc.T, ids, oks, energy

    row_spec = P(MESH_AXES, None)
    id_spec = P(MESH_AXES)
    return jax.shard_map(local_step, mesh=mesh, in_specs=(row_spec, row_spec, row_spec, id_spec, id_spec, P()), out_specs=(row_spec, row_spec, row_spec, id_spec, id_spec, P()), check_vma=False)
```

```python
import jax
import jax.numpy as jnp
from jax import lax
from jax.experimental import pallas as pl
from jax.experimental.pallas import tpu as pltpu
from jax.sharding import PartitionSpec as P

DT = 0.005
HALF_DT = 0.5 * DT
RC = 2.5
UPC = -48.0 * RC ** -13 + 24.0 * RC ** -7
MESH_AXES = ("z", "y", "x")
MESH = pl.DeviceIdType.MESH
NZ, NY, NX = 2, 2, 4
CAP = 729
LANES = 128
TILE = (8, LANES)
BLOCKS = 6
WIDE = BLOCKS * LANES
MOVE_CAP = CAP // 100
FAR_OWN = 1.0e4
FAR_OTHER = -1.0e4
NOWHERE = 1.0e9
GHOST_SQ = RC * RC + 0.01
PEERS = [(dz, dy, dx) for dz in range(NZ) for dy in range(NY) for dx in range(NX)][:0:-1]
SIDES = [(1, 1), (1, 0), (0, 1), (0, 0)]
GROUPS = [(gx, *side) for side in SIDES for gx in (1, -1)] + [(0, *side) for side in SIDES[:3]]
N_GROUPS = len(GROUPS)
DISTANT = [(2, *side) for side in SIDES]
N_PACKETS = N_GROUPS + len(DISTANT)


def lane_plan():
    starts, base = [], {}
    block, lane = 0, 0
    for index, (gx, gy, gz) in enumerate(GROUPS):
        if index == 8:
            block, lane = 1, 0
        dirs = [(gx, sy, sz) for sz in ((-1, 1) if gz else (0,)) for sy in ((-1, 1) if gy else (0,))]
        starts.append((block, lane, lane + MOVE_CAP * len(dirs)))
        for dx, dy, dz in dirs:
            base[(dz + 1) * 9 + (dy + 1) * 3 + dx + 1] = block * LANES + lane
            lane += MOVE_CAP
    return starts, base


LANE_STARTS, LANE_BASE = lane_plan()
STAY = 13
NT_DIMS = (((1,), (1,)), ((), ()))
NN_DIMS = (((1,), (0,)), ((), ()))


def split3(values):
    hi = values.astype(jnp.bfloat16).astype(jnp.float32)
    rest = values - hi
    mid = rest.astype(jnp.bfloat16).astype(jnp.float32)
    return jnp.concatenate([hi, mid, rest - mid], axis=0)


def join3(parts):
    rows = parts.shape[0] // 3
    return (parts[0:rows] + parts[rows:2 * rows]) + parts[2 * rows:3 * rows]


def dot_nt(a, b):
    return lax.dot_general(a, b, NT_DIMS, preferred_element_type=jnp.float32)


def dot_nn(a, b):
    return lax.dot_general(a, b, NN_DIMS, preferred_element_type=jnp.float32)


def down(values):
    return jnp.sum(values, axis=0, keepdims=True)


def across(values):
    return jnp.sum(values, axis=1, keepdims=True)


def stack(values):
    return jnp.concatenate(values, axis=0)


def beside(values):
    return jnp.concatenate(values, axis=1)


def iota(shape, axis):
    return lax.broadcasted_iota(jnp.int32, shape, axis)


def my_coords():
    return lax.axis_index("z"), lax.axis_index("y"), lax.axis_index("x")


def peer_id(coords, offset):
    mz, my, mx = coords
    return (lax.rem(mz + offset[0], NZ), lax.rem(my + offset[1], NY), lax.rem(mx + offset[2] + NX, NX))


def entry_signals(coords):
    barrier = pltpu.get_barrier_semaphore()
    for offset in PEERS:
        pl.semaphore_signal(barrier, inc=1, device_id=peer_id(coords, offset), device_id_type=MESH)
    return barrier


def exchange_kernel(brick_ref, pos_ref, vel_ref, frc_ref, id_ref, ok_ref, gat_ref, pkt_ref, own_ref, raw, ids_in, oks_in, pad_ref, int_ref, send_pos, send_pkt, in_sem, pos_send_sem, pos_recv_sem, pkt_send_sem, pkt_recv_sem):
    coords = my_coords()
    fetches = [pltpu.make_async_copy(src, dst, in_sem.at[index]) for index, (src, dst) in enumerate(((pos_ref, raw.at[0]), (vel_ref, raw.at[1]), (frc_ref, raw.at[2]), (id_ref, ids_in), (ok_ref, oks_in)))]
    for fetch in fetches:
        fetch.start()
    barrier = entry_signals(coords)
    tail = slice(WIDE - LANES, WIDE)
    pad_ref[:, :, tail] = jnp.zeros((3, 4, LANES), jnp.float32)
    int_ref[:, tail] = jnp.zeros((2, LANES), jnp.int32)
    for fetch in fetches:
        fetch.wait()
    brick = brick_ref[...]
    for index in range(3):
        pad_ref[index, 0:3, 0:CAP] = raw[index]
    int_ref[0:1, 0:CAP] = ids_in[...].reshape(1, CAP)
    int_ref[1:2, 0:CAP] = oks_in[...].reshape(1, CAP)
    owned = int_ref[1:2, :] > 0
    moved, half, code = [], [], jnp.zeros((1, WIDE), jnp.int32)
    for axis, (mine, size, weight) in enumerate(((coords[2], NX, 1), (coords[1], NY, 3), (coords[0], NZ, 9))):
        box = brick * float(size)
        low = mine.astype(jnp.float32) * brick
        high = (mine + 1).astype(jnp.float32) * brick
        half_v = pad_ref[1, axis:axis + 1, :] + HALF_DT * pad_ref[2, axis:axis + 1, :]
        drift = pad_ref[0, axis:axis + 1, :] + DT * half_v
        step = jnp.where(drift >= high, 2, jnp.where(drift < low, 0, 1))
        code = code + step * weight
        wrapped = jnp.where(drift < 0.0, drift + box, jnp.where(drift >= box, drift - box, drift))
        moved.append(wrapped)
        half.append(half_v)
    code = jnp.where(owned, code, -1)
    for axis in range(3):
        for block in range(BLOCKS):
            lanes = slice(block * LANES, (block + 1) * LANES)
            send_pos[axis, block:block + 1, :] = jnp.where(owned[:, lanes], moved[axis][:, lanes], NOWHERE)
    ids = int_ref[0:1, :]
    id_hi = (lax.shift_right_logical(ids, 16) + 1).astype(jnp.float32)
    id_lo = (ids & 65535).astype(jnp.float32)
    data = stack(moved + [id_hi] + half + [id_lo])
    member = (jnp.broadcast_to(code, (32, WIDE)) == iota((32, WIDE), 0)).astype(jnp.float32)
    tri = (iota((LANES, LANES), 0) < iota((LANES, LANES), 1)).astype(jnp.bfloat16)
    codes = iota((32, LANES), 0)
    running = jnp.zeros((32, LANES), jnp.float32)
    for move, first in LANE_BASE.items():
        running = jnp.where(codes == move, float(first), running)
    slots = []
    for block in range(BLOCKS):
        part = member[:, block * LANES:(block + 1) * LANES]
        before = dot_nn(part.astype(jnp.bfloat16), tri)
        slots.append(down(part * (before + running)))
        running = running + across(part)
    slot = beside(slots)
    stay = code == STAY
    mover_slot = jnp.where(owned & jnp.logical_not(stay), slot, -1.0).astype(jnp.int32)
    pick = (iota((2 * LANES, WIDE), 0) == mover_slot).astype(jnp.float32).astype(jnp.bfloat16)
    packet = join3(dot_nt(split3(data).astype(jnp.bfloat16), pick))
    send_pkt[0] = packet[:, 0:LANES]
    send_pkt[1] = packet[:, LANES:2 * LANES]
    own_ref[0:8, :] = data
    own_ref[8:16, :] = stack([jnp.where(stay, slot, -1.0), jnp.full((7, WIDE), brick, jnp.float32)])
    pl.semaphore_wait(barrier, len(PEERS))
    copies = []
    for index, (gx, gy, gz) in enumerate(GROUPS + DISTANT):
        peer = peer_id(coords, (gz, gy, gx))
        if index < N_GROUPS:
            copies.append(pltpu.make_async_remote_copy(src_ref=send_pos, dst_ref=gat_ref.at[index], send_sem=pos_send_sem.at[index], recv_sem=pos_recv_sem.at[index], device_id=peer, device_id_type=MESH))
            copies[-1].start()
            source, target = send_pkt.at[LANE_STARTS[index][0]], pkt_ref.at[index]
        else:
            source, target = send_pkt.at[0, 0:4], pkt_ref.at[index, 0:4]
        copies.append(pltpu.make_async_remote_copy(src_ref=source, dst_ref=target, send_sem=pkt_send_sem.at[index], recv_sem=pkt_recv_sem.at[index], device_id=peer, device_id_type=MESH))
        copies[-1].start()
    gat_ref[N_GROUPS] = send_pos[...]
    for copy in copies:
        copy.wait()


CAND_ROWS = 8 * (N_GROUPS + 1) + 8
MAX_ROWS = BLOCKS + CAND_ROWS
GROUPS_OWN = BLOCKS * 16
QUAD = 4
FIXED_BLOCKS = 4
PER_BLOCK = 16
FIXED_QUADS = FIXED_BLOCKS * PER_BLOCK // QUAD
FIXED_ROWS = 11
ENERGY_ROWS = 8


def pair_tools(mine, others, rc2, wrap_box):
    def powers(dist_sq):
        inv_r = lax.rsqrt(dist_sq)
        inv_2 = inv_r * inv_r
        inv_4 = inv_2 * inv_2
        term = inv_4 * inv_2 - 0.5
        return inv_r, term, term * (inv_4 * inv_4)

    cut_inv_r, cut_term, cut_core = powers(rc2)
    kappa = -RC * cut_core
    for ulps in (-3, -2, -1, 1, 2, 3):
        trial = ulps * 2.0 ** -34 - RC * cut_core
        kappa = jnp.where(trial * cut_inv_r == -cut_core, trial, kappa)

    def quad_energy(dist_sqs):
        terms, tails = [], []
        for dist_sq in dist_sqs:
            inv_r = lax.rsqrt(dist_sq)
            inv_2 = inv_r * inv_r
            term = inv_2 * inv_2 * inv_2 - 0.5
            terms.append(term * term)
            tails.append(kappa * inv_r * dist_sq)
        return ((terms[0] + terms[1]) + (terms[2] + terms[3])) - 12.0 * ((tails[0] + tails[1]) + (tails[2] + tails[3]))

    cut_energy = quad_energy([rc2] * QUAD)
    own_minus_lane = iota(TILE, 0) - iota(TILE, 1)

    def load_own(first):
        return [[mine[axis, first + k] for axis in range(3)] for k in range(QUAD)]

    def gaps(own, first, row, with_self):
        other = [others[axis, row] for axis in range(3)]
        deltas, dist_sqs = [], []
        for k in range(QUAD):
            delta = [own[k][axis] - other[axis] for axis in range(3)]
            for axis, box, inv_box in wrap_box:
                delta[axis] = delta[axis] - box * jnp.floor(delta[axis] * inv_box + 0.5)
            dist_sq = delta[0] * delta[0] + delta[1] * delta[1] + delta[2] * delta[2]
            if with_self:
                dist_sq = jnp.where(own_minus_lane == row * LANES - (first + k) * 8, rc2, dist_sq)
            deltas.append(delta)
            dist_sqs.append(jnp.minimum(dist_sq, rc2))
        return deltas, dist_sqs

    def energy_row(own, first, row, total, with_self, weight=None):
        gain = quad_energy(gaps(own, first, row, with_self)[1]) - cut_energy
        return total + (gain if weight is None else gain * weight)

    def force_row(own, first, row, force, with_self, react=None):
        force, pulls = list(force), []
        deltas, dist_sqs = gaps(own, first, row, with_self)
        for k in range(QUAD):
            inv_r, term, core = powers(dist_sqs[k])
            scale = core + kappa * inv_r
            pulls.append([scale * deltas[k][axis] for axis in range(3)])
            for axis in range(3):
                force[3 * k + axis] = force[3 * k + axis] + pulls[k][axis]
        if react is not None:
            for axis in range(3):
                react[axis, row] = react[axis, row] + ((pulls[0][axis] + pulls[1][axis]) + (pulls[2][axis] + pulls[3][axis]))
        return tuple(force)

    return load_own, energy_row, force_row


def prepare_kernel(gat_ref, pkt_ref, own_ref, sorted_ref, mine, others, acc, eng_ref):
    mz, my, mx = my_coords()
    brick = own_ref[9:10, 0:LANES]
    half_l = 0.5 * brick
    sizes = (NX, NY, NZ)
    centre = [(index.astype(jnp.float32) + 0.5) * brick for index in (mx, my, mz)]
    box = [brick * float(size) for size in sizes]
    lane_1 = iota((1, LANES), 1)
    acc[:, pl.ds(0, FIXED_QUADS * QUAD)] = jnp.zeros((3, FIXED_QUADS * QUAD, 8, LANES), jnp.float32)

    arrived = []
    for block in range(2):
        total = jnp.zeros(TILE, jnp.float32)
        for index in range(N_GROUPS):
            where_block, first, last = LANE_STARTS[index]
            if where_block == block:
                total = total + jnp.where((lane_1 >= first) & (lane_1 < last), pkt_ref[index], 0.0)
        arrived.append(total)
    arr = beside(arrived)
    arr_ok = arr[3:4] > 0.5
    stay_all = own_ref[8:9, :] >= 0.0
    n_vec = across(stay_all.astype(jnp.float32)) + across(arr_ok.astype(jnp.float32))
    n_own = jnp.max(n_vec).astype(jnp.int32)
    n_int = n_vec.astype(jnp.int32)
    quads = lax.div(n_own + (8 * QUAD - 1), 8 * QUAD)
    own_rows = lax.div(n_own + (LANES - 1), LANES)
    beyond = gat_ref[0, 0, 4:6, :]
    for slot in range(1, N_GROUPS + 1):
        beyond = jnp.minimum(beyond, gat_ref[slot, 0, 4:6, :])
    small = (jnp.min(beyond) > 0.5 * NOWHERE) & (n_own <= FIXED_BLOCKS * LANES)
    eng_ref[1] = jnp.broadcast_to(n_vec, TILE)
    wide = jnp.max(brick) >= 2.0 * RC
    int_max = 2147483647
    rc2 = RC * RC + 0.0 * own_ref[8:16, 0:LANES]
    zero = jnp.zeros(TILE, jnp.float32)
    far = jnp.full(TILE, FAR_OTHER, jnp.float32)

    def build(blocks, tile_rows):
        span = blocks * LANES
        data = beside([own_ref[0:8, 0:span], arr])
        ids = lax.shift_left(data[3:4].astype(jnp.int32) - 1, 16) + data[7:8].astype(jnp.int32)
        stay_rank = own_ref[8:9, 0:span]
        stay = stay_rank >= 0.0
        arr_id = jnp.where(arr_ok, ids[:, span:], int_max)
        own_id = jnp.where(stay, ids[:, :span], int_max)

        count_rows = (N_GROUPS + 1) * tile_rows
        cand = -(-(count_rows + len(DISTANT)) // 8) * 8
        rel = []
        for axis in range(3):
            near = [gat_ref[slot, axis, 0:tile_rows, :] for slot in range(N_GROUPS + 1)]
            distant = [jnp.where(pkt_ref[N_GROUPS + k, 3:4, :] > 0.5, pkt_ref[N_GROUPS + k, axis:axis + 1, :], NOWHERE) for k in range(len(DISTANT))]
            values = stack(near + distant + [jnp.full((cand - count_rows - len(DISTANT), LANES), NOWHERE, jnp.float32)]) - centre[axis]
            rel.append(jnp.where(values > 0.5 * box[axis], values - box[axis], jnp.where(values < -0.5 * box[axis], values + box[axis], values)))
        over = [jnp.maximum(jnp.abs(values) - half_l, 0.0) for values in rel]
        gap_sq = over[0] * over[0] + over[1] * over[1] + over[2] * over[2]
        side = jnp.zeros((cand, LANES), jnp.float32)
        for axis in range(3):
            side = 3.0 * side + jnp.where(over[2 - axis] > 0.0, jnp.where(rel[2 - axis] > 0.0, 1.0, -1.0), 0.0)
        near = gap_sq < GHOST_SQ
        mixed = jnp.where(near & (side > 0.0), 256.0, jnp.where(near & (side < 0.0), 1.0, 0.0)).astype(jnp.bfloat16)
        row_l, col_l = iota((LANES, LANES), 0), iota((LANES, LANES), 1)

        def counts(chosen):
            return dot_nn(mixed, chosen.astype(jnp.bfloat16)).astype(jnp.int32)

        cum = counts(row_l <= col_l)
        total = counts(row_l >= 0)
        marks = [counts(row_l < 16 * k) for k in range(1, 8)]
        arr_col = jnp.broadcast_to(arr_id, (8, 2 * LANES)).T[:, 0:1]
        arr_first = (arr_col < beside([own_id, arr_id])).astype(jnp.float32)
        arr_before = down(arr_first)
        stay_after = dot_nt(jnp.broadcast_to(stay.astype(jnp.float32), (8, span)).astype(jnp.bfloat16), arr_first[:, :span].astype(jnp.bfloat16))[0:1]
        stay_before = across(stay.astype(jnp.float32)) - stay_after
        rank = beside([jnp.where(stay, stay_rank + arr_before[:, :span], -1.0), jnp.where(arr_ok, stay_before + arr_before[:, span:], -1.0)]).astype(jnp.int32)
        earlier = (iota((cand, cand), 1) < iota((cand, cand), 0)).astype(jnp.bfloat16)
        uppers, lowers = lax.shift_right_logical(total, 8), total & 255

        def starts(each, first):
            base = dot_nn(earlier, each.astype(jnp.float32).astype(jnp.bfloat16)).astype(jnp.int32) + first
            return base, base[cand - 1:] + each[cand - 1:]

        upper_base, upper_end = starts(uppers, n_int)
        lower_base, all_end = starts(lowers, upper_end)
        n_upper, n_all = jnp.max(upper_end), jnp.max(all_end)
        eng_ref[2] = jnp.broadcast_to(upper_end.astype(jnp.float32), TILE)
        fits = n_upper <= ENERGY_ROWS * LANES
        parts = split3(data).astype(jnp.bfloat16)
        spread = ((iota((24, 3 * LANES), 0) & 7) == lax.shift_right_logical(iota((24, 3 * LANES), 1), 7)).astype(jnp.bfloat16)

        def place_block(block):
            pick = (iota((LANES, span + 2 * LANES), 0) + block * LANES == rank).astype(jnp.float32).astype(jnp.bfloat16)
            rows_s = join3((dot_nt(pick, parts)).T)
            sorted_ref[block] = rows_s
            valid = lane_1 + block * LANES < n_int
            own_rel = stack([rows_s[axis:axis + 1] - centre[axis] for axis in range(3)] + [rows_s[3:8]])
            tiles = dot_nn(split3(jnp.where(valid, own_rel, FAR_OWN)).T.astype(jnp.bfloat16), spread)
            for axis in range(3):
                others[axis, block] = jnp.broadcast_to(jnp.where(valid, own_rel[axis:axis + 1], 0.0), TILE)
                mine[axis, pl.ds(block * PER_BLOCK, PER_BLOCK)] = tiles[:, axis * LANES:(axis + 1) * LANES].reshape(16, 8, LANES)

        lane_c = iota((cand, LANES), 1)
        is_upper = lane_c < uppers
        keep = jnp.where(is_upper, -1, 255)
        bound = jnp.where(is_upper, lane_c * 256 + 255, lane_c - uppers)

        def passed(probes):
            return sum(((probe & keep) <= bound).astype(jnp.int32) for probe in probes)

        def probe_at(source, stride, number):
            return [jnp.take_along_axis(cum, source + (stride * k - 1), axis=1) for k in range(1, number + 1)]

        source = 16 * passed(marks)
        place_block(0)
        place_block(1)
        source = source + 2 * passed(probe_at(source, 2, 7))
        for block in range(2, blocks):
            place_block(block)
        source = source + passed(probe_at(source, 1, 1))
        for block in range(blocks, BLOCKS):
            sorted_ref[block] = zero

        def turned(base, each, first):
            place = (lane_c - base) & (LANES - 1)
            lane = jnp.take_along_axis(source, (first + place) & (LANES - 1), axis=1)
            target = jnp.where(place < each, lax.shift_right_logical(base + place, 7), -1)
            return target, [jnp.take_along_axis(values, lane, axis=1) for values in rel]

        def pack(target, packed, start, stop, held_rows, empty):
            def pack_row(row, carry):
                hit = target == row
                filled = lane_1 + row * LANES < n_all
                for axis in range(3):
                    held = jnp.where(row < held_rows, others[axis, row], 0.0)
                    values = held + down(jnp.where(hit, packed[axis], 0.0))
                    others[axis, row] = jnp.where(filled, values, empty)
                return carry

            lax.fori_loop(lax.div(start, LANES), lax.div(stop + (LANES - 1), LANES), pack_row, 0)

        upper_rows = lax.div(n_upper + (LANES - 1), LANES)
        rows = lax.div(n_all + (LANES - 1), LANES)
        upper_set, lower_set = turned(upper_base, uppers, 0), turned(lower_base, lowers, uppers)
        pack(*upper_set, n_own, n_upper, own_rows, 0.0)
        pack(*lower_set, n_upper, n_all, upper_rows, FAR_OTHER)

        def set_far(row, carry):
            for axis in range(3):
                others[axis, row] = far
            return carry

        def excess(first_quad, last_quad, first_row, wrap_box, energy):
            slot_8 = iota(TILE, 1)
            load_own, energy_row, force_row = pair_tools(mine, others, rc2, wrap_box)

            def quad(index, total):
                first = index * QUAD
                own = load_own(first)
                sums = (zero,) * (3 * QUAD) + (total,)

                def both(row, part):
                    slot = slot_8 + row * LANES
                    weight = 1.0 if wrap_box else jnp.where(slot < n_int, 1.0, jnp.where(slot < upper_end, 2.0, 0.0))
                    return force_row(own, first, row, part[:-1], True) + (energy_row(own, first, row, part[-1], True, weight),)

                sums = lax.fori_loop(first_row, rows, both, sums)
                for k in range(QUAD):
                    for axis in range(3):
                        acc[axis, first + k] = sums[3 * k + axis]
                return sums[-1]

            return lax.fori_loop(first_quad, last_quad, quad, energy)

        def plain():
            short = jnp.where(rows > FIXED_ROWS, jnp.minimum(quads, FIXED_QUADS), 0)
            energy = excess(0, short, FIXED_ROWS, [], zero)
            if blocks > FIXED_BLOCKS:
                energy = excess(FIXED_QUADS, quads, 0, [], energy)
            eng_ref[0] = energy
            lax.fori_loop(rows, FIXED_ROWS, set_far, 0)

        def alone(wrap_box):
            eng_ref[0] = excess(0, quads, 0, wrap_box, zero)
            lax.fori_loop(0, FIXED_ROWS, set_far, 0)

        pl.when(wide & fits)(plain)
        pl.when(wide & jnp.logical_not(fits))(lambda: alone([]))
        pl.when(jnp.logical_not(wide))(lambda: alone([(axis, box[axis], 1.0 / box[axis]) for axis in (1, 2)]))

    pl.when(small)(lambda: build(FIXED_BLOCKS, 4))
    pl.when(jnp.logical_not(small))(lambda: build(BLOCKS, BLOCKS))


def tile_kernel(mine, others, part, eng_ref, frc_ref, out_ref, acc, react, eng, slots, send_sem, recv_sem):
    coords = my_coords()
    mz, my, mx = coords
    barrier = entry_signals(coords)
    rc2 = RC * RC + 0.0 * mine[0, 0]
    load_own, energy_row, force_row = pair_tools(mine, others, rc2, [])

    lane_8 = iota(TILE, 1).astype(jnp.float32)
    energy = eng_ref[0]

    def weight_of(row, own_weight):
        slot = lane_8 + float(row * LANES)
        return jnp.where(slot < eng_ref[1], own_weight, jnp.where(slot < eng_ref[2], 2.0, 0.0))

    for block in range(FIXED_BLOCKS):

        def energy_quad(index, total, block=block):
            first = block * PER_BLOCK + index * QUAD
            own = load_own(first)
            for row in range(block, ENERGY_ROWS):
                weight = weight_of(row, 2.0 if block < row < FIXED_BLOCKS else 1.0)
                total = energy_row(own, first, row, total, row == block, weight)
            return total

        energy = lax.fori_loop(0, PER_BLOCK // QUAD, energy_quad, energy)
    eng[...] = 2.0 * down(energy)
    pl.semaphore_wait(barrier, len(PEERS))
    place = (mz * NY + my) * NX + mx
    copies = []
    for index, offset in enumerate(PEERS):
        copies.append(pltpu.make_async_remote_copy(src_ref=eng, dst_ref=slots.at[place], send_sem=send_sem.at[index], recv_sem=recv_sem.at[index], device_id=peer_id(coords, offset), device_id_type=MESH))
        copies[-1].start()
    slots[place] = eng[...]
    react[...] = jnp.zeros_like(react)
    for block in range(FIXED_BLOCKS):

        def force_quad(index, carry, block=block):
            first = block * PER_BLOCK + index * QUAD
            own = load_own(first)
            force = force_row(own, first, block, [part[axis, first + k] for k in range(QUAD) for axis in range(3)], True)
            for row in range(block + 1, FIXED_ROWS):
                force = force_row(own, first, row, force, False, react if row < FIXED_BLOCKS else None)
            for k in range(QUAD):
                for axis in range(3):
                    acc[axis, first + k] = force[3 * k + axis]
            return carry

        lax.fori_loop(0, PER_BLOCK // QUAD, force_quad, 0)
    for block in range(BLOCKS):
        held = acc if block < FIXED_BLOCKS else part
        for axis in range(3):
            turned = (held[axis, pl.ds(block * PER_BLOCK, PER_BLOCK)].reshape(LANES, LANES)).T
            force = down(turned)
            if 0 < block < FIXED_BLOCKS:
                force = force - down(react[axis, block])
            frc_ref[axis:axis + 1, block * LANES:(block + 1) * LANES] = 48.0 * force
    for copy in copies:
        copy.wait()
    total = slots[0]
    for index in range(1, NZ * NY * NX):
        total = total + slots[index]
    out_ref[...] = total


def finish_kernel(sorted_ref, frc_ref, total_ref, pos_out, vel_out, frc_out, id_out, ok_out, eng_out):
    eng_out[...] = jnp.sum(total_ref[...])
    for block in range(BLOCKS):
        width = min(LANES, CAP - block * LANES)
        lanes = slice(block * LANES, block * LANES + width)
        rows_s = sorted_ref[block]
        valid = rows_s[3:4] > 0.5
        for axis in range(3):
            force = jnp.where(valid, frc_ref[axis:axis + 1, block * LANES:(block + 1) * LANES], 0.0)
            frc_out[axis:axis + 1, lanes] = force[:, :width]
            vel_out[axis:axis + 1, lanes] = (rows_s[4 + axis:5 + axis] + HALF_DT * force)[:, :width]
            pos_out[axis:axis + 1, lanes] = rows_s[axis:axis + 1, :width]
        new_id = lax.shift_left(rows_s[3:4].astype(jnp.int32) - 1, 16) + rows_s[7:8].astype(jnp.int32)
        id_out[lanes] = jnp.where(valid, new_id, 0)[:, :width].reshape(width)
        ok_out[lanes] = valid.astype(jnp.int32)[:, :width].reshape(width)


VMEM_SPEC = pl.BlockSpec(memory_space=pltpu.VMEM)
HBM_SPEC = pl.BlockSpec(memory_space=pltpu.HBM)
VMEM_LIMIT = 8 * 1024 * 1024
SMEM_SPEC = pl.BlockSpec(memory_space=pltpu.SMEM)


def solution(mesh):
    def local_step(atom_pos, atom_vel, atom_frc, atom_id, atom_ok, brick_side):
        f32 = jnp.float32
        n_dev = NZ * NY * NX
        gat, pkt, own = pl.pallas_call(
            exchange_kernel,
            out_shape=(jax.ShapeDtypeStruct((N_GROUPS + 1, 3, BLOCKS, LANES), f32), jax.ShapeDtypeStruct((N_PACKETS, 8, LANES), f32), jax.ShapeDtypeStruct((16, WIDE), f32)),
            in_specs=[SMEM_SPEC] + [HBM_SPEC] * 5,
            out_specs=(VMEM_SPEC,) * 3,
            scratch_shapes=[
                pltpu.VMEM((3, 3, CAP), f32),
                pltpu.VMEM((CAP,), jnp.int32),
                pltpu.VMEM((CAP,), jnp.int32),
                pltpu.VMEM((3, 4, WIDE), f32),
                pltpu.VMEM((2, WIDE), jnp.int32),
                pltpu.VMEM((3, BLOCKS, LANES), f32),
                pltpu.VMEM((2, 8, LANES), f32),
                pltpu.SemaphoreType.DMA((5,)),
                pltpu.SemaphoreType.DMA((N_GROUPS,)),
                pltpu.SemaphoreType.DMA((N_GROUPS,)),
                pltpu.SemaphoreType.DMA((N_PACKETS,)),
                pltpu.SemaphoreType.DMA((N_PACKETS,)),
            ],
            compiler_params=pltpu.CompilerParams(collective_id=0, has_side_effects=True, vmem_limit_bytes=VMEM_LIMIT),
            name="exchange",
        )(brick_side, *(pltpu.with_memory_space_constraint(value, pltpu.HBM) for value in (atom_pos.T, atom_vel.T, atom_frc.T, atom_id, atom_ok)))
        own_tiles = jax.ShapeDtypeStruct((3, GROUPS_OWN, 8, LANES), f32)
        placed, mine, others, part, eng = pl.pallas_call(
            prepare_kernel,
            out_shape=(jax.ShapeDtypeStruct((BLOCKS, 8, LANES), f32), own_tiles, jax.ShapeDtypeStruct((3, MAX_ROWS, 8, LANES), f32), own_tiles, jax.ShapeDtypeStruct((3, 8, LANES), f32)),
            in_specs=[VMEM_SPEC] * 3,
            out_specs=(VMEM_SPEC,) * 5,
            compiler_params=pltpu.CompilerParams(vmem_limit_bytes=VMEM_LIMIT),
            name="prepare",
        )(gat, pkt, own)
        frc_rows, total = pl.pallas_call(
            tile_kernel,
            out_shape=(jax.ShapeDtypeStruct((8, WIDE), f32), jax.ShapeDtypeStruct((1, LANES), f32)),
            in_specs=[VMEM_SPEC] * 4,
            out_specs=(VMEM_SPEC,) * 2,
            scratch_shapes=[pltpu.VMEM((3, FIXED_BLOCKS * 16, 8, LANES), f32), pltpu.VMEM((3, FIXED_BLOCKS, 8, LANES), f32), pltpu.VMEM((1, LANES), f32), pltpu.VMEM((n_dev, 1, LANES), f32), pltpu.SemaphoreType.DMA((n_dev - 1,)), pltpu.SemaphoreType.DMA((n_dev - 1,))],
            compiler_params=pltpu.CompilerParams(collective_id=1, has_side_effects=True, vmem_limit_bytes=VMEM_LIMIT),
            name="tile",
        )(mine, others, part, eng)
        pos, vel, frc, ids, oks, energy = pl.pallas_call(
            finish_kernel,
            out_shape=(jax.ShapeDtypeStruct((3, CAP), f32),) * 3 + (jax.ShapeDtypeStruct((CAP,), jnp.int32),) * 2 + (jax.ShapeDtypeStruct((), f32),),
            in_specs=[VMEM_SPEC] * 3,
            out_specs=(VMEM_SPEC,) * 5 + (SMEM_SPEC,),
            compiler_params=pltpu.CompilerParams(vmem_limit_bytes=VMEM_LIMIT),
            name="finish",
        )(placed, frc_rows, total)
        return pos.T, vel.T, frc.T, ids, oks, energy

    row_spec = P(MESH_AXES, None)
    id_spec = P(MESH_AXES)
    return jax.shard_map(local_step, mesh=mesh, in_specs=(row_spec, row_spec, row_spec, id_spec, id_spec, P()), out_specs=(row_spec, row_spec, row_spec, id_spec, id_spec, P()), check_vma=False)
```

```python
import jax
import jax.numpy as jnp
from jax import lax
from jax.experimental import pallas as pl
from jax.experimental.pallas import tpu as pltpu
from jax.sharding import PartitionSpec as P

DT = 0.005
HALF_DT = 0.5 * DT
RC = 2.5
UPC = -48.0 * RC ** -13 + 24.0 * RC ** -7
MESH_AXES = ("z", "y", "x")
MESH = pl.DeviceIdType.MESH
NZ, NY, NX = 2, 2, 4
CAP = 729
LANES = 128
TILE = (8, LANES)
BLOCKS = 6
WIDE = BLOCKS * LANES
MOVE_CAP = CAP // 100
FAR_OWN = 1.0e4
FAR_OTHER = -1.0e4
NOWHERE = 1.0e9
GHOST_SQ = RC * RC + 0.01
PEERS = [(dz, dy, dx) for dz in range(NZ) for dy in range(NY) for dx in range(NX)][:0:-1]
SIDES = [(1, 1), (1, 0), (0, 1), (0, 0)]
GROUPS = [(gx, *side) for side in SIDES for gx in (1, -1)] + [(0, *side) for side in SIDES[:3]]
N_GROUPS = len(GROUPS)
DISTANT = [(2, *side) for side in SIDES]
N_PACKETS = N_GROUPS + len(DISTANT)


def lane_plan():
    starts, base = [], {}
    block, lane = 0, 0
    for index, (gx, gy, gz) in enumerate(GROUPS):
        if index == 8:
            block, lane = 1, 0
        dirs = [(gx, sy, sz) for sz in ((-1, 1) if gz else (0,)) for sy in ((-1, 1) if gy else (0,))]
        starts.append((block, lane, lane + MOVE_CAP * len(dirs)))
        for dx, dy, dz in dirs:
            base[(dz + 1) * 9 + (dy + 1) * 3 + dx + 1] = block * LANES + lane
            lane += MOVE_CAP
    return starts, base


LANE_STARTS, LANE_BASE = lane_plan()
STAY = 13
NT_DIMS = (((1,), (1,)), ((), ()))
NN_DIMS = (((1,), (0,)), ((), ()))


def split3(values):
    hi = values.astype(jnp.bfloat16).astype(jnp.float32)
    rest = values - hi
    mid = rest.astype(jnp.bfloat16).astype(jnp.float32)
    return jnp.concatenate([hi, mid, rest - mid], axis=0).astype(jnp.bfloat16)


def join3(parts):
    rows = parts.shape[0] // 3
    return (parts[0:rows] + parts[rows:2 * rows]) + parts[2 * rows:3 * rows]


def dot_nt(a, b):
    return lax.dot_general(a, b, NT_DIMS, preferred_element_type=jnp.float32)


def dot_nn(a, b):
    return lax.dot_general(a, b, NN_DIMS, preferred_element_type=jnp.float32)


def down(values):
    return jnp.sum(values, axis=0, keepdims=True)


def across(values):
    return jnp.sum(values, axis=1, keepdims=True)


def stack(values):
    return jnp.concatenate(values, axis=0)


def beside(values):
    return jnp.concatenate(values, axis=1)


def iota(shape, axis):
    return lax.broadcasted_iota(jnp.int32, shape, axis)


def my_coords():
    return lax.axis_index("z"), lax.axis_index("y"), lax.axis_index("x")


def peer_id(coords, offset):
    mz, my, mx = coords
    return (lax.rem(mz + offset[0], NZ), lax.rem(my + offset[1], NY), lax.rem(mx + offset[2] + NX, NX))


def entry_signals(coords):
    barrier = pltpu.get_barrier_semaphore()
    for offset in PEERS:
        pl.semaphore_signal(barrier, inc=1, device_id=peer_id(coords, offset), device_id_type=MESH)
    return barrier


def exchange_kernel(brick_ref, pos_ref, vel_ref, frc_ref, id_ref, ok_ref, gat_ref, pkt_ref, own_ref, raw, ids_in, oks_in, pad_ref, int_ref, send_pos, send_pkt, in_sem, pos_send_sem, pos_recv_sem, pkt_send_sem, pkt_recv_sem):
    coords = my_coords()
    fetches = [pltpu.make_async_copy(src, dst, in_sem.at[index]) for index, (src, dst) in enumerate(((pos_ref, raw.at[0]), (vel_ref, raw.at[1]), (frc_ref, raw.at[2]), (id_ref, ids_in), (ok_ref, oks_in)))]
    for fetch in fetches:
        fetch.start()
    barrier = entry_signals(coords)
    tail = slice(WIDE - LANES, WIDE)
    pad_ref[:, :, tail] = jnp.zeros((3, 4, LANES), jnp.float32)
    int_ref[:, tail] = jnp.zeros((2, LANES), jnp.int32)
    for fetch in fetches:
        fetch.wait()
    brick = brick_ref[...]
    for index in range(3):
        pad_ref[index, 0:3, 0:CAP] = raw[index]
    int_ref[0:1, 0:CAP] = ids_in[...].reshape(1, CAP)
    int_ref[1:2, 0:CAP] = oks_in[...].reshape(1, CAP)
    owned = int_ref[1:2, :] > 0
    moved, half, code = [], [], jnp.zeros((1, WIDE), jnp.int32)
    for axis, (mine, size, weight) in enumerate(((coords[2], NX, 1), (coords[1], NY, 3), (coords[0], NZ, 9))):
        box = brick * float(size)
        low = mine.astype(jnp.float32) * brick
        high = (mine + 1).astype(jnp.float32) * brick
        half_v = pad_ref[1, axis:axis + 1, :] + HALF_DT * pad_ref[2, axis:axis + 1, :]
        drift = pad_ref[0, axis:axis + 1, :] + DT * half_v
        step = jnp.where(drift >= high, 2, jnp.where(drift < low, 0, 1))
        code = code + step * weight
        wrapped = jnp.where(drift < 0.0, drift + box, jnp.where(drift >= box, drift - box, drift))
        moved.append(wrapped)
        half.append(half_v)
    code = jnp.where(owned, code, -1)
    for axis in range(3):
        for block in range(BLOCKS):
            lanes = slice(block * LANES, (block + 1) * LANES)
            send_pos[axis, block:block + 1, :] = jnp.where(owned[:, lanes], moved[axis][:, lanes], NOWHERE)
    ids = int_ref[0:1, :]
    id_hi = (lax.shift_right_logical(ids, 16) + 1).astype(jnp.float32)
    id_lo = (ids & 65535).astype(jnp.float32)
    data = stack(moved + [id_hi] + half + [id_lo])
    member = (jnp.broadcast_to(code, (32, WIDE)) == iota((32, WIDE), 0)).astype(jnp.float32)
    tri = (iota((LANES, LANES), 0) < iota((LANES, LANES), 1)).astype(jnp.bfloat16)
    codes = iota((32, LANES), 0)
    running = jnp.zeros((32, LANES), jnp.float32)
    for move, first in LANE_BASE.items():
        running = jnp.where(codes == move, float(first), running)
    slots = []
    for block in range(BLOCKS):
        part = member[:, block * LANES:(block + 1) * LANES]
        before = dot_nn(part.astype(jnp.bfloat16), tri)
        slots.append(down(part * (before + running)))
        running = running + across(part)
    slot = beside(slots)
    stay = code == STAY
    mover_slot = jnp.where(owned & jnp.logical_not(stay), slot, -1.0).astype(jnp.int32)
    pick = (iota((2 * LANES, WIDE), 0) == mover_slot).astype(jnp.float32).astype(jnp.bfloat16)
    packet = join3(dot_nt(split3(data), pick))
    send_pkt[0] = packet[:, 0:LANES]
    send_pkt[1] = packet[:, LANES:2 * LANES]
    own_ref[0:8, :] = data
    own_ref[8:16, :] = stack([jnp.where(stay, slot, -1.0), jnp.full((7, WIDE), brick, jnp.float32)])
    pl.semaphore_wait(barrier, len(PEERS))
    copies = []
    for index, (gx, gy, gz) in enumerate(GROUPS + DISTANT):
        peer = peer_id(coords, (gz, gy, gx))
        if index < N_GROUPS:
            copies.append(pltpu.make_async_remote_copy(src_ref=send_pos, dst_ref=gat_ref.at[index], send_sem=pos_send_sem.at[index], recv_sem=pos_recv_sem.at[index], device_id=peer, device_id_type=MESH))
            copies[-1].start()
            source, target = send_pkt.at[LANE_STARTS[index][0]], pkt_ref.at[index]
        else:
            source, target = send_pkt.at[0, 0:4], pkt_ref.at[index, 0:4]
        copies.append(pltpu.make_async_remote_copy(src_ref=source, dst_ref=target, send_sem=pkt_send_sem.at[index], recv_sem=pkt_recv_sem.at[index], device_id=peer, device_id_type=MESH))
        copies[-1].start()
    gat_ref[N_GROUPS] = send_pos[...]
    for copy in copies:
        copy.wait()


CAND_ROWS = 8 * (N_GROUPS + 1) + 8
MAX_ROWS = BLOCKS + CAND_ROWS
GROUPS_OWN = BLOCKS * 16
QUAD = 4
FIXED_BLOCKS = 4
PER_BLOCK = 16
FIXED_QUADS = FIXED_BLOCKS * PER_BLOCK // QUAD
FIXED_ROWS = 11
ENERGY_ROWS = 8


def pair_tools(mine, others, rc2, wrap_box):
    def powers(dist_sq):
        inv_r = lax.rsqrt(dist_sq)
        inv_2 = inv_r * inv_r
        inv_4 = inv_2 * inv_2
        term = inv_4 * inv_2 - 0.5
        return inv_r, term, term * (inv_4 * inv_4)

    cut_inv_r, cut_term, cut_core = powers(rc2)
    kappa = -RC * cut_core
    for ulps in (-3, -2, -1, 1, 2, 3):
        trial = ulps * 2.0 ** -34 - RC * cut_core
        kappa = jnp.where(trial * cut_inv_r == -cut_core, trial, kappa)

    def quad_energy(dist_sqs):
        terms, tails = [], []
        for dist_sq in dist_sqs:
            inv_r = lax.rsqrt(dist_sq)
            inv_2 = inv_r * inv_r
            term = inv_2 * inv_2 * inv_2 - 0.5
            terms.append(term * term)
            tails.append(kappa * inv_r * dist_sq)
        return ((terms[0] + terms[1]) + (terms[2] + terms[3])) - 12.0 * ((tails[0] + tails[1]) + (tails[2] + tails[3]))

    cut_energy = quad_energy([rc2] * QUAD)
    own_minus_lane = iota(TILE, 0) - iota(TILE, 1)

    def load_own(first):
        return [[mine[axis, first + k] for axis in range(3)] for k in range(QUAD)]

    def gaps(own, first, row, with_self):
        other = [others[axis, row] for axis in range(3)]
        deltas, dist_sqs = [], []
        for k in range(QUAD):
            delta = [own[k][axis] - other[axis] for axis in range(3)]
            for axis, box, inv_box in wrap_box:
                delta[axis] = delta[axis] - box * jnp.floor(delta[axis] * inv_box + 0.5)
            dist_sq = delta[0] * delta[0] + delta[1] * delta[1] + delta[2] * delta[2]
            if with_self:
                dist_sq = jnp.where(own_minus_lane == row * LANES - (first + k) * 8, rc2, dist_sq)
            deltas.append(delta)
            dist_sqs.append(jnp.minimum(dist_sq, rc2))
        return deltas, dist_sqs

    def energy_row(own, first, row, total, with_self, weight=None):
        gain = quad_energy(gaps(own, first, row, with_self)[1]) - cut_energy
        return total + (gain if weight is None else gain * weight)

    def force_row(own, first, row, force, with_self, react=None):
        force, pulls = list(force), []
        deltas, dist_sqs = gaps(own, first, row, with_self)
        for k in range(QUAD):
            inv_r, term, core = powers(dist_sqs[k])
            scale = core + kappa * inv_r
            pulls.append([scale * deltas[k][axis] for axis in range(3)])
            for axis in range(3):
                force[3 * k + axis] = force[3 * k + axis] + pulls[k][axis]
        if react is not None:
            for axis in range(3):
                react[axis, row] = react[axis, row] + ((pulls[0][axis] + pulls[1][axis]) + (pulls[2][axis] + pulls[3][axis]))
        return tuple(force)

    return load_own, energy_row, force_row


def prepare_kernel(gat_ref, pkt_ref, own_ref, sorted_ref, mine, others, acc, eng_ref):
    mz, my, mx = my_coords()
    brick = own_ref[9:10, 0:LANES]
    half_l = 0.5 * brick
    sizes = (NX, NY, NZ)
    centre = [(index.astype(jnp.float32) + 0.5) * brick for index in (mx, my, mz)]
    box = [brick * float(size) for size in sizes]
    lane_1 = iota((1, LANES), 1)
    acc[:, pl.ds(0, FIXED_QUADS * QUAD)] = jnp.zeros((3, FIXED_QUADS * QUAD, 8, LANES), jnp.float32)

    arrived = []
    for block in range(2):
        total = jnp.zeros(TILE, jnp.float32)
        for index in range(N_GROUPS):
            where_block, first, last = LANE_STARTS[index]
            if where_block == block:
                total = total + jnp.where((lane_1 >= first) & (lane_1 < last), pkt_ref[index], 0.0)
        arrived.append(total)
    arr = beside(arrived)
    arr_ok = arr[3:4] > 0.5
    stay_all = own_ref[8:9, :] >= 0.0
    n_vec = across(stay_all.astype(jnp.float32)) + across(arr_ok.astype(jnp.float32))
    n_own = jnp.max(n_vec).astype(jnp.int32)
    n_int = n_vec.astype(jnp.int32)
    quads = lax.div(n_own + (8 * QUAD - 1), 8 * QUAD)
    own_rows = lax.div(n_own + (LANES - 1), LANES)
    beyond = gat_ref[0, 0, 4:6, :]
    for slot in range(1, N_GROUPS + 1):
        beyond = jnp.minimum(beyond, gat_ref[slot, 0, 4:6, :])
    small = (jnp.min(beyond) > 0.5 * NOWHERE) & (n_own <= FIXED_BLOCKS * LANES)
    eng_ref[1] = jnp.broadcast_to(n_vec, TILE)
    wide = jnp.max(brick) >= 2.0 * RC
    int_max = 2147483647
    rc2 = RC * RC + 0.0 * own_ref[8:16, 0:LANES]
    zero = jnp.zeros(TILE, jnp.float32)
    far = jnp.full(TILE, FAR_OTHER, jnp.float32)

    def build(blocks, tile_rows):
        span = blocks * LANES
        data = beside([own_ref[0:8, 0:span], arr])
        ids = lax.shift_left(data[3:4].astype(jnp.int32) - 1, 16) + data[7:8].astype(jnp.int32)
        stay_rank = own_ref[8:9, 0:span]
        stay = stay_rank >= 0.0
        arr_id = jnp.where(arr_ok, ids[:, span:], int_max)
        own_id = jnp.where(stay, ids[:, :span], int_max)

        count_rows = (N_GROUPS + 1) * tile_rows
        cand = -(-(count_rows + len(DISTANT)) // 8) * 8
        rel = []
        for axis in range(3):
            near = [gat_ref[slot, axis, 0:tile_rows, :] for slot in range(N_GROUPS + 1)]
            distant = [jnp.where(pkt_ref[N_GROUPS + k, 3:4, :] > 0.5, pkt_ref[N_GROUPS + k, axis:axis + 1, :], NOWHERE) for k in range(len(DISTANT))]
            values = stack(near + distant + [jnp.full((cand - count_rows - len(DISTANT), LANES), NOWHERE, jnp.float32)]) - centre[axis]
            rel.append(jnp.where(values > 0.5 * box[axis], values - box[axis], jnp.where(values < -0.5 * box[axis], values + box[axis], values)))
        over = [jnp.maximum(jnp.abs(values) - half_l, 0.0) for values in rel]
        gap_sq = over[0] * over[0] + over[1] * over[1] + over[2] * over[2]
        side = jnp.zeros((cand, LANES), jnp.float32)
        for axis in range(3):
            side = 3.0 * side + jnp.where(over[2 - axis] > 0.0, jnp.where(rel[2 - axis] > 0.0, 1.0, -1.0), 0.0)
        near = gap_sq < GHOST_SQ
        mixed = jnp.where(near & (side > 0.0), 256.0, jnp.where(near & (side < 0.0), 1.0, 0.0)).astype(jnp.bfloat16)
        row_l, col_l = iota((LANES, LANES), 0), iota((LANES, LANES), 1)

        def counts(chosen):
            return dot_nn(mixed, chosen.astype(jnp.bfloat16)).astype(jnp.int32)

        cum = counts(row_l <= col_l)
        total = counts(row_l >= 0)
        marks = [counts(row_l < 16 * k) for k in range(1, 8)]
        arr_col = jnp.broadcast_to(arr_id, (8, 2 * LANES)).T[:, 0:1]
        arr_first = (arr_col < beside([own_id, arr_id])).astype(jnp.float32)
        arr_before = down(arr_first)
        stay_after = dot_nt(jnp.broadcast_to(stay.astype(jnp.float32), (8, span)).astype(jnp.bfloat16), arr_first[:, :span].astype(jnp.bfloat16))[0:1]
        stay_before = across(stay.astype(jnp.float32)) - stay_after
        rank = beside([jnp.where(stay, stay_rank + arr_before[:, :span], -1.0), jnp.where(arr_ok, stay_before + arr_before[:, span:], -1.0)]).astype(jnp.int32)
        earlier = (iota((cand, cand), 1) < iota((cand, cand), 0)).astype(jnp.bfloat16)
        uppers, lowers = lax.shift_right_logical(total, 8), total & 255

        def starts(each, first):
            base = dot_nn(earlier, each.astype(jnp.float32).astype(jnp.bfloat16)).astype(jnp.int32) + first
            return base, base[cand - 1:] + each[cand - 1:]

        upper_base, upper_end = starts(uppers, n_int)
        lower_base, all_end = starts(lowers, upper_end)
        n_upper, n_all = jnp.max(upper_end), jnp.max(all_end)
        eng_ref[2] = jnp.broadcast_to(upper_end.astype(jnp.float32), TILE)
        fits = n_upper <= ENERGY_ROWS * LANES
        parts = split3(data)

        pick = (iota((span, span + 2 * LANES), 0) == rank).astype(jnp.float32).astype(jnp.bfloat16)
        chosen = dot_nt(pick, parts)

        def place_block(block):
            rows_s = join3(chosen[block * LANES:(block + 1) * LANES].T)
            sorted_ref[block] = rows_s
            valid = lane_1 + block * LANES < n_int
            own_rel = stack([rows_s[axis:axis + 1] - centre[axis] for axis in range(3)] + [rows_s[3:8]])
            columns = jnp.where(valid, own_rel, FAR_OWN).T
            for axis in range(3):
                others[axis, block] = jnp.broadcast_to(jnp.where(valid, own_rel[axis:axis + 1], 0.0), TILE)
                mine[axis, pl.ds(block * PER_BLOCK, PER_BLOCK)] = jnp.broadcast_to(columns[:, axis:axis + 1], (LANES, LANES)).reshape(16, 8, LANES)

        lane_c = iota((cand, LANES), 1)
        is_upper = lane_c < uppers
        keep = jnp.where(is_upper, -1, 255)
        bound = jnp.where(is_upper, lane_c * 256 + 255, lane_c - uppers)

        def passed(probes):
            return sum(((probe & keep) <= bound).astype(jnp.int32) for probe in probes)

        def probe_at(source, stride, number):
            return [jnp.take_along_axis(cum, source + (stride * k - 1), axis=1) for k in range(1, number + 1)]

        source = 16 * passed(marks)
        place_block(0)
        place_block(1)
        source = source + 2 * passed(probe_at(source, 2, 7))
        for block in range(2, blocks):
            place_block(block)
        source = source + passed(probe_at(source, 1, 1))
        for block in range(blocks, BLOCKS):
            sorted_ref[block] = zero

        def turned(base, each, first):
            place = (lane_c - base) & (LANES - 1)
            lane = jnp.take_along_axis(source, (first + place) & (LANES - 1), axis=1)
            target = jnp.where(place < each, lax.shift_right_logical(base + place, 7), -1)
            return target, [jnp.take_along_axis(values, lane, axis=1) for values in rel]

        def pack(target, packed, start, stop, held_rows, empty):
            def pack_row(row, carry):
                hit = target == row
                filled = lane_1 + row * LANES < n_all
                for axis in range(3):
                    held = jnp.where(row < held_rows, others[axis, row], 0.0)
                    values = held + down(jnp.where(hit, packed[axis], 0.0))
                    others[axis, row] = jnp.where(filled, values, empty)
                return carry

            lax.fori_loop(lax.div(start, LANES), lax.div(stop + (LANES - 1), LANES), pack_row, 0)

        upper_rows = lax.div(n_upper + (LANES - 1), LANES)
        rows = lax.div(n_all + (LANES - 1), LANES)
        upper_set, lower_set = turned(upper_base, uppers, 0), turned(lower_base, lowers, uppers)
        pack(*upper_set, n_own, n_upper, own_rows, 0.0)
        pack(*lower_set, n_upper, n_all, upper_rows, FAR_OTHER)

        def set_far(row, carry):
            for axis in range(3):
                others[axis, row] = far
            return carry

        def excess(first_quad, last_quad, first_row, wrap_box, energy):
            slot_8 = iota(TILE, 1)
            load_own, energy_row, force_row = pair_tools(mine, others, rc2, wrap_box)

            def quad(index, total):
                first = index * QUAD
                own = load_own(first)
                sums = (zero,) * (3 * QUAD) + (total,)

                def both(row, part):
                    slot = slot_8 + row * LANES
                    weight = 1.0 if wrap_box else jnp.where(slot < n_int, 1.0, jnp.where(slot < upper_end, 2.0, 0.0))
                    return force_row(own, first, row, part[:-1], True) + (energy_row(own, first, row, part[-1], True, weight),)

                sums = lax.fori_loop(first_row, rows, both, sums)
                for k in range(QUAD):
                    for axis in range(3):
                        acc[axis, first + k] = sums[3 * k + axis]
                return sums[-1]

            return lax.fori_loop(first_quad, last_quad, quad, energy)

        def plain():
            short = jnp.where(rows > FIXED_ROWS, jnp.minimum(quads, FIXED_QUADS), 0)
            energy = excess(0, short, FIXED_ROWS, [], zero)
            if blocks > FIXED_BLOCKS:
                energy = excess(FIXED_QUADS, quads, 0, [], energy)
            eng_ref[0] = energy
            lax.fori_loop(rows, FIXED_ROWS, set_far, 0)

        def alone(wrap_box):
            eng_ref[0] = excess(0, quads, 0, wrap_box, zero)
            lax.fori_loop(0, FIXED_ROWS, set_far, 0)

        pl.when(wide & fits)(plain)
        pl.when(wide & jnp.logical_not(fits))(lambda: alone([]))
        pl.when(jnp.logical_not(wide))(lambda: alone([(axis, box[axis], 1.0 / box[axis]) for axis in (1, 2)]))

    pl.when(small)(lambda: build(FIXED_BLOCKS, 4))
    pl.when(jnp.logical_not(small))(lambda: build(BLOCKS, BLOCKS))


def tile_kernel(mine, others, part, eng_ref, frc_ref, out_ref, acc, react, eng, slots, send_sem, recv_sem):
    coords = my_coords()
    mz, my, mx = coords
    barrier = entry_signals(coords)
    rc2 = RC * RC + 0.0 * mine[0, 0]
    load_own, energy_row, force_row = pair_tools(mine, others, rc2, [])

    lane_8 = iota(TILE, 1).astype(jnp.float32)
    energy = eng_ref[0]

    def weight_of(row, own_weight):
        slot = lane_8 + float(row * LANES)
        return jnp.where(slot < eng_ref[1], own_weight, jnp.where(slot < eng_ref[2], 2.0, 0.0))

    for block in range(FIXED_BLOCKS):

        def energy_quad(index, total, block=block):
            first = block * PER_BLOCK + index * QUAD
            own = load_own(first)
            for row in range(block, ENERGY_ROWS):
                weight = weight_of(row, 2.0 if block < row < FIXED_BLOCKS else 1.0)
                total = energy_row(own, first, row, total, row == block, weight)
            return total

        energy = lax.fori_loop(0, PER_BLOCK // QUAD, energy_quad, energy)
    eng[...] = 2.0 * down(energy)
    pl.semaphore_wait(barrier, len(PEERS))
    place = (mz * NY + my) * NX + mx
    copies = []
    for index, offset in enumerate(PEERS):
        copies.append(pltpu.make_async_remote_copy(src_ref=eng, dst_ref=slots.at[place], send_sem=send_sem.at[index], recv_sem=recv_sem.at[index], device_id=peer_id(coords, offset), device_id_type=MESH))
        copies[-1].start()
    slots[place] = eng[...]
    react[...] = jnp.zeros_like(react)
    for block in range(FIXED_BLOCKS):

        def force_quad(index, carry, block=block):
            first = block * PER_BLOCK + index * QUAD
            own = load_own(first)
            force = force_row(own, first, block, [part[axis, first + k] for k in range(QUAD) for axis in range(3)], True)
            for row in range(block + 1, FIXED_ROWS):
                force = force_row(own, first, row, force, False, react if row < FIXED_BLOCKS else None)
            for k in range(QUAD):
                for axis in range(3):
                    acc[axis, first + k] = force[3 * k + axis]
            return carry

        lax.fori_loop(0, PER_BLOCK // QUAD, force_quad, 0)
    for block in range(BLOCKS):
        held = acc if block < FIXED_BLOCKS else part
        for axis in range(3):
            turned = (held[axis, pl.ds(block * PER_BLOCK, PER_BLOCK)].reshape(LANES, LANES)).T
            force = down(turned)
            if 0 < block < FIXED_BLOCKS:
                force = force - down(react[axis, block])
            frc_ref[axis:axis + 1, block * LANES:(block + 1) * LANES] = 48.0 * force
    for copy in copies:
        copy.wait()
    total = slots[0]
    for index in range(1, NZ * NY * NX):
        total = total + slots[index]
    out_ref[...] = total


def finish_kernel(sorted_ref, frc_ref, total_ref, pos_out, vel_out, frc_out, id_out, ok_out, eng_out):
    eng_out[...] = jnp.sum(total_ref[...])
    for block in range(BLOCKS):
        width = min(LANES, CAP - block * LANES)
        lanes = slice(block * LANES, block * LANES + width)
        rows_s = sorted_ref[block]
        valid = rows_s[3:4] > 0.5
        for axis in range(3):
            force = jnp.where(valid, frc_ref[axis:axis + 1, block * LANES:(block + 1) * LANES], 0.0)
            frc_out[axis:axis + 1, lanes] = force[:, :width]
            vel_out[axis:axis + 1, lanes] = (rows_s[4 + axis:5 + axis] + HALF_DT * force)[:, :width]
            pos_out[axis:axis + 1, lanes] = rows_s[axis:axis + 1, :width]
        new_id = lax.shift_left(rows_s[3:4].astype(jnp.int32) - 1, 16) + rows_s[7:8].astype(jnp.int32)
        id_out[lanes] = jnp.where(valid, new_id, 0)[:, :width].reshape(width)
        ok_out[lanes] = valid.astype(jnp.int32)[:, :width].reshape(width)


VMEM_SPEC = pl.BlockSpec(memory_space=pltpu.VMEM)
HBM_SPEC = pl.BlockSpec(memory_space=pltpu.HBM)
VMEM_LIMIT = 8 * 1024 * 1024
SMEM_SPEC = pl.BlockSpec(memory_space=pltpu.SMEM)


def solution(mesh):
    def local_step(atom_pos, atom_vel, atom_frc, atom_id, atom_ok, brick_side):
        f32 = jnp.float32
        n_dev = NZ * NY * NX
        gat, pkt, own = pl.pallas_call(
            exchange_kernel,
            out_shape=(jax.ShapeDtypeStruct((N_GROUPS + 1, 3, BLOCKS, LANES), f32), jax.ShapeDtypeStruct((N_PACKETS, 8, LANES), f32), jax.ShapeDtypeStruct((16, WIDE), f32)),
            in_specs=[SMEM_SPEC] + [HBM_SPEC] * 5,
            out_specs=(VMEM_SPEC,) * 3,
            scratch_shapes=[
                pltpu.VMEM((3, 3, CAP), f32),
                pltpu.VMEM((CAP,), jnp.int32),
                pltpu.VMEM((CAP,), jnp.int32),
                pltpu.VMEM((3, 4, WIDE), f32),
                pltpu.VMEM((2, WIDE), jnp.int32),
                pltpu.VMEM((3, BLOCKS, LANES), f32),
                pltpu.VMEM((2, 8, LANES), f32),
                pltpu.SemaphoreType.DMA((5,)),
                pltpu.SemaphoreType.DMA((N_GROUPS,)),
                pltpu.SemaphoreType.DMA((N_GROUPS,)),
                pltpu.SemaphoreType.DMA((N_PACKETS,)),
                pltpu.SemaphoreType.DMA((N_PACKETS,)),
            ],
            compiler_params=pltpu.CompilerParams(collective_id=0, has_side_effects=True, vmem_limit_bytes=VMEM_LIMIT),
            name="exchange",
        )(brick_side, *(pltpu.with_memory_space_constraint(value, pltpu.HBM) for value in (atom_pos.T, atom_vel.T, atom_frc.T, atom_id, atom_ok)))
        own_tiles = jax.ShapeDtypeStruct((3, GROUPS_OWN, 8, LANES), f32)
        placed, mine, others, part, eng = pl.pallas_call(
            prepare_kernel,
            out_shape=(jax.ShapeDtypeStruct((BLOCKS, 8, LANES), f32), own_tiles, jax.ShapeDtypeStruct((3, MAX_ROWS, 8, LANES), f32), own_tiles, jax.ShapeDtypeStruct((3, 8, LANES), f32)),
            in_specs=[VMEM_SPEC] * 3,
            out_specs=(VMEM_SPEC,) * 5,
            compiler_params=pltpu.CompilerParams(vmem_limit_bytes=VMEM_LIMIT),
            name="prepare",
        )(gat, pkt, own)
        frc_rows, total = pl.pallas_call(
            tile_kernel,
            out_shape=(jax.ShapeDtypeStruct((8, WIDE), f32), jax.ShapeDtypeStruct((1, LANES), f32)),
            in_specs=[VMEM_SPEC] * 4,
            out_specs=(VMEM_SPEC,) * 2,
            scratch_shapes=[pltpu.VMEM((3, FIXED_BLOCKS * 16, 8, LANES), f32), pltpu.VMEM((3, FIXED_BLOCKS, 8, LANES), f32), pltpu.VMEM((1, LANES), f32), pltpu.VMEM((n_dev, 1, LANES), f32), pltpu.SemaphoreType.DMA((n_dev - 1,)), pltpu.SemaphoreType.DMA((n_dev - 1,))],
            compiler_params=pltpu.CompilerParams(collective_id=1, has_side_effects=True, vmem_limit_bytes=VMEM_LIMIT),
            name="tile",
        )(mine, others, part, eng)
        pos, vel, frc, ids, oks, energy = pl.pallas_call(
            finish_kernel,
            out_shape=(jax.ShapeDtypeStruct((3, CAP), f32),) * 3 + (jax.ShapeDtypeStruct((CAP,), jnp.int32),) * 2 + (jax.ShapeDtypeStruct((), f32),),
            in_specs=[VMEM_SPEC] * 3,
            out_specs=(VMEM_SPEC,) * 5 + (SMEM_SPEC,),
            compiler_params=pltpu.CompilerParams(vmem_limit_bytes=VMEM_LIMIT),
            name="finish",
        )(placed, frc_rows, total)
        return pos.T, vel.T, frc.T, ids, oks, energy

    row_spec = P(MESH_AXES, None)
    id_spec = P(MESH_AXES)
    return jax.shard_map(local_step, mesh=mesh, in_specs=(row_spec, row_spec, row_spec, id_spec, id_spec, P()), out_specs=(row_spec, row_spec, row_spec, id_spec, id_spec, P()), check_vma=False)
```

```python
import jax
import jax.numpy as jnp
from jax import lax
from jax.experimental import pallas as pl
from jax.experimental.pallas import tpu as pltpu
from jax.sharding import PartitionSpec as P

DT = 0.005
HALF_DT = 0.5 * DT
RC = 2.5
UPC = -48.0 * RC ** -13 + 24.0 * RC ** -7
MESH_AXES = ("z", "y", "x")
MESH = pl.DeviceIdType.MESH
NZ, NY, NX = 2, 2, 4
CAP = 729
LANES = 128
TILE = (8, LANES)
BLOCKS = 6
WIDE = BLOCKS * LANES
MOVE_CAP = CAP // 100
FAR_OWN = 1.0e4
FAR_OTHER = -1.0e4
NOWHERE = 1.0e9
GHOST_SQ = RC * RC + 0.01
PEERS = [(dz, dy, dx) for dz in range(NZ) for dy in range(NY) for dx in range(NX)][:0:-1]
SIDES = [(1, 1), (1, 0), (0, 1), (0, 0)]
GROUPS = [(gx, *side) for side in SIDES for gx in (1, -1)] + [(0, *side) for side in SIDES[:3]]
N_GROUPS = len(GROUPS)
DISTANT = [(2, *side) for side in SIDES]
N_PACKETS = N_GROUPS + len(DISTANT)


def lane_plan():
    starts, base = [], {}
    block, lane = 0, 0
    for index, (gx, gy, gz) in enumerate(GROUPS):
        if index == 8:
            block, lane = 1, 0
        dirs = [(gx, sy, sz) for sz in ((-1, 1) if gz else (0,)) for sy in ((-1, 1) if gy else (0,))]
        starts.append((block, lane, lane + MOVE_CAP * len(dirs)))
        for dx, dy, dz in dirs:
            base[(dz + 1) * 9 + (dy + 1) * 3 + dx + 1] = block * LANES + lane
            lane += MOVE_CAP
    return starts, base


LANE_STARTS, LANE_BASE = lane_plan()
STAY = 13
NT_DIMS = (((1,), (1,)), ((), ()))
NN_DIMS = (((1,), (0,)), ((), ()))


def split3(values):
    hi = values.astype(jnp.bfloat16).astype(jnp.float32)
    rest = values - hi
    mid = rest.astype(jnp.bfloat16).astype(jnp.float32)
    return jnp.concatenate([hi, mid, rest - mid], axis=0).astype(jnp.bfloat16)


def join3(parts):
    rows = parts.shape[0] // 3
    return (parts[0:rows] + parts[rows:2 * rows]) + parts[2 * rows:3 * rows]


def dot_nt(a, b):
    return lax.dot_general(a, b, NT_DIMS, preferred_element_type=jnp.float32)


def dot_nn(a, b):
    return lax.dot_general(a, b, NN_DIMS, preferred_element_type=jnp.float32)


def down(values):
    return jnp.sum(values, axis=0, keepdims=True)


def across(values):
    return jnp.sum(values, axis=1, keepdims=True)


def stack(values):
    return jnp.concatenate(values, axis=0)


def beside(values):
    return jnp.concatenate(values, axis=1)


def iota(shape, axis):
    return lax.broadcasted_iota(jnp.int32, shape, axis)


def my_coords():
    return lax.axis_index("z"), lax.axis_index("y"), lax.axis_index("x")


def peer_id(coords, offset):
    mz, my, mx = coords
    return (lax.rem(mz + offset[0], NZ), lax.rem(my + offset[1], NY), lax.rem(mx + offset[2] + NX, NX))


def entry_signals(coords):
    barrier = pltpu.get_barrier_semaphore()
    for offset in PEERS:
        pl.semaphore_signal(barrier, inc=1, device_id=peer_id(coords, offset), device_id_type=MESH)
    return barrier


def exchange_kernel(brick_ref, pos_ref, vel_ref, frc_ref, id_ref, ok_ref, gat_ref, pkt_ref, own_ref, raw, ids_in, oks_in, pad_ref, int_ref, send_pos, send_pkt, in_sem, pos_send_sem, pos_recv_sem, pkt_send_sem, pkt_recv_sem):
    coords = my_coords()
    fetches = [pltpu.make_async_copy(src, dst, in_sem.at[index]) for index, (src, dst) in enumerate(((pos_ref, raw.at[0]), (vel_ref, raw.at[1]), (frc_ref, raw.at[2]), (id_ref, ids_in), (ok_ref, oks_in)))]
    for fetch in fetches:
        fetch.start()
    barrier = entry_signals(coords)
    tail = slice(WIDE - LANES, WIDE)
    pad_ref[:, :, tail] = jnp.zeros((3, 4, LANES), jnp.float32)
    int_ref[:, tail] = jnp.zeros((2, LANES), jnp.int32)
    for fetch in fetches:
        fetch.wait()
    brick = brick_ref[...]
    for index in range(3):
        pad_ref[index, 0:3, 0:CAP] = raw[index]
    int_ref[0:1, 0:CAP] = ids_in[...].reshape(1, CAP)
    int_ref[1:2, 0:CAP] = oks_in[...].reshape(1, CAP)
    owned = int_ref[1:2, :] > 0
    moved, half, code = [], [], jnp.zeros((1, WIDE), jnp.int32)
    for axis, (mine, size, weight) in enumerate(((coords[2], NX, 1), (coords[1], NY, 3), (coords[0], NZ, 9))):
        box = brick * float(size)
        low = mine.astype(jnp.float32) * brick
        high = (mine + 1).astype(jnp.float32) * brick
        half_v = pad_ref[1, axis:axis + 1, :] + HALF_DT * pad_ref[2, axis:axis + 1, :]
        drift = pad_ref[0, axis:axis + 1, :] + DT * half_v
        step = jnp.where(drift >= high, 2, jnp.where(drift < low, 0, 1))
        code = code + step * weight
        wrapped = jnp.where(drift < 0.0, drift + box, jnp.where(drift >= box, drift - box, drift))
        moved.append(wrapped)
        half.append(half_v)
    code = jnp.where(owned, code, -1)
    for axis in range(3):
        for block in range(BLOCKS):
            lanes = slice(block * LANES, (block + 1) * LANES)
            send_pos[axis, block:block + 1, :] = jnp.where(owned[:, lanes], moved[axis][:, lanes], NOWHERE)
    ids = int_ref[0:1, :]
    id_hi = (lax.shift_right_logical(ids, 16) + 1).astype(jnp.float32)
    id_lo = (ids & 65535).astype(jnp.float32)
    data = stack(moved + [id_hi] + half + [id_lo])
    member = (jnp.broadcast_to(code, (32, WIDE)) == iota((32, WIDE), 0)).astype(jnp.float32)
    tri = (iota((LANES, LANES), 0) < iota((LANES, LANES), 1)).astype(jnp.bfloat16)
    codes = iota((32, LANES), 0)
    running = jnp.zeros((32, LANES), jnp.float32)
    for move, first in LANE_BASE.items():
        running = jnp.where(codes == move, float(first), running)
    slots = []
    for block in range(BLOCKS):
        part = member[:, block * LANES:(block + 1) * LANES]
        before = dot_nn(part.astype(jnp.bfloat16), tri)
        slots.append(down(part * (before + running)))
        running = running + across(part)
    slot = beside(slots)
    stay = code == STAY
    mover_slot = jnp.where(owned & jnp.logical_not(stay), slot, -1.0).astype(jnp.int32)
    pick = (iota((2 * LANES, WIDE), 0) == mover_slot).astype(jnp.float32).astype(jnp.bfloat16)
    packet = join3(dot_nt(split3(data), pick))
    send_pkt[0] = packet[:, 0:LANES]
    send_pkt[1] = packet[:, LANES:2 * LANES]
    own_ref[0:8, :] = data
    own_ref[8:16, :] = stack([jnp.where(stay, slot, -1.0), jnp.full((7, WIDE), brick, jnp.float32)])
    pl.semaphore_wait(barrier, len(PEERS))
    copies = []
    for index, (gx, gy, gz) in enumerate(GROUPS + DISTANT):
        peer = peer_id(coords, (gz, gy, gx))
        if index < N_GROUPS:
            copies.append(pltpu.make_async_remote_copy(src_ref=send_pos, dst_ref=gat_ref.at[index], send_sem=pos_send_sem.at[index], recv_sem=pos_recv_sem.at[index], device_id=peer, device_id_type=MESH))
            copies[-1].start()
            source, target = send_pkt.at[LANE_STARTS[index][0]], pkt_ref.at[index]
        else:
            source, target = send_pkt.at[0, 0:4], pkt_ref.at[index, 0:4]
        copies.append(pltpu.make_async_remote_copy(src_ref=source, dst_ref=target, send_sem=pkt_send_sem.at[index], recv_sem=pkt_recv_sem.at[index], device_id=peer, device_id_type=MESH))
        copies[-1].start()
    gat_ref[N_GROUPS] = send_pos[...]
    for copy in copies:
        copy.wait()


CAND_ROWS = 8 * (N_GROUPS + 1) + 8
MAX_ROWS = BLOCKS + CAND_ROWS
GROUPS_OWN = BLOCKS * 16
QUAD = 4
FIXED_BLOCKS = 4
PER_BLOCK = 16
FIXED_QUADS = FIXED_BLOCKS * PER_BLOCK // QUAD
FIXED_ROWS = 11
ENERGY_ROWS = 8


def pair_tools(mine, others, rc2, wrap_box):
    def powers(dist_sq):
        inv_r = lax.rsqrt(dist_sq)
        inv_2 = inv_r * inv_r
        inv_4 = inv_2 * inv_2
        term = inv_4 * inv_2 - 0.5
        return inv_r, term, term * (inv_4 * inv_4)

    cut_inv_r, cut_term, cut_core = powers(rc2)
    kappa = -RC * cut_core
    for ulps in (-3, -2, -1, 1, 2, 3):
        trial = ulps * 2.0 ** -34 - RC * cut_core
        kappa = jnp.where(trial * cut_inv_r == -cut_core, trial, kappa)

    def quad_energy(dist_sqs):
        terms, tails = [], []
        for dist_sq in dist_sqs:
            inv_r = lax.rsqrt(dist_sq)
            inv_2 = inv_r * inv_r
            term = inv_2 * inv_2 * inv_2 - 0.5
            terms.append(term * term)
            tails.append(kappa * inv_r * dist_sq)
        return ((terms[0] + terms[1]) + (terms[2] + terms[3])) - 12.0 * ((tails[0] + tails[1]) + (tails[2] + tails[3]))

    cut_energy = quad_energy([rc2] * QUAD)
    own_minus_lane = iota(TILE, 0) - iota(TILE, 1)

    def load_own(first):
        return [[mine[axis, first + k] for axis in range(3)] for k in range(QUAD)]

    def gaps(own, first, row, with_self):
        other = [others[axis, row] for axis in range(3)]
        deltas, dist_sqs = [], []
        for k in range(QUAD):
            delta = [own[k][axis] - other[axis] for axis in range(3)]
            for axis, box, inv_box in wrap_box:
                delta[axis] = delta[axis] - box * jnp.floor(delta[axis] * inv_box + 0.5)
            dist_sq = delta[0] * delta[0] + delta[1] * delta[1] + delta[2] * delta[2]
            if with_self:
                dist_sq = jnp.where(own_minus_lane == row * LANES - (first + k) * 8, rc2, dist_sq)
            deltas.append(delta)
            dist_sqs.append(jnp.minimum(dist_sq, rc2))
        return deltas, dist_sqs

    def energy_row(own, first, row, total, with_self, weight=None):
        gain = quad_energy(gaps(own, first, row, with_self)[1]) - cut_energy
        return total + (gain if weight is None else gain * weight)

    def force_row(own, first, row, force, with_self, react=None):
        force, pulls = list(force), []
        deltas, dist_sqs = gaps(own, first, row, with_self)
        for k in range(QUAD):
            inv_r, term, core = powers(dist_sqs[k])
            scale = core + kappa * inv_r
            pulls.append([scale * deltas[k][axis] for axis in range(3)])
            for axis in range(3):
                force[3 * k + axis] = force[3 * k + axis] + pulls[k][axis]
        if react is not None:
            for axis in range(3):
                react[axis, row] = react[axis, row] + ((pulls[0][axis] + pulls[1][axis]) + (pulls[2][axis] + pulls[3][axis]))
        return tuple(force)

    return load_own, energy_row, force_row


def prepare_kernel(gat_ref, pkt_ref, own_ref, sorted_ref, mine, others, acc, eng_ref):
    mz, my, mx = my_coords()
    brick = own_ref[9:10, 0:LANES]
    half_l = 0.5 * brick
    sizes = (NX, NY, NZ)
    centre = [(index.astype(jnp.float32) + 0.5) * brick for index in (mx, my, mz)]
    box = [brick * float(size) for size in sizes]
    lane_1 = iota((1, LANES), 1)
    acc[:, pl.ds(0, FIXED_QUADS * QUAD)] = jnp.zeros((3, FIXED_QUADS * QUAD, 8, LANES), jnp.float32)

    arrived = []
    for block in range(2):
        total = jnp.zeros(TILE, jnp.float32)
        for index in range(N_GROUPS):
            where_block, first, last = LANE_STARTS[index]
            if where_block == block:
                total = total + jnp.where((lane_1 >= first) & (lane_1 < last), pkt_ref[index], 0.0)
        arrived.append(total)
    arr = beside(arrived)
    arr_ok = arr[3:4] > 0.5
    stay_all = own_ref[8:9, :] >= 0.0
    n_vec = across(stay_all.astype(jnp.float32)) + across(arr_ok.astype(jnp.float32))
    n_own = jnp.max(n_vec).astype(jnp.int32)
    n_int = n_vec.astype(jnp.int32)
    quads = lax.div(n_own + (8 * QUAD - 1), 8 * QUAD)
    own_rows = lax.div(n_own + (LANES - 1), LANES)
    beyond = gat_ref[0, 0, 4:6, :]
    for slot in range(1, N_GROUPS + 1):
        beyond = jnp.minimum(beyond, gat_ref[slot, 0, 4:6, :])
    small = (jnp.min(beyond) > 0.5 * NOWHERE) & (n_own <= FIXED_BLOCKS * LANES)
    eng_ref[1] = jnp.broadcast_to(n_vec, TILE)
    wide = jnp.max(brick) >= 2.0 * RC
    int_max = 2147483647
    rc2 = RC * RC + 0.0 * own_ref[8:16, 0:LANES]
    zero = jnp.zeros(TILE, jnp.float32)
    far = jnp.full(TILE, FAR_OTHER, jnp.float32)

    def build(blocks, tile_rows):
        span = blocks * LANES
        data = beside([own_ref[0:8, 0:span], arr])
        ids = lax.shift_left(data[3:4].astype(jnp.int32) - 1, 16) + data[7:8].astype(jnp.int32)
        stay_rank = own_ref[8:9, 0:span]
        stay = stay_rank >= 0.0
        arr_id = jnp.where(arr_ok, ids[:, span:], int_max)
        own_id = jnp.where(stay, ids[:, :span], int_max)

        count_rows = (N_GROUPS + 1) * tile_rows
        cand = -(-(count_rows + len(DISTANT)) // 8) * 8
        rel = []
        for axis in range(3):
            near = [gat_ref[slot, axis, 0:tile_rows, :] for slot in range(N_GROUPS + 1)]
            distant = [jnp.where(pkt_ref[N_GROUPS + k, 3:4, :] > 0.5, pkt_ref[N_GROUPS + k, axis:axis + 1, :], NOWHERE) for k in range(len(DISTANT))]
            values = stack(near + distant + [jnp.full((cand - count_rows - len(DISTANT), LANES), NOWHERE, jnp.float32)]) - centre[axis]
            rel.append(jnp.where(values > 0.5 * box[axis], values - box[axis], jnp.where(values < -0.5 * box[axis], values + box[axis], values)))
        over = [jnp.maximum(jnp.abs(values) - half_l, 0.0) for values in rel]
        gap_sq = over[0] * over[0] + over[1] * over[1] + over[2] * over[2]
        side = jnp.zeros((cand, LANES), jnp.float32)
        for axis in range(3):
            side = 3.0 * side + jnp.where(over[2 - axis] > 0.0, jnp.where(rel[2 - axis] > 0.0, 1.0, -1.0), 0.0)
        near = gap_sq < GHOST_SQ
        mixed = jnp.where(near & (side > 0.0), 256.0, jnp.where(near & (side < 0.0), 1.0, 0.0)).astype(jnp.bfloat16)
        row_l, col_l = iota((LANES, LANES), 0), iota((LANES, LANES), 1)

        levels = beside([(row_l <= col_l)] + [row_l < 16 * k for k in range(1, 9)]).astype(jnp.float32).astype(jnp.bfloat16)
        counts = dot_nn(mixed, levels).astype(jnp.int32)
        cum, *marks, total = [counts[:, k * LANES:(k + 1) * LANES] for k in range(9)]
        arr_col = jnp.broadcast_to(arr_id, (8, 2 * LANES)).T[:, 0:1]
        arr_first = (arr_col < beside([own_id, arr_id])).astype(jnp.float32)
        arr_before = down(arr_first)
        stay_after = dot_nt(jnp.broadcast_to(stay.astype(jnp.float32), (8, span)).astype(jnp.bfloat16), arr_first[:, :span].astype(jnp.bfloat16))[0:1]
        stay_before = across(stay.astype(jnp.float32)) - stay_after
        rank = beside([jnp.where(stay, stay_rank + arr_before[:, :span], -1.0), jnp.where(arr_ok, stay_before + arr_before[:, span:], -1.0)]).astype(jnp.int32)
        earlier = (iota((cand, cand), 1) < iota((cand, cand), 0)).astype(jnp.bfloat16)
        uppers, lowers = lax.shift_right_logical(total, 8), total & 255

        bases = dot_nn(earlier, beside([uppers, lowers]).astype(jnp.float32).astype(jnp.bfloat16)).astype(jnp.int32)
        upper_base = bases[:, :LANES] + n_int
        upper_end = upper_base[cand - 1:] + uppers[cand - 1:]
        lower_base = bases[:, LANES:] + upper_end
        all_end = lower_base[cand - 1:] + lowers[cand - 1:]
        n_upper, n_all = jnp.max(upper_end), jnp.max(all_end)
        eng_ref[2] = jnp.broadcast_to(upper_end.astype(jnp.float32), TILE)
        fits = n_upper <= ENERGY_ROWS * LANES
        parts = split3(data)

        pick = (iota((span, span + 2 * LANES), 0) == rank).astype(jnp.float32).astype(jnp.bfloat16)
        chosen = dot_nt(pick, parts)

        def place_block(block):
            rows_s = join3(chosen[block * LANES:(block + 1) * LANES].T)
            sorted_ref[block] = rows_s
            valid = lane_1 + block * LANES < n_int
            own_rel = stack([rows_s[axis:axis + 1] - centre[axis] for axis in range(3)] + [rows_s[3:8]])
            columns = jnp.where(valid, own_rel, FAR_OWN).T
            for axis in range(3):
                others[axis, block] = jnp.broadcast_to(jnp.where(valid, own_rel[axis:axis + 1], 0.0), TILE)
                mine[axis, pl.ds(block * PER_BLOCK, PER_BLOCK)] = jnp.broadcast_to(columns[:, axis:axis + 1], (LANES, LANES)).reshape(16, 8, LANES)

        lane_c = iota((cand, LANES), 1)
        is_upper = lane_c < uppers
        keep = jnp.where(is_upper, -1, 255)
        bound = jnp.where(is_upper, lane_c * 256 + 255, lane_c - uppers)

        def passed(probes):
            return sum(((probe & keep) <= bound).astype(jnp.int32) for probe in probes)

        def probe_at(source, stride, number):
            return [jnp.take_along_axis(cum, source + (stride * k - 1), axis=1) for k in range(1, number + 1)]

        source = 16 * passed(marks)
        place_block(0)
        place_block(1)
        source = source + 2 * passed(probe_at(source, 2, 7))
        for block in range(2, blocks):
            place_block(block)
        source = source + passed(probe_at(source, 1, 1))
        for block in range(blocks, BLOCKS):
            sorted_ref[block] = zero

        def turned(base, each, first):
            place = (lane_c - base) & (LANES - 1)
            lane = jnp.take_along_axis(source, (first + place) & (LANES - 1), axis=1)
            target = jnp.where(place < each, lax.shift_right_logical(base + place, 7), -1)
            return target, [jnp.take_along_axis(values, lane, axis=1) for values in rel]

        def pack(target, packed, start, stop, held_rows, empty):
            def pack_row(row, carry):
                hit = target == row
                filled = lane_1 + row * LANES < n_all
                for axis in range(3):
                    held = jnp.where(row < held_rows, others[axis, row], 0.0)
                    values = held + down(jnp.where(hit, packed[axis], 0.0))
                    others[axis, row] = jnp.where(filled, values, empty)
                return carry

            lax.fori_loop(lax.div(start, LANES), lax.div(stop + (LANES - 1), LANES), pack_row, 0)

        upper_rows = lax.div(n_upper + (LANES - 1), LANES)
        rows = lax.div(n_all + (LANES - 1), LANES)
        upper_set, lower_set = turned(upper_base, uppers, 0), turned(lower_base, lowers, uppers)
        pack(*upper_set, n_own, n_upper, own_rows, 0.0)
        pack(*lower_set, n_upper, n_all, upper_rows, FAR_OTHER)

        def set_far(row, carry):
            for axis in range(3):
                others[axis, row] = far
            return carry

        def excess(first_quad, last_quad, first_row, wrap_box, energy):
            slot_8 = iota(TILE, 1)
            load_own, energy_row, force_row = pair_tools(mine, others, rc2, wrap_box)

            def quad(index, total):
                first = index * QUAD
                own = load_own(first)
                sums = (zero,) * (3 * QUAD) + (total,)

                def both(row, part):
                    slot = slot_8 + row * LANES
                    weight = 1.0 if wrap_box else jnp.where(slot < n_int, 1.0, jnp.where(slot < upper_end, 2.0, 0.0))
                    return force_row(own, first, row, part[:-1], True) + (energy_row(own, first, row, part[-1], True, weight),)

                sums = lax.fori_loop(first_row, rows, both, sums)
                for k in range(QUAD):
                    for axis in range(3):
                        acc[axis, first + k] = sums[3 * k + axis]
                return sums[-1]

            return lax.fori_loop(first_quad, last_quad, quad, energy)

        def plain():
            short = jnp.where(rows > FIXED_ROWS, jnp.minimum(quads, FIXED_QUADS), 0)
            energy = excess(0, short, FIXED_ROWS, [], zero)
            if blocks > FIXED_BLOCKS:
                energy = excess(FIXED_QUADS, quads, 0, [], energy)
            eng_ref[0] = energy
            lax.fori_loop(rows, FIXED_ROWS, set_far, 0)

        def alone(wrap_box):
            eng_ref[0] = excess(0, quads, 0, wrap_box, zero)
            lax.fori_loop(0, FIXED_ROWS, set_far, 0)

        pl.when(wide & fits)(plain)
        pl.when(wide & jnp.logical_not(fits))(lambda: alone([]))
        pl.when(jnp.logical_not(wide))(lambda: alone([(axis, box[axis], 1.0 / box[axis]) for axis in (1, 2)]))

    pl.when(small)(lambda: build(FIXED_BLOCKS, 4))
    pl.when(jnp.logical_not(small))(lambda: build(BLOCKS, BLOCKS))


def tile_kernel(mine, others, part, eng_ref, frc_ref, out_ref, acc, react, eng, slots, send_sem, recv_sem):
    coords = my_coords()
    mz, my, mx = coords
    barrier = entry_signals(coords)
    rc2 = RC * RC + 0.0 * mine[0, 0]
    load_own, energy_row, force_row = pair_tools(mine, others, rc2, [])

    lane_8 = iota(TILE, 1).astype(jnp.float32)
    energy = eng_ref[0]

    def weight_of(row, own_weight):
        slot = lane_8 + float(row * LANES)
        return jnp.where(slot < eng_ref[1], own_weight, jnp.where(slot < eng_ref[2], 2.0, 0.0))

    for block in range(FIXED_BLOCKS):

        def energy_quad(index, total, block=block):
            first = block * PER_BLOCK + index * QUAD
            own = load_own(first)
            for row in range(block, ENERGY_ROWS):
                weight = weight_of(row, 2.0 if block < row < FIXED_BLOCKS else 1.0)
                total = energy_row(own, first, row, total, row == block, weight)
            return total

        energy = lax.fori_loop(0, PER_BLOCK // QUAD, energy_quad, energy)
    eng[...] = 2.0 * down(energy)
    pl.semaphore_wait(barrier, len(PEERS))
    place = (mz * NY + my) * NX + mx
    copies = []
    for index, offset in enumerate(PEERS):
        copies.append(pltpu.make_async_remote_copy(src_ref=eng, dst_ref=slots.at[place], send_sem=send_sem.at[index], recv_sem=recv_sem.at[index], device_id=peer_id(coords, offset), device_id_type=MESH))
        copies[-1].start()
    slots[place] = eng[...]
    react[...] = jnp.zeros_like(react)
    for block in range(FIXED_BLOCKS):

        def force_quad(index, carry, block=block):
            first = block * PER_BLOCK + index * QUAD
            own = load_own(first)
            force = force_row(own, first, block, [part[axis, first + k] for k in range(QUAD) for axis in range(3)], True)
            for row in range(block + 1, FIXED_ROWS):
                force = force_row(own, first, row, force, False, react if row < FIXED_BLOCKS else None)
            for k in range(QUAD):
                for axis in range(3):
                    acc[axis, first + k] = force[3 * k + axis]
            return carry

        lax.fori_loop(0, PER_BLOCK // QUAD, force_quad, 0)
    for block in range(BLOCKS):
        held = acc if block < FIXED_BLOCKS else part
        for axis in range(3):
            turned = (held[axis, pl.ds(block * PER_BLOCK, PER_BLOCK)].reshape(LANES, LANES)).T
            force = down(turned)
            if 0 < block < FIXED_BLOCKS:
                force = force - down(react[axis, block])
            frc_ref[axis:axis + 1, block * LANES:(block + 1) * LANES] = 48.0 * force
    for copy in copies:
        copy.wait()
    total = slots[0]
    for index in range(1, NZ * NY * NX):
        total = total + slots[index]
    out_ref[...] = total


def finish_kernel(sorted_ref, frc_ref, total_ref, pos_out, vel_out, frc_out, id_out, ok_out, eng_out):
    eng_out[...] = jnp.sum(total_ref[...])
    for block in range(BLOCKS):
        width = min(LANES, CAP - block * LANES)
        lanes = slice(block * LANES, block * LANES + width)
        rows_s = sorted_ref[block]
        valid = rows_s[3:4] > 0.5
        for axis in range(3):
            force = jnp.where(valid, frc_ref[axis:axis + 1, block * LANES:(block + 1) * LANES], 0.0)
            frc_out[axis:axis + 1, lanes] = force[:, :width]
            vel_out[axis:axis + 1, lanes] = (rows_s[4 + axis:5 + axis] + HALF_DT * force)[:, :width]
            pos_out[axis:axis + 1, lanes] = rows_s[axis:axis + 1, :width]
        new_id = lax.shift_left(rows_s[3:4].astype(jnp.int32) - 1, 16) + rows_s[7:8].astype(jnp.int32)
        id_out[lanes] = jnp.where(valid, new_id, 0)[:, :width].reshape(width)
        ok_out[lanes] = valid.astype(jnp.int32)[:, :width].reshape(width)


VMEM_SPEC = pl.BlockSpec(memory_space=pltpu.VMEM)
HBM_SPEC = pl.BlockSpec(memory_space=pltpu.HBM)
VMEM_LIMIT = 8 * 1024 * 1024
SMEM_SPEC = pl.BlockSpec(memory_space=pltpu.SMEM)


def solution(mesh):
    def local_step(atom_pos, atom_vel, atom_frc, atom_id, atom_ok, brick_side):
        f32 = jnp.float32
        n_dev = NZ * NY * NX
        gat, pkt, own = pl.pallas_call(
            exchange_kernel,
            out_shape=(jax.ShapeDtypeStruct((N_GROUPS + 1, 3, BLOCKS, LANES), f32), jax.ShapeDtypeStruct((N_PACKETS, 8, LANES), f32), jax.ShapeDtypeStruct((16, WIDE), f32)),
            in_specs=[SMEM_SPEC] + [HBM_SPEC] * 5,
            out_specs=(VMEM_SPEC,) * 3,
            scratch_shapes=[
                pltpu.VMEM((3, 3, CAP), f32),
                pltpu.VMEM((CAP,), jnp.int32),
                pltpu.VMEM((CAP,), jnp.int32),
                pltpu.VMEM((3, 4, WIDE), f32),
                pltpu.VMEM((2, WIDE), jnp.int32),
                pltpu.VMEM((3, BLOCKS, LANES), f32),
                pltpu.VMEM((2, 8, LANES), f32),
                pltpu.SemaphoreType.DMA((5,)),
                pltpu.SemaphoreType.DMA((N_GROUPS,)),
                pltpu.SemaphoreType.DMA((N_GROUPS,)),
                pltpu.SemaphoreType.DMA((N_PACKETS,)),
                pltpu.SemaphoreType.DMA((N_PACKETS,)),
            ],
            compiler_params=pltpu.CompilerParams(collective_id=0, has_side_effects=True, vmem_limit_bytes=VMEM_LIMIT),
            name="exchange",
        )(brick_side, *(pltpu.with_memory_space_constraint(value, pltpu.HBM) for value in (atom_pos.T, atom_vel.T, atom_frc.T, atom_id, atom_ok)))
        own_tiles = jax.ShapeDtypeStruct((3, GROUPS_OWN, 8, LANES), f32)
        placed, mine, others, part, eng = pl.pallas_call(
            prepare_kernel,
            out_shape=(jax.ShapeDtypeStruct((BLOCKS, 8, LANES), f32), own_tiles, jax.ShapeDtypeStruct((3, MAX_ROWS, 8, LANES), f32), own_tiles, jax.ShapeDtypeStruct((3, 8, LANES), f32)),
            in_specs=[VMEM_SPEC] * 3,
            out_specs=(VMEM_SPEC,) * 5,
            compiler_params=pltpu.CompilerParams(vmem_limit_bytes=VMEM_LIMIT),
            name="prepare",
        )(gat, pkt, own)
        frc_rows, total = pl.pallas_call(
            tile_kernel,
            out_shape=(jax.ShapeDtypeStruct((8, WIDE), f32), jax.ShapeDtypeStruct((1, LANES), f32)),
            in_specs=[VMEM_SPEC] * 4,
            out_specs=(VMEM_SPEC,) * 2,
            scratch_shapes=[pltpu.VMEM((3, FIXED_BLOCKS * 16, 8, LANES), f32), pltpu.VMEM((3, FIXED_BLOCKS, 8, LANES), f32), pltpu.VMEM((1, LANES), f32), pltpu.VMEM((n_dev, 1, LANES), f32), pltpu.SemaphoreType.DMA((n_dev - 1,)), pltpu.SemaphoreType.DMA((n_dev - 1,))],
            compiler_params=pltpu.CompilerParams(collective_id=1, has_side_effects=True, vmem_limit_bytes=VMEM_LIMIT),
            name="tile",
        )(mine, others, part, eng)
        pos, vel, frc, ids, oks, energy = pl.pallas_call(
            finish_kernel,
            out_shape=(jax.ShapeDtypeStruct((3, CAP), f32),) * 3 + (jax.ShapeDtypeStruct((CAP,), jnp.int32),) * 2 + (jax.ShapeDtypeStruct((), f32),),
            in_specs=[VMEM_SPEC] * 3,
            out_specs=(VMEM_SPEC,) * 5 + (SMEM_SPEC,),
            compiler_params=pltpu.CompilerParams(vmem_limit_bytes=VMEM_LIMIT),
            name="finish",
        )(placed, frc_rows, total)
        return pos.T, vel.T, frc.T, ids, oks, energy

    row_spec = P(MESH_AXES, None)
    id_spec = P(MESH_AXES)
    return jax.shard_map(local_step, mesh=mesh, in_specs=(row_spec, row_spec, row_spec, id_spec, id_spec, P()), out_specs=(row_spec, row_spec, row_spec, id_spec, id_spec, P()), check_vma=False)
```

```python
import jax
import jax.numpy as jnp
from jax import lax
from jax.experimental import pallas as pl
from jax.experimental.pallas import tpu as pltpu
from jax.sharding import PartitionSpec as P

DT = 0.005
HALF_DT = 0.5 * DT
RC = 2.5
UPC = -48.0 * RC ** -13 + 24.0 * RC ** -7
MESH_AXES = ("z", "y", "x")
MESH = pl.DeviceIdType.MESH
NZ, NY, NX = 2, 2, 4
CAP = 729
LANES = 128
TILE = (8, LANES)
BLOCKS = 6
WIDE = BLOCKS * LANES
MOVE_CAP = CAP // 100
FAR_OWN = 1.0e4
FAR_OTHER = -1.0e4
NOWHERE = 1.0e9
GHOST_SQ = RC * RC + 0.01
PEERS = [(dz, dy, dx) for dz in range(NZ) for dy in range(NY) for dx in range(NX)][:0:-1]
SIDES = [(1, 1), (1, 0), (0, 1), (0, 0)]
GROUPS = [(gx, *side) for side in SIDES for gx in (1, -1)] + [(0, *side) for side in SIDES[:3]]
N_GROUPS = len(GROUPS)
DISTANT = [(2, *side) for side in SIDES]
N_PACKETS = N_GROUPS + len(DISTANT)


def lane_plan():
    starts, base = [], {}
    block, lane = 0, 0
    for index, (gx, gy, gz) in enumerate(GROUPS):
        if index == 8:
            block, lane = 1, 0
        dirs = [(gx, sy, sz) for sz in ((-1, 1) if gz else (0,)) for sy in ((-1, 1) if gy else (0,))]
        starts.append((block, lane, lane + MOVE_CAP * len(dirs)))
        for dx, dy, dz in dirs:
            base[(dz + 1) * 9 + (dy + 1) * 3 + dx + 1] = block * LANES + lane
            lane += MOVE_CAP
    return starts, base


LANE_STARTS, LANE_BASE = lane_plan()
STAY = 13
NT_DIMS = (((1,), (1,)), ((), ()))
NN_DIMS = (((1,), (0,)), ((), ()))


def split3(values):
    hi = values.astype(jnp.bfloat16).astype(jnp.float32)
    rest = values - hi
    mid = rest.astype(jnp.bfloat16).astype(jnp.float32)
    return jnp.concatenate([hi, mid, rest - mid], axis=0).astype(jnp.bfloat16)


def join3(parts):
    rows = parts.shape[0] // 3
    return (parts[0:rows] + parts[rows:2 * rows]) + parts[2 * rows:3 * rows]


def dot_nt(a, b):
    return lax.dot_general(a, b, NT_DIMS, preferred_element_type=jnp.float32)


def dot_nn(a, b):
    return lax.dot_general(a, b, NN_DIMS, preferred_element_type=jnp.float32)


def down(values):
    return jnp.sum(values, axis=0, keepdims=True)


def across(values):
    return jnp.sum(values, axis=1, keepdims=True)


def stack(values):
    return jnp.concatenate(values, axis=0)


def beside(values):
    return jnp.concatenate(values, axis=1)


def iota(shape, axis):
    return lax.broadcasted_iota(jnp.int32, shape, axis)


def my_coords():
    return lax.axis_index("z"), lax.axis_index("y"), lax.axis_index("x")


def peer_id(coords, offset):
    mz, my, mx = coords
    return (lax.rem(mz + offset[0], NZ), lax.rem(my + offset[1], NY), lax.rem(mx + offset[2] + NX, NX))


def entry_signals(coords):
    barrier = pltpu.get_barrier_semaphore()
    for offset in PEERS:
        pl.semaphore_signal(barrier, inc=1, device_id=peer_id(coords, offset), device_id_type=MESH)
    return barrier


def exchange_kernel(brick_ref, pos_ref, vel_ref, frc_ref, id_ref, ok_ref, gat_ref, pkt_ref, own_ref, raw, ids_in, oks_in, pad_ref, int_ref, send_pos, send_pkt, in_sem, pos_send_sem, pos_recv_sem, pkt_send_sem, pkt_recv_sem):
    coords = my_coords()
    fetches = [pltpu.make_async_copy(src, dst, in_sem.at[index]) for index, (src, dst) in enumerate(((pos_ref, raw.at[0]), (vel_ref, raw.at[1]), (frc_ref, raw.at[2]), (id_ref, ids_in), (ok_ref, oks_in)))]
    for fetch in fetches:
        fetch.start()
    barrier = entry_signals(coords)
    tail = slice(WIDE - LANES, WIDE)
    pad_ref[:, :, tail] = jnp.zeros((3, 4, LANES), jnp.float32)
    int_ref[:, tail] = jnp.zeros((2, LANES), jnp.int32)
    for fetch in fetches:
        fetch.wait()
    brick = brick_ref[...]
    for index in range(3):
        pad_ref[index, 0:3, 0:CAP] = raw[index]
    int_ref[0:1, 0:CAP] = ids_in[...].reshape(1, CAP)
    int_ref[1:2, 0:CAP] = oks_in[...].reshape(1, CAP)
    owned = int_ref[1:2, :] > 0
    moved, half, code = [], [], jnp.zeros((1, WIDE), jnp.int32)
    for axis, (mine, size, weight) in enumerate(((coords[2], NX, 1), (coords[1], NY, 3), (coords[0], NZ, 9))):
        box = brick * float(size)
        low = mine.astype(jnp.float32) * brick
        high = (mine + 1).astype(jnp.float32) * brick
        half_v = pad_ref[1, axis:axis + 1, :] + HALF_DT * pad_ref[2, axis:axis + 1, :]
        drift = pad_ref[0, axis:axis + 1, :] + DT * half_v
        step = jnp.where(drift >= high, 2, jnp.where(drift < low, 0, 1))
        code = code + step * weight
        wrapped = jnp.where(drift < 0.0, drift + box, jnp.where(drift >= box, drift - box, drift))
        moved.append(wrapped)
        half.append(half_v)
    code = jnp.where(owned, code, -1)
    for axis in range(3):
        for block in range(BLOCKS):
            lanes = slice(block * LANES, (block + 1) * LANES)
            send_pos[axis, block:block + 1, :] = jnp.where(owned[:, lanes], moved[axis][:, lanes], NOWHERE)
    ids = int_ref[0:1, :]
    id_hi = (lax.shift_right_logical(ids, 16) + 1).astype(jnp.float32)
    id_lo = (ids & 65535).astype(jnp.float32)
    data = stack(moved + [id_hi] + half + [id_lo])
    member = (jnp.broadcast_to(code, (32, WIDE)) == iota((32, WIDE), 0)).astype(jnp.float32)
    tri = (iota((LANES, LANES), 0) < iota((LANES, LANES), 1)).astype(jnp.bfloat16)
    codes = iota((32, LANES), 0)
    running = jnp.zeros((32, LANES), jnp.float32)
    for move, first in LANE_BASE.items():
        running = jnp.where(codes == move, float(first), running)
    slots = []
    for block in range(BLOCKS):
        part = member[:, block * LANES:(block + 1) * LANES]
        before = dot_nn(part.astype(jnp.bfloat16), tri)
        slots.append(down(part * (before + running)))
        running = running + across(part)
    slot = beside(slots)
    stay = code == STAY
    mover_slot = jnp.where(owned & jnp.logical_not(stay), slot, -1.0).astype(jnp.int32)
    pick = (iota((2 * LANES, WIDE), 0) == mover_slot).astype(jnp.float32).astype(jnp.bfloat16)
    packet = join3(dot_nt(split3(data), pick))
    send_pkt[0] = packet[:, 0:LANES]
    send_pkt[1] = packet[:, LANES:2 * LANES]
    own_ref[0:8, :] = data
    own_ref[8:16, :] = stack([jnp.where(stay, slot, -1.0), jnp.full((7, WIDE), brick, jnp.float32)])
    pl.semaphore_wait(barrier, len(PEERS))
    copies = []
    for index, (gx, gy, gz) in enumerate(GROUPS + DISTANT):
        peer = peer_id(coords, (gz, gy, gx))
        if index < N_GROUPS:
            copies.append(pltpu.make_async_remote_copy(src_ref=send_pos, dst_ref=gat_ref.at[index], send_sem=pos_send_sem.at[index], recv_sem=pos_recv_sem.at[index], device_id=peer, device_id_type=MESH))
            copies[-1].start()
            source, target = send_pkt.at[LANE_STARTS[index][0]], pkt_ref.at[index]
        else:
            source, target = send_pkt.at[0, 0:4], pkt_ref.at[index, 0:4]
        copies.append(pltpu.make_async_remote_copy(src_ref=source, dst_ref=target, send_sem=pkt_send_sem.at[index], recv_sem=pkt_recv_sem.at[index], device_id=peer, device_id_type=MESH))
        copies[-1].start()
    gat_ref[N_GROUPS] = send_pos[...]
    for copy in copies:
        copy.wait()


CAND_ROWS = 8 * (N_GROUPS + 1) + 8
MAX_ROWS = BLOCKS + CAND_ROWS
GROUPS_OWN = BLOCKS * 16
QUAD = 4
FIXED_BLOCKS = 4
PER_BLOCK = 16
FIXED_QUADS = FIXED_BLOCKS * PER_BLOCK // QUAD
FIXED_ROWS = 11
ENERGY_ROWS = 8


def pair_tools(mine, others, rc2, wrap_box):
    def powers(dist_sq):
        inv_r = lax.rsqrt(dist_sq)
        inv_2 = inv_r * inv_r
        inv_4 = inv_2 * inv_2
        term = inv_4 * inv_2 - 0.5
        return inv_r, term, term * (inv_4 * inv_4)

    cut_inv_r, cut_term, cut_core = powers(rc2)
    kappa = -RC * cut_core
    for ulps in (-3, -2, -1, 1, 2, 3):
        trial = ulps * 2.0 ** -34 - RC * cut_core
        kappa = jnp.where(trial * cut_inv_r == -cut_core, trial, kappa)

    def quad_energy(dist_sqs):
        terms, tails = [], []
        for dist_sq in dist_sqs:
            inv_r = lax.rsqrt(dist_sq)
            inv_2 = inv_r * inv_r
            term = inv_2 * inv_2 * inv_2 - 0.5
            terms.append(term * term)
            tails.append(kappa * inv_r * dist_sq)
        return ((terms[0] + terms[1]) + (terms[2] + terms[3])) - 12.0 * ((tails[0] + tails[1]) + (tails[2] + tails[3]))

    cut_energy = quad_energy([rc2] * QUAD)
    own_minus_lane = iota(TILE, 0) - iota(TILE, 1)

    def load_own(first):
        return [[mine[axis, first + k] for axis in range(3)] for k in range(QUAD)]

    def gaps(own, first, row, with_self):
        other = [others[axis, row] for axis in range(3)]
        deltas, dist_sqs = [], []
        for k in range(QUAD):
            delta = [own[k][axis] - other[axis] for axis in range(3)]
            for axis, box, inv_box in wrap_box:
                delta[axis] = delta[axis] - box * jnp.floor(delta[axis] * inv_box + 0.5)
            dist_sq = delta[0] * delta[0] + delta[1] * delta[1] + delta[2] * delta[2]
            if with_self:
                dist_sq = jnp.where(own_minus_lane == row * LANES - (first + k) * 8, rc2, dist_sq)
            deltas.append(delta)
            dist_sqs.append(jnp.minimum(dist_sq, rc2))
        return deltas, dist_sqs

    def energy_row(own, first, row, total, with_self, weight=None):
        gain = quad_energy(gaps(own, first, row, with_self)[1]) - cut_energy
        return total + (gain if weight is None else gain * weight)

    def force_row(own, first, row, force, with_self, react=None):
        force, pulls = list(force), []
        deltas, dist_sqs = gaps(own, first, row, with_self)
        for k in range(QUAD):
            inv_r, term, core = powers(dist_sqs[k])
            scale = core + kappa * inv_r
            pulls.append([scale * deltas[k][axis] for axis in range(3)])
            for axis in range(3):
                force[3 * k + axis] = force[3 * k + axis] + pulls[k][axis]
        if react is not None:
            for axis in range(3):
                react[axis, row] = react[axis, row] + ((pulls[0][axis] + pulls[1][axis]) + (pulls[2][axis] + pulls[3][axis]))
        return tuple(force)

    return load_own, energy_row, force_row


def spread_own(rel_ref, mine, blocks):
    for block in range(blocks):
        columns = rel_ref[block].T
        for axis in range(3):
            mine[axis, pl.ds(block * PER_BLOCK, PER_BLOCK)] = jnp.broadcast_to(columns[:, axis:axis + 1], (LANES, LANES)).reshape(PER_BLOCK, *TILE)


def prepare_kernel(gat_ref, pkt_ref, own_ref, sorted_ref, rel_ref, others, acc, eng_ref, mine):
    mz, my, mx = my_coords()
    brick = own_ref[9:10, 0:LANES]
    half_l = 0.5 * brick
    sizes = (NX, NY, NZ)
    centre = [(index.astype(jnp.float32) + 0.5) * brick for index in (mx, my, mz)]
    box = [brick * float(size) for size in sizes]
    lane_1 = iota((1, LANES), 1)
    acc[:, pl.ds(0, FIXED_QUADS * QUAD)] = jnp.zeros((3, FIXED_QUADS * QUAD, 8, LANES), jnp.float32)

    arrived = []
    for block in range(2):
        total = jnp.zeros(TILE, jnp.float32)
        for index in range(N_GROUPS):
            where_block, first, last = LANE_STARTS[index]
            if where_block == block:
                total = total + jnp.where((lane_1 >= first) & (lane_1 < last), pkt_ref[index], 0.0)
        arrived.append(total)
    arr = beside(arrived)
    arr_ok = arr[3:4] > 0.5
    stay_all = own_ref[8:9, :] >= 0.0
    n_vec = across(stay_all.astype(jnp.float32)) + across(arr_ok.astype(jnp.float32))
    n_own = jnp.max(n_vec).astype(jnp.int32)
    n_int = n_vec.astype(jnp.int32)
    quads = lax.div(n_own + (8 * QUAD - 1), 8 * QUAD)
    own_rows = lax.div(n_own + (LANES - 1), LANES)
    beyond = gat_ref[0, 0, 4:6, :]
    for slot in range(1, N_GROUPS + 1):
        beyond = jnp.minimum(beyond, gat_ref[slot, 0, 4:6, :])
    small = (jnp.min(beyond) > 0.5 * NOWHERE) & (n_own <= FIXED_BLOCKS * LANES)
    eng_ref[1] = jnp.broadcast_to(n_vec, TILE)
    wide = jnp.max(brick) >= 2.0 * RC
    int_max = 2147483647
    rc2 = RC * RC + 0.0 * own_ref[8:16, 0:LANES]
    zero = jnp.zeros(TILE, jnp.float32)
    far = jnp.full(TILE, FAR_OTHER, jnp.float32)

    def build(blocks, tile_rows):
        span = blocks * LANES
        data = beside([own_ref[0:8, 0:span], arr])
        ids = lax.shift_left(data[3:4].astype(jnp.int32) - 1, 16) + data[7:8].astype(jnp.int32)
        stay_rank = own_ref[8:9, 0:span]
        stay = stay_rank >= 0.0
        arr_id = jnp.where(arr_ok, ids[:, span:], int_max)
        own_id = jnp.where(stay, ids[:, :span], int_max)

        count_rows = (N_GROUPS + 1) * tile_rows
        cand = -(-(count_rows + len(DISTANT)) // 8) * 8
        rel = []
        for axis in range(3):
            near = [gat_ref[slot, axis, 0:tile_rows, :] for slot in range(N_GROUPS + 1)]
            distant = [jnp.where(pkt_ref[N_GROUPS + k, 3:4, :] > 0.5, pkt_ref[N_GROUPS + k, axis:axis + 1, :], NOWHERE) for k in range(len(DISTANT))]
            values = stack(near + distant + [jnp.full((cand - count_rows - len(DISTANT), LANES), NOWHERE, jnp.float32)]) - centre[axis]
            rel.append(jnp.where(values > 0.5 * box[axis], values - box[axis], jnp.where(values < -0.5 * box[axis], values + box[axis], values)))
        over = [jnp.maximum(jnp.abs(values) - half_l, 0.0) for values in rel]
        gap_sq = over[0] * over[0] + over[1] * over[1] + over[2] * over[2]
        side = jnp.zeros((cand, LANES), jnp.float32)
        for axis in range(3):
            side = 3.0 * side + jnp.where(over[2 - axis] > 0.0, jnp.where(rel[2 - axis] > 0.0, 1.0, -1.0), 0.0)
        near = gap_sq < GHOST_SQ
        mixed = jnp.where(near & (side > 0.0), 256.0, jnp.where(near & (side < 0.0), 1.0, 0.0)).astype(jnp.bfloat16)
        row_l, col_l = iota((LANES, LANES), 0), iota((LANES, LANES), 1)

        def counts(chosen):
            return dot_nn(mixed, chosen.astype(jnp.bfloat16)).astype(jnp.int32)

        cum = counts(row_l <= col_l)
        total = counts(row_l >= 0)
        marks = [counts(row_l < 16 * k) for k in range(1, 8)]
        arr_col = jnp.broadcast_to(arr_id, (8, 2 * LANES)).T[:, 0:1]
        arr_first = (arr_col < beside([own_id, arr_id])).astype(jnp.float32)
        arr_before = down(arr_first)
        stay_after = dot_nt(jnp.broadcast_to(stay.astype(jnp.float32), (8, span)).astype(jnp.bfloat16), arr_first[:, :span].astype(jnp.bfloat16))[0:1]
        stay_before = across(stay.astype(jnp.float32)) - stay_after
        rank = beside([jnp.where(stay, stay_rank + arr_before[:, :span], -1.0), jnp.where(arr_ok, stay_before + arr_before[:, span:], -1.0)]).astype(jnp.int32)
        earlier = (iota((cand, cand), 1) < iota((cand, cand), 0)).astype(jnp.bfloat16)
        uppers, lowers = lax.shift_right_logical(total, 8), total & 255

        def starts(each, first):
            base = dot_nn(earlier, each.astype(jnp.float32).astype(jnp.bfloat16)).astype(jnp.int32) + first
            return base, base[cand - 1:] + each[cand - 1:]

        upper_base, upper_end = starts(uppers, n_int)
        lower_base, all_end = starts(lowers, upper_end)
        n_upper, n_all = jnp.max(upper_end), jnp.max(all_end)
        eng_ref[2] = jnp.broadcast_to(upper_end.astype(jnp.float32), TILE)
        fits = n_upper <= ENERGY_ROWS * LANES
        parts = split3(data)

        pick = (iota((span, span + 2 * LANES), 0) == rank).astype(jnp.float32).astype(jnp.bfloat16)
        chosen = dot_nt(pick, parts)

        def place_block(block):
            rows_s = join3(chosen[block * LANES:(block + 1) * LANES].T)
            sorted_ref[block] = rows_s
            valid = lane_1 + block * LANES < n_int
            own_rel = stack([rows_s[axis:axis + 1] - centre[axis] for axis in range(3)] + [rows_s[3:8]])
            rel_ref[block] = jnp.where(valid, own_rel, FAR_OWN)
            for axis in range(3):
                others[axis, block] = jnp.broadcast_to(jnp.where(valid, own_rel[axis:axis + 1], 0.0), TILE)

        lane_c = iota((cand, LANES), 1)
        is_upper = lane_c < uppers
        keep = jnp.where(is_upper, -1, 255)
        bound = jnp.where(is_upper, lane_c * 256 + 255, lane_c - uppers)

        def passed(probes):
            return sum(((probe & keep) <= bound).astype(jnp.int32) for probe in probes)

        def probe_at(source, stride, number):
            return [jnp.take_along_axis(cum, source + (stride * k - 1), axis=1) for k in range(1, number + 1)]

        source = 16 * passed(marks)
        place_block(0)
        place_block(1)
        source = source + 2 * passed(probe_at(source, 2, 7))
        for block in range(2, blocks):
            place_block(block)
        source = source + passed(probe_at(source, 1, 1))
        for block in range(blocks, BLOCKS):
            sorted_ref[block] = zero

        def turned(base, each, first):
            place = (lane_c - base) & (LANES - 1)
            lane = jnp.take_along_axis(source, (first + place) & (LANES - 1), axis=1)
            target = jnp.where(place < each, lax.shift_right_logical(base + place, 7), -1)
            return target, [jnp.take_along_axis(values, lane, axis=1) for values in rel]

        def pack(target, packed, start, stop, held_rows, empty):
            def pack_row(row, carry):
                hit = target == row
                filled = lane_1 + row * LANES < n_all
                for axis in range(3):
                    held = jnp.where(row < held_rows, others[axis, row], 0.0)
                    values = held + down(jnp.where(hit, packed[axis], 0.0))
                    others[axis, row] = jnp.where(filled, values, empty)
                return carry

            lax.fori_loop(lax.div(start, LANES), lax.div(stop + (LANES - 1), LANES), pack_row, 0)

        upper_rows = lax.div(n_upper + (LANES - 1), LANES)
        rows = lax.div(n_all + (LANES - 1), LANES)
        upper_set, lower_set = turned(upper_base, uppers, 0), turned(lower_base, lowers, uppers)
        pack(*upper_set, n_own, n_upper, own_rows, 0.0)
        pack(*lower_set, n_upper, n_all, upper_rows, FAR_OTHER)

        def set_far(row, carry):
            for axis in range(3):
                others[axis, row] = far
            return carry

        def excess(first_quad, last_quad, first_row, wrap_box, energy):
            slot_8 = iota(TILE, 1)
            load_own, energy_row, force_row = pair_tools(mine, others, rc2, wrap_box)

            def quad(index, total):
                first = index * QUAD
                own = load_own(first)
                sums = (zero,) * (3 * QUAD) + (total,)

                def both(row, part):
                    slot = slot_8 + row * LANES
                    weight = 1.0 if wrap_box else jnp.where(slot < n_int, 1.0, jnp.where(slot < upper_end, 2.0, 0.0))
                    return force_row(own, first, row, part[:-1], True) + (energy_row(own, first, row, part[-1], True, weight),)

                sums = lax.fori_loop(first_row, rows, both, sums)
                for k in range(QUAD):
                    for axis in range(3):
                        acc[axis, first + k] = sums[3 * k + axis]
                return sums[-1]

            return lax.fori_loop(first_quad, last_quad, quad, energy)

        def leftover():
            spread_own(rel_ref, mine, blocks)
            short = jnp.where(rows > FIXED_ROWS, jnp.minimum(quads, FIXED_QUADS), 0)
            energy = excess(0, short, FIXED_ROWS, [], zero)
            if blocks > FIXED_BLOCKS:
                energy = excess(FIXED_QUADS, quads, 0, [], energy)
            eng_ref[0] = energy

        def plain():
            eng_ref[0] = zero
            pl.when((rows > FIXED_ROWS) | (quads > FIXED_QUADS))(leftover)
            lax.fori_loop(rows, FIXED_ROWS, set_far, 0)

        def alone(wrap_box):
            spread_own(rel_ref, mine, blocks)
            eng_ref[0] = excess(0, quads, 0, wrap_box, zero)
            lax.fori_loop(0, FIXED_ROWS, set_far, 0)

        pl.when(wide & fits)(plain)
        pl.when(wide & jnp.logical_not(fits))(lambda: alone([]))
        pl.when(jnp.logical_not(wide))(lambda: alone([(axis, box[axis], 1.0 / box[axis]) for axis in (1, 2)]))

    pl.when(small)(lambda: build(FIXED_BLOCKS, 4))
    pl.when(jnp.logical_not(small))(lambda: build(BLOCKS, BLOCKS))


def tile_kernel(rel_ref, others, part, eng_ref, frc_ref, out_ref, mine, acc, react, eng, slots, send_sem, recv_sem):
    coords = my_coords()
    mz, my, mx = coords
    barrier = entry_signals(coords)
    rc2 = RC * RC + 0.0 * rel_ref[0]
    spread_own(rel_ref, mine, FIXED_BLOCKS)
    load_own, energy_row, force_row = pair_tools(mine, others, rc2, [])

    lane_8 = iota(TILE, 1).astype(jnp.float32)
    energy = eng_ref[0]

    def weight_of(row, own_weight):
        slot = lane_8 + float(row * LANES)
        return jnp.where(slot < eng_ref[1], own_weight, jnp.where(slot < eng_ref[2], 2.0, 0.0))

    for block in range(FIXED_BLOCKS):

        def energy_quad(index, total, block=block):
            first = block * PER_BLOCK + index * QUAD
            own = load_own(first)
            for row in range(block, ENERGY_ROWS):
                weight = weight_of(row, 2.0 if block < row < FIXED_BLOCKS else 1.0)
                total = energy_row(own, first, row, total, row == block, weight)
            return total

        energy = lax.fori_loop(0, PER_BLOCK // QUAD, energy_quad, energy)
    eng[...] = 2.0 * down(energy)
    pl.semaphore_wait(barrier, len(PEERS))
    place = (mz * NY + my) * NX + mx
    copies = []
    for index, offset in enumerate(PEERS):
        copies.append(pltpu.make_async_remote_copy(src_ref=eng, dst_ref=slots.at[place], send_sem=send_sem.at[index], recv_sem=recv_sem.at[index], device_id=peer_id(coords, offset), device_id_type=MESH))
        copies[-1].start()
    slots[place] = eng[...]
    react[...] = jnp.zeros_like(react)
    for block in range(FIXED_BLOCKS):

        def force_quad(index, carry, block=block):
            first = block * PER_BLOCK + index * QUAD
            own = load_own(first)
            force = force_row(own, first, block, [part[axis, first + k] for k in range(QUAD) for axis in range(3)], True)
            for row in range(block + 1, FIXED_ROWS):
                force = force_row(own, first, row, force, False, react if row < FIXED_BLOCKS else None)
            for k in range(QUAD):
                for axis in range(3):
                    acc[axis, first + k] = force[3 * k + axis]
            return carry

        lax.fori_loop(0, PER_BLOCK // QUAD, force_quad, 0)
    for block in range(BLOCKS):
        held = acc if block < FIXED_BLOCKS else part
        for axis in range(3):
            turned = (held[axis, pl.ds(block * PER_BLOCK, PER_BLOCK)].reshape(LANES, LANES)).T
            force = down(turned)
            if 0 < block < FIXED_BLOCKS:
                force = force - down(react[axis, block])
            frc_ref[axis:axis + 1, block * LANES:(block + 1) * LANES] = 48.0 * force
    for copy in copies:
        copy.wait()
    total = slots[0]
    for index in range(1, NZ * NY * NX):
        total = total + slots[index]
    out_ref[...] = total


def finish_kernel(sorted_ref, frc_ref, total_ref, pos_out, vel_out, frc_out, id_out, ok_out, eng_out):
    eng_out[...] = jnp.sum(total_ref[...])
    for block in range(BLOCKS):
        width = min(LANES, CAP - block * LANES)
        lanes = slice(block * LANES, block * LANES + width)
        rows_s = sorted_ref[block]
        valid = rows_s[3:4] > 0.5
        for axis in range(3):
            force = jnp.where(valid, frc_ref[axis:axis + 1, block * LANES:(block + 1) * LANES], 0.0)
            frc_out[axis:axis + 1, lanes] = force[:, :width]
            vel_out[axis:axis + 1, lanes] = (rows_s[4 + axis:5 + axis] + HALF_DT * force)[:, :width]
            pos_out[axis:axis + 1, lanes] = rows_s[axis:axis + 1, :width]
        new_id = lax.shift_left(rows_s[3:4].astype(jnp.int32) - 1, 16) + rows_s[7:8].astype(jnp.int32)
        id_out[lanes] = jnp.where(valid, new_id, 0)[:, :width].reshape(width)
        ok_out[lanes] = valid.astype(jnp.int32)[:, :width].reshape(width)


VMEM_SPEC = pl.BlockSpec(memory_space=pltpu.VMEM)
HBM_SPEC = pl.BlockSpec(memory_space=pltpu.HBM)
VMEM_LIMIT = 8 * 1024 * 1024
SMEM_SPEC = pl.BlockSpec(memory_space=pltpu.SMEM)


def solution(mesh):
    def local_step(atom_pos, atom_vel, atom_frc, atom_id, atom_ok, brick_side):
        f32 = jnp.float32
        n_dev = NZ * NY * NX
        gat, pkt, own = pl.pallas_call(
            exchange_kernel,
            out_shape=(jax.ShapeDtypeStruct((N_GROUPS + 1, 3, BLOCKS, LANES), f32), jax.ShapeDtypeStruct((N_PACKETS, 8, LANES), f32), jax.ShapeDtypeStruct((16, WIDE), f32)),
            in_specs=[SMEM_SPEC] + [HBM_SPEC] * 5,
            out_specs=(VMEM_SPEC,) * 3,
            scratch_shapes=[
                pltpu.VMEM((3, 3, CAP), f32),
                pltpu.VMEM((CAP,), jnp.int32),
                pltpu.VMEM((CAP,), jnp.int32),
                pltpu.VMEM((3, 4, WIDE), f32),
                pltpu.VMEM((2, WIDE), jnp.int32),
                pltpu.VMEM((3, BLOCKS, LANES), f32),
                pltpu.VMEM((2, 8, LANES), f32),
                pltpu.SemaphoreType.DMA((5,)),
                pltpu.SemaphoreType.DMA((N_GROUPS,)),
                pltpu.SemaphoreType.DMA((N_GROUPS,)),
                pltpu.SemaphoreType.DMA((N_PACKETS,)),
                pltpu.SemaphoreType.DMA((N_PACKETS,)),
            ],
            compiler_params=pltpu.CompilerParams(collective_id=0, has_side_effects=True, vmem_limit_bytes=VMEM_LIMIT),
            name="exchange",
        )(brick_side, *(pltpu.with_memory_space_constraint(value, pltpu.HBM) for value in (atom_pos.T, atom_vel.T, atom_frc.T, atom_id, atom_ok)))
        own_tiles = jax.ShapeDtypeStruct((3, GROUPS_OWN, 8, LANES), f32)
        block_rows = jax.ShapeDtypeStruct((BLOCKS, 8, LANES), f32)
        placed, rel, others, part, eng = pl.pallas_call(
            prepare_kernel,
            out_shape=(block_rows, block_rows, jax.ShapeDtypeStruct((3, MAX_ROWS, 8, LANES), f32), own_tiles, jax.ShapeDtypeStruct((3, 8, LANES), f32)),
            in_specs=[VMEM_SPEC] * 3,
            out_specs=(VMEM_SPEC,) * 5,
            scratch_shapes=[pltpu.VMEM(own_tiles.shape, f32)],
            compiler_params=pltpu.CompilerParams(vmem_limit_bytes=VMEM_LIMIT),
            name="prepare",
        )(gat, pkt, own)
        frc_rows, total = pl.pallas_call(
            tile_kernel,
            out_shape=(jax.ShapeDtypeStruct((8, WIDE), f32), jax.ShapeDtypeStruct((1, LANES), f32)),
            in_specs=[VMEM_SPEC] * 4,
            out_specs=(VMEM_SPEC,) * 2,
            scratch_shapes=[pltpu.VMEM((3, FIXED_BLOCKS * PER_BLOCK, 8, LANES), f32)] * 2 + [pltpu.VMEM((3, FIXED_BLOCKS, 8, LANES), f32), pltpu.VMEM((1, LANES), f32), pltpu.VMEM((n_dev, 1, LANES), f32), pltpu.SemaphoreType.DMA((n_dev - 1,)), pltpu.SemaphoreType.DMA((n_dev - 1,))],
            compiler_params=pltpu.CompilerParams(collective_id=1, has_side_effects=True, vmem_limit_bytes=VMEM_LIMIT),
            name="tile",
        )(rel, others, part, eng)
        pos, vel, frc, ids, oks, energy = pl.pallas_call(
            finish_kernel,
            out_shape=(jax.ShapeDtypeStruct((3, CAP), f32),) * 3 + (jax.ShapeDtypeStruct((CAP,), jnp.int32),) * 2 + (jax.ShapeDtypeStruct((), f32),),
            in_specs=[VMEM_SPEC] * 3,
            out_specs=(VMEM_SPEC,) * 5 + (SMEM_SPEC,),
            compiler_params=pltpu.CompilerParams(vmem_limit_bytes=VMEM_LIMIT),
            name="finish",
        )(placed, frc_rows, total)
        return pos.T, vel.T, frc.T, ids, oks, energy

    row_spec = P(MESH_AXES, None)
    id_spec = P(MESH_AXES)
    return jax.shard_map(local_step, mesh=mesh, in_specs=(row_spec, row_spec, row_spec, id_spec, id_spec, P()), out_specs=(row_spec, row_spec, row_spec, id_spec, id_spec, P()), check_vma=False)
```

```python
import jax
import jax.numpy as jnp
from jax import lax
from jax.experimental import pallas as pl
from jax.experimental.pallas import tpu as pltpu
from jax.sharding import PartitionSpec as P

DT = 0.005
HALF_DT = 0.5 * DT
RC = 2.5
UPC = -48.0 * RC ** -13 + 24.0 * RC ** -7
MESH_AXES = ("z", "y", "x")
MESH = pl.DeviceIdType.MESH
NZ, NY, NX = 2, 2, 4
CAP = 729
LANES = 128
TILE = (8, LANES)
BLOCKS = 6
WIDE = BLOCKS * LANES
MOVE_CAP = CAP // 100
FAR_OWN = 1.0e4
FAR_OTHER = -1.0e4
NOWHERE = 1.0e9
GHOST_SQ = RC * RC + 0.01
PEERS = [(dz, dy, dx) for dz in range(NZ) for dy in range(NY) for dx in range(NX)][:0:-1]
SIDES = [(1, 1), (1, 0), (0, 1), (0, 0)]
GROUPS = [(gx, *side) for side in SIDES for gx in (1, -1)] + [(0, *side) for side in SIDES[:3]]
N_GROUPS = len(GROUPS)
DISTANT = [(2, *side) for side in SIDES]
N_PACKETS = N_GROUPS + len(DISTANT)


def lane_plan():
    starts, base = [], {}
    block, lane = 0, 0
    for index, (gx, gy, gz) in enumerate(GROUPS):
        if index == 8:
            block, lane = 1, 0
        dirs = [(gx, sy, sz) for sz in ((-1, 1) if gz else (0,)) for sy in ((-1, 1) if gy else (0,))]
        starts.append((block, lane, lane + MOVE_CAP * len(dirs)))
        for dx, dy, dz in dirs:
            base[(dz + 1) * 9 + (dy + 1) * 3 + dx + 1] = block * LANES + lane
            lane += MOVE_CAP
    return starts, base


LANE_STARTS, LANE_BASE = lane_plan()
STAY = 13
NT_DIMS = (((1,), (1,)), ((), ()))
NN_DIMS = (((1,), (0,)), ((), ()))


def split3(values):
    hi = values.astype(jnp.bfloat16).astype(jnp.float32)
    rest = values - hi
    mid = rest.astype(jnp.bfloat16).astype(jnp.float32)
    return jnp.concatenate([hi, mid, rest - mid], axis=0).astype(jnp.bfloat16)


def join3(parts):
    rows = parts.shape[0] // 3
    return (parts[0:rows] + parts[rows:2 * rows]) + parts[2 * rows:3 * rows]


def dot_nt(a, b):
    return lax.dot_general(a, b, NT_DIMS, preferred_element_type=jnp.float32)


def dot_nn(a, b):
    return lax.dot_general(a, b, NN_DIMS, preferred_element_type=jnp.float32)


def down(values):
    return jnp.sum(values, axis=0, keepdims=True)


def across(values):
    return jnp.sum(values, axis=1, keepdims=True)


def stack(values):
    return jnp.concatenate(values, axis=0)


def beside(values):
    return jnp.concatenate(values, axis=1)


def iota(shape, axis):
    return lax.broadcasted_iota(jnp.int32, shape, axis)


def my_coords():
    return lax.axis_index("z"), lax.axis_index("y"), lax.axis_index("x")


def peer_id(coords, offset):
    mz, my, mx = coords
    return (lax.rem(mz + offset[0], NZ), lax.rem(my + offset[1], NY), lax.rem(mx + offset[2] + NX, NX))


def entry_signals(coords):
    barrier = pltpu.get_barrier_semaphore()
    for offset in PEERS:
        pl.semaphore_signal(barrier, inc=1, device_id=peer_id(coords, offset), device_id_type=MESH)
    return barrier


def exchange_kernel(brick_ref, pos_ref, vel_ref, frc_ref, id_ref, ok_ref, gat_ref, pkt_ref, own_ref, raw, ids_in, oks_in, pad_ref, int_ref, send_pos, send_pkt, in_sem, pos_send_sem, pos_recv_sem, pkt_send_sem, pkt_recv_sem):
    coords = my_coords()
    fetches = [pltpu.make_async_copy(src, dst, in_sem.at[index]) for index, (src, dst) in enumerate(((pos_ref, raw.at[0]), (vel_ref, raw.at[1]), (frc_ref, raw.at[2]), (id_ref, ids_in), (ok_ref, oks_in)))]
    for fetch in fetches:
        fetch.start()
    barrier = entry_signals(coords)
    tail = slice(WIDE - LANES, WIDE)
    pad_ref[:, :, tail] = jnp.zeros((3, 4, LANES), jnp.float32)
    int_ref[:, tail] = jnp.zeros((2, LANES), jnp.int32)
    for fetch in fetches:
        fetch.wait()
    brick = brick_ref[...]
    for index in range(3):
        pad_ref[index, 0:3, 0:CAP] = raw[index]
    int_ref[0:1, 0:CAP] = ids_in[...].reshape(1, CAP)
    int_ref[1:2, 0:CAP] = oks_in[...].reshape(1, CAP)
    owned = int_ref[1:2, :] > 0
    moved, half, code = [], [], jnp.zeros((1, WIDE), jnp.int32)
    for axis, (mine, size, weight) in enumerate(((coords[2], NX, 1), (coords[1], NY, 3), (coords[0], NZ, 9))):
        box = brick * float(size)
        low = mine.astype(jnp.float32) * brick
        high = (mine + 1).astype(jnp.float32) * brick
        half_v = pad_ref[1, axis:axis + 1, :] + HALF_DT * pad_ref[2, axis:axis + 1, :]
        drift = pad_ref[0, axis:axis + 1, :] + DT * half_v
        step = jnp.where(drift >= high, 2, jnp.where(drift < low, 0, 1))
        code = code + step * weight
        wrapped = jnp.where(drift < 0.0, drift + box, jnp.where(drift >= box, drift - box, drift))
        moved.append(wrapped)
        half.append(half_v)
    code = jnp.where(owned, code, -1)
    for axis in range(3):
        for block in range(BLOCKS):
            lanes = slice(block * LANES, (block + 1) * LANES)
            send_pos[axis, block:block + 1, :] = jnp.where(owned[:, lanes], moved[axis][:, lanes], NOWHERE)
    ids = int_ref[0:1, :]
    id_hi = (lax.shift_right_logical(ids, 16) + 1).astype(jnp.float32)
    id_lo = (ids & 65535).astype(jnp.float32)
    data = stack(moved + [id_hi] + half + [id_lo])
    member = (jnp.broadcast_to(code, (32, WIDE)) == iota((32, WIDE), 0)).astype(jnp.float32)
    tri = (iota((LANES, LANES), 0) < iota((LANES, LANES), 1)).astype(jnp.bfloat16)
    codes = iota((32, LANES), 0)
    running = jnp.zeros((32, LANES), jnp.float32)
    for move, first in LANE_BASE.items():
        running = jnp.where(codes == move, float(first), running)
    pieces = [member[:, block * LANES:(block + 1) * LANES] for block in range(BLOCKS)]
    before = dot_nn(stack(pieces).astype(jnp.bfloat16), tri)
    slots = []
    for block, part in enumerate(pieces):
        slots.append(down(part * (before[32 * block:32 * block + 32] + running)))
        running = running + across(part)
    slot = beside(slots)
    stay = code == STAY
    mover_slot = jnp.where(owned & jnp.logical_not(stay), slot, -1.0).astype(jnp.int32)
    pick = (iota((2 * LANES, WIDE), 0) == mover_slot).astype(jnp.float32).astype(jnp.bfloat16)
    packet = join3(dot_nt(split3(data), pick))
    send_pkt[0] = packet[:, 0:LANES]
    send_pkt[1] = packet[:, LANES:2 * LANES]
    own_ref[0:8, :] = data
    own_ref[8:16, :] = stack([jnp.where(stay, slot, -1.0), jnp.full((7, WIDE), brick, jnp.float32)])
    pl.semaphore_wait(barrier, len(PEERS))
    copies = []
    for index, (gx, gy, gz) in enumerate(GROUPS + DISTANT):
        peer = peer_id(coords, (gz, gy, gx))
        if index < N_GROUPS:
            copies.append(pltpu.make_async_remote_copy(src_ref=send_pos, dst_ref=gat_ref.at[index], send_sem=pos_send_sem.at[index], recv_sem=pos_recv_sem.at[index], device_id=peer, device_id_type=MESH))
            copies[-1].start()
            source, target = send_pkt.at[LANE_STARTS[index][0]], pkt_ref.at[index]
        else:
            source, target = send_pkt.at[0, 0:4], pkt_ref.at[index, 0:4]
        copies.append(pltpu.make_async_remote_copy(src_ref=source, dst_ref=target, send_sem=pkt_send_sem.at[index], recv_sem=pkt_recv_sem.at[index], device_id=peer, device_id_type=MESH))
        copies[-1].start()
    gat_ref[N_GROUPS] = send_pos[...]
    for copy in copies:
        copy.wait()


CAND_ROWS = 8 * (N_GROUPS + 1) + 8
MAX_ROWS = BLOCKS + CAND_ROWS
GROUPS_OWN = BLOCKS * 16
QUAD = 4
FIXED_BLOCKS = 4
PER_BLOCK = 16
FIXED_QUADS = FIXED_BLOCKS * PER_BLOCK // QUAD
FIXED_ROWS = 11
ENERGY_ROWS = 8


def pair_tools(mine, others, rc2, wrap_box):
    def powers(dist_sq):
        inv_r = lax.rsqrt(dist_sq)
        inv_2 = inv_r * inv_r
        inv_4 = inv_2 * inv_2
        term = inv_4 * inv_2 - 0.5
        return inv_r, term, term * (inv_4 * inv_4)

    cut_inv_r, cut_term, cut_core = powers(rc2)
    kappa = -RC * cut_core
    for ulps in (-3, -2, -1, 1, 2, 3):
        trial = ulps * 2.0 ** -34 - RC * cut_core
        kappa = jnp.where(trial * cut_inv_r == -cut_core, trial, kappa)

    def quad_energy(dist_sqs):
        terms, tails = [], []
        for dist_sq in dist_sqs:
            inv_r = lax.rsqrt(dist_sq)
            inv_2 = inv_r * inv_r
            term = inv_2 * inv_2 * inv_2 - 0.5
            terms.append(term * term)
            tails.append(kappa * inv_r * dist_sq)
        return ((terms[0] + terms[1]) + (terms[2] + terms[3])) - 12.0 * ((tails[0] + tails[1]) + (tails[2] + tails[3]))

    cut_energy = quad_energy([rc2] * QUAD)
    own_minus_lane = iota(TILE, 0) - iota(TILE, 1)

    def load_own(first):
        return [[mine[axis, first + k] for axis in range(3)] for k in range(QUAD)]

    def gaps(own, first, row, with_self):
        other = [others[axis, row] for axis in range(3)]
        deltas, dist_sqs = [], []
        for k in range(QUAD):
            delta = [own[k][axis] - other[axis] for axis in range(3)]
            for axis, box, inv_box in wrap_box:
                delta[axis] = delta[axis] - box * jnp.floor(delta[axis] * inv_box + 0.5)
            dist_sq = delta[0] * delta[0] + delta[1] * delta[1] + delta[2] * delta[2]
            if with_self:
                dist_sq = jnp.where(own_minus_lane == row * LANES - (first + k) * 8, rc2, dist_sq)
            deltas.append(delta)
            dist_sqs.append(jnp.minimum(dist_sq, rc2))
        return deltas, dist_sqs

    def energy_row(own, first, row, total, with_self, weight=None):
        gain = quad_energy(gaps(own, first, row, with_self)[1]) - cut_energy
        return total + (gain if weight is None else gain * weight)

    def force_row(own, first, row, force, with_self, react=None):
        force, pulls = list(force), []
        deltas, dist_sqs = gaps(own, first, row, with_self)
        for k in range(QUAD):
            inv_r, term, core = powers(dist_sqs[k])
            scale = core + kappa * inv_r
            pulls.append([scale * deltas[k][axis] for axis in range(3)])
            for axis in range(3):
                force[3 * k + axis] = force[3 * k + axis] + pulls[k][axis]
        if react is not None:
            for axis in range(3):
                react[axis, row] = react[axis, row] + ((pulls[0][axis] + pulls[1][axis]) + (pulls[2][axis] + pulls[3][axis]))
        return tuple(force)

    return load_own, energy_row, force_row


def spread_own(rel_ref, mine, blocks):
    for block in range(blocks):
        columns = rel_ref[block].T
        for axis in range(3):
            mine[axis, pl.ds(block * PER_BLOCK, PER_BLOCK)] = jnp.broadcast_to(columns[:, axis:axis + 1], (LANES, LANES)).reshape(PER_BLOCK, *TILE)


def prepare_kernel(gat_ref, pkt_ref, own_ref, sorted_ref, rel_ref, others, acc, eng_ref, mine):
    mz, my, mx = my_coords()
    brick = own_ref[9:10, 0:LANES]
    half_l = 0.5 * brick
    sizes = (NX, NY, NZ)
    centre = [(index.astype(jnp.float32) + 0.5) * brick for index in (mx, my, mz)]
    box = [brick * float(size) for size in sizes]
    lane_1 = iota((1, LANES), 1)
    acc[:, pl.ds(0, FIXED_QUADS * QUAD)] = jnp.zeros((3, FIXED_QUADS * QUAD, 8, LANES), jnp.float32)

    arrived = []
    for block in range(2):
        total = jnp.zeros(TILE, jnp.float32)
        for index in range(N_GROUPS):
            where_block, first, last = LANE_STARTS[index]
            if where_block == block:
                total = total + jnp.where((lane_1 >= first) & (lane_1 < last), pkt_ref[index], 0.0)
        arrived.append(total)
    arr = beside(arrived)
    arr_ok = arr[3:4] > 0.5
    stay_all = own_ref[8:9, :] >= 0.0
    n_vec = across(stay_all.astype(jnp.float32)) + across(arr_ok.astype(jnp.float32))
    n_own = jnp.max(n_vec).astype(jnp.int32)
    n_int = n_vec.astype(jnp.int32)
    quads = lax.div(n_own + (8 * QUAD - 1), 8 * QUAD)
    own_rows = lax.div(n_own + (LANES - 1), LANES)
    beyond = gat_ref[0, 0, 4:6, :]
    for slot in range(1, N_GROUPS + 1):
        beyond = jnp.minimum(beyond, gat_ref[slot, 0, 4:6, :])
    small = (jnp.min(beyond) > 0.5 * NOWHERE) & (n_own <= FIXED_BLOCKS * LANES)
    eng_ref[1] = jnp.broadcast_to(n_vec, TILE)
    wide = jnp.max(brick) >= 2.0 * RC
    int_max = 2147483647
    rc2 = RC * RC + 0.0 * own_ref[8:16, 0:LANES]
    zero = jnp.zeros(TILE, jnp.float32)
    far = jnp.full(TILE, FAR_OTHER, jnp.float32)

    def build(blocks, tile_rows):
        span = blocks * LANES
        data = beside([own_ref[0:8, 0:span], arr])
        ids = lax.shift_left(data[3:4].astype(jnp.int32) - 1, 16) + data[7:8].astype(jnp.int32)
        stay_rank = own_ref[8:9, 0:span]
        stay = stay_rank >= 0.0
        arr_id = jnp.where(arr_ok, ids[:, span:], int_max)
        own_id = jnp.where(stay, ids[:, :span], int_max)

        count_rows = (N_GROUPS + 1) * tile_rows
        cand = -(-(count_rows + len(DISTANT)) // 8) * 8
        rel = []
        for axis in range(3):
            near = [gat_ref[slot, axis, 0:tile_rows, :] for slot in range(N_GROUPS + 1)]
            distant = [jnp.where(pkt_ref[N_GROUPS + k, 3:4, :] > 0.5, pkt_ref[N_GROUPS + k, axis:axis + 1, :], NOWHERE) for k in range(len(DISTANT))]
            values = stack(near + distant + [jnp.full((cand - count_rows - len(DISTANT), LANES), NOWHERE, jnp.float32)]) - centre[axis]
            rel.append(jnp.where(values > 0.5 * box[axis], values - box[axis], jnp.where(values < -0.5 * box[axis], values + box[axis], values)))
        over = [jnp.maximum(jnp.abs(values) - half_l, 0.0) for values in rel]
        gap_sq = over[0] * over[0] + over[1] * over[1] + over[2] * over[2]
        side = jnp.zeros((cand, LANES), jnp.float32)
        for axis in range(3):
            side = 3.0 * side + jnp.where(over[2 - axis] > 0.0, jnp.where(rel[2 - axis] > 0.0, 1.0, -1.0), 0.0)
        near = gap_sq < GHOST_SQ
        mixed = jnp.where(near & (side > 0.0), 256.0, jnp.where(near & (side < 0.0), 1.0, 0.0)).astype(jnp.bfloat16)
        row_l, col_l = iota((LANES, LANES), 0), iota((LANES, LANES), 1)

        def counts(chosen):
            return dot_nn(mixed, chosen.astype(jnp.bfloat16)).astype(jnp.int32)

        cum = counts(row_l <= col_l)
        total = counts(row_l >= 0)
        marks = [counts(row_l < 16 * k) for k in range(1, 8)]
        arr_col = jnp.broadcast_to(arr_id, (8, 2 * LANES)).T[:, 0:1]
        arr_first = (arr_col < beside([own_id, arr_id])).astype(jnp.float32)
        arr_before = down(arr_first)
        stay_after = dot_nt(jnp.broadcast_to(stay.astype(jnp.float32), (8, span)).astype(jnp.bfloat16), arr_first[:, :span].astype(jnp.bfloat16))[0:1]
        stay_before = across(stay.astype(jnp.float32)) - stay_after
        rank = beside([jnp.where(stay, stay_rank + arr_before[:, :span], -1.0), jnp.where(arr_ok, stay_before + arr_before[:, span:], -1.0)]).astype(jnp.int32)
        earlier = (iota((cand, cand), 1) < iota((cand, cand), 0)).astype(jnp.bfloat16)
        uppers, lowers = lax.shift_right_logical(total, 8), total & 255

        def starts(each, first):
            base = dot_nn(earlier, each.astype(jnp.float32).astype(jnp.bfloat16)).astype(jnp.int32) + first
            return base, base[cand - 1:] + each[cand - 1:]

        upper_base, upper_end = starts(uppers, n_int)
        lower_base, all_end = starts(lowers, upper_end)
        n_upper, n_all = jnp.max(upper_end), jnp.max(all_end)
        eng_ref[2] = jnp.broadcast_to(upper_end.astype(jnp.float32), TILE)
        fits = n_upper <= ENERGY_ROWS * LANES
        parts = split3(data)

        pick = (iota((span, span + 2 * LANES), 0) == rank).astype(jnp.float32).astype(jnp.bfloat16)
        chosen = dot_nt(pick, parts)

        def place_block(block):
            rows_s = join3(chosen[block * LANES:(block + 1) * LANES].T)
            sorted_ref[block] = rows_s
            valid = lane_1 + block * LANES < n_int
            own_rel = stack([rows_s[axis:axis + 1] - centre[axis] for axis in range(3)] + [rows_s[3:8]])
            rel_ref[block] = jnp.where(valid, own_rel, FAR_OWN)
            for axis in range(3):
                others[axis, block] = jnp.broadcast_to(jnp.where(valid, own_rel[axis:axis + 1], 0.0), TILE)

        lane_c = iota((cand, LANES), 1)
        is_upper = lane_c < uppers
        keep = jnp.where(is_upper, -1, 255)
        bound = jnp.where(is_upper, lane_c * 256 + 255, lane_c - uppers)

        def passed(probes):
            return sum(((probe & keep) <= bound).astype(jnp.int32) for probe in probes)

        def probe_at(source, stride, number):
            return [jnp.take_along_axis(cum, source + (stride * k - 1), axis=1) for k in range(1, number + 1)]

        source = 16 * passed(marks)
        place_block(0)
        place_block(1)
        source = source + 2 * passed(probe_at(source, 2, 7))
        for block in range(2, blocks):
            place_block(block)
        source = source + passed(probe_at(source, 1, 1))
        for block in range(blocks, BLOCKS):
            sorted_ref[block] = zero

        def turned(base, each, first):
            place = (lane_c - base) & (LANES - 1)
            lane = jnp.take_along_axis(source, (first + place) & (LANES - 1), axis=1)
            target = jnp.where(place < each, lax.shift_right_logical(base + place, 7), -1)
            return target, [jnp.take_along_axis(values, lane, axis=1) for values in rel]

        def pack(target, packed, start, stop, held_rows, empty):
            def pack_row(row, carry):
                hit = target == row
                filled = lane_1 + row * LANES < n_all
                for axis in range(3):
                    held = jnp.where(row < held_rows, others[axis, row], 0.0)
                    values = held + down(jnp.where(hit, packed[axis], 0.0))
                    others[axis, row] = jnp.where(filled, values, empty)
                return carry

            lax.fori_loop(lax.div(start, LANES), lax.div(stop + (LANES - 1), LANES), pack_row, 0)

        upper_rows = lax.div(n_upper + (LANES - 1), LANES)
        rows = lax.div(n_all + (LANES - 1), LANES)
        upper_set, lower_set = turned(upper_base, uppers, 0), turned(lower_base, lowers, uppers)
        pack(*upper_set, n_own, n_upper, own_rows, 0.0)
        pack(*lower_set, n_upper, n_all, upper_rows, FAR_OTHER)

        def set_far(row, carry):
            for axis in range(3):
                others[axis, row] = far
            return carry

        def excess(first_quad, last_quad, first_row, wrap_box, energy):
            slot_8 = iota(TILE, 1)
            load_own, energy_row, force_row = pair_tools(mine, others, rc2, wrap_box)

            def quad(index, total):
                first = index * QUAD
                own = load_own(first)
                sums = (zero,) * (3 * QUAD) + (total,)

                def both(row, part):
                    slot = slot_8 + row * LANES
                    weight = 1.0 if wrap_box else jnp.where(slot < n_int, 1.0, jnp.where(slot < upper_end, 2.0, 0.0))
                    return force_row(own, first, row, part[:-1], True) + (energy_row(own, first, row, part[-1], True, weight),)

                sums = lax.fori_loop(first_row, rows, both, sums)
                for k in range(QUAD):
                    for axis in range(3):
                        acc[axis, first + k] = sums[3 * k + axis]
                return sums[-1]

            return lax.fori_loop(first_quad, last_quad, quad, energy)

        def leftover():
            spread_own(rel_ref, mine, blocks)
            short = jnp.where(rows > FIXED_ROWS, jnp.minimum(quads, FIXED_QUADS), 0)
            energy = excess(0, short, FIXED_ROWS, [], zero)
            if blocks > FIXED_BLOCKS:
                energy = excess(FIXED_QUADS, quads, 0, [], energy)
            eng_ref[0] = energy

        def plain():
            eng_ref[0] = zero
            pl.when((rows > FIXED_ROWS) | (quads > FIXED_QUADS))(leftover)
            lax.fori_loop(rows, FIXED_ROWS, set_far, 0)

        def alone(wrap_box):
            spread_own(rel_ref, mine, blocks)
            eng_ref[0] = excess(0, quads, 0, wrap_box, zero)
            lax.fori_loop(0, FIXED_ROWS, set_far, 0)

        pl.when(wide & fits)(plain)
        pl.when(wide & jnp.logical_not(fits))(lambda: alone([]))
        pl.when(jnp.logical_not(wide))(lambda: alone([(axis, box[axis], 1.0 / box[axis]) for axis in (1, 2)]))

    pl.when(small)(lambda: build(FIXED_BLOCKS, 4))
    pl.when(jnp.logical_not(small))(lambda: build(BLOCKS, BLOCKS))


def tile_kernel(rel_ref, others, part, eng_ref, frc_ref, out_ref, mine, acc, react, eng, slots, send_sem, recv_sem):
    coords = my_coords()
    mz, my, mx = coords
    barrier = entry_signals(coords)
    rc2 = RC * RC + 0.0 * rel_ref[0]
    spread_own(rel_ref, mine, FIXED_BLOCKS)
    load_own, energy_row, force_row = pair_tools(mine, others, rc2, [])

    lane_8 = iota(TILE, 1).astype(jnp.float32)
    energy = eng_ref[0]

    def weight_of(row, own_weight):
        slot = lane_8 + float(row * LANES)
        return jnp.where(slot < eng_ref[1], own_weight, jnp.where(slot < eng_ref[2], 2.0, 0.0))

    for block in range(FIXED_BLOCKS):

        def energy_quad(index, total, block=block):
            first = block * PER_BLOCK + index * QUAD
            own = load_own(first)
            for row in range(block, ENERGY_ROWS):
                weight = weight_of(row, 2.0 if block < row < FIXED_BLOCKS else 1.0)
                total = energy_row(own, first, row, total, row == block, weight)
            return total

        energy = lax.fori_loop(0, PER_BLOCK // QUAD, energy_quad, energy)
    eng[...] = 2.0 * down(energy)
    pl.semaphore_wait(barrier, len(PEERS))
    place = (mz * NY + my) * NX + mx
    copies = []
    for index, offset in enumerate(PEERS):
        copies.append(pltpu.make_async_remote_copy(src_ref=eng, dst_ref=slots.at[place], send_sem=send_sem.at[index], recv_sem=recv_sem.at[index], device_id=peer_id(coords, offset), device_id_type=MESH))
        copies[-1].start()
    slots[place] = eng[...]
    react[...] = jnp.zeros_like(react)
    for block in range(FIXED_BLOCKS):

        def force_quad(index, carry, block=block):
            first = block * PER_BLOCK + index * QUAD
            own = load_own(first)
            force = force_row(own, first, block, [part[axis, first + k] for k in range(QUAD) for axis in range(3)], True)
            for row in range(block + 1, FIXED_ROWS):
                force = force_row(own, first, row, force, False, react if row < FIXED_BLOCKS else None)
            for k in range(QUAD):
                for axis in range(3):
                    acc[axis, first + k] = force[3 * k + axis]
            return carry

        lax.fori_loop(0, PER_BLOCK // QUAD, force_quad, 0)
    for block in range(BLOCKS):
        held = acc if block < FIXED_BLOCKS else part
        for axis in range(3):
            turned = (held[axis, pl.ds(block * PER_BLOCK, PER_BLOCK)].reshape(LANES, LANES)).T
            force = down(turned)
            if 0 < block < FIXED_BLOCKS:
                force = force - down(react[axis, block])
            frc_ref[axis:axis + 1, block * LANES:(block + 1) * LANES] = 48.0 * force
    for copy in copies:
        copy.wait()
    total = slots[0]
    for index in range(1, NZ * NY * NX):
        total = total + slots[index]
    out_ref[...] = total


def finish_kernel(sorted_ref, frc_ref, total_ref, pos_out, vel_out, frc_out, id_out, ok_out, eng_out):
    eng_out[...] = jnp.sum(total_ref[...])
    for block in range(BLOCKS):
        width = min(LANES, CAP - block * LANES)
        lanes = slice(block * LANES, block * LANES + width)
        rows_s = sorted_ref[block]
        valid = rows_s[3:4] > 0.5
        for axis in range(3):
            force = jnp.where(valid, frc_ref[axis:axis + 1, block * LANES:(block + 1) * LANES], 0.0)
            frc_out[axis:axis + 1, lanes] = force[:, :width]
            vel_out[axis:axis + 1, lanes] = (rows_s[4 + axis:5 + axis] + HALF_DT * force)[:, :width]
            pos_out[axis:axis + 1, lanes] = rows_s[axis:axis + 1, :width]
        new_id = lax.shift_left(rows_s[3:4].astype(jnp.int32) - 1, 16) + rows_s[7:8].astype(jnp.int32)
        id_out[lanes] = jnp.where(valid, new_id, 0)[:, :width].reshape(width)
        ok_out[lanes] = valid.astype(jnp.int32)[:, :width].reshape(width)


VMEM_SPEC = pl.BlockSpec(memory_space=pltpu.VMEM)
HBM_SPEC = pl.BlockSpec(memory_space=pltpu.HBM)
VMEM_LIMIT = 8 * 1024 * 1024
SMEM_SPEC = pl.BlockSpec(memory_space=pltpu.SMEM)


def solution(mesh):
    def local_step(atom_pos, atom_vel, atom_frc, atom_id, atom_ok, brick_side):
        f32 = jnp.float32
        n_dev = NZ * NY * NX
        gat, pkt, own = pl.pallas_call(
            exchange_kernel,
            out_shape=(jax.ShapeDtypeStruct((N_GROUPS + 1, 3, BLOCKS, LANES), f32), jax.ShapeDtypeStruct((N_PACKETS, 8, LANES), f32), jax.ShapeDtypeStruct((16, WIDE), f32)),
            in_specs=[SMEM_SPEC] + [HBM_SPEC] * 5,
            out_specs=(VMEM_SPEC,) * 3,
            scratch_shapes=[
                pltpu.VMEM((3, 3, CAP), f32),
                pltpu.VMEM((CAP,), jnp.int32),
                pltpu.VMEM((CAP,), jnp.int32),
                pltpu.VMEM((3, 4, WIDE), f32),
                pltpu.VMEM((2, WIDE), jnp.int32),
                pltpu.VMEM((3, BLOCKS, LANES), f32),
                pltpu.VMEM((2, 8, LANES), f32),
                pltpu.SemaphoreType.DMA((5,)),
                pltpu.SemaphoreType.DMA((N_GROUPS,)),
                pltpu.SemaphoreType.DMA((N_GROUPS,)),
                pltpu.SemaphoreType.DMA((N_PACKETS,)),
                pltpu.SemaphoreType.DMA((N_PACKETS,)),
            ],
            compiler_params=pltpu.CompilerParams(collective_id=0, has_side_effects=True, vmem_limit_bytes=VMEM_LIMIT),
            name="exchange",
        )(brick_side, *(pltpu.with_memory_space_constraint(value, pltpu.HBM) for value in (atom_pos.T, atom_vel.T, atom_frc.T, atom_id, atom_ok)))
        own_tiles = jax.ShapeDtypeStruct((3, GROUPS_OWN, 8, LANES), f32)
        block_rows = jax.ShapeDtypeStruct((BLOCKS, 8, LANES), f32)
        placed, rel, others, part, eng = pl.pallas_call(
            prepare_kernel,
            out_shape=(block_rows, block_rows, jax.ShapeDtypeStruct((3, MAX_ROWS, 8, LANES), f32), own_tiles, jax.ShapeDtypeStruct((3, 8, LANES), f32)),
            in_specs=[VMEM_SPEC] * 3,
            out_specs=(VMEM_SPEC,) * 5,
            scratch_shapes=[pltpu.VMEM(own_tiles.shape, f32)],
            compiler_params=pltpu.CompilerParams(vmem_limit_bytes=VMEM_LIMIT),
            name="prepare",
        )(gat, pkt, own)
        frc_rows, total = pl.pallas_call(
            tile_kernel,
            out_shape=(jax.ShapeDtypeStruct((8, WIDE), f32), jax.ShapeDtypeStruct((1, LANES), f32)),
            in_specs=[VMEM_SPEC] * 4,
            out_specs=(VMEM_SPEC,) * 2,
            scratch_shapes=[pltpu.VMEM((3, FIXED_BLOCKS * PER_BLOCK, 8, LANES), f32)] * 2 + [pltpu.VMEM((3, FIXED_BLOCKS, 8, LANES), f32), pltpu.VMEM((1, LANES), f32), pltpu.VMEM((n_dev, 1, LANES), f32), pltpu.SemaphoreType.DMA((n_dev - 1,)), pltpu.SemaphoreType.DMA((n_dev - 1,))],
            compiler_params=pltpu.CompilerParams(collective_id=1, has_side_effects=True, vmem_limit_bytes=VMEM_LIMIT),
            name="tile",
        )(rel, others, part, eng)
        pos, vel, frc, ids, oks, energy = pl.pallas_call(
            finish_kernel,
            out_shape=(jax.ShapeDtypeStruct((3, CAP), f32),) * 3 + (jax.ShapeDtypeStruct((CAP,), jnp.int32),) * 2 + (jax.ShapeDtypeStruct((), f32),),
            in_specs=[VMEM_SPEC] * 3,
            out_specs=(VMEM_SPEC,) * 5 + (SMEM_SPEC,),
            compiler_params=pltpu.CompilerParams(vmem_limit_bytes=VMEM_LIMIT),
            name="finish",
        )(placed, frc_rows, total)
        return pos.T, vel.T, frc.T, ids, oks, energy

    row_spec = P(MESH_AXES, None)
    id_spec = P(MESH_AXES)
    return jax.shard_map(local_step, mesh=mesh, in_specs=(row_spec, row_spec, row_spec, id_spec, id_spec, P()), out_specs=(row_spec, row_spec, row_spec, id_spec, id_spec, P()), check_vma=False)
```

```python
import jax
import jax.numpy as jnp
from jax import lax
from jax.experimental import pallas as pl
from jax.experimental.pallas import tpu as pltpu
from jax.sharding import PartitionSpec as P

DT = 0.005
HALF_DT = 0.5 * DT
RC = 2.5
UPC = -48.0 * RC ** -13 + 24.0 * RC ** -7
MESH_AXES = ("z", "y", "x")
MESH = pl.DeviceIdType.MESH
NZ, NY, NX = 2, 2, 4
CAP = 729
LANES = 128
TILE = (8, LANES)
BLOCKS = 6
WIDE = BLOCKS * LANES
MOVE_CAP = CAP // 100
FAR_OWN = 1.0e4
FAR_OTHER = -1.0e4
NOWHERE = 1.0e9
GHOST_SQ = RC * RC + 0.01
PEERS = [(dz, dy, dx) for dz in range(NZ) for dy in range(NY) for dx in range(NX)][:0:-1]
SIDES = [(1, 1), (1, 0), (0, 1), (0, 0)]
GROUPS = [(gx, *side) for side in SIDES for gx in (1, -1)] + [(0, *side) for side in SIDES[:3]]
N_GROUPS = len(GROUPS)
DISTANT = [(2, *side) for side in SIDES]
N_PACKETS = N_GROUPS + len(DISTANT)


def lane_plan():
    starts, base = [], {}
    block, lane = 0, 0
    for index, (gx, gy, gz) in enumerate(GROUPS):
        if index == 8:
            block, lane = 1, 0
        dirs = [(gx, sy, sz) for sz in ((-1, 1) if gz else (0,)) for sy in ((-1, 1) if gy else (0,))]
        starts.append((block, lane, lane + MOVE_CAP * len(dirs)))
        for dx, dy, dz in dirs:
            base[(dz + 1) * 9 + (dy + 1) * 3 + dx + 1] = block * LANES + lane
            lane += MOVE_CAP
    return starts, base


LANE_STARTS, LANE_BASE = lane_plan()
STAY = 13
NT_DIMS = (((1,), (1,)), ((), ()))
NN_DIMS = (((1,), (0,)), ((), ()))


def split3(values):
    hi = values.astype(jnp.bfloat16).astype(jnp.float32)
    rest = values - hi
    mid = rest.astype(jnp.bfloat16).astype(jnp.float32)
    return jnp.concatenate([hi, mid, rest - mid], axis=0).astype(jnp.bfloat16)


def join3(parts):
    rows = parts.shape[0] // 3
    return (parts[0:rows] + parts[rows:2 * rows]) + parts[2 * rows:3 * rows]


def dot_nt(a, b):
    return lax.dot_general(a, b, NT_DIMS, preferred_element_type=jnp.float32)


def dot_nn(a, b):
    return lax.dot_general(a, b, NN_DIMS, preferred_element_type=jnp.float32)


def down(values):
    return jnp.sum(values, axis=0, keepdims=True)


def across(values):
    return jnp.sum(values, axis=1, keepdims=True)


def stack(values):
    return jnp.concatenate(values, axis=0)


def beside(values):
    return jnp.concatenate(values, axis=1)


def iota(shape, axis):
    return lax.broadcasted_iota(jnp.int32, shape, axis)


def my_coords():
    return lax.axis_index("z"), lax.axis_index("y"), lax.axis_index("x")


def peer_id(coords, offset):
    mz, my, mx = coords
    return (lax.rem(mz + offset[0], NZ), lax.rem(my + offset[1], NY), lax.rem(mx + offset[2] + NX, NX))


def entry_signals(coords):
    barrier = pltpu.get_barrier_semaphore()
    for offset in PEERS:
        pl.semaphore_signal(barrier, inc=1, device_id=peer_id(coords, offset), device_id_type=MESH)
    return barrier


def exchange_kernel(brick_ref, pos_ref, vel_ref, frc_ref, id_ref, ok_ref, gat_ref, pkt_ref, own_ref, raw, ids_in, oks_in, pad_ref, int_ref, send_pos, send_pkt, in_sem, pos_send_sem, pos_recv_sem, pkt_send_sem, pkt_recv_sem):
    coords = my_coords()
    fetches = [pltpu.make_async_copy(src, dst, in_sem.at[index]) for index, (src, dst) in enumerate(((pos_ref, raw.at[0]), (vel_ref, raw.at[1]), (frc_ref, raw.at[2]), (id_ref, ids_in), (ok_ref, oks_in)))]
    for fetch in fetches:
        fetch.start()
    barrier = entry_signals(coords)
    tail = slice(WIDE - LANES, WIDE)
    pad_ref[:, :, tail] = jnp.zeros((3, 4, LANES), jnp.float32)
    int_ref[:, tail] = jnp.zeros((2, LANES), jnp.int32)
    for fetch in fetches:
        fetch.wait()
    brick = brick_ref[...]
    for index in range(3):
        pad_ref[index, 0:3, 0:CAP] = raw[index]
    int_ref[0:1, 0:CAP] = ids_in[...].reshape(1, CAP)
    int_ref[1:2, 0:CAP] = oks_in[...].reshape(1, CAP)
    owned = int_ref[1:2, :] > 0
    moved, half, code = [], [], jnp.zeros((1, WIDE), jnp.int32)
    for axis, (mine, size, weight) in enumerate(((coords[2], NX, 1), (coords[1], NY, 3), (coords[0], NZ, 9))):
        box = brick * float(size)
        low = mine.astype(jnp.float32) * brick
        high = (mine + 1).astype(jnp.float32) * brick
        half_v = pad_ref[1, axis:axis + 1, :] + HALF_DT * pad_ref[2, axis:axis + 1, :]
        drift = pad_ref[0, axis:axis + 1, :] + DT * half_v
        step = jnp.where(drift >= high, 2, jnp.where(drift < low, 0, 1))
        code = code + step * weight
        wrapped = jnp.where(drift < 0.0, drift + box, jnp.where(drift >= box, drift - box, drift))
        moved.append(wrapped)
        half.append(half_v)
    code = jnp.where(owned, code, -1)
    for axis in range(3):
        for block in range(BLOCKS):
            lanes = slice(block * LANES, (block + 1) * LANES)
            send_pos[axis, block:block + 1, :] = jnp.where(owned[:, lanes], moved[axis][:, lanes], NOWHERE)
    ids = int_ref[0:1, :]
    id_hi = (lax.shift_right_logical(ids, 16) + 1).astype(jnp.float32)
    id_lo = (ids & 65535).astype(jnp.float32)
    data = stack(moved + [id_hi] + half + [id_lo])
    member = (jnp.broadcast_to(code, (32, WIDE)) == iota((32, WIDE), 0)).astype(jnp.float32)
    tri = (iota((LANES, LANES), 0) < iota((LANES, LANES), 1)).astype(jnp.bfloat16)
    codes = iota((32, LANES), 0)
    running = jnp.zeros((32, LANES), jnp.float32)
    for move, first in LANE_BASE.items():
        running = jnp.where(codes == move, float(first), running)
    pieces = [member[:, block * LANES:(block + 1) * LANES] for block in range(BLOCKS)]
    before = dot_nn(stack(pieces).astype(jnp.bfloat16), tri)
    slots = []
    for block, part in enumerate(pieces):
        slots.append(down(part * (before[32 * block:32 * block + 32] + running)))
        running = running + across(part)
    slot = beside(slots)
    stay = code == STAY
    mover_slot = jnp.where(owned & jnp.logical_not(stay), slot, -1.0).astype(jnp.int32)
    pick = (iota((2 * LANES, WIDE), 0) == mover_slot).astype(jnp.float32).astype(jnp.bfloat16)
    packet = join3(dot_nt(split3(data), pick))
    send_pkt[0] = packet[:, 0:LANES]
    send_pkt[1] = packet[:, LANES:2 * LANES]
    own_ref[0:8, :] = data
    own_ref[8:16, :] = stack([jnp.where(stay, slot, -1.0), jnp.full((7, WIDE), brick, jnp.float32)])
    pl.semaphore_wait(barrier, len(PEERS))
    copies = []
    order = list(enumerate(GROUPS + DISTANT))
    for index, (gx, gy, gz) in order[N_GROUPS:] + order[:N_GROUPS]:
        peer = peer_id(coords, (gz, gy, gx))
        if index < N_GROUPS:
            copies.append(pltpu.make_async_remote_copy(src_ref=send_pos, dst_ref=gat_ref.at[index], send_sem=pos_send_sem.at[index], recv_sem=pos_recv_sem.at[index], device_id=peer, device_id_type=MESH))
            copies[-1].start()
            source, target = send_pkt.at[LANE_STARTS[index][0]], pkt_ref.at[index]
        else:
            source, target = send_pkt.at[0, 0:4], pkt_ref.at[index, 0:4]
        copies.append(pltpu.make_async_remote_copy(src_ref=source, dst_ref=target, send_sem=pkt_send_sem.at[index], recv_sem=pkt_recv_sem.at[index], device_id=peer, device_id_type=MESH))
        copies[-1].start()
    gat_ref[N_GROUPS] = send_pos[...]
    for copy in copies:
        copy.wait()


CAND_ROWS = 8 * (N_GROUPS + 1) + 8
MAX_ROWS = BLOCKS + CAND_ROWS
GROUPS_OWN = BLOCKS * 16
QUAD = 4
FIXED_BLOCKS = 4
PER_BLOCK = 16
FIXED_QUADS = FIXED_BLOCKS * PER_BLOCK // QUAD
FIXED_ROWS = 11
ENERGY_ROWS = 8


def pair_tools(mine, others, rc2, wrap_box):
    def powers(dist_sq):
        inv_r = lax.rsqrt(dist_sq)
        inv_2 = inv_r * inv_r
        inv_4 = inv_2 * inv_2
        term = inv_4 * inv_2 - 0.5
        return inv_r, term, term * (inv_4 * inv_4)

    cut_inv_r, cut_term, cut_core = powers(rc2)
    kappa = -RC * cut_core
    for ulps in (-3, -2, -1, 1, 2, 3):
        trial = ulps * 2.0 ** -34 - RC * cut_core
        kappa = jnp.where(trial * cut_inv_r == -cut_core, trial, kappa)

    kappa_12 = 12.0 * kappa

    def quad_energy(dist_sqs):
        terms, tails = [], []
        for dist_sq in dist_sqs:
            inv_r = lax.rsqrt(dist_sq)
            inv_2 = inv_r * inv_r
            term = inv_2 * inv_2 * inv_2 - 0.5
            terms.append(term * term)
            tails.append(kappa_12 * inv_r * dist_sq)
        return ((terms[0] + terms[1]) + (terms[2] + terms[3])) - ((tails[0] + tails[1]) + (tails[2] + tails[3]))

    cut_energy = quad_energy([rc2] * QUAD)
    own_minus_lane = iota(TILE, 0) - iota(TILE, 1)

    def load_own(first):
        return [[mine[axis, first + k] for axis in range(3)] for k in range(QUAD)]

    def gaps(own, first, row, with_self):
        other = [others[axis, row] for axis in range(3)]
        deltas, dist_sqs = [], []
        for k in range(QUAD):
            delta = [own[k][axis] - other[axis] for axis in range(3)]
            for axis, box, inv_box in wrap_box:
                delta[axis] = delta[axis] - box * jnp.floor(delta[axis] * inv_box + 0.5)
            dist_sq = delta[0] * delta[0] + delta[1] * delta[1] + delta[2] * delta[2]
            if with_self:
                dist_sq = jnp.where(own_minus_lane == row * LANES - (first + k) * 8, rc2, dist_sq)
            deltas.append(delta)
            dist_sqs.append(jnp.minimum(dist_sq, rc2))
        return deltas, dist_sqs

    def energy_row(own, first, row, total, with_self, weight=None):
        gain = quad_energy(gaps(own, first, row, with_self)[1]) - cut_energy
        return total + (gain if weight is None else gain * weight)

    def force_row(own, first, row, force, with_self, react=None):
        force, pulls = list(force), []
        deltas, dist_sqs = gaps(own, first, row, with_self)
        for k in range(QUAD):
            inv_r, term, core = powers(dist_sqs[k])
            scale = core + kappa * inv_r
            pulls.append([scale * deltas[k][axis] for axis in range(3)])
            for axis in range(3):
                force[3 * k + axis] = force[3 * k + axis] + pulls[k][axis]
        if react is not None:
            for axis in range(3):
                react[axis, row] = react[axis, row] + ((pulls[0][axis] + pulls[1][axis]) + (pulls[2][axis] + pulls[3][axis]))
        return tuple(force)

    return load_own, energy_row, force_row


def spread_own(rel_ref, mine, blocks):
    for block in range(blocks):
        columns = rel_ref[block].T
        for axis in range(3):
            mine[axis, pl.ds(block * PER_BLOCK, PER_BLOCK)] = jnp.broadcast_to(columns[:, axis:axis + 1], (LANES, LANES)).reshape(PER_BLOCK, *TILE)


def prepare_kernel(gat_ref, pkt_ref, own_ref, sorted_ref, rel_ref, others, acc, eng_ref, mine):
    mz, my, mx = my_coords()
    brick = own_ref[9:10, 0:LANES]
    half_l = 0.5 * brick
    sizes = (NX, NY, NZ)
    centre = [(index.astype(jnp.float32) + 0.5) * brick for index in (mx, my, mz)]
    box = [brick * float(size) for size in sizes]
    lane_1 = iota((1, LANES), 1)
    acc[:, pl.ds(0, FIXED_QUADS * QUAD)] = jnp.zeros((3, FIXED_QUADS * QUAD, 8, LANES), jnp.float32)

    arrived = []
    for block in range(2):
        total = jnp.zeros(TILE, jnp.float32)
        for index in range(N_GROUPS):
            where_block, first, last = LANE_STARTS[index]
            if where_block == block:
                total = total + jnp.where((lane_1 >= first) & (lane_1 < last), pkt_ref[index], 0.0)
        arrived.append(total)
    arr = beside(arrived)
    arr_ok = arr[3:4] > 0.5
    stay_all = own_ref[8:9, :] >= 0.0
    n_vec = across(stay_all.astype(jnp.float32)) + across(arr_ok.astype(jnp.float32))
    n_own = jnp.max(n_vec).astype(jnp.int32)
    n_int = n_vec.astype(jnp.int32)
    quads = lax.div(n_own + (8 * QUAD - 1), 8 * QUAD)
    own_rows = lax.div(n_own + (LANES - 1), LANES)
    beyond = gat_ref[0, 0, 4:6, :]
    for slot in range(1, N_GROUPS + 1):
        beyond = jnp.minimum(beyond, gat_ref[slot, 0, 4:6, :])
    small = (jnp.min(beyond) > 0.5 * NOWHERE) & (n_own <= FIXED_BLOCKS * LANES)
    eng_ref[1] = jnp.broadcast_to(n_vec, TILE)
    wide = jnp.max(brick) >= 2.0 * RC
    int_max = 2147483647
    rc2 = RC * RC + 0.0 * own_ref[8:16, 0:LANES]
    zero = jnp.zeros(TILE, jnp.float32)
    far = jnp.full(TILE, FAR_OTHER, jnp.float32)

    def build(blocks, tile_rows):
        span = blocks * LANES
        data = beside([own_ref[0:8, 0:span], arr])
        ids = lax.shift_left(data[3:4].astype(jnp.int32) - 1, 16) + data[7:8].astype(jnp.int32)
        stay_rank = own_ref[8:9, 0:span]
        stay = stay_rank >= 0.0
        arr_id = jnp.where(arr_ok, ids[:, span:], int_max)
        own_id = jnp.where(stay, ids[:, :span], int_max)

        count_rows = (N_GROUPS + 1) * tile_rows
        cand = -(-(count_rows + len(DISTANT)) // 8) * 8
        rel = []
        for axis in range(3):
            near = [gat_ref[slot, axis, 0:tile_rows, :] for slot in range(N_GROUPS + 1)]
            distant = [jnp.where(pkt_ref[N_GROUPS + k, 3:4, :] > 0.5, pkt_ref[N_GROUPS + k, axis:axis + 1, :], NOWHERE) for k in range(len(DISTANT))]
            values = stack(near + distant + [jnp.full((cand - count_rows - len(DISTANT), LANES), NOWHERE, jnp.float32)]) - centre[axis]
            rel.append(jnp.where(values > 0.5 * box[axis], values - box[axis], jnp.where(values < -0.5 * box[axis], values + box[axis], values)))
        over = [jnp.maximum(jnp.abs(values) - half_l, 0.0) for values in rel]
        gap_sq = over[0] * over[0] + over[1] * over[1] + over[2] * over[2]
        side = jnp.zeros((cand, LANES), jnp.float32)
        for axis in range(3):
            side = 3.0 * side + jnp.where(over[2 - axis] > 0.0, jnp.where(rel[2 - axis] > 0.0, 1.0, -1.0), 0.0)
        near = gap_sq < GHOST_SQ
        mixed = jnp.where(near & (side > 0.0), 256.0, jnp.where(near & (side < 0.0), 1.0, 0.0)).astype(jnp.bfloat16)
        row_l, col_l = iota((LANES, LANES), 0), iota((LANES, LANES), 1)

        def counts(chosen):
            return dot_nn(mixed, chosen.astype(jnp.bfloat16)).astype(jnp.int32)

        cum = counts(row_l <= col_l)
        total = counts(row_l >= 0)
        marks = [counts(row_l < 16 * k) for k in range(1, 8)]
        arr_col = jnp.broadcast_to(arr_id, (8, 2 * LANES)).T[:, 0:1]
        arr_first = (arr_col < beside([own_id, arr_id])).astype(jnp.float32)
        arr_before = down(arr_first)
        stay_after = dot_nt(jnp.broadcast_to(stay.astype(jnp.float32), (8, span)).astype(jnp.bfloat16), arr_first[:, :span].astype(jnp.bfloat16))[0:1]
        stay_before = across(stay.astype(jnp.float32)) - stay_after
        rank = beside([jnp.where(stay, stay_rank + arr_before[:, :span], -1.0), jnp.where(arr_ok, stay_before + arr_before[:, span:], -1.0)]).astype(jnp.int32)
        earlier = (iota((cand, cand), 1) < iota((cand, cand), 0)).astype(jnp.bfloat16)
        uppers, lowers = lax.shift_right_logical(total, 8), total & 255

        def starts(each, first):
            base = dot_nn(earlier, each.astype(jnp.float32).astype(jnp.bfloat16)).astype(jnp.int32) + first
            return base, base[cand - 1:] + each[cand - 1:]

        upper_base, upper_end = starts(uppers, n_int)
        lower_base, all_end = starts(lowers, upper_end)
        n_upper, n_all = jnp.max(upper_end), jnp.max(all_end)
        eng_ref[2] = jnp.broadcast_to(upper_end.astype(jnp.float32), TILE)
        fits = n_upper <= ENERGY_ROWS * LANES
        parts = split3(data)

        pick = (iota((span, span + 2 * LANES), 0) == rank).astype(jnp.float32).astype(jnp.bfloat16)
        chosen = dot_nt(pick, parts)

        def place_block(block):
            rows_s = join3(chosen[block * LANES:(block + 1) * LANES].T)
            sorted_ref[block] = rows_s
            valid = lane_1 + block * LANES < n_int
            own_rel = stack([rows_s[axis:axis + 1] - centre[axis] for axis in range(3)] + [rows_s[3:8]])
            rel_ref[block] = jnp.where(valid, own_rel, FAR_OWN)
            for axis in range(3):
                others[axis, block] = jnp.broadcast_to(jnp.where(valid, own_rel[axis:axis + 1], 0.0), TILE)

        lane_c = iota((cand, LANES), 1)
        is_upper = lane_c < uppers
        keep = jnp.where(is_upper, -1, 255)
        bound = jnp.where(is_upper, lane_c * 256 + 255, lane_c - uppers)

        def passed(probes):
            return sum(((probe & keep) <= bound).astype(jnp.int32) for probe in probes)

        def probe_at(source, stride, number):
            return [jnp.take_along_axis(cum, source + (stride * k - 1), axis=1) for k in range(1, number + 1)]

        source = 16 * passed(marks)
        place_block(0)
        place_block(1)
        source = source + 2 * passed(probe_at(source, 2, 7))
        for block in range(2, blocks):
            place_block(block)
        source = source + passed(probe_at(source, 1, 1))
        for block in range(blocks, BLOCKS):
            sorted_ref[block] = zero

        def turned(base, each, first):
            place = (lane_c - base) & (LANES - 1)
            lane = jnp.take_along_axis(source, (first + place) & (LANES - 1), axis=1)
            target = jnp.where(place < each, lax.shift_right_logical(base + place, 7), -1)
            return target, [jnp.take_along_axis(values, lane, axis=1) for values in rel]

        def pack(target, packed, start, stop, held_rows, empty):
            def pack_row(row, carry):
                hit = target == row
                filled = lane_1 + row * LANES < n_all
                for axis in range(3):
                    held = jnp.where(row < held_rows, others[axis, row], 0.0)
                    values = held + down(jnp.where(hit, packed[axis], 0.0))
                    others[axis, row] = jnp.where(filled, values, empty)
                return carry

            lax.fori_loop(lax.div(start, LANES), lax.div(stop + (LANES - 1), LANES), pack_row, 0)

        upper_rows = lax.div(n_upper + (LANES - 1), LANES)
        rows = lax.div(n_all + (LANES - 1), LANES)
        upper_set, lower_set = turned(upper_base, uppers, 0), turned(lower_base, lowers, uppers)
        pack(*upper_set, n_own, n_upper, own_rows, 0.0)
        pack(*lower_set, n_upper, n_all, upper_rows, FAR_OTHER)

        def set_far(row, carry):
            for axis in range(3):
                others[axis, row] = far
            return carry

        def excess(first_quad, last_quad, first_row, wrap_box, energy):
            slot_8 = iota(TILE, 1)
            load_own, energy_row, force_row = pair_tools(mine, others, rc2, wrap_box)

            def quad(index, total):
                first = index * QUAD
                own = load_own(first)
                sums = (zero,) * (3 * QUAD) + (total,)

                def both(row, part):
                    slot = slot_8 + row * LANES
                    weight = 1.0 if wrap_box else jnp.where(slot < n_int, 1.0, jnp.where(slot < upper_end, 2.0, 0.0))
                    return force_row(own, first, row, part[:-1], True) + (energy_row(own, first, row, part[-1], True, weight),)

                sums = lax.fori_loop(first_row, rows, both, sums)
                for k in range(QUAD):
                    for axis in range(3):
                        acc[axis, first + k] = sums[3 * k + axis]
                return sums[-1]

            return lax.fori_loop(first_quad, last_quad, quad, energy)

        def leftover():
            spread_own(rel_ref, mine, blocks)
            short = jnp.where(rows > FIXED_ROWS, jnp.minimum(quads, FIXED_QUADS), 0)
            energy = excess(0, short, FIXED_ROWS, [], zero)
            if blocks > FIXED_BLOCKS:
                energy = excess(FIXED_QUADS, quads, 0, [], energy)
            eng_ref[0] = energy

        def plain():
            eng_ref[0] = zero
            pl.when((rows > FIXED_ROWS) | (quads > FIXED_QUADS))(leftover)
            lax.fori_loop(rows, FIXED_ROWS, set_far, 0)

        def alone(wrap_box):
            spread_own(rel_ref, mine, blocks)
            eng_ref[0] = excess(0, quads, 0, wrap_box, zero)
            lax.fori_loop(0, FIXED_ROWS, set_far, 0)

        pl.when(wide & fits)(plain)
        pl.when(wide & jnp.logical_not(fits))(lambda: alone([]))
        pl.when(jnp.logical_not(wide))(lambda: alone([(axis, box[axis], 1.0 / box[axis]) for axis in (1, 2)]))

    pl.when(small)(lambda: build(FIXED_BLOCKS, 4))
    pl.when(jnp.logical_not(small))(lambda: build(BLOCKS, BLOCKS))


def tile_kernel(rel_ref, others, part, eng_ref, frc_ref, out_ref, mine, acc, react, eng, slots, send_sem, recv_sem):
    coords = my_coords()
    mz, my, mx = coords
    barrier = entry_signals(coords)
    rc2 = RC * RC + 0.0 * rel_ref[0]
    spread_own(rel_ref, mine, FIXED_BLOCKS)
    load_own, energy_row, force_row = pair_tools(mine, others, rc2, [])

    lane_8 = iota(TILE, 1).astype(jnp.float32)
    energy = eng_ref[0]

    def weight_of(row, own_weight):
        slot = lane_8 + float(row * LANES)
        return jnp.where(slot < eng_ref[1], own_weight, jnp.where(slot < eng_ref[2], 2.0, 0.0))

    for block in range(FIXED_BLOCKS):

        def energy_quad(index, total, block=block):
            first = block * PER_BLOCK + index * QUAD
            own = load_own(first)
            for row in range(block, ENERGY_ROWS):
                weight = weight_of(row, 2.0 if block < row < FIXED_BLOCKS else 1.0)
                total = energy_row(own, first, row, total, row == block, weight)
            return total

        energy = lax.fori_loop(0, PER_BLOCK // QUAD, energy_quad, energy)
    eng[...] = 2.0 * down(energy)
    pl.semaphore_wait(barrier, len(PEERS))
    place = (mz * NY + my) * NX + mx
    copies = []
    for index, offset in enumerate(PEERS):
        copies.append(pltpu.make_async_remote_copy(src_ref=eng, dst_ref=slots.at[place], send_sem=send_sem.at[index], recv_sem=recv_sem.at[index], device_id=peer_id(coords, offset), device_id_type=MESH))
        copies[-1].start()
    slots[place] = eng[...]
    react[...] = jnp.zeros_like(react)
    for block in range(FIXED_BLOCKS):

        def force_quad(index, carry, block=block):
            first = block * PER_BLOCK + index * QUAD
            own = load_own(first)
            force = force_row(own, first, block, [part[axis, first + k] for k in range(QUAD) for axis in range(3)], True)
            for row in range(block + 1, FIXED_ROWS):
                force = force_row(own, first, row, force, False, react if row < FIXED_BLOCKS else None)
            for k in range(QUAD):
                for axis in range(3):
                    acc[axis, first + k] = force[3 * k + axis]
            return carry

        lax.fori_loop(0, PER_BLOCK // QUAD, force_quad, 0)
    for block in range(BLOCKS):
        held = acc if block < FIXED_BLOCKS else part
        for axis in range(3):
            turned = (held[axis, pl.ds(block * PER_BLOCK, PER_BLOCK)].reshape(LANES, LANES)).T
            force = down(turned)
            if 0 < block < FIXED_BLOCKS:
                force = force - down(react[axis, block])
            frc_ref[axis:axis + 1, block * LANES:(block + 1) * LANES] = 48.0 * force
    for copy in copies:
        copy.wait()
    total = slots[0]
    for index in range(1, NZ * NY * NX):
        total = total + slots[index]
    out_ref[...] = total


def finish_kernel(sorted_ref, frc_ref, total_ref, pos_out, vel_out, frc_out, id_out, ok_out, eng_out):
    eng_out[...] = jnp.sum(total_ref[...])
    for block in range(BLOCKS):
        width = min(LANES, CAP - block * LANES)
        lanes = slice(block * LANES, block * LANES + width)
        rows_s = sorted_ref[block]
        valid = rows_s[3:4] > 0.5
        for axis in range(3):
            force = jnp.where(valid, frc_ref[axis:axis + 1, block * LANES:(block + 1) * LANES], 0.0)
            frc_out[axis:axis + 1, lanes] = force[:, :width]
            vel_out[axis:axis + 1, lanes] = (rows_s[4 + axis:5 + axis] + HALF_DT * force)[:, :width]
            pos_out[axis:axis + 1, lanes] = rows_s[axis:axis + 1, :width]
        new_id = lax.shift_left(rows_s[3:4].astype(jnp.int32) - 1, 16) + rows_s[7:8].astype(jnp.int32)
        id_out[lanes] = jnp.where(valid, new_id, 0)[:, :width].reshape(width)
        ok_out[lanes] = valid.astype(jnp.int32)[:, :width].reshape(width)


VMEM_SPEC = pl.BlockSpec(memory_space=pltpu.VMEM)
HBM_SPEC = pl.BlockSpec(memory_space=pltpu.HBM)
VMEM_LIMIT = 8 * 1024 * 1024
SMEM_SPEC = pl.BlockSpec(memory_space=pltpu.SMEM)


def solution(mesh):
    def local_step(atom_pos, atom_vel, atom_frc, atom_id, atom_ok, brick_side):
        f32 = jnp.float32
        n_dev = NZ * NY * NX
        gat, pkt, own = pl.pallas_call(
            exchange_kernel,
            out_shape=(jax.ShapeDtypeStruct((N_GROUPS + 1, 3, BLOCKS, LANES), f32), jax.ShapeDtypeStruct((N_PACKETS, 8, LANES), f32), jax.ShapeDtypeStruct((16, WIDE), f32)),
            in_specs=[SMEM_SPEC] + [HBM_SPEC] * 5,
            out_specs=(VMEM_SPEC,) * 3,
            scratch_shapes=[
                pltpu.VMEM((3, 3, CAP), f32),
                pltpu.VMEM((CAP,), jnp.int32),
                pltpu.VMEM((CAP,), jnp.int32),
                pltpu.VMEM((3, 4, WIDE), f32),
                pltpu.VMEM((2, WIDE), jnp.int32),
                pltpu.VMEM((3, BLOCKS, LANES), f32),
                pltpu.VMEM((2, 8, LANES), f32),
                pltpu.SemaphoreType.DMA((5,)),
                pltpu.SemaphoreType.DMA((N_GROUPS,)),
                pltpu.SemaphoreType.DMA((N_GROUPS,)),
                pltpu.SemaphoreType.DMA((N_PACKETS,)),
                pltpu.SemaphoreType.DMA((N_PACKETS,)),
            ],
            compiler_params=pltpu.CompilerParams(collective_id=0, has_side_effects=True, vmem_limit_bytes=VMEM_LIMIT),
            name="exchange",
        )(brick_side, *(pltpu.with_memory_space_constraint(value, pltpu.HBM) for value in (atom_pos.T, atom_vel.T, atom_frc.T, atom_id, atom_ok)))
        own_tiles = jax.ShapeDtypeStruct((3, GROUPS_OWN, 8, LANES), f32)
        block_rows = jax.ShapeDtypeStruct((BLOCKS, 8, LANES), f32)
        placed, rel, others, part, eng = pl.pallas_call(
            prepare_kernel,
            out_shape=(block_rows, block_rows, jax.ShapeDtypeStruct((3, MAX_ROWS, 8, LANES), f32), own_tiles, jax.ShapeDtypeStruct((3, 8, LANES), f32)),
            in_specs=[VMEM_SPEC] * 3,
            out_specs=(VMEM_SPEC,) * 5,
            scratch_shapes=[pltpu.VMEM(own_tiles.shape, f32)],
            compiler_params=pltpu.CompilerParams(vmem_limit_bytes=VMEM_LIMIT),
            name="prepare",
        )(gat, pkt, own)
        frc_rows, total = pl.pallas_call(
            tile_kernel,
            out_shape=(jax.ShapeDtypeStruct((8, WIDE), f32), jax.ShapeDtypeStruct((1, LANES), f32)),
            in_specs=[VMEM_SPEC] * 4,
            out_specs=(VMEM_SPEC,) * 2,
            scratch_shapes=[pltpu.VMEM((3, FIXED_BLOCKS * PER_BLOCK, 8, LANES), f32)] * 2 + [pltpu.VMEM((3, FIXED_BLOCKS, 8, LANES), f32), pltpu.VMEM((1, LANES), f32), pltpu.VMEM((n_dev, 1, LANES), f32), pltpu.SemaphoreType.DMA((n_dev - 1,)), pltpu.SemaphoreType.DMA((n_dev - 1,))],
            compiler_params=pltpu.CompilerParams(collective_id=1, has_side_effects=True, vmem_limit_bytes=VMEM_LIMIT),
            name="tile",
        )(rel, others, part, eng)
        pos, vel, frc, ids, oks, energy = pl.pallas_call(
            finish_kernel,
            out_shape=(jax.ShapeDtypeStruct((3, CAP), f32),) * 3 + (jax.ShapeDtypeStruct((CAP,), jnp.int32),) * 2 + (jax.ShapeDtypeStruct((), f32),),
            in_specs=[VMEM_SPEC] * 3,
            out_specs=(VMEM_SPEC,) * 5 + (SMEM_SPEC,),
            compiler_params=pltpu.CompilerParams(vmem_limit_bytes=VMEM_LIMIT),
            name="finish",
        )(placed, frc_rows, total)
        return pos.T, vel.T, frc.T, ids, oks, energy

    row_spec = P(MESH_AXES, None)
    id_spec = P(MESH_AXES)
    return jax.shard_map(local_step, mesh=mesh, in_specs=(row_spec, row_spec, row_spec, id_spec, id_spec, P()), out_specs=(row_spec, row_spec, row_spec, id_spec, id_spec, P()), check_vma=False)
```

```python
import jax
import jax.numpy as jnp
from jax import lax
from jax.experimental import pallas as pl
from jax.experimental.pallas import tpu as pltpu
from jax.sharding import PartitionSpec as P

DT = 0.005
HALF_DT = 0.5 * DT
RC = 2.5
UPC = -48.0 * RC ** -13 + 24.0 * RC ** -7
MESH_AXES = ("z", "y", "x")
MESH = pl.DeviceIdType.MESH
NZ, NY, NX = 2, 2, 4
CAP = 729
LANES = 128
TILE = (8, LANES)
BLOCKS = 6
WIDE = BLOCKS * LANES
MOVE_CAP = CAP // 100
FAR_OWN = 1.0e4
FAR_OTHER = -1.0e4
NOWHERE = 1.0e9
GHOST_SQ = RC * RC + 0.01
PEERS = [(dz, dy, dx) for dz in range(NZ) for dy in range(NY) for dx in range(NX)][1:]
PEERS.sort(key=lambda offset: -2 * (offset[0] + offset[1]) - (1, 2, 3, 2)[offset[2]])
SIDES = [(1, 1), (1, 0), (0, 1), (0, 0)]
GROUPS = [(gx, *side) for side in SIDES for gx in (1, -1)] + [(0, *side) for side in SIDES[:3]]
N_GROUPS = len(GROUPS)
DISTANT = [(2, *side) for side in SIDES]
N_PACKETS = N_GROUPS + len(DISTANT)


def lane_plan():
    starts, base = [], {}
    block, lane = 0, 0
    for index, (gx, gy, gz) in enumerate(GROUPS):
        if index == 8:
            block, lane = 1, 0
        dirs = [(gx, sy, sz) for sz in ((-1, 1) if gz else (0,)) for sy in ((-1, 1) if gy else (0,))]
        starts.append((block, lane, lane + MOVE_CAP * len(dirs)))
        for dx, dy, dz in dirs:
            base[(dz + 1) * 9 + (dy + 1) * 3 + dx + 1] = block * LANES + lane
            lane += MOVE_CAP
    return starts, base


LANE_STARTS, LANE_BASE = lane_plan()
STAY = 13
NT_DIMS = (((1,), (1,)), ((), ()))
NN_DIMS = (((1,), (0,)), ((), ()))


def split3(values):
    hi = values.astype(jnp.bfloat16).astype(jnp.float32)
    rest = values - hi
    mid = rest.astype(jnp.bfloat16).astype(jnp.float32)
    return jnp.concatenate([hi, mid, rest - mid], axis=0).astype(jnp.bfloat16)


def join3(parts):
    rows = parts.shape[0] // 3
    return (parts[0:rows] + parts[rows:2 * rows]) + parts[2 * rows:3 * rows]


def dot_nt(a, b):
    return lax.dot_general(a, b, NT_DIMS, preferred_element_type=jnp.float32)


def dot_nn(a, b):
    return lax.dot_general(a, b, NN_DIMS, preferred_element_type=jnp.float32)


def down(values):
    return jnp.sum(values, axis=0, keepdims=True)


def across(values):
    return jnp.sum(values, axis=1, keepdims=True)


def stack(values):
    return jnp.concatenate(values, axis=0)


def beside(values):
    return jnp.concatenate(values, axis=1)


def iota(shape, axis):
    return lax.broadcasted_iota(jnp.int32, shape, axis)


def my_coords():
    return lax.axis_index("z"), lax.axis_index("y"), lax.axis_index("x")


def peer_id(coords, offset):
    mz, my, mx = coords
    return (lax.rem(mz + offset[0], NZ), lax.rem(my + offset[1], NY), lax.rem(mx + offset[2] + NX, NX))


def entry_signals(coords):
    barrier = pltpu.get_barrier_semaphore()
    for offset in PEERS:
        pl.semaphore_signal(barrier, inc=1, device_id=peer_id(coords, offset), device_id_type=MESH)
    return barrier


def exchange_kernel(brick_ref, pos_ref, vel_ref, frc_ref, id_ref, ok_ref, gat_ref, pkt_ref, own_ref, raw, ids_in, oks_in, pad_ref, int_ref, send_pos, send_pkt, in_sem, pos_send_sem, pos_recv_sem, pkt_send_sem, pkt_recv_sem):
    coords = my_coords()
    fetches = [pltpu.make_async_copy(src, dst, in_sem.at[index]) for index, (src, dst) in enumerate(((pos_ref, raw.at[0]), (vel_ref, raw.at[1]), (frc_ref, raw.at[2]), (id_ref, ids_in), (ok_ref, oks_in)))]
    for fetch in fetches:
        fetch.start()
    barrier = entry_signals(coords)
    tail = slice(WIDE - LANES, WIDE)
    pad_ref[:, :, tail] = jnp.zeros((3, 4, LANES), jnp.float32)
    int_ref[:, tail] = jnp.zeros((2, LANES), jnp.int32)
    for fetch in fetches:
        fetch.wait()
    brick = brick_ref[...]
    for index in range(3):
        pad_ref[index, 0:3, 0:CAP] = raw[index]
    int_ref[0:1, 0:CAP] = ids_in[...].reshape(1, CAP)
    int_ref[1:2, 0:CAP] = oks_in[...].reshape(1, CAP)
    owned = int_ref[1:2, :] > 0
    moved, half, code = [], [], jnp.zeros((1, WIDE), jnp.int32)
    for axis, (mine, size, weight) in enumerate(((coords[2], NX, 1), (coords[1], NY, 3), (coords[0], NZ, 9))):
        box = brick * float(size)
        low = mine.astype(jnp.float32) * brick
        high = (mine + 1).astype(jnp.float32) * brick
        half_v = pad_ref[1, axis:axis + 1, :] + HALF_DT * pad_ref[2, axis:axis + 1, :]
        drift = pad_ref[0, axis:axis + 1, :] + DT * half_v
        step = jnp.where(drift >= high, 2, jnp.where(drift < low, 0, 1))
        code = code + step * weight
        wrapped = jnp.where(drift < 0.0, drift + box, jnp.where(drift >= box, drift - box, drift))
        moved.append(wrapped)
        half.append(half_v)
    code = jnp.where(owned, code, -1)
    for axis in range(3):
        for block in range(BLOCKS):
            lanes = slice(block * LANES, (block + 1) * LANES)
            send_pos[axis, block:block + 1, :] = jnp.where(owned[:, lanes], moved[axis][:, lanes], NOWHERE)
    ids = int_ref[0:1, :]
    id_hi = (lax.shift_right_logical(ids, 16) + 1).astype(jnp.float32)
    id_lo = (ids & 65535).astype(jnp.float32)
    data = stack(moved + [id_hi] + half + [id_lo])
    member = (jnp.broadcast_to(code, (32, WIDE)) == iota((32, WIDE), 0)).astype(jnp.float32)
    tri = (iota((LANES, LANES), 0) < iota((LANES, LANES), 1)).astype(jnp.bfloat16)
    codes = iota((32, LANES), 0)
    running = jnp.zeros((32, LANES), jnp.float32)
    for move, first in LANE_BASE.items():
        running = jnp.where(codes == move, float(first), running)
    pieces = [member[:, block * LANES:(block + 1) * LANES] for block in range(BLOCKS)]
    before = dot_nn(stack(pieces).astype(jnp.bfloat16), tri)
    slots = []
    for block, part in enumerate(pieces):
        slots.append(down(part * (before[32 * block:32 * block + 32] + running)))
        running = running + across(part)
    slot = beside(slots)
    stay = code == STAY
    mover_slot = jnp.where(owned & jnp.logical_not(stay), slot, -1.0).astype(jnp.int32)
    pick = (iota((2 * LANES, WIDE), 0) == mover_slot).astype(jnp.float32).astype(jnp.bfloat16)
    packet = join3(dot_nt(split3(data), pick))
    send_pkt[0] = packet[:, 0:LANES]
    send_pkt[1] = packet[:, LANES:2 * LANES]
    own_ref[0:8, :] = data
    own_ref[8:16, :] = stack([jnp.where(stay, slot, -1.0), jnp.full((7, WIDE), brick, jnp.float32)])
    pl.semaphore_wait(barrier, len(PEERS))
    copies = []
    order = sorted(enumerate(GROUPS + DISTANT), key=lambda item: (item[0] < N_GROUPS, -2 * (item[1][1] + item[1][2]) - abs(item[1][0])))
    for index, (gx, gy, gz) in order:
        peer = peer_id(coords, (gz, gy, gx))
        if index < N_GROUPS:
            copies.append(pltpu.make_async_remote_copy(src_ref=send_pos, dst_ref=gat_ref.at[index], send_sem=pos_send_sem.at[index], recv_sem=pos_recv_sem.at[index], device_id=peer, device_id_type=MESH))
            copies[-1].start()
            source, target = send_pkt.at[LANE_STARTS[index][0]], pkt_ref.at[index]
        else:
            source, target = send_pkt.at[0, 0:4], pkt_ref.at[index, 0:4]
        copies.append(pltpu.make_async_remote_copy(src_ref=source, dst_ref=target, send_sem=pkt_send_sem.at[index], recv_sem=pkt_recv_sem.at[index], device_id=peer, device_id_type=MESH))
        copies[-1].start()
    gat_ref[N_GROUPS] = send_pos[...]
    for copy in copies:
        copy.wait()


CAND_ROWS = 8 * (N_GROUPS + 1) + 8
MAX_ROWS = BLOCKS + CAND_ROWS
GROUPS_OWN = BLOCKS * 16
QUAD = 4
FIXED_BLOCKS = 4
PER_BLOCK = 16
FIXED_QUADS = FIXED_BLOCKS * PER_BLOCK // QUAD
FIXED_ROWS = 11
ENERGY_ROWS = 8


def pair_tools(mine, others, rc2, wrap_box):
    def powers(dist_sq):
        inv_r = lax.rsqrt(dist_sq)
        inv_2 = inv_r * inv_r
        inv_4 = inv_2 * inv_2
        term = inv_4 * inv_2 - 0.5
        return inv_r, term, term * (inv_4 * inv_4)

    cut_inv_r, cut_term, cut_core = powers(rc2)
    kappa = -RC * cut_core
    for ulps in (-3, -2, -1, 1, 2, 3):
        trial = ulps * 2.0 ** -34 - RC * cut_core
        kappa = jnp.where(trial * cut_inv_r == -cut_core, trial, kappa)

    kappa_12 = 12.0 * kappa

    def quad_energy(dist_sqs):
        terms, tails = [], []
        for dist_sq in dist_sqs:
            inv_r = lax.rsqrt(dist_sq)
            inv_2 = inv_r * inv_r
            term = inv_2 * inv_2 * inv_2 - 0.5
            terms.append(term * term)
            tails.append(kappa_12 * inv_r * dist_sq)
        return ((terms[0] + terms[1]) + (terms[2] + terms[3])) - ((tails[0] + tails[1]) + (tails[2] + tails[3]))

    cut_energy = quad_energy([rc2] * QUAD)
    own_minus_lane = iota(TILE, 0) - iota(TILE, 1)

    def load_own(first):
        return [[mine[axis, first + k] for axis in range(3)] for k in range(QUAD)]

    def gaps(own, first, row, with_self):
        other = [others[axis, row] for axis in range(3)]
        deltas, dist_sqs = [], []
        for k in range(QUAD):
            delta = [own[k][axis] - other[axis] for axis in range(3)]
            for axis, box, inv_box in wrap_box:
                delta[axis] = delta[axis] - box * jnp.floor(delta[axis] * inv_box + 0.5)
            dist_sq = delta[0] * delta[0] + delta[1] * delta[1] + delta[2] * delta[2]
            if with_self:
                dist_sq = jnp.where(own_minus_lane == row * LANES - (first + k) * 8, rc2, dist_sq)
            deltas.append(delta)
            dist_sqs.append(jnp.minimum(dist_sq, rc2))
        return deltas, dist_sqs

    def energy_row(own, first, row, total, with_self, weight=None):
        gain = quad_energy(gaps(own, first, row, with_self)[1]) - cut_energy
        return total + (gain if weight is None else gain * weight)

    def force_row(own, first, row, force, with_self, react=None):
        force, pulls = list(force), []
        deltas, dist_sqs = gaps(own, first, row, with_self)
        for k in range(QUAD):
            inv_r, term, core = powers(dist_sqs[k])
            scale = core + kappa * inv_r
            pulls.append([scale * deltas[k][axis] for axis in range(3)])
            for axis in range(3):
                force[3 * k + axis] = force[3 * k + axis] + pulls[k][axis]
        if react is not None:
            for axis in range(3):
                react[axis, row] = react[axis, row] + ((pulls[0][axis] + pulls[1][axis]) + (pulls[2][axis] + pulls[3][axis]))
        return tuple(force)

    return load_own, energy_row, force_row


def spread_own(rel_ref, mine, blocks):
    for block in range(blocks):
        columns = rel_ref[block].T
        for axis in range(3):
            mine[axis, pl.ds(block * PER_BLOCK, PER_BLOCK)] = jnp.broadcast_to(columns[:, axis:axis + 1], (LANES, LANES)).reshape(PER_BLOCK, *TILE)


def prepare_kernel(gat_ref, pkt_ref, own_ref, sorted_ref, rel_ref, others, acc, eng_ref, mine):
    mz, my, mx = my_coords()
    brick = own_ref[9:10, 0:LANES]
    half_l = 0.5 * brick
    sizes = (NX, NY, NZ)
    centre = [(index.astype(jnp.float32) + 0.5) * brick for index in (mx, my, mz)]
    box = [brick * float(size) for size in sizes]
    lane_1 = iota((1, LANES), 1)
    acc[:, pl.ds(0, FIXED_QUADS * QUAD)] = jnp.zeros((3, FIXED_QUADS * QUAD, 8, LANES), jnp.float32)

    arrived = []
    for block in range(2):
        total = jnp.zeros(TILE, jnp.float32)
        for index in range(N_GROUPS):
            where_block, first, last = LANE_STARTS[index]
            if where_block == block:
                total = total + jnp.where((lane_1 >= first) & (lane_1 < last), pkt_ref[index], 0.0)
        arrived.append(total)
    arr = beside(arrived)
    arr_ok = arr[3:4] > 0.5
    stay_all = own_ref[8:9, :] >= 0.0
    n_vec = across(stay_all.astype(jnp.float32)) + across(arr_ok.astype(jnp.float32))
    n_own = jnp.max(n_vec).astype(jnp.int32)
    n_int = n_vec.astype(jnp.int32)
    quads = lax.div(n_own + (8 * QUAD - 1), 8 * QUAD)
    own_rows = lax.div(n_own + (LANES - 1), LANES)
    beyond = gat_ref[0, 0, 4:6, :]
    for slot in range(1, N_GROUPS + 1):
        beyond = jnp.minimum(beyond, gat_ref[slot, 0, 4:6, :])
    small = (jnp.min(beyond) > 0.5 * NOWHERE) & (n_own <= FIXED_BLOCKS * LANES)
    eng_ref[1] = jnp.broadcast_to(n_vec, TILE)
    wide = jnp.max(brick) >= 2.0 * RC
    int_max = 2147483647
    rc2 = RC * RC + 0.0 * own_ref[8:16, 0:LANES]
    zero = jnp.zeros(TILE, jnp.float32)
    far = jnp.full(TILE, FAR_OTHER, jnp.float32)

    def build(blocks, tile_rows):
        span = blocks * LANES
        data = beside([own_ref[0:8, 0:span], arr])
        ids = lax.shift_left(data[3:4].astype(jnp.int32) - 1, 16) + data[7:8].astype(jnp.int32)
        stay_rank = own_ref[8:9, 0:span]
        stay = stay_rank >= 0.0
        arr_id = jnp.where(arr_ok, ids[:, span:], int_max)
        own_id = jnp.where(stay, ids[:, :span], int_max)

        count_rows = (N_GROUPS + 1) * tile_rows
        cand = -(-(count_rows + len(DISTANT)) // 8) * 8
        rel = []
        for axis in range(3):
            near = [gat_ref[slot, axis, 0:tile_rows, :] for slot in range(N_GROUPS + 1)]
            distant = [jnp.where(pkt_ref[N_GROUPS + k, 3:4, :] > 0.5, pkt_ref[N_GROUPS + k, axis:axis + 1, :], NOWHERE) for k in range(len(DISTANT))]
            values = stack(near + distant + [jnp.full((cand - count_rows - len(DISTANT), LANES), NOWHERE, jnp.float32)]) - centre[axis]
            rel.append(jnp.where(values > 0.5 * box[axis], values - box[axis], jnp.where(values < -0.5 * box[axis], values + box[axis], values)))
        over = [jnp.maximum(jnp.abs(values) - half_l, 0.0) for values in rel]
        gap_sq = over[0] * over[0] + over[1] * over[1] + over[2] * over[2]
        side = jnp.zeros((cand, LANES), jnp.float32)
        for axis in range(3):
            side = 3.0 * side + jnp.where(over[2 - axis] > 0.0, jnp.where(rel[2 - axis] > 0.0, 1.0, -1.0), 0.0)
        near = gap_sq < GHOST_SQ
        mixed = jnp.where(near & (side > 0.0), 256.0, jnp.where(near & (side < 0.0), 1.0, 0.0)).astype(jnp.bfloat16)
        row_l, col_l = iota((LANES, LANES), 0), iota((LANES, LANES), 1)

        def counts(chosen):
            return dot_nn(mixed, chosen.astype(jnp.bfloat16)).astype(jnp.int32)

        cum = counts(row_l <= col_l)
        total = counts(row_l >= 0)
        marks = [counts(row_l < 16 * k) for k in range(1, 8)]
        arr_col = jnp.broadcast_to(arr_id, (8, 2 * LANES)).T[:, 0:1]
        arr_first = (arr_col < beside([own_id, arr_id])).astype(jnp.float32)
        arr_before = down(arr_first)
        stay_after = dot_nt(jnp.broadcast_to(stay.astype(jnp.float32), (8, span)).astype(jnp.bfloat16), arr_first[:, :span].astype(jnp.bfloat16))[0:1]
        stay_before = across(stay.astype(jnp.float32)) - stay_after
        rank = beside([jnp.where(stay, stay_rank + arr_before[:, :span], -1.0), jnp.where(arr_ok, stay_before + arr_before[:, span:], -1.0)]).astype(jnp.int32)
        earlier = (iota((cand, cand), 1) < iota((cand, cand), 0)).astype(jnp.bfloat16)
        uppers, lowers = lax.shift_right_logical(total, 8), total & 255

        def starts(each, first):
            base = dot_nn(earlier, each.astype(jnp.float32).astype(jnp.bfloat16)).astype(jnp.int32) + first
            return base, base[cand - 1:] + each[cand - 1:]

        upper_base, upper_end = starts(uppers, n_int)
        lower_base, all_end = starts(lowers, upper_end)
        n_upper, n_all = jnp.max(upper_end), jnp.max(all_end)
        eng_ref[2] = jnp.broadcast_to(upper_end.astype(jnp.float32), TILE)
        fits = n_upper <= ENERGY_ROWS * LANES
        parts = split3(data)

        pick = (iota((span, span + 2 * LANES), 0) == rank).astype(jnp.float32).astype(jnp.bfloat16)
        chosen = dot_nt(pick, parts)

        def place_block(block):
            rows_s = join3(chosen[block * LANES:(block + 1) * LANES].T)
            sorted_ref[block] = rows_s
            valid = lane_1 + block * LANES < n_int
            own_rel = stack([rows_s[axis:axis + 1] - centre[axis] for axis in range(3)] + [rows_s[3:8]])
            rel_ref[block] = jnp.where(valid, own_rel, FAR_OWN)
            for axis in range(3):
                others[axis, block] = jnp.broadcast_to(jnp.where(valid, own_rel[axis:axis + 1], 0.0), TILE)

        lane_c = iota((cand, LANES), 1)
        is_upper = lane_c < uppers
        keep = jnp.where(is_upper, -1, 255)
        bound = jnp.where(is_upper, lane_c * 256 + 255, lane_c - uppers)

        def passed(probes):
            return sum(((probe & keep) <= bound).astype(jnp.int32) for probe in probes)

        def probe_at(source, stride, number):
            return [jnp.take_along_axis(cum, source + (stride * k - 1), axis=1) for k in range(1, number + 1)]

        source = 16 * passed(marks)
        place_block(0)
        place_block(1)
        source = source + 2 * passed(probe_at(source, 2, 7))
        for block in range(2, blocks):
            place_block(block)
        source = source + passed(probe_at(source, 1, 1))
        for block in range(blocks, BLOCKS):
            sorted_ref[block] = zero

        def turned(base, each, first):
            place = (lane_c - base) & (LANES - 1)
            lane = jnp.take_along_axis(source, (first + place) & (LANES - 1), axis=1)
            target = jnp.where(place < each, lax.shift_right_logical(base + place, 7), -1)
            return target, [jnp.take_along_axis(values, lane, axis=1) for values in rel]

        def pack(target, packed, start, stop, held_rows, empty):
            def pack_row(row, carry):
                hit = target == row
                filled = lane_1 + row * LANES < n_all
                for axis in range(3):
                    held = jnp.where(row < held_rows, others[axis, row], 0.0)
                    values = held + down(jnp.where(hit, packed[axis], 0.0))
                    others[axis, row] = jnp.where(filled, values, empty)
                return carry

            lax.fori_loop(lax.div(start, LANES), lax.div(stop + (LANES - 1), LANES), pack_row, 0)

        upper_rows = lax.div(n_upper + (LANES - 1), LANES)
        rows = lax.div(n_all + (LANES - 1), LANES)
        upper_set, lower_set = turned(upper_base, uppers, 0), turned(lower_base, lowers, uppers)
        pack(*upper_set, n_own, n_upper, own_rows, 0.0)
        pack(*lower_set, n_upper, n_all, upper_rows, FAR_OTHER)

        def set_far(row, carry):
            for axis in range(3):
                others[axis, row] = far
            return carry

        def excess(first_quad, last_quad, first_row, wrap_box, energy):
            slot_8 = iota(TILE, 1)
            load_own, energy_row, force_row = pair_tools(mine, others, rc2, wrap_box)

            def quad(index, total):
                first = index * QUAD
                own = load_own(first)
                sums = (zero,) * (3 * QUAD) + (total,)

                def both(row, part):
                    slot = slot_8 + row * LANES
                    weight = 1.0 if wrap_box else jnp.where(slot < n_int, 1.0, jnp.where(slot < upper_end, 2.0, 0.0))
                    return force_row(own, first, row, part[:-1], True) + (energy_row(own, first, row, part[-1], True, weight),)

                sums = lax.fori_loop(first_row, rows, both, sums)
                for k in range(QUAD):
                    for axis in range(3):
                        acc[axis, first + k] = sums[3 * k + axis]
                return sums[-1]

            return lax.fori_loop(first_quad, last_quad, quad, energy)

        def leftover():
            spread_own(rel_ref, mine, blocks)
            short = jnp.where(rows > FIXED_ROWS, jnp.minimum(quads, FIXED_QUADS), 0)
            energy = excess(0, short, FIXED_ROWS, [], zero)
            if blocks > FIXED_BLOCKS:
                energy = excess(FIXED_QUADS, quads, 0, [], energy)
            eng_ref[0] = energy

        def plain():
            eng_ref[0] = zero
            pl.when((rows > FIXED_ROWS) | (quads > FIXED_QUADS))(leftover)
            lax.fori_loop(rows, FIXED_ROWS, set_far, 0)

        def alone(wrap_box):
            spread_own(rel_ref, mine, blocks)
            eng_ref[0] = excess(0, quads, 0, wrap_box, zero)
            lax.fori_loop(0, FIXED_ROWS, set_far, 0)

        pl.when(wide & fits)(plain)
        pl.when(wide & jnp.logical_not(fits))(lambda: alone([]))
        pl.when(jnp.logical_not(wide))(lambda: alone([(axis, box[axis], 1.0 / box[axis]) for axis in (1, 2)]))

    pl.when(small)(lambda: build(FIXED_BLOCKS, 4))
    pl.when(jnp.logical_not(small))(lambda: build(BLOCKS, BLOCKS))


def tile_kernel(rel_ref, others, part, eng_ref, frc_ref, out_ref, mine, acc, react, eng, slots, send_sem, recv_sem):
    coords = my_coords()
    mz, my, mx = coords
    barrier = entry_signals(coords)
    rc2 = RC * RC + 0.0 * rel_ref[0]
    spread_own(rel_ref, mine, FIXED_BLOCKS)
    load_own, energy_row, force_row = pair_tools(mine, others, rc2, [])

    lane_8 = iota(TILE, 1).astype(jnp.float32)
    energy = eng_ref[0]

    def weight_of(row, own_weight):
        slot = lane_8 + float(row * LANES)
        return jnp.where(slot < eng_ref[1], own_weight, jnp.where(slot < eng_ref[2], 2.0, 0.0))

    for block in range(FIXED_BLOCKS):

        def energy_quad(index, total, block=block):
            first = block * PER_BLOCK + index * QUAD
            own = load_own(first)
            for row in range(block, ENERGY_ROWS):
                weight = weight_of(row, 2.0 if block < row < FIXED_BLOCKS else 1.0)
                total = energy_row(own, first, row, total, row == block, weight)
            return total

        energy = lax.fori_loop(0, PER_BLOCK // QUAD, energy_quad, energy)
    eng[...] = 2.0 * down(energy)
    pl.semaphore_wait(barrier, len(PEERS))
    place = (mz * NY + my) * NX + mx
    copies = []
    for index, offset in enumerate(PEERS):
        copies.append(pltpu.make_async_remote_copy(src_ref=eng, dst_ref=slots.at[place], send_sem=send_sem.at[index], recv_sem=recv_sem.at[index], device_id=peer_id(coords, offset), device_id_type=MESH))
        copies[-1].start()
    slots[place] = eng[...]
    react[...] = jnp.zeros_like(react)
    for block in range(FIXED_BLOCKS):

        def force_quad(index, carry, block=block):
            first = block * PER_BLOCK + index * QUAD
            own = load_own(first)
            force = force_row(own, first, block, [part[axis, first + k] for k in range(QUAD) for axis in range(3)], True)
            for row in range(block + 1, FIXED_ROWS):
                force = force_row(own, first, row, force, False, react if row < FIXED_BLOCKS else None)
            for k in range(QUAD):
                for axis in range(3):
                    acc[axis, first + k] = force[3 * k + axis]
            return carry

        lax.fori_loop(0, PER_BLOCK // QUAD, force_quad, 0)
    for block in range(BLOCKS):
        held = acc if block < FIXED_BLOCKS else part
        for axis in range(3):
            turned = (held[axis, pl.ds(block * PER_BLOCK, PER_BLOCK)].reshape(LANES, LANES)).T
            force = down(turned)
            if 0 < block < FIXED_BLOCKS:
                force = force - down(react[axis, block])
            frc_ref[axis:axis + 1, block * LANES:(block + 1) * LANES] = 48.0 * force
    for copy in copies:
        copy.wait()
    total = slots[0]
    for index in range(1, NZ * NY * NX):
        total = total + slots[index]
    out_ref[...] = total


def finish_kernel(sorted_ref, frc_ref, total_ref, pos_out, vel_out, frc_out, id_out, ok_out, eng_out):
    eng_out[...] = jnp.sum(total_ref[...])
    for block in range(BLOCKS):
        width = min(LANES, CAP - block * LANES)
        lanes = slice(block * LANES, block * LANES + width)
        rows_s = sorted_ref[block]
        valid = rows_s[3:4] > 0.5
        for axis in range(3):
            force = jnp.where(valid, frc_ref[axis:axis + 1, block * LANES:(block + 1) * LANES], 0.0)
            frc_out[axis:axis + 1, lanes] = force[:, :width]
            vel_out[axis:axis + 1, lanes] = (rows_s[4 + axis:5 + axis] + HALF_DT * force)[:, :width]
            pos_out[axis:axis + 1, lanes] = rows_s[axis:axis + 1, :width]
        new_id = lax.shift_left(rows_s[3:4].astype(jnp.int32) - 1, 16) + rows_s[7:8].astype(jnp.int32)
        id_out[lanes] = jnp.where(valid, new_id, 0)[:, :width].reshape(width)
        ok_out[lanes] = valid.astype(jnp.int32)[:, :width].reshape(width)


VMEM_SPEC = pl.BlockSpec(memory_space=pltpu.VMEM)
HBM_SPEC = pl.BlockSpec(memory_space=pltpu.HBM)
VMEM_LIMIT = 8 * 1024 * 1024
SMEM_SPEC = pl.BlockSpec(memory_space=pltpu.SMEM)


def solution(mesh):
    def local_step(atom_pos, atom_vel, atom_frc, atom_id, atom_ok, brick_side):
        f32 = jnp.float32
        n_dev = NZ * NY * NX
        gat, pkt, own = pl.pallas_call(
            exchange_kernel,
            out_shape=(jax.ShapeDtypeStruct((N_GROUPS + 1, 3, BLOCKS, LANES), f32), jax.ShapeDtypeStruct((N_PACKETS, 8, LANES), f32), jax.ShapeDtypeStruct((16, WIDE), f32)),
            in_specs=[SMEM_SPEC] + [HBM_SPEC] * 5,
            out_specs=(VMEM_SPEC,) * 3,
            scratch_shapes=[
                pltpu.VMEM((3, 3, CAP), f32),
                pltpu.VMEM((CAP,), jnp.int32),
                pltpu.VMEM((CAP,), jnp.int32),
                pltpu.VMEM((3, 4, WIDE), f32),
                pltpu.VMEM((2, WIDE), jnp.int32),
                pltpu.VMEM((3, BLOCKS, LANES), f32),
                pltpu.VMEM((2, 8, LANES), f32),
                pltpu.SemaphoreType.DMA((5,)),
                pltpu.SemaphoreType.DMA((N_GROUPS,)),
                pltpu.SemaphoreType.DMA((N_GROUPS,)),
                pltpu.SemaphoreType.DMA((N_PACKETS,)),
                pltpu.SemaphoreType.DMA((N_PACKETS,)),
            ],
            compiler_params=pltpu.CompilerParams(collective_id=0, has_side_effects=True, vmem_limit_bytes=VMEM_LIMIT),
            name="exchange",
        )(brick_side, *(pltpu.with_memory_space_constraint(value, pltpu.HBM) for value in (atom_pos.T, atom_vel.T, atom_frc.T, atom_id, atom_ok)))
        own_tiles = jax.ShapeDtypeStruct((3, GROUPS_OWN, 8, LANES), f32)
        block_rows = jax.ShapeDtypeStruct((BLOCKS, 8, LANES), f32)
        placed, rel, others, part, eng = pl.pallas_call(
            prepare_kernel,
            out_shape=(block_rows, block_rows, jax.ShapeDtypeStruct((3, MAX_ROWS, 8, LANES), f32), own_tiles, jax.ShapeDtypeStruct((3, 8, LANES), f32)),
            in_specs=[VMEM_SPEC] * 3,
            out_specs=(VMEM_SPEC,) * 5,
            scratch_shapes=[pltpu.VMEM(own_tiles.shape, f32)],
            compiler_params=pltpu.CompilerParams(vmem_limit_bytes=VMEM_LIMIT),
            name="prepare",
        )(gat, pkt, own)
        frc_rows, total = pl.pallas_call(
            tile_kernel,
            out_shape=(jax.ShapeDtypeStruct((8, WIDE), f32), jax.ShapeDtypeStruct((1, LANES), f32)),
            in_specs=[VMEM_SPEC] * 4,
            out_specs=(VMEM_SPEC,) * 2,
            scratch_shapes=[pltpu.VMEM((3, FIXED_BLOCKS * PER_BLOCK, 8, LANES), f32)] * 2 + [pltpu.VMEM((3, FIXED_BLOCKS, 8, LANES), f32), pltpu.VMEM((1, LANES), f32), pltpu.VMEM((n_dev, 1, LANES), f32), pltpu.SemaphoreType.DMA((n_dev - 1,)), pltpu.SemaphoreType.DMA((n_dev - 1,))],
            compiler_params=pltpu.CompilerParams(collective_id=1, has_side_effects=True, vmem_limit_bytes=VMEM_LIMIT),
            name="tile",
        )(rel, others, part, eng)
        pos, vel, frc, ids, oks, energy = pl.pallas_call(
            finish_kernel,
            out_shape=(jax.ShapeDtypeStruct((3, CAP), f32),) * 3 + (jax.ShapeDtypeStruct((CAP,), jnp.int32),) * 2 + (jax.ShapeDtypeStruct((), f32),),
            in_specs=[VMEM_SPEC] * 3,
            out_specs=(VMEM_SPEC,) * 5 + (SMEM_SPEC,),
            compiler_params=pltpu.CompilerParams(vmem_limit_bytes=VMEM_LIMIT),
            name="finish",
        )(placed, frc_rows, total)
        return pos.T, vel.T, frc.T, ids, oks, energy

    row_spec = P(MESH_AXES, None)
    id_spec = P(MESH_AXES)
    return jax.shard_map(local_step, mesh=mesh, in_specs=(row_spec, row_spec, row_spec, id_spec, id_spec, P()), out_specs=(row_spec, row_spec, row_spec, id_spec, id_spec, P()), check_vma=False)
```
